32 devices in a mesh: data: 1 (over z), seq: 32 (over y, x, core).
Axes of the slice: x: 4, y: 4, z: 1, core: 2. Of those that a mesh axis runs over, the one named last changes fastest.
The devices are a block of a 4x4x8 slice.
Arguments:
- dec_in: bfloat16 [2048, 1024], P(('data', 'seq'))
- memory: bfloat16 [32768, 1024], P(('data', 'seq'))
- mem_len: int32 [1], P('data')
- grad_out: float32 [2048, 1024], P(('data', 'seq'))
- norm_attn: bfloat16 [1024], replicated
- wq_cross: bfloat16 [1024, 16, 64], replicated
- wk_cross: bfloat16 [1024, 16, 64], replicated
- wv_cross: bfloat16 [1024, 16, 64], replicated
- wo_cross: bfloat16 [16, 64, 1024], replicated
- norm_mlp: bfloat16 [1024], replicated
- w_gate: bfloat16 [1024, 2816], replicated
- w_up: bfloat16 [1024, 2816], replicated
- w_down: bfloat16 [2816, 1024], replicated
Outputs:
- output 1: float32 [2048, 1024], P(('data', 'seq'))
- output 2: float32 [32768, 1024], P(('data', 'seq'))
- output 3: float32 [1024], P('data')
- output 4: float32 [1024, 16, 64], P('data')
- output 5: float32 [1024, 16, 64], P('data')
- output 6: float32 [1024, 16, 64], P('data')
- output 7: float32 [16, 64, 1024], P('data')
- output 8: float32 [1024], P('data')
- output 9: float32 [1024, 2816], P('data')
- output 10: float32 [1024, 2816], P('data')
- output 11: float32 [2816, 1024], P('data')
All inputs are finite; a program needn't handle non-finite values.
Results may differ from the reference program's by a relative error of at most 0.0157327.
Values are sent between devices in bfloat16 or wider.
A program may use at most 768 MiB of HBM per device.

```python
import functools
import jax
import jax.numpy as jnp
from jax import lax

TQ = 2048
TM = 32768
D = 1024
HEADS = 16
KV_HEADS = 16
HEAD = 64
FF = 2816
QBLK = 64
SEGMENTS = 16


def setup_inputs(seed: int = 0, part: int = 0) -> dict:
    part_keys = jax.random.split(jax.random.fold_in(jax.random.key(seed), part), 5)
    shared_keys = jax.random.split(jax.random.key(seed + 1), 11)
    inv_width = D ** -0.5

    def normal_draw(key, shape, spread):
        return spread * jax.random.normal(key, shape, jnp.float32)

    topics = normal_draw(part_keys[1], (SEGMENTS, D), 1.0)
    memory = normal_draw(part_keys[2], (TM, D), 0.6) + 0.8 * jnp.repeat(topics, TM // SEGMENTS, axis=0)
    quarter = TM // 4
    mem_len = jax.random.randint(part_keys[3], (1,), quarter, TM - quarter + 1, dtype=jnp.int32)
    return {
        'dec_in': normal_draw(part_keys[0], (TQ, D), 1.0).astype(jnp.bfloat16),
        'memory': memory.astype(jnp.bfloat16),
        'mem_len': mem_len,
        'grad_out': normal_draw(part_keys[4], (TQ, D), 1.0),
        'norm_attn': (1.0 + normal_draw(shared_keys[0], (D,), 0.3)).astype(jnp.bfloat16),
        'wq_cross': normal_draw(shared_keys[1], (D, HEADS, HEAD), 1.2 * inv_width).astype(jnp.bfloat16),
        'wk_cross': normal_draw(shared_keys[2], (D, KV_HEADS, HEAD), 1.2 * inv_width).astype(jnp.bfloat16),
        'wv_cross': normal_draw(shared_keys[3], (D, KV_HEADS, HEAD), inv_width).astype(jnp.bfloat16),
        'wo_cross': normal_draw(shared_keys[4], (HEADS, HEAD, D), 1.5 * inv_width).astype(jnp.bfloat16),
        'norm_mlp': (1.0 + normal_draw(shared_keys[5], (D,), 0.3)).astype(jnp.bfloat16),
        'w_gate': normal_draw(shared_keys[6], (D, FF), inv_width).astype(jnp.bfloat16),
        'w_up': normal_draw(shared_keys[7], (D, FF), inv_width).astype(jnp.bfloat16),
        'w_down': normal_draw(shared_keys[8], (FF, D), FF ** -0.5).astype(jnp.bfloat16),
    }


def to_bf16(tensor):
    return tensor + lax.stop_gradient(tensor.astype(jnp.bfloat16).astype(jnp.float32) - tensor)


def rms_norm(tensor, gain):
    mean_sq = jnp.mean(tensor * tensor, axis=-1, keepdims=True)
    return tensor * lax.rsqrt(mean_sq + 1e-6) * gain


def layer_forward(valid_mask, dec_in, memory, norm_attn, wq_cross, wk_cross, wv_cross, wo_cross, norm_mlp, w_gate, w_up, w_down):
    normed = to_bf16(rms_norm(dec_in, norm_attn))
    dec_query = to_bf16(jnp.einsum('td,dhe->the', normed, wq_cross))
    dec_query = dec_query.reshape(TQ // QBLK, QBLK, KV_HEADS, HEADS // KV_HEADS, HEAD)
    mem_keys = to_bf16(jnp.einsum('td,dke->tke', memory, wk_cross))
    mem_vals = to_bf16(jnp.einsum('td,dke->tke', memory, wv_cross))

    def block_attention(query_block):
        scores = jnp.einsum('qkge,tke->qkgt', query_block, mem_keys) * (HEAD ** -0.5)
        scores = jnp.where(valid_mask, scores, -1e30)
        attn_prob = jax.nn.softmax(scores, axis=-1)
        return jnp.einsum('qkgt,tke->qkge', attn_prob, mem_vals)

    attended = to_bf16(lax.map(jax.checkpoint(block_attention), dec_query).reshape(TQ, HEADS, HEAD))
    hidden = to_bf16(dec_in + jnp.einsum('the,hed->td', attended, wo_cross))
    normed_mlp = to_bf16(rms_norm(hidden, norm_mlp))
    gate_pre = jnp.dot(normed_mlp, w_gate, preferred_element_type=jnp.float32)
    up_pre = jnp.dot(normed_mlp, w_up, preferred_element_type=jnp.float32)
    mlp_act = to_bf16(jax.nn.silu(gate_pre) * up_pre)
    return hidden + jnp.dot(mlp_act, w_down, preferred_element_type=jnp.float32)


def reference(dec_in, memory, mem_len, grad_out, norm_attn, wq_cross, wk_cross, wv_cross, wo_cross, norm_mlp, w_gate, w_up, w_down):
    valid_mask = jnp.arange(TM) < mem_len[0]
    primals = [tensor.astype(jnp.float32) for tensor in (dec_in, memory, norm_attn, wq_cross, wk_cross, wv_cross, wo_cross, norm_mlp, w_gate, w_up, w_down)]
    _, pullback = jax.vjp(functools.partial(layer_forward, valid_mask), *primals)
    (g_dec, g_mem, g_norm_attn, g_wq, g_wk, g_wv, g_wo, g_norm_mlp, g_gate, g_up, g_down) = pullback(grad_out.astype(jnp.float32))
    return (g_dec, g_mem, g_norm_attn, g_wq, g_wk, g_wv, g_wo, g_norm_mlp, g_gate, g_up, g_down)
```

```python
import functools

import jax
import jax.numpy as jnp
from jax import lax
from jax.experimental import pallas as pl
from jax.experimental.pallas import tpu as pltpu
from jax.sharding import PartitionSpec as P

LOG2E = 1.4426950408889634
NEG = -1e30
VMEM_LIMIT = 60 * 1024 * 1024


def rms_norm(tensor, gain):
    mean_sq = jnp.mean(tensor * tensor, axis=-1, keepdims=True)
    return tensor * lax.rsqrt(mean_sq + 1e-6) * gain


def gated_unit(gate_pre, up_pre):
    return jax.nn.silu(gate_pre) * up_pre


def dot(a, b):
    return jnp.dot(a, b, preferred_element_type=jnp.float32)


def exchange_kernel(n, count, *refs):
    srcs, dsts, send, recv = refs[:count], refs[count:2 * count], refs[2 * count], refs[2 * count + 1]
    me = lax.axis_index('seq')
    barrier = pltpu.get_barrier_semaphore()
    for step in range(1, n):
        pl.semaphore_signal(barrier, inc=1, device_id={'seq': lax.rem(me + step, n)}, device_id_type=pl.DeviceIdType.MESH)
    pl.semaphore_wait(barrier, n - 1)

    def copy(i, src, dst, peer):
        return pltpu.make_async_remote_copy(src_ref=srcs[i].at[src], dst_ref=dsts[i].at[dst], send_sem=send.at[i],
                                            recv_sem=recv.at[i], device_id={'seq': peer},
                                            device_id_type=pl.DeviceIdType.MESH)

    for i in range(count):
        for step in range(1, n):
            peer = lax.rem(me + step, n)
            copy(i, peer, me, peer).start()
    for i in range(count):
        dsts[i][me] = srcs[i][me]
    for i in range(count):
        whole = copy(i, pl.ds(0, n - 1), pl.ds(0, n - 1), me)
        whole.wait_send()
        whole.wait_recv()


def exchange(n, collective_id, *arrays):
    count = len(arrays)
    return pl.pallas_call(
        functools.partial(exchange_kernel, n, count),
        out_shape=[jax.ShapeDtypeStruct(a.shape, a.dtype) for a in arrays],
        in_specs=[pl.BlockSpec(memory_space=pltpu.VMEM)] * count,
        out_specs=[pl.BlockSpec(memory_space=pltpu.VMEM)] * count,
        scratch_shapes=[pltpu.SemaphoreType.DMA((count,)), pltpu.SemaphoreType.DMA((count,))],
        compiler_params=pltpu.CompilerParams(collective_id=collective_id, has_side_effects=True,
                                             vmem_limit_bytes=VMEM_LIMIT),
        name='exchange',
    )(*arrays)


def forward_kernel(scale, head_dim, q_block, bounds_ref, kv_ref, qt_ref, out_ref):
    blocks, last_valid = bounds_ref[0], bounds_ref[1]
    rows, total_q = kv_ref.shape[1], qt_ref.shape[1]
    out_ref[:head_dim + 8, :] = jnp.zeros((head_dim + 8, total_q), jnp.float32)
    out_ref[head_dim + 8:, :] = jnp.full((8, total_q), NEG, jnp.float32)

    def block(index, masked):
        keys = kv_ref[index]
        values = jnp.concatenate([keys.T[head_dim:], jnp.ones((16, rows), keys.dtype)], axis=0)
        for first in range(0, total_q, q_block):
            cols = slice(first, first + q_block)
            scores = dot(keys, qt_ref[:, cols]) * scale
            if masked:
                position = lax.broadcasted_iota(jnp.int32, scores.shape, 0)
                scores = jnp.where(position < last_valid, scores, NEG)
            old = out_ref[head_dim + 8:head_dim + 9, cols]
            new = jnp.maximum(old, jnp.max(scores, axis=0, keepdims=True))
            weights = jnp.exp2(scores - new).astype(keys.dtype)
            update = dot(values, weights)
            out_ref[:head_dim + 8, cols] = out_ref[:head_dim + 8, cols] * jnp.exp2(old - new) + update[:head_dim + 8]
            out_ref[head_dim + 8:, cols] = jnp.broadcast_to(new, (8, q_block))

    def step(index, carry):
        block(index, False)
        return carry

    lax.fori_loop(0, blocks - 1, step, 0)
    block(blocks - 1, True)


def attention_forward(scale, head_dim, sources, bounds, kv, qt):
    rows, total_q = kv.shape[1], qt.shape[1]
    return pl.pallas_call(
        functools.partial(forward_kernel, scale, head_dim, min(512, total_q)),
        out_shape=jax.ShapeDtypeStruct((head_dim + 16, total_q), jnp.float32),
        grid=(1,),
        in_specs=[pl.BlockSpec(memory_space=pltpu.SMEM),
                  pl.BlockSpec((sources, rows, kv.shape[2]), lambda i: (0, 0, 0), pipeline_mode=pl.Buffered(1)),
                  pl.BlockSpec(qt.shape, lambda i: (0, 0), pipeline_mode=pl.Buffered(1))],
        out_specs=pl.BlockSpec((head_dim + 16, total_q), lambda i: (0, 0)),
        compiler_params=pltpu.CompilerParams(vmem_limit_bytes=VMEM_LIMIT),
        cost_estimate=pl.CostEstimate(flops=4 * total_q * sources * rows * head_dim, bytes_accessed=kv.size * 2,
                                      transcendentals=total_q * sources * rows),
        name='attention_forward',
    )(bounds, kv, qt)


def backward_kernel(scale, key_scale, head_dim, q_block, bounds_ref, kv_ref, qt_ref, dot_ref, q_ref, do_ref, lse_ref,
                    delta_ref, dkv_ref, dq_ref):
    blocks, last_valid = bounds_ref[0], bounds_ref[1]
    rows, total_q = kv_ref.shape[1], qt_ref.shape[1]
    width = kv_ref.shape[2]
    dq_ref[...] = jnp.zeros_like(dq_ref)
    lane_scale = jnp.where(lax.broadcasted_iota(jnp.int32, (1, width), 1) < head_dim, key_scale, 1.0)

    def block(index, masked):
        keys = kv_ref[index]
        keys_t = keys.T[:head_dim]
        total = jnp.zeros((rows, width), jnp.float32)
        for first in range(0, total_q, q_block):
            cols = slice(first, first + q_block)
            scores = dot(keys, qt_ref[:, cols]) * scale
            grads = dot(keys, dot_ref[:, cols])
            prob = jnp.exp2(scores - lse_ref[:, cols])
            if masked:
                position = lax.broadcasted_iota(jnp.int32, scores.shape, 0)
                prob = jnp.where(position < last_valid, prob, 0.0)
            grad_scores = (prob * (grads - delta_ref[:, cols])).astype(keys.dtype)
            total += dot(grad_scores, q_ref[cols, :]) + dot(prob.astype(keys.dtype), do_ref[cols, :])
            dq_ref[:, cols] += dot(keys_t, grad_scores)
        dkv_ref[index] = (total * lane_scale).astype(dkv_ref.dtype)

    def step(index, carry):
        block(index, False)
        return carry

    def clear(index, carry):
        dkv_ref[index] = jnp.zeros((rows, width), dkv_ref.dtype)
        return carry

    lax.fori_loop(0, blocks - 1, step, 0)
    block(blocks - 1, True)
    lax.fori_loop(blocks, dkv_ref.shape[0], clear, 0)
    dq_ref[...] = dq_ref[...] * key_scale


def attention_backward(scale, key_scale, head_dim, sources, bounds, kv, qt, do_t, q, do, lse, delta):
    n, rows, width = kv.shape
    total_q = qt.shape[1]
    whole = lambda a: pl.BlockSpec(a.shape, lambda i: (0,) * a.ndim, pipeline_mode=pl.Buffered(1))
    return pl.pallas_call(
        functools.partial(backward_kernel, scale, key_scale, head_dim, min(512, total_q)),
        out_shape=[jax.ShapeDtypeStruct((n, rows, width), jnp.bfloat16),
                   jax.ShapeDtypeStruct((head_dim, total_q), jnp.float32)],
        grid=(1,),
        in_specs=[pl.BlockSpec(memory_space=pltpu.SMEM),
                  pl.BlockSpec((sources, rows, width), lambda i: (0, 0, 0), pipeline_mode=pl.Buffered(1)),
                  whole(qt), whole(do_t), whole(q), whole(do), whole(lse), whole(delta)],
        out_specs=[pl.BlockSpec((n, rows, width), lambda i: (0, 0, 0)),
                   pl.BlockSpec((head_dim, total_q), lambda i: (0, 0))],
        compiler_params=pltpu.CompilerParams(vmem_limit_bytes=VMEM_LIMIT),
        cost_estimate=pl.CostEstimate(flops=10 * total_q * sources * rows * head_dim, bytes_accessed=kv.size * 4,
                                      transcendentals=total_q * sources * rows),
        name='attention_backward',
    )(bounds, kv, qt, do_t, q, do, lse, delta)


def mlp_kernel(chunk, n2_ref, n2t_ref, top_ref, w1_ref, w3_ref, w2_ref, g1_ref, g3_ref, g2_ref, d1_ref, d3_ref, act_ref):
    rows = n2_ref.shape[0]
    w1, w3, w2t = w1_ref[...], w3_ref[...], w2_ref[...].T
    for first in range(0, rows, chunk):
        part = slice(first, first + chunk)
        gate = dot(n2_ref[part, :], w1)
        up = dot(n2_ref[part, :], w3)
        grad = dot(top_ref[part, :], w2t)
        sig = jax.nn.sigmoid(gate)
        silu = gate * sig
        act_ref[part, :] = (silu * up).astype(act_ref.dtype)
        d3_ref[part, :] = (grad * silu).astype(d3_ref.dtype)
        d1_ref[part, :] = (grad * up * (sig + silu * (1.0 - sig))).astype(d1_ref.dtype)
    g1_ref[...] = dot(n2t_ref[...], d1_ref[...])
    g3_ref[...] = dot(n2t_ref[...], d3_ref[...])
    g2_ref[...] = lax.dot_general(act_ref[...], top_ref[...], (((0,), (0,)), ((), ())), preferred_element_type=jnp.float32)


def mlp_weight_grads(n2, n2t, top, w_gate, w_up, w_down):
    rows, dim = n2.shape
    ff = w_gate.shape[1]
    tile = 256
    whole = lambda a: pl.BlockSpec(a.shape, lambda i: (0, 0), pipeline_mode=pl.Buffered(1))
    cols = pl.BlockSpec((dim, tile), lambda i: (0, i))
    tall = pl.BlockSpec((tile, dim), lambda i: (i, 0))
    return pl.pallas_call(
        functools.partial(mlp_kernel, min(512, rows)),
        out_shape=[jax.ShapeDtypeStruct((dim, ff), jnp.float32), jax.ShapeDtypeStruct((dim, ff), jnp.float32),
                   jax.ShapeDtypeStruct((ff, dim), jnp.float32)],
        grid=(ff // tile,),
        in_specs=[whole(n2), whole(n2t), whole(top), cols, cols, tall],
        out_specs=[cols, cols, tall],
        scratch_shapes=[pltpu.VMEM((rows, tile), jnp.bfloat16)] * 3,
        compiler_params=pltpu.CompilerParams(vmem_limit_bytes=VMEM_LIMIT),
        cost_estimate=pl.CostEstimate(flops=12 * rows * dim * ff, bytes_accessed=18 * dim * ff, transcendentals=rows * ff),
        name='mlp_weight_grads',
    )(n2, n2t, top, w_gate, w_up, w_down)


def solution(mesh):
    n = mesh.shape['seq']
    row_spec = P(('data', 'seq'), None)
    weight_spec = P()
    part_vec = P('data')
    part_mat = P('data', None)
    part_cube = P('data', None, None)

    def device_step(dec_in, memory, mem_len, grad_out, norm_attn, wq_cross, wk_cross, wv_cross, wo_cross, norm_mlp, w_gate, w_up, w_down):
        q_rows, dim = dec_in.shape
        m_rows = memory.shape[0]
        heads, hd = wq_cross.shape[1], wq_cross.shape[2]
        parts = n // heads
        half = m_rows // parts
        sources = -(-3 * n // 4)
        total_q = q_rows * n
        key_scale = hd ** -0.5
        scale = key_scale * LOG2E
        bf16, f32 = jnp.bfloat16, jnp.float32
        me = lax.axis_index('seq')
        part = lax.rem(me, parts)
        pair = [(i, i + 1 - 2 * (i % 2)) for i in range(n)]

        reach = mem_len[0] - part * half
        blocks = jnp.minimum((reach + m_rows - 1) // m_rows, sources)
        bounds = jnp.stack([blocks, jnp.minimum(reach - (blocks - 1) * m_rows, half)]).astype(jnp.int32)

        x_in = dec_in.astype(f32)
        normed_f, norm_pull = jax.vjp(rms_norm, x_in, norm_attn.astype(f32))
        normed = normed_f.astype(bf16)
        local_q = jnp.einsum('td,dhe->hte', normed, wq_cross, preferred_element_type=f32).astype(bf16)
        w_kv = jnp.concatenate([wk_cross, wv_cross], axis=-1)
        local_kv = jnp.einsum('td,dhe->hte', memory, w_kv, preferred_element_type=f32).astype(bf16)
        q_out = jnp.broadcast_to(local_q[:, None], (heads, parts, q_rows, hd)).reshape(n, q_rows, hd)
        kv, q_in = exchange(n, 0, local_kv.reshape(n, half, 2 * hd), q_out)

        grad_top = grad_out.astype(bf16)
        gate_dep, _ = lax.optimization_barrier((jnp.concatenate([dec_in, grad_top], axis=1), q_in))
        early = lax.all_gather(gate_dep, 'seq', axis=0, tiled=True)

        head_q = q_in.reshape(total_q, hd)
        zeros = jnp.zeros((total_q, hd), bf16)
        q_wide = jnp.concatenate([head_q, zeros], axis=1)
        qt_wide = jnp.concatenate([head_q.T, zeros.T], axis=0)

        mine = attention_forward(scale, hd, sources, bounds, kv, qt_wide)
        other = lax.ppermute(mine, 'seq', pair)
        m_a, m_b = mine[hd + 8:hd + 9], other[hd + 8:hd + 9]
        m_all = jnp.maximum(m_a, m_b)
        s_a, s_b = jnp.exp2(m_a - m_all), jnp.exp2(m_b - m_all)
        den = mine[hd:hd + 1] * s_a + other[hd:hd + 1] * s_b
        out_t = (mine[:hd] * s_a + other[:hd] * s_b) / den
        lse = m_all + jnp.log2(den)
        out_blocks = out_t.astype(bf16).reshape(hd, n, q_rows).transpose(1, 2, 0)
        (att_in,) = exchange(n, 1, out_blocks)
        attended = att_in[::parts]

        hidden_f = x_in + jnp.einsum('hqe,hed->qd', attended, wo_cross, preferred_element_type=f32)
        hidden = hidden_f.astype(bf16)
        normed_mlp_f, mlp_norm_pull = jax.vjp(rms_norm, hidden.astype(f32), norm_mlp.astype(f32))
        normed_mlp = normed_mlp_f.astype(bf16)
        gate_pre = jnp.dot(normed_mlp, w_gate, preferred_element_type=f32)
        up_pre = jnp.dot(normed_mlp, w_up, preferred_element_type=f32)
        _, gated_pull = jax.vjp(gated_unit, gate_pre, up_pre)
        grad_act = jnp.einsum('qd,fd->qf', grad_top, w_down, preferred_element_type=f32)
        grad_gate, grad_up = gated_pull(grad_act)
        grad_normed_mlp = (jnp.einsum('qf,df->qd', grad_gate.astype(bf16), w_gate, preferred_element_type=f32)
                           + jnp.einsum('qf,df->qd', grad_up.astype(bf16), w_up, preferred_element_type=f32))
        grad_hidden_norm, g_norm_mlp = mlp_norm_pull(grad_normed_mlp)
        grad_hidden = grad_out + grad_hidden_norm
        grad_hidden_b = grad_hidden.astype(bf16)
        grad_att = jnp.einsum('qd,hed->hqe', grad_hidden_b, wo_cross, preferred_element_type=f32).astype(bf16)
        (do_in,) = exchange(n, 2, jnp.broadcast_to(grad_att[:, None], (heads, parts, q_rows, hd)).reshape(n, q_rows, hd))

        late_local = jnp.concatenate([attended.transpose(1, 0, 2).reshape(q_rows, heads * hd), grad_hidden_b], axis=1)
        late_local, _ = lax.optimization_barrier((late_local, do_in))
        late = lax.all_gather(late_local, 'seq', axis=0, tiled=True)

        head_do = do_in.reshape(total_q, hd)
        do_wide = jnp.concatenate([zeros, head_do], axis=1)
        do_t = head_do.T
        dot_wide = jnp.concatenate([zeros.T, do_t], axis=0)
        delta = jnp.sum(do_t.astype(f32) * out_t, axis=0, keepdims=True)
        dkv, dq_part = attention_backward(scale, key_scale, hd, sources, bounds, kv, qt_wide, dot_wide, q_wide, do_wide, lse, delta)

        share = total_q // parts
        dq_shares = dq_part.reshape(hd, parts, share).transpose(1, 2, 0)
        keep = lax.dynamic_index_in_dim(dq_shares, part, 0, keepdims=False)
        give = lax.dynamic_index_in_dim(dq_shares, 1 - part, 0, keepdims=False)
        dq_share = (keep + lax.ppermute(give, 'seq', pair)).astype(bf16)

        (dkv_in,) = exchange(n, 3, dkv)
        dkv_in = dkv_in.reshape(heads, m_rows, 2 * hd)
        dq_all = lax.all_gather(dq_share, 'seq', axis=0, tiled=True).reshape(heads, total_q, hd)
        dq_rows = lax.dynamic_slice_in_dim(dq_all, me * q_rows, q_rows, axis=1)
        grad_normed = jnp.einsum('hte,dhe->td', dq_rows, wq_cross, preferred_element_type=f32)
        grad_x_norm, g_norm_attn = norm_pull(grad_normed)
        g_dec = grad_hidden + grad_x_norm

        g_kv = jnp.einsum('td,hte->dhe', memory, dkv_in, preferred_element_type=f32)
        g_kv, norms = lax.psum((g_kv, jnp.stack([g_norm_attn, g_norm_mlp])), 'seq')
        g_mem = jnp.einsum('hte,dhe->td', dkv_in, w_kv, preferred_element_type=f32)

        dec_all, top_all = early[:, :dim], early[:, dim:]
        att_all, gh_all = late[:, :heads * hd], late[:, heads * hd:]
        hidden_all = (dec_all.astype(f32) + jnp.dot(att_all, wo_cross.reshape(heads * hd, dim), preferred_element_type=f32)).astype(bf16)
        n2_all = rms_norm(hidden_all.astype(f32), norm_mlp.astype(f32)).astype(bf16)
        n1_all = rms_norm(dec_all.astype(f32), norm_attn.astype(f32)).astype(bf16)
        g_gate, g_up, g_down = mlp_weight_grads(n2_all, n2_all.T, top_all, w_gate, w_up, w_down)
        g_wo = jnp.einsum('tf,td->fd', att_all, gh_all, preferred_element_type=f32).reshape(heads, hd, dim)
        g_wq = jnp.einsum('td,hte->dhe', n1_all, dq_all, preferred_element_type=f32)
        return (g_dec, g_mem, norms[0], g_wq, g_kv[:, :, :hd], g_kv[:, :, hd:], g_wo, norms[1], g_gate, g_up, g_down)

    return jax.shard_map(device_step, mesh=mesh,
                         in_specs=(row_spec, row_spec, part_vec, row_spec) + (weight_spec,) * 9,
                         out_specs=(row_spec, row_spec, part_vec, part_cube, part_cube, part_cube, part_cube, part_vec, part_mat, part_mat, part_mat),
                         check_vma=False)
```

```python
import functools

import jax
import jax.numpy as jnp
from jax import lax
from jax.experimental import pallas as pl
from jax.experimental.pallas import tpu as pltpu
from jax.sharding import PartitionSpec as P

LOG2E = 1.4426950408889634
NEG = -1e30
VMEM_LIMIT = 60 * 1024 * 1024
MESH = pl.DeviceIdType.MESH
BF16, F32 = jnp.bfloat16, jnp.float32


def rms_norm(tensor, gain):
    mean_sq = jnp.mean(tensor * tensor, axis=-1, keepdims=True)
    return tensor * lax.rsqrt(mean_sq + 1e-6) * gain


def gated_unit(gate_pre, up_pre):
    return jax.nn.silu(gate_pre) * up_pre


def dot(a, b):
    return jnp.dot(a, b, preferred_element_type=F32)


def dot_nt(a, b):
    return lax.dot_general(a, b, (((1,), (1,)), ((), ())), preferred_element_type=F32)


def dot_tn(a, b):
    return lax.dot_general(a, b, (((0,), (0,)), ((), ())), preferred_element_type=F32)


def full(array):
    return pl.BlockSpec(array.shape, lambda *_: (0,) * array.ndim, pipeline_mode=pl.Buffered(1))


def vmem(count):
    return [pl.BlockSpec(memory_space=pltpu.VMEM)] * count


def plain(semantics=None):
    return pltpu.CompilerParams(vmem_limit_bytes=VMEM_LIMIT, dimension_semantics=semantics)


def remote(collective_id):
    return pltpu.CompilerParams(collective_id=collective_id, has_side_effects=True, vmem_limit_bytes=VMEM_LIMIT)


def shape(dims, dtype):
    return jax.ShapeDtypeStruct(dims, dtype)


def meet(peers):
    barrier = pltpu.get_barrier_semaphore()
    for peer in peers:
        pl.semaphore_signal(barrier, inc=1, device_id={'seq': peer}, device_id_type=MESH)
    pl.semaphore_wait(barrier, len(peers))


def send(src, dst, send_sem, recv_sem, peer):
    return pltpu.make_async_remote_copy(src_ref=src, dst_ref=dst, send_sem=send_sem, recv_sem=recv_sem,
                                        device_id={'seq': peer}, device_id_type=MESH)


def project_kernel(memory_ref, dec_ref, gain_ref, wk_ref, wv_ref, wq_ref, kv_ref, q_ref, normed_ref):
    group, hd = wk_ref.shape[0], wk_ref.shape[1]

    @pl.when(pl.program_id(0) == 0)
    def _():
        normed_ref[...] = rms_norm(dec_ref[...].astype(F32), gain_ref[...].astype(F32)).astype(BF16)

    weights = jnp.concatenate([part[i] for i in range(group) for part in (wk_ref, wv_ref)], axis=0)
    both = dot_nt(memory_ref[...], weights).astype(BF16)
    queries = dot_nt(normed_ref[...], jnp.concatenate([wq_ref[i] for i in range(group)], axis=0)).astype(BF16)
    zeros = jnp.zeros((queries.shape[0], hd), BF16)
    for i in range(group):
        kv_ref[i] = both[:, 2 * hd * i:2 * hd * (i + 1)]
        q_ref[i] = jnp.concatenate([queries[:, hd * i:hd * (i + 1)], zeros], axis=1)


def project(memory, dec_in, gain, wk_t, wv_t, wq_t):
    heads, hd, dim = wk_t.shape
    rows, q_rows = memory.shape[0], dec_in.shape[0]
    group = 2
    weight = pl.BlockSpec((group, hd, dim), lambda i: (i, 0, 0))
    return pl.pallas_call(
        project_kernel,
        out_shape=[shape((heads, rows, 2 * hd), BF16), shape((heads, q_rows, 2 * hd), BF16)],
        grid=(heads // group,),
        in_specs=[full(memory), full(dec_in), full(gain), weight, weight, weight],
        out_specs=[pl.BlockSpec((group, rows, 2 * hd), lambda i: (i, 0, 0)),
                   pl.BlockSpec((group, q_rows, 2 * hd), lambda i: (i, 0, 0))],
        scratch_shapes=[pltpu.VMEM(dec_in.shape, BF16)],
        compiler_params=plain(),
        cost_estimate=pl.CostEstimate(flops=4 * rows * dim * heads * hd, bytes_accessed=8 * rows * dim, transcendentals=0),
        name='project',
    )(memory, dec_in, gain, wk_t, wv_t, wq_t)


def exchange_kernel(n, counts, *refs):
    total = len(counts)
    srcs, dsts, send_sem, recv_sem = refs[:total], refs[total:2 * total], refs[2 * total], refs[2 * total + 1]
    me = lax.axis_index('seq')
    meet([lax.rem(me + step, n) for step in range(1, n)])

    def block(i, peer):
        return srcs[i].at[peer // (n // counts[i])]

    for i in range(total):
        for step in range(1, n):
            peer = lax.rem(me + step, n)
            send(block(i, peer), dsts[i].at[me], send_sem.at[i], recv_sem.at[i], peer).start()
    for i in range(total):
        dsts[i][me] = srcs[i][me // (n // counts[i])]
    for i in range(total):
        others = dsts[i].at[pl.ds(0, n - 1)]
        whole = send(others, others, send_sem.at[i], recv_sem.at[i], me)
        whole.wait_send()
        whole.wait_recv()


def exchange(n, collective_id, *arrays):
    total = len(arrays)
    return pl.pallas_call(
        functools.partial(exchange_kernel, n, [a.shape[0] for a in arrays]),
        out_shape=[shape((n,) + a.shape[1:], a.dtype) for a in arrays],
        in_specs=vmem(total),
        out_specs=vmem(total),
        scratch_shapes=[pltpu.SemaphoreType.DMA((total,)), pltpu.SemaphoreType.DMA((total,))],
        compiler_params=remote(collective_id),
        name='exchange',
    )(*arrays)


def to_rows(n, heads, q_rows, me, part, wide_ref, rows_ref, send_sem, recv_sem):
    parts = n // heads
    head = me // parts
    for step in range(1, heads):
        peer = lax.rem(head + step, heads) * parts + part
        send(wide_ref.at[peer], rows_ref.at[head], send_sem, recv_sem, peer).start()
    rows_ref[head] = wide_ref[me]
    others = rows_ref.at[pl.ds(0, heads - 1)]
    whole = send(others, others, send_sem, recv_sem, me)
    whole.wait_send()
    whole.wait_recv()


def pair_peers(n, heads, me, part):
    parts = n // heads
    head = me // parts
    partner = head * parts + (parts - 1 - part)
    return partner, [partner] + [lax.rem(head + step, heads) * parts + part for step in range(1, heads)]


def spread(values, n, q_rows):
    rows = values.T.astype(BF16)
    return jnp.concatenate([rows, jnp.zeros_like(rows)], axis=1).reshape(n, q_rows, 2 * rows.shape[1])


def combine_kernel(n, heads, hd, q_rows, mine_ref, rows_ref, out_ref, lse_ref, theirs_ref, wide_ref, send_sem, recv_sem):
    me = lax.axis_index('seq')
    part = lax.rem(me, n // heads)
    partner, peers = pair_peers(n, heads, me, part)
    meet(peers)
    swap = send(mine_ref, theirs_ref, send_sem.at[0], recv_sem.at[0], partner)
    swap.start()
    swap.wait()
    m_a, m_b = mine_ref[hd + 8:hd + 9], theirs_ref[hd + 8:hd + 9]
    top = jnp.maximum(m_a, m_b)
    s_a, s_b = jnp.exp2(m_a - top), jnp.exp2(m_b - top)
    den = mine_ref[hd:hd + 1] * s_a + theirs_ref[hd:hd + 1] * s_b
    out = (mine_ref[:hd] * s_a + theirs_ref[:hd] * s_b) / den
    out_ref[...] = out
    lse_ref[...] = top + jnp.log2(den)
    wide_ref[...] = spread(out, n, q_rows)
    to_rows(n, heads, q_rows, me, part, wide_ref, rows_ref, send_sem.at[1], recv_sem.at[1])


def combine(n, heads, hd, q_rows, collective_id, mine):
    total_q = mine.shape[1]
    return pl.pallas_call(
        functools.partial(combine_kernel, n, heads, hd, q_rows),
        out_shape=[shape((heads, q_rows, 2 * hd), BF16), shape((hd, total_q), F32), shape((1, total_q), F32)],
        in_specs=vmem(1),
        out_specs=vmem(3),
        scratch_shapes=[pltpu.VMEM(mine.shape, F32), pltpu.VMEM((n, q_rows, 2 * hd), BF16),
                        pltpu.SemaphoreType.DMA((2,)), pltpu.SemaphoreType.DMA((2,))],
        compiler_params=remote(collective_id),
        name='combine',
    )(mine)


def pair_sum_kernel(n, heads, q_rows, mine_ref, rows_ref, share_ref, theirs_ref, wide_ref, send_sem, recv_sem):
    me = lax.axis_index('seq')
    parts = n // heads
    part = lax.rem(me, parts)
    partner, peers = pair_peers(n, heads, me, part)
    meet(peers)
    swap = send(mine_ref, theirs_ref, send_sem.at[0], recv_sem.at[0], partner)
    swap.start()
    swap.wait()
    total = mine_ref[...] + theirs_ref[...]
    wide_ref[...] = spread(total, n, q_rows)
    width = share_ref.shape[1]
    share_ref[...] = jnp.where(part == 0, total[:, :width], total[:, width:]).astype(BF16)
    to_rows(n, heads, q_rows, me, part, wide_ref, rows_ref, send_sem.at[1], recv_sem.at[1])


def pair_sum(n, heads, q_rows, collective_id, mine):
    hd, total_q = mine.shape
    return pl.pallas_call(
        functools.partial(pair_sum_kernel, n, heads, q_rows),
        out_shape=[shape((heads, q_rows, 2 * hd), BF16), shape((hd, total_q * heads // n), BF16)],
        in_specs=vmem(1),
        out_specs=vmem(2),
        scratch_shapes=[pltpu.VMEM(mine.shape, F32), pltpu.VMEM((n, q_rows, 2 * hd), BF16),
                        pltpu.SemaphoreType.DMA((2,)), pltpu.SemaphoreType.DMA((2,))],
        compiler_params=remote(collective_id),
        name='pair_sum',
    )(mine)


def small_sum_kernel(n, mine_ref, total_ref, all_ref, send_sem, recv_sem):
    me = lax.axis_index('seq')
    meet([lax.rem(me + step, n) for step in range(1, n)])
    for step in range(1, n):
        send(mine_ref, all_ref.at[me], send_sem, recv_sem, lax.rem(me + step, n)).start()
    all_ref[me] = mine_ref[...]
    others = all_ref.at[pl.ds(0, n - 1)]
    whole = send(others, others, send_sem, recv_sem, me)
    whole.wait_send()
    whole.wait_recv()
    total_ref[...] = jnp.sum(all_ref[...], axis=0)


def small_sum(n, collective_id, mine):
    return pl.pallas_call(
        functools.partial(small_sum_kernel, n),
        out_shape=shape(mine.shape, F32),
        in_specs=vmem(1),
        out_specs=vmem(1)[0],
        scratch_shapes=[pltpu.VMEM((n,) + mine.shape, F32), pltpu.SemaphoreType.DMA, pltpu.SemaphoreType.DMA],
        compiler_params=remote(collective_id),
        name='small_sum',
    )(mine)


def forward_kernel(scale, hd, q_block, bounds_ref, kv_ref, q_ref, out_ref, qt_ref):
    blocks, last_valid = bounds_ref[0], bounds_ref[1]
    rows, total_q = kv_ref.shape[1], q_ref.shape[0]
    qt_ref[...] = q_ref[...].T
    out_ref[:hd + 8, :] = jnp.zeros((hd + 8, total_q), F32)
    out_ref[hd + 8:, :] = jnp.full((8, total_q), NEG, F32)

    def block(index, masked):
        keys = kv_ref[index]
        values = jnp.concatenate([keys.T[hd:], jnp.ones((16, rows), keys.dtype)], axis=0)
        for first in range(0, total_q, q_block):
            cols = slice(first, first + q_block)
            scores = dot(keys, qt_ref[:, cols]) * scale
            if masked:
                position = lax.broadcasted_iota(jnp.int32, scores.shape, 0)
                scores = jnp.where(position < last_valid, scores, NEG)
            old = out_ref[hd + 8:hd + 9, cols]
            new = jnp.maximum(old, jnp.max(scores, axis=0, keepdims=True))
            weights = jnp.exp2(scores - new).astype(keys.dtype)
            update = dot(values, weights)
            out_ref[:hd + 8, cols] = out_ref[:hd + 8, cols] * jnp.exp2(old - new) + update[:hd + 8]
            out_ref[hd + 8:, cols] = jnp.broadcast_to(new, (8, q_block))

    def step(index, carry):
        block(index, False)
        return carry

    lax.fori_loop(0, blocks - 1, step, 0)
    block(blocks - 1, True)


def attention_forward(scale, hd, sources, bounds, kv, q):
    rows, width = kv.shape[1], kv.shape[2]
    total_q = q.shape[0]
    return pl.pallas_call(
        functools.partial(forward_kernel, scale, hd, min(512, total_q)),
        out_shape=shape((hd + 16, total_q), F32),
        grid=(1,),
        in_specs=[pl.BlockSpec(memory_space=pltpu.SMEM),
                  pl.BlockSpec((sources, rows, width), lambda i: (0, 0, 0), pipeline_mode=pl.Buffered(1)), full(q)],
        out_specs=pl.BlockSpec((hd + 16, total_q), lambda i: (0, 0)),
        scratch_shapes=[pltpu.VMEM((width, total_q), BF16)],
        compiler_params=plain(),
        cost_estimate=pl.CostEstimate(flops=4 * total_q * sources * rows * hd, bytes_accessed=kv.size * 2,
                                      transcendentals=total_q * sources * rows),
        name='attention_forward',
    )(bounds, kv, q)


def backward_kernel(scale, key_scale, hd, q_block, bounds_ref, kv_ref, q_ref, do_ref, out_ref, lse_ref, dkv_ref, dq_ref,
                    qt_ref, dot_ref, delta_ref):
    blocks, last_valid = bounds_ref[0], bounds_ref[1]
    rows, total_q = kv_ref.shape[1], q_ref.shape[0]
    width = kv_ref.shape[2]
    dq_ref[...] = jnp.zeros_like(dq_ref)
    qt_ref[...] = q_ref[...].T
    do_t = do_ref[...].T
    dot_ref[...] = do_t
    delta_ref[...] = jnp.sum(do_t[hd:].astype(F32) * out_ref[...], axis=0, keepdims=True)
    lane_scale = jnp.where(lax.broadcasted_iota(jnp.int32, (1, width), 1) < hd, key_scale, 1.0)

    def block(index, masked):
        keys = kv_ref[index]
        keys_t = keys.T[:hd]
        total = jnp.zeros((rows, width), F32)
        for first in range(0, total_q, q_block):
            cols = slice(first, first + q_block)
            scores = dot(keys, qt_ref[:, cols]) * scale
            grads = dot(keys, dot_ref[:, cols])
            prob = jnp.exp2(scores - lse_ref[:, cols])
            if masked:
                position = lax.broadcasted_iota(jnp.int32, scores.shape, 0)
                prob = jnp.where(position < last_valid, prob, 0.0)
            grad_scores = (prob * (grads - delta_ref[:, cols])).astype(keys.dtype)
            total += dot(grad_scores, q_ref[cols, :]) + dot(prob.astype(keys.dtype), do_ref[cols, :])
            dq_ref[:, cols] += dot(keys_t, grad_scores)
        dkv_ref[index] = (total * lane_scale).astype(dkv_ref.dtype)

    def step(index, carry):
        block(index, False)
        return carry

    def clear(index, carry):
        dkv_ref[index] = jnp.zeros((rows, width), dkv_ref.dtype)
        return carry

    lax.fori_loop(0, blocks - 1, step, 0)
    block(blocks - 1, True)
    lax.fori_loop(blocks, dkv_ref.shape[0], clear, 0)
    dq_ref[...] = dq_ref[...] * key_scale


def attention_backward(scale, key_scale, hd, sources, bounds, kv, q, do, out_t, lse):
    n, rows, width = kv.shape
    total_q = q.shape[0]
    return pl.pallas_call(
        functools.partial(backward_kernel, scale, key_scale, hd, min(512, total_q)),
        out_shape=[shape((n, rows, width), BF16), shape((hd, total_q), F32)],
        grid=(1,),
        in_specs=[pl.BlockSpec(memory_space=pltpu.SMEM),
                  pl.BlockSpec((sources, rows, width), lambda i: (0, 0, 0), pipeline_mode=pl.Buffered(1)),
                  full(q), full(do), full(out_t), full(lse)],
        out_specs=[pl.BlockSpec((n, rows, width), lambda i: (0, 0, 0)),
                   pl.BlockSpec((hd, total_q), lambda i: (0, 0))],
        scratch_shapes=[pltpu.VMEM((width, total_q), BF16), pltpu.VMEM((width, total_q), BF16), pltpu.VMEM((1, total_q), F32)],
        compiler_params=plain(),
        cost_estimate=pl.CostEstimate(flops=10 * total_q * sources * rows * hd, bytes_accessed=kv.size * 4,
                                      transcendentals=total_q * sources * rows),
        name='attention_backward',
    )(bounds, kv, q, do, out_t, lse)


def prepare_kernel(dec_ref, att_ref, wo_ref, gain_ref, n2_ref, n2t_ref):
    hidden = (dec_ref[...].astype(F32) + dot(att_ref[...], wo_ref[...])).astype(BF16)
    normed = rms_norm(hidden.astype(F32), gain_ref[...].astype(F32)).astype(BF16)
    n2_ref[...] = normed
    n2t_ref[...] = normed.T


def prepare(early, late, wo, gain):
    rows, dim = early.shape[0], wo.shape[1]
    chunk = min(512, rows)
    left = pl.BlockSpec((chunk, dim), lambda i: (i, 0))
    return pl.pallas_call(
        prepare_kernel,
        out_shape=[shape((rows, dim), BF16), shape((dim, rows), BF16)],
        grid=(rows // chunk,),
        in_specs=[left, pl.BlockSpec((chunk, wo.shape[0]), lambda i: (i, 0)), full(wo), full(gain)],
        out_specs=[left, pl.BlockSpec((dim, chunk), lambda i: (0, i))],
        compiler_params=plain(),
        cost_estimate=pl.CostEstimate(flops=2 * rows * dim * dim, bytes_accessed=8 * rows * dim, transcendentals=0),
        name='prepare',
    )(early, late, wo, gain)


def mlp_kernel(chunk, n2_ref, n2t_ref, top_ref, w1_ref, w3_ref, w2_ref, g1_ref, g3_ref, g2_ref, d1_ref, d3_ref, act_ref):
    rows = n2_ref.shape[0]
    w1, w3, w2t = w1_ref[...], w3_ref[...], w2_ref[...].T
    for first in range(0, rows, chunk):
        part = slice(first, first + chunk)
        gate = dot(n2_ref[part, :], w1)
        up = dot(n2_ref[part, :], w3)
        grad = dot(top_ref[part, :], w2t)
        sig = jax.nn.sigmoid(gate)
        silu = gate * sig
        act_ref[part, :] = (silu * up).astype(act_ref.dtype)
        d3_ref[part, :] = (grad * silu).astype(d3_ref.dtype)
        d1_ref[part, :] = (grad * up * (sig + silu * (1.0 - sig))).astype(d1_ref.dtype)
    g1_ref[...] = dot(n2t_ref[...], d1_ref[...])
    g3_ref[...] = dot(n2t_ref[...], d3_ref[...])
    g2_ref[...] = dot_tn(act_ref[...], top_ref[...])


def mlp_weight_grads(n2, n2t, early, w_gate, w_up, w_down):
    rows, dim = n2.shape
    ff = w_gate.shape[1]
    tile = 256
    cols = pl.BlockSpec((dim, tile), lambda i: (0, i))
    tall = pl.BlockSpec((tile, dim), lambda i: (i, 0))
    return pl.pallas_call(
        functools.partial(mlp_kernel, min(512, rows)),
        out_shape=[shape((dim, ff), F32), shape((dim, ff), F32), shape((ff, dim), F32)],
        grid=(ff // tile,),
        in_specs=[full(n2), full(n2t), pl.BlockSpec((rows, dim), lambda i: (0, 1), pipeline_mode=pl.Buffered(1)), cols, cols, tall],
        out_specs=[cols, cols, tall],
        scratch_shapes=[pltpu.VMEM((rows, tile), BF16)] * 3,
        compiler_params=plain(),
        cost_estimate=pl.CostEstimate(flops=12 * rows * dim * ff, bytes_accessed=18 * dim * ff, transcendentals=rows * ff),
        name='mlp_weight_grads',
    )(n2, n2t, early, w_gate, w_up, w_down)


def solution(mesh):
    n = mesh.shape['seq']
    row_spec = P(('data', 'seq'), None)
    weight_spec = P()
    part_vec = P('data')
    part_mat = P('data', None)
    part_cube = P('data', None, None)

    def device_step(dec_in, memory, mem_len, grad_out, norm_attn, wq_cross, wk_cross, wv_cross, wo_cross, norm_mlp, w_gate, w_up, w_down):
        q_rows, dim = dec_in.shape
        m_rows = memory.shape[0]
        heads, hd = wq_cross.shape[1], wq_cross.shape[2]
        parts = n // heads
        half = m_rows // parts
        sources = -(-3 * n // 4)
        total_q = q_rows * n
        key_scale = hd ** -0.5
        scale = key_scale * LOG2E
        me = lax.axis_index('seq')
        part = lax.rem(me, parts)

        reach = mem_len[0] - part * half
        blocks = jnp.minimum((reach + m_rows - 1) // m_rows, sources)
        bounds = jnp.stack([blocks, jnp.minimum(reach - (blocks - 1) * m_rows, half)]).astype(jnp.int32)

        wq_t, wk_t, wv_t = (jnp.transpose(w, (1, 2, 0)) for w in (wq_cross, wk_cross, wv_cross))
        gain_attn, gain_mlp = norm_attn.reshape(1, dim), norm_mlp.reshape(1, dim)
        local_kv, local_q = project(memory, dec_in, gain_attn, wk_t, wv_t, wq_t)
        kv, q_in = exchange(n, 0, local_kv.reshape(n, half, 2 * hd), local_q)
        head_q = q_in.reshape(total_q, 2 * hd)

        grad_top = grad_out.astype(BF16)
        early_local, kv = lax.optimization_barrier((jnp.concatenate([dec_in, grad_top], axis=1), kv))
        early = lax.all_gather(early_local, 'seq', axis=0, tiled=True)

        mine = attention_forward(scale, hd, sources, bounds, kv, head_q)
        att_in, out_t, lse = combine(n, heads, hd, q_rows, 1, mine)
        attended = att_in[:, :, :hd]

        x_in = dec_in.astype(F32)
        hidden_f = x_in + jnp.einsum('hqe,hed->qd', attended, wo_cross, preferred_element_type=F32)
        hidden = hidden_f.astype(BF16)
        normed_mlp_f, mlp_norm_pull = jax.vjp(rms_norm, hidden.astype(F32), norm_mlp.astype(F32))
        normed_mlp = normed_mlp_f.astype(BF16)
        gate_pre = jnp.dot(normed_mlp, w_gate, preferred_element_type=F32)
        up_pre = jnp.dot(normed_mlp, w_up, preferred_element_type=F32)
        _, gated_pull = jax.vjp(gated_unit, gate_pre, up_pre)
        grad_act = jnp.einsum('qd,fd->qf', grad_top, w_down, preferred_element_type=F32)
        grad_gate, grad_up = gated_pull(grad_act)
        grad_normed_mlp = (jnp.einsum('qf,df->qd', grad_gate.astype(BF16), w_gate, preferred_element_type=F32)
                           + jnp.einsum('qf,df->qd', grad_up.astype(BF16), w_up, preferred_element_type=F32))
        grad_hidden_norm, g_norm_mlp = mlp_norm_pull(grad_normed_mlp)
        grad_hidden = grad_out + grad_hidden_norm
        grad_hidden_b = grad_hidden.astype(BF16)
        grad_att = jnp.einsum('qd,hed->hqe', grad_hidden_b, wo_cross, preferred_element_type=F32).astype(BF16)
        (do_in,) = exchange(n, 2, jnp.concatenate([jnp.zeros_like(grad_att), grad_att], axis=-1))
        head_do = do_in.reshape(total_q, 2 * hd)

        late_local = jnp.concatenate([attended.transpose(1, 0, 2).reshape(q_rows, heads * hd), grad_hidden_b], axis=1)
        head_do, late_local, early = lax.optimization_barrier((head_do, late_local, early))
        late = lax.all_gather(late_local, 'seq', axis=0, tiled=True)

        dkv, dq_part = attention_backward(scale, key_scale, hd, sources, bounds, kv, head_q, head_do, out_t, lse)
        dq_rows, dq_share = pair_sum(n, heads, q_rows, 3, dq_part)
        dkv, dq_share, late = lax.optimization_barrier((dkv, dq_share, late))
        dq_all = lax.all_gather(dq_share, 'seq', axis=0, tiled=False).reshape(heads, parts, hd, total_q // parts)
        (dkv_in,) = exchange(n, 4, dkv)
        dkv_in, dq_all = lax.optimization_barrier((dkv_in, dq_all))
        dkv_in = dkv_in.reshape(heads, m_rows, 2 * hd)

        g_kv = lax.psum(jnp.einsum('td,hte->dhe', memory, dkv_in, preferred_element_type=F32), 'seq')

        dq_rows, _ = lax.optimization_barrier((dq_rows, dkv_in))
        grad_normed = jnp.einsum('hte,dhe->td', dq_rows[:, :, :hd], wq_cross, preferred_element_type=F32)
        _, norm_pull = jax.vjp(rms_norm, x_in, norm_attn.astype(F32))
        grad_x_norm, g_norm_attn = norm_pull(grad_normed)
        g_dec = grad_hidden + grad_x_norm
        norms = small_sum(n, 5, jnp.concatenate([g_norm_attn, g_norm_mlp]).reshape(-1, 128)).reshape(2, dim)
        w_kv = jnp.concatenate([wk_t, wv_t], axis=1)
        g_mem = jnp.einsum('hte,hed->td', dkv_in, w_kv, preferred_element_type=F32)

        dec_all = early[:, :dim]
        att_all, gh_all = late[:, :heads * hd], late[:, heads * hd:]
        n2_all, n2_all_t = prepare(early, late, wo_cross.reshape(heads * hd, dim), gain_mlp)
        n1_all = rms_norm(dec_all.astype(F32), norm_attn.astype(F32)).astype(BF16)
        g_gate, g_up, g_down = mlp_weight_grads(n2_all, n2_all_t, early, w_gate, w_up, w_down)
        g_wo = jnp.einsum('tf,td->fd', att_all, gh_all, preferred_element_type=F32).reshape(heads, hd, dim)
        g_wq = sum(jnp.einsum('het,td->dhe', dq_all[:, p], n1_all[p * (total_q // parts):(p + 1) * (total_q // parts)],
                              preferred_element_type=F32) for p in range(parts))
        return (g_dec, g_mem, norms[0], g_wq, g_kv[:, :, :hd], g_kv[:, :, hd:], g_wo, norms[1], g_gate, g_up, g_down)

    return jax.shard_map(device_step, mesh=mesh,
                         in_specs=(row_spec, row_spec, part_vec, row_spec) + (weight_spec,) * 9,
                         out_specs=(row_spec, row_spec, part_vec, part_cube, part_cube, part_cube, part_cube, part_vec, part_mat, part_mat, part_mat),
                         check_vma=False)
```

```python
import functools

import jax
import jax.numpy as jnp
from jax import lax
from jax.experimental import pallas as pl
from jax.experimental.pallas import tpu as pltpu
from jax.sharding import PartitionSpec as P

LOG2E = 1.4426950408889634
NEG = -1e30
VMEM_LIMIT = 60 * 1024 * 1024
MESH = pl.DeviceIdType.MESH
BF16, F32 = jnp.bfloat16, jnp.float32


def rms_norm(tensor, gain):
    mean_sq = jnp.mean(tensor * tensor, axis=-1, keepdims=True)
    return tensor * lax.rsqrt(mean_sq + 1e-6) * gain


def gated_unit(gate_pre, up_pre):
    return jax.nn.silu(gate_pre) * up_pre


def dot(a, b):
    return jnp.dot(a, b, preferred_element_type=F32)


def dot_nt(a, b):
    return lax.dot_general(a, b, (((1,), (1,)), ((), ())), preferred_element_type=F32)


def dot_tn(a, b):
    return lax.dot_general(a, b, (((0,), (0,)), ((), ())), preferred_element_type=F32)


def full(array):
    return pl.BlockSpec(array.shape, lambda *_: (0,) * array.ndim, pipeline_mode=pl.Buffered(1))


def vmem(count):
    return [pl.BlockSpec(memory_space=pltpu.VMEM)] * count


def plain(semantics=None):
    return pltpu.CompilerParams(vmem_limit_bytes=VMEM_LIMIT, dimension_semantics=semantics)


def remote(collective_id):
    return pltpu.CompilerParams(collective_id=collective_id, has_side_effects=True, vmem_limit_bytes=VMEM_LIMIT)


def shape(dims, dtype):
    return jax.ShapeDtypeStruct(dims, dtype)


def meet(peers):
    barrier = pltpu.get_barrier_semaphore()
    for peer in peers:
        pl.semaphore_signal(barrier, inc=1, device_id={'seq': peer}, device_id_type=MESH)
    pl.semaphore_wait(barrier, len(peers))


def send(src, dst, send_sem, recv_sem, peer):
    return pltpu.make_async_remote_copy(src_ref=src, dst_ref=dst, send_sem=send_sem, recv_sem=recv_sem,
                                        device_id={'seq': peer}, device_id_type=MESH)


def project_kernel(memory_ref, dec_ref, gain_ref, wk_ref, wv_ref, wq_ref, kv_ref, q_ref, normed_ref):
    group, hd = wk_ref.shape[0], wk_ref.shape[1]

    @pl.when(pl.program_id(0) == 0)
    def _():
        normed_ref[...] = rms_norm(dec_ref[...].astype(F32), gain_ref[...].astype(F32)).astype(BF16)

    weights = jnp.concatenate([part[i] for i in range(group) for part in (wk_ref, wv_ref)], axis=0)
    both = dot_nt(memory_ref[...], weights).astype(BF16)
    queries = dot_nt(normed_ref[...], jnp.concatenate([wq_ref[i] for i in range(group)], axis=0)).astype(BF16)
    for i in range(group):
        kv_ref[i] = both[:, 2 * hd * i:2 * hd * (i + 1)]
        q_ref[i] = queries[:, hd * i:hd * (i + 1)]


def project(memory, dec_in, gain, wk_t, wv_t, wq_t):
    heads, hd, dim = wk_t.shape
    rows, q_rows = memory.shape[0], dec_in.shape[0]
    group = 2
    weight = pl.BlockSpec((group, hd, dim), lambda i: (i, 0, 0))
    return pl.pallas_call(
        project_kernel,
        out_shape=[shape((heads, rows, 2 * hd), BF16), shape((heads, q_rows, hd), BF16)],
        grid=(heads // group,),
        in_specs=[full(memory), full(dec_in), full(gain), weight, weight, weight],
        out_specs=[pl.BlockSpec((group, rows, 2 * hd), lambda i: (i, 0, 0)),
                   pl.BlockSpec((group, q_rows, hd), lambda i: (i, 0, 0))],
        scratch_shapes=[pltpu.VMEM(dec_in.shape, BF16)],
        compiler_params=plain(),
        cost_estimate=pl.CostEstimate(flops=4 * rows * dim * heads * hd, bytes_accessed=8 * rows * dim, transcendentals=0),
        name='project',
    )(memory, dec_in, gain, wk_t, wv_t, wq_t)


def pair_peers(n, heads, me, part):
    parts = n // heads
    head = me // parts
    partner = head * parts + (parts - 1 - part)
    return partner, [partner] + [lax.rem(head + step, heads) * parts + part for step in range(1, heads)]


def pack(rows):
    middle = rows.shape[-2] // 2
    return jnp.concatenate([rows[..., :middle, :], rows[..., middle:, :]], axis=-1)


def unpack(packed):
    middle = packed.shape[-1] // 2
    return jnp.concatenate([packed[..., :middle], packed[..., middle:]], axis=-2)


def start_rows(n, heads, me, part, src, src_of, dst_ref, send_sem, recv_sem):
    parts = n // heads
    head = me // parts
    for step in range(1, heads):
        peer = lax.rem(head + step, heads) * parts + part
        send(src.at[src_of(peer)], dst_ref.at[head], send_sem, recv_sem, peer).start()
    dst_ref[head] = src[src_of(me)]


def wait_rows(heads, me, dst_ref, send_sem, recv_sem):
    others = dst_ref.at[pl.ds(0, heads - 1)]
    whole = send(others, others, send_sem, recv_sem, me)
    whole.wait_send()
    whole.wait_recv()


def swap(src, dst, send_sem, recv_sem, partner):
    copy = send(src, dst, send_sem, recv_sem, partner)
    copy.start()
    copy.wait()


def place(n, heads, part, mine_ref, theirs_ref, wide_ref, low):
    parts = n // heads
    for source, index in ((mine_ref, part), (theirs_ref, parts - 1 - part)):
        for head in range(heads):
            rows = unpack(source[head])
            zeros = jnp.zeros_like(rows)
            wide_ref[head * parts + index] = jnp.concatenate([rows, zeros] if low else [zeros, rows], axis=-1)


def exchange_kernel(n, heads, kv_ref, q_ref, kv_out_ref, q_out_ref, packed_ref, got_ref, swapped_ref, send_sem, recv_sem):
    me = lax.axis_index('seq')
    part = lax.rem(me, n // heads)
    partner, _ = pair_peers(n, heads, me, part)
    packed_ref[...] = pack(q_ref[...])
    meet([lax.rem(me + step, n) for step in range(1, n)])
    start_rows(n, heads, me, part, packed_ref, lambda peer: peer // (n // heads), got_ref, send_sem.at[1], recv_sem.at[1])
    for step in range(1, n):
        peer = lax.rem(me + step, n)
        send(kv_ref.at[peer], kv_out_ref.at[me], send_sem.at[0], recv_sem.at[0], peer).start()
    kv_out_ref[me] = kv_ref[me]
    wait_rows(heads, me, got_ref, send_sem.at[1], recv_sem.at[1])
    swap(got_ref, swapped_ref, send_sem.at[2], recv_sem.at[2], partner)
    place(n, heads, part, got_ref, swapped_ref, q_out_ref, True)
    others = kv_out_ref.at[pl.ds(0, n - 1)]
    whole = send(others, others, send_sem.at[0], recv_sem.at[0], me)
    whole.wait_send()
    whole.wait_recv()


def row_scratch(heads, q_rows, hd):
    return [pltpu.VMEM((heads, q_rows // 2, 2 * hd), BF16)] * 3


def exchange(n, heads, collective_id, kv, q):
    q_rows, hd = q.shape[1], q.shape[2]
    return pl.pallas_call(
        functools.partial(exchange_kernel, n, heads),
        out_shape=[shape(kv.shape, BF16), shape((n, q_rows, 2 * hd), BF16)],
        in_specs=vmem(2),
        out_specs=vmem(2),
        scratch_shapes=row_scratch(heads, q_rows, hd) + [pltpu.SemaphoreType.DMA((3,)), pltpu.SemaphoreType.DMA((3,))],
        compiler_params=remote(collective_id),
        name='exchange',
    )(kv, q)


def return_kernel(n, src_ref, dst_ref, send_sem, recv_sem):
    me = lax.axis_index('seq')
    meet([lax.rem(me + step, n) for step in range(1, n)])
    for step in range(1, n):
        peer = lax.rem(me + step, n)
        send(src_ref.at[peer], dst_ref.at[me], send_sem, recv_sem, peer).start()
    dst_ref[me] = src_ref[me]
    others = dst_ref.at[pl.ds(0, n - 1)]
    whole = send(others, others, send_sem, recv_sem, me)
    whole.wait_send()
    whole.wait_recv()


def return_blocks(n, collective_id, blocks):
    return pl.pallas_call(
        functools.partial(return_kernel, n),
        out_shape=shape(blocks.shape, BF16),
        in_specs=vmem(1),
        out_specs=vmem(1)[0],
        scratch_shapes=[pltpu.SemaphoreType.DMA, pltpu.SemaphoreType.DMA],
        compiler_params=remote(collective_id),
        name='return_blocks',
    )(blocks)


def to_heads_kernel(n, heads, rows_ref, wide_ref, packed_ref, got_ref, swapped_ref, send_sem, recv_sem):
    me = lax.axis_index('seq')
    part = lax.rem(me, n // heads)
    partner, peers = pair_peers(n, heads, me, part)
    packed_ref[...] = pack(rows_ref[...])
    meet(peers)
    start_rows(n, heads, me, part, packed_ref, lambda peer: peer // (n // heads), got_ref, send_sem.at[0], recv_sem.at[0])
    wait_rows(heads, me, got_ref, send_sem.at[0], recv_sem.at[0])
    swap(got_ref, swapped_ref, send_sem.at[1], recv_sem.at[1], partner)
    place(n, heads, part, got_ref, swapped_ref, wide_ref, False)


def to_heads(n, heads, collective_id, rows):
    q_rows, hd = rows.shape[1], rows.shape[2]
    return pl.pallas_call(
        functools.partial(to_heads_kernel, n, heads),
        out_shape=shape((n, q_rows, 2 * hd), BF16),
        in_specs=vmem(1),
        out_specs=vmem(1)[0],
        scratch_shapes=row_scratch(heads, q_rows, hd) + [pltpu.SemaphoreType.DMA((2,)), pltpu.SemaphoreType.DMA((2,))],
        compiler_params=remote(collective_id),
        name='to_heads',
    )(rows)


def to_rows(n, heads, q_rows, me, part, values, packed_ref, got_ref, rows_ref, send_sem, recv_sem):
    packed_ref[...] = pack(values.T.astype(BF16).reshape(n, q_rows, values.shape[0]))
    start_rows(n, heads, me, part, packed_ref, lambda peer: peer, got_ref, send_sem, recv_sem)
    wait_rows(heads, me, got_ref, send_sem, recv_sem)
    rows_ref[...] = unpack(got_ref[...])


def combine_kernel(n, heads, hd, q_rows, mine_ref, rows_ref, out_ref, lse_ref, theirs_ref, packed_ref, got_ref, send_sem, recv_sem):
    me = lax.axis_index('seq')
    part = lax.rem(me, n // heads)
    partner, peers = pair_peers(n, heads, me, part)
    meet(peers)
    swap(mine_ref, theirs_ref, send_sem.at[0], recv_sem.at[0], partner)
    m_a, m_b = mine_ref[hd + 8:hd + 9], theirs_ref[hd + 8:hd + 9]
    top = jnp.maximum(m_a, m_b)
    s_a, s_b = jnp.exp2(m_a - top), jnp.exp2(m_b - top)
    den = mine_ref[hd:hd + 1] * s_a + theirs_ref[hd:hd + 1] * s_b
    out = (mine_ref[:hd] * s_a + theirs_ref[:hd] * s_b) / den
    out_ref[...] = out
    lse_ref[...] = top + jnp.log2(den)
    to_rows(n, heads, q_rows, me, part, out, packed_ref, got_ref, rows_ref, send_sem.at[1], recv_sem.at[1])


def pair_scratch(n, heads, hd, q_rows, mine):
    return [pltpu.VMEM(mine.shape, F32), pltpu.VMEM((n, q_rows // 2, 2 * hd), BF16), pltpu.VMEM((heads, q_rows // 2, 2 * hd), BF16),
            pltpu.SemaphoreType.DMA((2,)), pltpu.SemaphoreType.DMA((2,))]


def combine(n, heads, hd, q_rows, collective_id, mine):
    total_q = mine.shape[1]
    return pl.pallas_call(
        functools.partial(combine_kernel, n, heads, hd, q_rows),
        out_shape=[shape((heads, q_rows, hd), BF16), shape((hd, total_q), F32), shape((1, total_q), F32)],
        in_specs=vmem(1),
        out_specs=vmem(3),
        scratch_shapes=pair_scratch(n, heads, hd, q_rows, mine),
        compiler_params=remote(collective_id),
        name='combine',
    )(mine)


def pair_sum_kernel(n, heads, q_rows, mine_ref, rows_ref, share_ref, theirs_ref, packed_ref, got_ref, send_sem, recv_sem):
    me = lax.axis_index('seq')
    part = lax.rem(me, n // heads)
    partner, peers = pair_peers(n, heads, me, part)
    meet(peers)
    swap(mine_ref, theirs_ref, send_sem.at[0], recv_sem.at[0], partner)
    total = mine_ref[...] + theirs_ref[...]
    width = share_ref.shape[1]
    share_ref[...] = jnp.where(part == 0, total[:, :width], total[:, width:]).astype(BF16)
    to_rows(n, heads, q_rows, me, part, total, packed_ref, got_ref, rows_ref, send_sem.at[1], recv_sem.at[1])


def pair_sum(n, heads, q_rows, collective_id, mine):
    hd, total_q = mine.shape
    return pl.pallas_call(
        functools.partial(pair_sum_kernel, n, heads, q_rows),
        out_shape=[shape((heads, q_rows, hd), BF16), shape((hd, total_q * heads // n), BF16)],
        in_specs=vmem(1),
        out_specs=vmem(2),
        scratch_shapes=pair_scratch(n, heads, hd, q_rows, mine),
        compiler_params=remote(collective_id),
        name='pair_sum',
    )(mine)


def small_sum_kernel(n, mine_ref, total_ref, all_ref, send_sem, recv_sem):
    me = lax.axis_index('seq')
    meet([lax.rem(me + step, n) for step in range(1, n)])
    for step in range(1, n):
        send(mine_ref, all_ref.at[me], send_sem, recv_sem, lax.rem(me + step, n)).start()
    all_ref[me] = mine_ref[...]
    others = all_ref.at[pl.ds(0, n - 1)]
    whole = send(others, others, send_sem, recv_sem, me)
    whole.wait_send()
    whole.wait_recv()
    total_ref[...] = jnp.sum(all_ref[...], axis=0)


def small_sum(n, collective_id, mine):
    return pl.pallas_call(
        functools.partial(small_sum_kernel, n),
        out_shape=shape(mine.shape, F32),
        in_specs=vmem(1),
        out_specs=vmem(1)[0],
        scratch_shapes=[pltpu.VMEM((n,) + mine.shape, F32), pltpu.SemaphoreType.DMA, pltpu.SemaphoreType.DMA],
        compiler_params=remote(collective_id),
        name='small_sum',
    )(mine)


def forward_kernel(scale, hd, q_block, bounds_ref, kv_ref, q_ref, out_ref, qt_ref, top_ref):
    blocks, last_valid = bounds_ref[0], bounds_ref[1]
    rows, total_q = kv_ref.shape[1], q_ref.shape[0]
    groups = [slice(first, first + q_block) for first in range(0, total_q, q_block)]
    base = slice(hd + 8, hd + 9)
    qt_ref[...] = q_ref[...].T

    def masked_scores(scores):
        position = lax.broadcasted_iota(jnp.int32, scores.shape, 0)
        return jnp.where(position < last_valid, scores, NEG)

    def values_of(keys):
        return jnp.concatenate([keys.T[hd:], jnp.ones((16, rows), keys.dtype)], axis=0)

    for cols in groups:
        top = jnp.max(dot(kv_ref[0], qt_ref[:, cols]), axis=0, keepdims=True)
        out_ref[hd + 8:, cols] = jnp.broadcast_to(top * scale, (8, q_block))
        top_ref[:, cols] = jnp.broadcast_to(top, (8, q_block))
    out_ref[:hd + 8, :] = jnp.zeros((hd + 8, total_q), F32)

    def block(index, masked):
        keys = kv_ref[index]
        values = values_of(keys)
        ahead = dot(keys, qt_ref[:, groups[0]])
        for i, cols in enumerate(groups):
            scores = masked_scores(ahead) if masked else ahead
            if i + 1 < len(groups):
                ahead = dot(keys, qt_ref[:, groups[i + 1]])
            top_ref[:, cols] = jnp.maximum(top_ref[:, cols], jnp.max(scores.reshape(rows // 8, 8, q_block), axis=0))
            weights = jnp.exp2(scores * scale - out_ref[base, cols]).astype(keys.dtype)
            out_ref[:hd + 8, cols] += dot(values, weights)[:hd + 8]

    def step(index, carry):
        block(index, False)
        return carry

    lax.fori_loop(0, blocks - 1, step, 0)
    block(blocks - 1, True)

    excess = jnp.max(top_ref[...] * scale - out_ref[hd + 8:, :])

    @pl.when(excess > 16.0)
    def _():
        out_ref[:hd + 8, :] = jnp.zeros((hd + 8, total_q), F32)
        out_ref[hd + 8:, :] = jnp.full((8, total_q), NEG, F32)

        def running(step_index, carry):
            index, group = step_index // len(groups), lax.rem(step_index, len(groups))
            cols = pl.ds(pl.multiple_of(group * q_block, q_block), q_block)
            keys = kv_ref[index]
            limit = jnp.where(index == blocks - 1, last_valid, rows)
            scores = dot(keys, qt_ref[:, cols]) * scale
            position = lax.broadcasted_iota(jnp.int32, scores.shape, 0)
            scores = jnp.where(position < limit, scores, NEG)
            old = out_ref[base, cols]
            new = jnp.maximum(old, jnp.max(scores, axis=0, keepdims=True))
            weights = jnp.exp2(scores - new).astype(keys.dtype)
            out_ref[:hd + 8, cols] = out_ref[:hd + 8, cols] * jnp.exp2(old - new) + dot(values_of(keys), weights)[:hd + 8]
            out_ref[hd + 8:, cols] = jnp.broadcast_to(new, (8, q_block))
            return carry

        lax.fori_loop(0, blocks * len(groups), running, 0)


def attention_forward(scale, hd, sources, bounds, kv, q):
    rows, width = kv.shape[1], kv.shape[2]
    total_q = q.shape[0]
    return pl.pallas_call(
        functools.partial(forward_kernel, scale, hd, min(512, total_q)),
        out_shape=shape((hd + 16, total_q), F32),
        grid=(1,),
        in_specs=[pl.BlockSpec(memory_space=pltpu.SMEM),
                  pl.BlockSpec((sources, rows, width), lambda i: (0, 0, 0), pipeline_mode=pl.Buffered(1)), full(q)],
        out_specs=pl.BlockSpec((hd + 16, total_q), lambda i: (0, 0)),
        scratch_shapes=[pltpu.VMEM((width, total_q), BF16), pltpu.VMEM((8, total_q), F32)],
        compiler_params=plain(),
        cost_estimate=pl.CostEstimate(flops=4 * total_q * sources * rows * hd, bytes_accessed=kv.size * 2,
                                      transcendentals=total_q * sources * rows),
        name='attention_forward',
    )(bounds, kv, q)


def backward_kernel(scale, key_scale, hd, q_block, bounds_ref, kv_ref, q_ref, do_ref, out_ref, lse_ref, dkv_ref, dq_ref,
                    qt_ref, dot_ref, delta_ref):
    blocks, last_valid = bounds_ref[0], bounds_ref[1]
    rows, total_q = kv_ref.shape[1], q_ref.shape[0]
    width = kv_ref.shape[2]
    groups = [slice(first, first + q_block) for first in range(0, total_q, q_block)]
    dq_ref[...] = jnp.zeros_like(dq_ref)
    qt_ref[...] = q_ref[...].T
    do_t = do_ref[...].T
    dot_ref[...] = do_t
    delta_ref[...] = jnp.sum(do_t[hd:].astype(F32) * out_ref[...], axis=0, keepdims=True)

    def step(index, carry):
        keys = kv_ref[index]
        keys_t = keys.T[:hd]
        limit = jnp.where(index == blocks - 1, last_valid, rows)
        grad_k, grad_v = jnp.zeros((hd, rows), F32), jnp.zeros((hd, rows), F32)
        ahead = dot(keys, qt_ref[:, groups[0]]), dot(keys, dot_ref[:, groups[0]])
        for i, cols in enumerate(groups):
            scores, grads = ahead
            if i + 1 < len(groups):
                ahead = dot(keys, qt_ref[:, groups[i + 1]]), dot(keys, dot_ref[:, groups[i + 1]])
            position = lax.broadcasted_iota(jnp.int32, scores.shape, 0)
            prob = jnp.exp2(jnp.where(position < limit, scores * scale - lse_ref[:, cols], NEG))
            grad_scores = (prob * (grads - delta_ref[:, cols])).astype(keys.dtype)
            dq_ref[:, cols] += dot(keys_t, grad_scores)
            grad_k += dot_nt(qt_ref[:hd, cols], grad_scores)
            grad_v += dot_nt(dot_ref[hd:, cols], prob.astype(keys.dtype))
        dkv_ref[index] = jnp.concatenate([grad_k * key_scale, grad_v], axis=0).T.astype(dkv_ref.dtype)
        return carry

    def clear(index, carry):
        dkv_ref[index] = jnp.zeros((rows, width), dkv_ref.dtype)
        return carry

    lax.fori_loop(0, blocks, step, 0)
    lax.fori_loop(blocks, dkv_ref.shape[0], clear, 0)
    dq_ref[...] = dq_ref[...] * key_scale


def attention_backward(scale, key_scale, hd, sources, bounds, kv, q, do, out_t, lse):
    n, rows, width = kv.shape
    total_q = q.shape[0]
    return pl.pallas_call(
        functools.partial(backward_kernel, scale, key_scale, hd, min(512, total_q)),
        out_shape=[shape((n, rows, width), BF16), shape((hd, total_q), F32)],
        grid=(1,),
        in_specs=[pl.BlockSpec(memory_space=pltpu.SMEM),
                  pl.BlockSpec((sources, rows, width), lambda i: (0, 0, 0), pipeline_mode=pl.Buffered(1)),
                  full(q), full(do), full(out_t), full(lse)],
        out_specs=[pl.BlockSpec((n, rows, width), lambda i: (0, 0, 0)),
                   pl.BlockSpec((hd, total_q), lambda i: (0, 0))],
        scratch_shapes=[pltpu.VMEM((width, total_q), BF16), pltpu.VMEM((width, total_q), BF16), pltpu.VMEM((1, total_q), F32)],
        compiler_params=plain(),
        cost_estimate=pl.CostEstimate(flops=10 * total_q * sources * rows * hd, bytes_accessed=kv.size * 4,
                                      transcendentals=total_q * sources * rows),
        name='attention_backward',
    )(bounds, kv, q, do, out_t, lse)


def prepare_kernel(dec_ref, att_ref, wo_ref, gain_ref, n2_ref, n2t_ref):
    hidden = (dec_ref[...].astype(F32) + dot(att_ref[...], wo_ref[...])).astype(BF16)
    normed = rms_norm(hidden.astype(F32), gain_ref[...].astype(F32)).astype(BF16)
    n2_ref[...] = normed
    n2t_ref[...] = normed.T


def prepare(early, late, wo, gain):
    rows, dim = early.shape[0], wo.shape[1]
    chunk = min(512, rows)
    left = pl.BlockSpec((chunk, dim), lambda i: (i, 0))
    return pl.pallas_call(
        prepare_kernel,
        out_shape=[shape((rows, dim), BF16), shape((dim, rows), BF16)],
        grid=(rows // chunk,),
        in_specs=[left, pl.BlockSpec((chunk, wo.shape[0]), lambda i: (i, 0)), full(wo), full(gain)],
        out_specs=[left, pl.BlockSpec((dim, chunk), lambda i: (0, i))],
        compiler_params=plain(),
        cost_estimate=pl.CostEstimate(flops=2 * rows * dim * dim, bytes_accessed=8 * rows * dim, transcendentals=0),
        name='prepare',
    )(early, late, wo, gain)


def mlp_kernel(chunk, n2_ref, n2t_ref, top_ref, w1_ref, w3_ref, w2_ref, g1_ref, g3_ref, g2_ref, d1_ref, d3_ref, act_ref):
    rows = n2_ref.shape[0]
    w1, w3, w2t = w1_ref[...], w3_ref[...], w2_ref[...].T
    for first in range(0, rows, chunk):
        part = slice(first, first + chunk)
        gate = dot(n2_ref[part, :], w1)
        up = dot(n2_ref[part, :], w3)
        grad = dot(top_ref[part, :], w2t)
        sig = jax.nn.sigmoid(gate)
        silu = gate * sig
        act_ref[part, :] = (silu * up).astype(act_ref.dtype)
        d3_ref[part, :] = (grad * silu).astype(d3_ref.dtype)
        d1_ref[part, :] = (grad * up * (sig + silu * (1.0 - sig))).astype(d1_ref.dtype)
    g1_ref[...] = dot(n2t_ref[...], d1_ref[...])
    g3_ref[...] = dot(n2t_ref[...], d3_ref[...])
    g2_ref[...] = dot_tn(act_ref[...], top_ref[...])


def mlp_weight_grads(n2, n2t, early, w_gate, w_up, w_down):
    rows, dim = n2.shape
    ff = w_gate.shape[1]
    tile = 256
    cols = pl.BlockSpec((dim, tile), lambda i: (0, i))
    tall = pl.BlockSpec((tile, dim), lambda i: (i, 0))
    return pl.pallas_call(
        functools.partial(mlp_kernel, min(512, rows)),
        out_shape=[shape((dim, ff), F32), shape((dim, ff), F32), shape((ff, dim), F32)],
        grid=(ff // tile,),
        in_specs=[full(n2), full(n2t), pl.BlockSpec((rows, dim), lambda i: (0, 1), pipeline_mode=pl.Buffered(1)), cols, cols, tall],
        out_specs=[cols, cols, tall],
        scratch_shapes=[pltpu.VMEM((rows, tile), BF16)] * 3,
        compiler_params=plain(),
        cost_estimate=pl.CostEstimate(flops=12 * rows * dim * ff, bytes_accessed=18 * dim * ff, transcendentals=rows * ff),
        name='mlp_weight_grads',
    )(n2, n2t, early, w_gate, w_up, w_down)


def memory_weight_kernel(memory_ref, dkv_ref, gk_ref, gv_ref):
    group, hd = dkv_ref.shape[0], dkv_ref.shape[2] // 2
    for i in range(group):
        both = dot_tn(dkv_ref[i], memory_ref[...])
        gk_ref[i * hd:(i + 1) * hd, :] = both[:hd]
        gv_ref[i * hd:(i + 1) * hd, :] = both[hd:]


def memory_weight_grads(memory, dkv):
    heads, rows, width = dkv.shape
    dim, hd = memory.shape[1], width // 2
    group = 4
    out = pl.BlockSpec((group * hd, dim), lambda i: (i, 0))
    return pl.pallas_call(
        memory_weight_kernel,
        out_shape=[shape((heads * hd, dim), F32)] * 2,
        grid=(heads // group,),
        in_specs=[full(memory), pl.BlockSpec((group, rows, width), lambda i: (i, 0, 0))],
        out_specs=[out, out],
        compiler_params=plain(),
        cost_estimate=pl.CostEstimate(flops=2 * rows * dim * heads * width, bytes_accessed=16 * rows * dim, transcendentals=0),
        name='memory_weight_grads',
    )(memory, dkv)


def memory_grad_kernel(dkv_ref, wk_ref, wv_ref, out_ref):
    group = dkv_ref.shape[0]
    left = jnp.concatenate([dkv_ref[i] for i in range(group)], axis=1)
    right = jnp.concatenate([part[i] for i in range(group) for part in (wk_ref, wv_ref)], axis=0)

    @pl.when(pl.program_id(0) == 0)
    def _():
        out_ref[...] = dot(left, right)

    @pl.when(pl.program_id(0) > 0)
    def _():
        out_ref[...] += dot(left, right)


def memory_grad(dkv, wk_t, wv_t):
    heads, rows, width = dkv.shape
    hd, dim = wk_t.shape[1], wk_t.shape[2]
    group = 4
    weight = pl.BlockSpec((group, hd, dim), lambda i: (i, 0, 0))
    return pl.pallas_call(
        memory_grad_kernel,
        out_shape=shape((rows, dim), F32),
        grid=(heads // group,),
        in_specs=[pl.BlockSpec((group, rows, width), lambda i: (i, 0, 0)), weight, weight],
        out_specs=pl.BlockSpec((rows, dim), lambda i: (0, 0)),
        compiler_params=plain(),
        cost_estimate=pl.CostEstimate(flops=2 * rows * dim * heads * width, bytes_accessed=12 * rows * dim, transcendentals=0),
        name='memory_grad',
    )(dkv, wk_t, wv_t)


def outer_kernel(dec_ref, gain_ref, att_ref, gh_ref, dq_ref, gwo_ref, gwq_ref, n1_ref):
    @pl.when(pl.program_id(0) == 0)
    def _():
        n1_ref[...] = rms_norm(dec_ref[...].astype(F32), gain_ref[...].astype(F32)).astype(BF16)

    group, parts, hd, share = dq_ref.shape
    gwo_ref[...] = dot_tn(att_ref[...], gh_ref[...])
    total = None
    for p in range(parts):
        left = jnp.concatenate([dq_ref[i, p] for i in range(group)], axis=0)
        term = dot(left, n1_ref[p * share:(p + 1) * share, :])
        total = term if total is None else total + term
    gwq_ref[...] = total


def outer_weight_grads(early, late, gain, dq_all):
    heads, parts, hd, share = dq_all.shape
    rows, dim = early.shape[0], gain.shape[1]
    group = 4
    out = pl.BlockSpec((group * hd, dim), lambda i: (i, 0))
    return pl.pallas_call(
        outer_kernel,
        out_shape=[shape((heads * hd, dim), F32)] * 2,
        grid=(heads // group,),
        in_specs=[pl.BlockSpec((rows, dim), lambda i: (0, 0), pipeline_mode=pl.Buffered(1)), full(gain),
                  pl.BlockSpec((rows, group * hd), lambda i: (0, i)),
                  pl.BlockSpec((rows, dim), lambda i: (0, 1), pipeline_mode=pl.Buffered(1)),
                  pl.BlockSpec((group, parts, hd, share), lambda i: (i, 0, 0, 0))],
        out_specs=[out, out],
        scratch_shapes=[pltpu.VMEM((rows, dim), BF16)],
        compiler_params=plain(),
        cost_estimate=pl.CostEstimate(flops=4 * rows * dim * heads * hd, bytes_accessed=16 * rows * dim, transcendentals=0),
        name='outer_weight_grads',
    )(early, gain, late, late, dq_all)


def solution(mesh):
    n = mesh.shape['seq']
    row_spec = P(('data', 'seq'), None)
    weight_spec = P()
    part_vec = P('data')
    part_mat = P('data', None)
    part_cube = P('data', None, None)

    def device_step(dec_in, memory, mem_len, grad_out, norm_attn, wq_cross, wk_cross, wv_cross, wo_cross, norm_mlp, w_gate, w_up, w_down):
        q_rows, dim = dec_in.shape
        m_rows = memory.shape[0]
        heads, hd = wq_cross.shape[1], wq_cross.shape[2]
        parts = n // heads
        half = m_rows // parts
        sources = -(-3 * n // 4)
        total_q = q_rows * n
        key_scale = hd ** -0.5
        scale = key_scale * LOG2E
        me = lax.axis_index('seq')
        part = lax.rem(me, parts)

        reach = mem_len[0] - part * half
        blocks = jnp.minimum((reach + m_rows - 1) // m_rows, sources)
        bounds = jnp.stack([blocks, jnp.minimum(reach - (blocks - 1) * m_rows, half)]).astype(jnp.int32)

        wq_t, wk_t, wv_t = (jnp.transpose(w, (1, 2, 0)) for w in (wq_cross, wk_cross, wv_cross))
        gain_attn, gain_mlp = norm_attn.reshape(1, dim), norm_mlp.reshape(1, dim)
        local_kv, local_q = project(memory, dec_in, gain_attn, wk_t, wv_t, wq_t)
        kv, q_in = exchange(n, heads, 0, local_kv.reshape(n, half, 2 * hd), local_q)
        head_q = q_in.reshape(total_q, 2 * hd)

        grad_top = grad_out.astype(BF16)
        early_local, kv = lax.optimization_barrier((jnp.concatenate([dec_in, grad_top], axis=1), kv))
        early = lax.all_gather(early_local, 'seq', axis=0, tiled=True)

        mine = attention_forward(scale, hd, sources, bounds, kv, head_q)
        attended, out_t, lse = combine(n, heads, hd, q_rows, 1, mine)

        x_in = dec_in.astype(F32)
        hidden_f = x_in + jnp.einsum('hqe,hed->qd', attended, wo_cross, preferred_element_type=F32)
        hidden = hidden_f.astype(BF16)
        normed_mlp_f, mlp_norm_pull = jax.vjp(rms_norm, hidden.astype(F32), norm_mlp.astype(F32))
        normed_mlp = normed_mlp_f.astype(BF16)
        gate_pre = jnp.dot(normed_mlp, w_gate, preferred_element_type=F32)
        up_pre = jnp.dot(normed_mlp, w_up, preferred_element_type=F32)
        _, gated_pull = jax.vjp(gated_unit, gate_pre, up_pre)
        grad_act = jnp.einsum('qd,fd->qf', grad_top, w_down, preferred_element_type=F32)
        grad_gate, grad_up = gated_pull(grad_act)
        grad_normed_mlp = (jnp.einsum('qf,df->qd', grad_gate.astype(BF16), w_gate, preferred_element_type=F32)
                           + jnp.einsum('qf,df->qd', grad_up.astype(BF16), w_up, preferred_element_type=F32))
        grad_hidden_norm, g_norm_mlp = mlp_norm_pull(grad_normed_mlp)
        grad_hidden = grad_out + grad_hidden_norm
        grad_hidden_b = grad_hidden.astype(BF16)
        grad_att = jnp.einsum('qd,hed->hqe', grad_hidden_b, wo_cross, preferred_element_type=F32).astype(BF16)
        head_do = to_heads(n, heads, 2, grad_att).reshape(total_q, 2 * hd)

        late_local = jnp.concatenate([attended.transpose(1, 0, 2).reshape(q_rows, heads * hd), grad_hidden_b], axis=1)
        head_do, late_local, early = lax.optimization_barrier((head_do, late_local, early))
        late = lax.all_gather(late_local, 'seq', axis=0, tiled=True)

        dkv, dq_part = attention_backward(scale, key_scale, hd, sources, bounds, kv, head_q, head_do, out_t, lse)
        dq_rows, dq_share = pair_sum(n, heads, q_rows, 3, dq_part)
        dkv, dq_share, late = lax.optimization_barrier((dkv, dq_share, late))
        dq_all = lax.all_gather(dq_share, 'seq', axis=0, tiled=False).reshape(heads, parts, hd, total_q // parts)
        dkv_in = return_blocks(n, 4, dkv).reshape(heads, m_rows, 2 * hd)
        dkv_in, dq_all, dq_rows = lax.optimization_barrier((dkv_in, dq_all, dq_rows))

        gk_part, gv_part = memory_weight_grads(memory, dkv_in)
        gk_part, gv_part, dkv_in, dq_all, dq_rows, early, late = lax.optimization_barrier(
            (gk_part, gv_part, dkv_in, dq_all, dq_rows, early, late))
        g_wk, g_wv = lax.psum((gk_part, gv_part), 'seq')

        n2_all, n2_all_t = prepare(early, late, wo_cross.reshape(heads * hd, dim), gain_mlp)
        g_gate, g_up, g_down = mlp_weight_grads(n2_all, n2_all_t, early, w_gate, w_up, w_down)
        g_wo, g_wq = outer_weight_grads(early, late, gain_attn, dq_all)

        grad_normed = jnp.einsum('hte,dhe->td', dq_rows, wq_cross, preferred_element_type=F32)
        _, norm_pull = jax.vjp(rms_norm, x_in, norm_attn.astype(F32))
        grad_x_norm, g_norm_attn = norm_pull(grad_normed)
        g_dec = grad_hidden + grad_x_norm
        norms = small_sum(n, 5, jnp.concatenate([g_norm_attn, g_norm_mlp]).reshape(-1, 128)).reshape(2, dim)
        g_mem = memory_grad(dkv_in, wk_t, wv_t)
        cube = lambda g: jnp.transpose(g.reshape(heads, hd, dim), (2, 0, 1))
        return (g_dec, g_mem, norms[0], cube(g_wq), cube(g_wk), cube(g_wv), g_wo.reshape(heads, hd, dim), norms[1], g_gate, g_up, g_down)

    return jax.shard_map(device_step, mesh=mesh,
                         in_specs=(row_spec, row_spec, part_vec, row_spec) + (weight_spec,) * 9,
                         out_specs=(row_spec, row_spec, part_vec, part_cube, part_cube, part_cube, part_cube, part_vec, part_mat, part_mat, part_mat),
                         check_vma=False)
```

```python
import functools
import math

import jax
import jax.numpy as jnp
from jax import lax
from jax.experimental import pallas as pl
from jax.experimental.pallas import tpu as pltpu
from jax.sharding import PartitionSpec as P

LOG2E = 1.4426950408889634
NEG = -1e30
VMEM_LIMIT = 60 * 1024 * 1024
MESH = pl.DeviceIdType.MESH
BF16, F32 = jnp.bfloat16, jnp.float32


def rms_norm(tensor, gain):
    mean_sq = jnp.mean(tensor * tensor, axis=-1, keepdims=True)
    return tensor * lax.rsqrt(mean_sq + 1e-6) * gain


def gated_unit(gate_pre, up_pre):
    return jax.nn.silu(gate_pre) * up_pre


def dot(a, b):
    return jnp.dot(a, b, preferred_element_type=F32)


def dot_nt(a, b):
    return lax.dot_general(a, b, (((1,), (1,)), ((), ())), preferred_element_type=F32)


def dot_tn(a, b):
    return lax.dot_general(a, b, (((0,), (0,)), ((), ())), preferred_element_type=F32)


def full(array):
    return pl.BlockSpec(array.shape, lambda *_: (0,) * array.ndim, pipeline_mode=pl.Buffered(1))


def vmem(count):
    return [pl.BlockSpec(memory_space=pltpu.VMEM)] * count


def plain(semantics=None):
    return pltpu.CompilerParams(vmem_limit_bytes=VMEM_LIMIT, dimension_semantics=semantics)


def remote(collective_id):
    return pltpu.CompilerParams(collective_id=collective_id, has_side_effects=True, vmem_limit_bytes=VMEM_LIMIT)


def shape(dims, dtype):
    return jax.ShapeDtypeStruct(dims, dtype)


def meet(peers):
    barrier = pltpu.get_barrier_semaphore()
    for peer in peers:
        pl.semaphore_signal(barrier, inc=1, device_id={'seq': peer}, device_id_type=MESH)
    pl.semaphore_wait(barrier, len(peers))


def send(src, dst, send_sem, recv_sem, peer):
    return pltpu.make_async_remote_copy(src_ref=src, dst_ref=dst, send_sem=send_sem, recv_sem=recv_sem,
                                        device_id={'seq': peer}, device_id_type=MESH)


class Grid:
    def __init__(self, n, heads, source_rows):
        self.n, self.heads, self.source_rows = n, heads, source_rows
        self.parts = n // heads
        self.side = math.isqrt(heads)
        self.me = lax.axis_index('seq')
        self.part = lax.rem(self.me, self.parts)
        self.chip = self.me // self.parts
        self.col = lax.rem(self.chip, self.side)
        self.row = self.chip // self.side
        self.partner = self.chip * self.parts + (self.parts - 1 - self.part)
        self.ties = self.side == 4
        self.direct = (1, 3) if self.ties else (1,)

    def wrap(self, value):
        return lax.rem(value + self.side, self.side)

    def device(self, row, col, part):
        return (row * self.side + col) * self.parts + part

    def near(self, drow, dcol, part=None):
        return self.device(self.wrap(self.row + drow), self.wrap(self.col + dcol), self.part if part is None else part)

    def hop(self, offset):
        return 1 if offset == 1 else -1

    def is_source(self, row):
        return self.wrap(row) < self.source_rows

    def row_peers(self):
        return [lax.rem(self.chip + step, self.heads) * self.parts + self.part for step in range(1, self.heads)]

    def peers(self):
        return self.row_peers() + [self.partner] + [self.near(0, self.hop(d), self.parts - 1 - self.part) for d in self.direct]


def pair_peers(n, heads, me, part):
    parts = n // heads
    head = me // parts
    partner = head * parts + (parts - 1 - part)
    return partner, [partner] + [lax.rem(head + step, heads) * parts + part for step in range(1, heads)]


def pack(rows):
    middle = rows.shape[-2] // 2
    return jnp.concatenate([rows[..., :middle, :], rows[..., middle:, :]], axis=-1)


def unpack(packed):
    middle = packed.shape[-1] // 2
    return jnp.concatenate([packed[..., :middle], packed[..., middle:]], axis=-2)


def start_rows(n, heads, me, part, src, src_of, dst_ref, send_sem, recv_sem):
    parts = n // heads
    head = me // parts
    for step in range(1, heads):
        peer = lax.rem(head + step, heads) * parts + part
        send(src.at[src_of(peer)], dst_ref.at[head], send_sem, recv_sem, peer).start()
    dst_ref[head] = src[src_of(me)]


def wait_rows(heads, me, dst_ref, send_sem, recv_sem):
    others = dst_ref.at[pl.ds(0, heads - 1)]
    whole = send(others, others, send_sem, recv_sem, me)
    whole.wait_send()
    whole.wait_recv()


def swap(src, dst, send_sem, recv_sem, partner):
    copy = send(src, dst, send_sem, recv_sem, partner)
    copy.start()
    copy.wait()


def place(n, heads, part, mine_ref, theirs_ref, wide_ref, low):
    parts = n // heads
    for source, index in ((mine_ref, part), (theirs_ref, parts - 1 - part)):
        for head in range(heads):
            rows = unpack(source[head])
            zeros = jnp.zeros_like(rows)
            wide_ref[head * parts + index] = jnp.concatenate([rows, zeros] if low else [zeros, rows], axis=-1)


def exchange_kernel(n, heads, source_rows, memory_ref, dec_ref, gain_ref, wk_ref, wv_ref, wq_ref, kv_out_ref, q_out_ref,
                    kv_ref, stage_ref, up_ref, down_ref, right_ref, left_ref, packed_ref, got_ref, swapped_ref,
                    row_send, row_recv, y_send, pass_send, x_send, fwd_send, stage_recv, up_recv, down_recv, right_recv,
                    left_recv, out_recv):
    g = Grid(n, heads, source_rows)
    side, hd = g.side, wk_ref.shape[1]
    half = kv_out_ref.shape[1]
    chunk_rows = min(256, kv_ref.shape[1])
    barrier = pltpu.get_barrier_semaphore()
    peers = g.peers()
    for peer in peers:
        pl.semaphore_signal(barrier, inc=1, device_id={'seq': peer}, device_id_type=MESH)

    normed = rms_norm(dec_ref[...].astype(F32), gain_ref[...].astype(F32)).astype(BF16)
    for i in range(0, heads, 4):
        queries = dot_nt(normed, jnp.concatenate([wq_ref[i + j] for j in range(4)], axis=0)).astype(BF16)
        for j in range(4):
            packed_ref[i + j] = pack(queries[:, hd * j:hd * (j + 1)])

    def head(drow, dcol):
        return g.wrap(g.row + drow) * side + g.wrap(g.col + dcol)

    def project(drow, dcols):
        weights = jnp.concatenate([ref[head(drow, d)] for d in dcols for ref in (wk_ref, wv_ref)], axis=0)

        def rows(index, carry):
            at = pl.ds(pl.multiple_of(index * chunk_rows, chunk_rows), chunk_rows)
            both = dot_nt(memory_ref[at, :], weights).astype(BF16)
            for i, d in enumerate(dcols):
                kv_ref[head(drow, d), at, :] = both[:, 2 * hd * i:2 * hd * (i + 1)]
            return carry

        lax.fori_loop(0, kv_ref.shape[1] // chunk_rows, rows, 0)

    def along_column(drow, dcol):
        chunk = kv_ref.at[head(drow, dcol)]
        if drow in g.direct:
            send(chunk, stage_ref.at[drow - 1, dcol], y_send.at[drow - 1], stage_recv.at[drow - 1, dcol], g.near(g.hop(drow), 0)).start()
        elif dcol % 2 == 0:
            send(chunk, up_ref.at[dcol // 2], y_send.at[drow - 1], up_recv.at[dcol // 2], g.near(1, 0)).start()
        else:
            send(chunk, down_ref.at[dcol // 2], y_send.at[drow - 1], down_recv.at[dcol // 2], g.near(-1, 0)).start()

    def along_row(o, dcol):
        chunk = kv_ref.at[head(0, dcol)] if o == 0 else stage_ref.at[o - 1, dcol]
        source = g.device(g.wrap(g.row - o), g.col, g.part)
        if dcol == 0:
            kv_out_ref[source] = chunk[pl.ds(pl.multiple_of(g.part * half, half), half), :]
            away = pl.ds(pl.multiple_of((g.parts - 1 - g.part) * half, half), half)
            send(chunk.at[away], kv_out_ref.at[source], x_send.at[o], out_recv, g.partner).start()
        elif dcol in g.direct:
            for part in range(g.parts):
                send(chunk.at[pl.ds(part * half, half)], kv_out_ref.at[source], x_send.at[o], out_recv,
                     g.near(0, g.hop(dcol), part)).start()
        else:
            send(chunk.at[pl.ds(0, half)], right_ref.at[o], x_send.at[o], right_recv.at[o], g.near(0, 1)).start()
            send(chunk.at[pl.ds(half, half)], left_ref.at[o], x_send.at[o], left_recv.at[o], g.near(0, -1)).start()

    def pass_row(o):
        for ref, sem, come in ((right_ref, right_recv, -1), (left_ref, left_recv, 1)):
            source = g.device(g.wrap(g.row - o), g.wrap(g.col + come), g.part)
            send(ref.at[o], ref.at[o], fwd_send.at[o], sem.at[o], g.me).wait_recv()
            send(ref.at[o], kv_out_ref.at[source], fwd_send.at[o], out_recv, g.near(0, -come, 0 if come < 0 else 1)).start()

    def when_source(row, body):
        pl.when(g.is_source(row))(body)

    order = ((2, 1), (3, 0)) if g.ties else ((1, 0),)
    drows = (2, 1, 3, 0) if g.ties else (1, 0)
    pending = None
    for drow in drows:
        for dcols in order:
            project(drow, dcols)
            if pending is None:
                pl.semaphore_wait(barrier, len(peers))
                start_rows(n, heads, g.me, g.part, packed_ref, lambda peer: peer // g.parts, got_ref, row_send.at[0], row_recv.at[0])
            else:
                pending()

            def issue(drow=drow, dcols=dcols):
                def body():
                    for d in dcols:
                        along_row(0, d) if drow == 0 else along_column(drow, d)
                when_source(g.row, body)
            pending = issue
    pending()

    if g.ties:
        for i in range(2):
            def up(i=i):
                send(up_ref.at[i], up_ref.at[i], pass_send.at[0], up_recv.at[i], g.me).wait_recv()
                send(up_ref.at[i], stage_ref.at[1, 2 * i], pass_send.at[0], stage_recv.at[1, 2 * i], g.near(1, 0)).start()
            def down(i=i):
                send(down_ref.at[i], down_ref.at[i], pass_send.at[1], down_recv.at[i], g.me).wait_recv()
                send(down_ref.at[i], stage_ref.at[1, 2 * i + 1], pass_send.at[1], stage_recv.at[1, 2 * i + 1], g.near(-1, 0)).start()
            when_source(g.row - 1, up)
            when_source(g.row + 1, down)
        when_source(g.row, lambda: pass_row(0))

    wait_rows(heads, g.me, got_ref, row_send.at[0], row_recv.at[0])
    swap(got_ref, swapped_ref, row_send.at[1], row_recv.at[1], g.partner)
    place(n, heads, g.part, got_ref, swapped_ref, q_out_ref, True)

    def arrived(o, dcol):
        send(stage_ref.at[o - 1, dcol], stage_ref.at[o - 1, dcol], y_send.at[0], stage_recv.at[o - 1, dcol], g.me).wait_recv()
        along_row(o, dcol)

    for dcols in order:
        for d in dcols:
            for o in g.direct:
                when_source(g.row - o, lambda o=o, d=d: arrived(o, d))
    if g.ties:
        for o in g.direct:
            when_source(g.row - o, lambda o=o: pass_row(o))
        for d in (2, 1, 0, 3):
            when_source(g.row - 2, lambda d=d: arrived(2, d))
        when_source(g.row - 2, lambda: pass_row(2))

    def sent(sem, ref):
        send(ref, ref, sem, out_recv, g.me).wait_send()

    def mine():
        for drow in range(1, side):
            sent(y_send.at[drow - 1], stage_ref.at[0])
    when_source(g.row, mine)
    for o in range(side):
        def passed(o=o):
            sent(x_send.at[o], kv_out_ref.at[pl.ds(0, g.parts * side - 1)])
            if g.ties:
                sent(fwd_send.at[o], kv_out_ref.at[pl.ds(0, 2)])
        when_source(g.row - o, passed)
    if g.ties:
        when_source(g.row - 1, lambda: sent(pass_send.at[0], up_ref))
        when_source(g.row + 1, lambda: sent(pass_send.at[1], down_ref))
    blocks = source_rows * side * g.parts
    others = kv_out_ref.at[pl.ds(0, blocks - source_rows)]
    send(others, others, y_send.at[0], out_recv, g.me).wait_recv()


def row_scratch(heads, q_rows, hd):
    return [pltpu.VMEM((heads, q_rows // 2, 2 * hd), BF16)] * 3


def dma(*dims):
    return pltpu.SemaphoreType.DMA(dims)


def exchange(n, heads, source_rows, collective_id, memory, dec_in, gain, wk_t, wv_t, wq_t):
    m_rows, q_rows, hd = memory.shape[0], dec_in.shape[0], wk_t.shape[1]
    side, parts = math.isqrt(heads), n // heads
    half = m_rows // parts
    chunk = lambda *lead: pltpu.VMEM(lead + (m_rows, 2 * hd), BF16)
    block = lambda *lead: pltpu.VMEM(lead + (half, 2 * hd), BF16)
    return pl.pallas_call(
        functools.partial(exchange_kernel, n, heads, source_rows),
        out_shape=[shape((n, half, 2 * hd), BF16), shape((n, q_rows, 2 * hd), BF16)],
        in_specs=vmem(6),
        out_specs=vmem(2),
        scratch_shapes=[chunk(heads), chunk(side - 1, side), chunk(2), chunk(2), block(side), block(side)]
        + row_scratch(heads, q_rows, hd)
        + [dma(2), dma(2), dma(side - 1), dma(2), dma(side), dma(side), dma(side - 1, side), dma(2), dma(2), dma(side), dma(side),
           pltpu.SemaphoreType.DMA],
        compiler_params=remote(collective_id),
        name='exchange',
    )(memory, dec_in, gain, wk_t, wv_t, wq_t)


def return_kernel(n, heads, source_rows, src_ref, dst_ref, stage_ref, right_ref, left_ref, up_ref, down_ref,
                  x_send, fwd_send, y_send, pass_send, stage_recv, right_recv, left_recv, up_recv, down_recv, out_recv):
    g = Grid(n, heads, source_rows)
    side = g.side
    half = src_ref.shape[1]
    meet(g.peers())
    mine = pl.ds(pl.multiple_of(g.part * half, half), half)

    def landing(drow, dcol, head_col):
        if drow == 0:
            return dst_ref.at[g.row * side + head_col, mine], out_recv
        return stage_ref.at[drow - 1, dcol, mine], stage_recv.at[drow - 1, dcol]

    def along_row(drow, dcol):
        row = g.wrap(g.row + drow)
        col = g.wrap(g.col + dcol)
        for part in range(g.parts):
            source = src_ref.at[g.device(row, col, part)]
            if dcol in g.direct:
                dst, sem = landing(drow, dcol, g.col)
                send(source, dst, x_send.at[drow], sem, g.near(0, g.hop(dcol), part)).start()
            elif part == 0:
                send(source, right_ref.at[drow], x_send.at[drow], right_recv.at[drow], g.near(0, 1)).start()
            else:
                send(source, left_ref.at[drow], x_send.at[drow], left_recv.at[drow], g.near(0, -1)).start()

    def own_chip(drow):
        row = g.wrap(g.row + drow)
        away = src_ref.at[g.device(row, g.col, g.parts - 1 - g.part)]
        dst, sem = landing(drow, 0, g.col)
        dst[...] = src_ref[g.device(row, g.col, g.part)]
        send(away, dst, x_send.at[drow], sem, g.partner).start()

    def pass_row(drow):
        for ref, come_sem, come in ((right_ref, right_recv, -1), (left_ref, left_recv, 1)):
            send(ref.at[drow], ref.at[drow], fwd_send.at[drow], come_sem.at[drow], g.me).wait_recv()
            dst, sem = landing(drow, 2, g.wrap(g.col + come))
            send(ref.at[drow], dst, fwd_send.at[drow], sem, g.near(0, -come, 0 if come < 0 else 1)).start()

    def along_column(drow, dcol):
        chunk = stage_ref.at[drow - 1, dcol]
        got = chunk.at[pl.ds(0, half)] if dcol == 0 else chunk
        send(got, got, y_send.at[drow - 1], stage_recv.at[drow - 1, dcol], g.me).wait_recv()
        head = g.row * side + g.wrap(g.col - dcol)
        if drow in g.direct:
            send(chunk, dst_ref.at[head], y_send.at[drow - 1], out_recv, g.near(g.hop(drow), 0)).start()
        elif dcol % 2 == 0:
            send(chunk, up_ref.at[dcol // 2], y_send.at[drow - 1], up_recv.at[dcol // 2], g.near(1, 0)).start()
        else:
            send(chunk, down_ref.at[dcol // 2], y_send.at[drow - 1], down_recv.at[dcol // 2], g.near(-1, 0)).start()

    def when_source(row, body):
        pl.when(g.is_source(row))(body)

    drows = (2, 1, 3, 0) if g.ties else (1, 0)
    dcols = (2, 1, 3) if g.ties else (1,)
    for drow in drows:
        def issue(drow=drow):
            for d in dcols:
                along_row(drow, d)
            own_chip(drow)
        when_source(g.row + drow, issue)
    if g.ties:
        when_source(g.row + 2, lambda: pass_row(2))
        for d in (0, 1, 3, 2):
            when_source(g.row + 2, lambda d=d: along_column(2, d))
        for drow in g.direct:
            when_source(g.row + drow, lambda drow=drow: pass_row(drow))
    for d in (0, 1, 3, 2) if g.ties else (0, 1):
        for drow in g.direct:
            when_source(g.row + drow, lambda drow=drow, d=d: along_column(drow, d))
    if g.ties:
        when_source(g.row, lambda: pass_row(0))
        for i in (0, 1):
            def up(i=i):
                send(up_ref.at[i], up_ref.at[i], pass_send.at[0], up_recv.at[i], g.me).wait_recv()
                head = g.wrap(g.row - 1) * side + g.wrap(g.col - 2 * i)
                send(up_ref.at[i], dst_ref.at[head], pass_send.at[0], out_recv, g.near(1, 0)).start()
            def down(i=i):
                send(down_ref.at[i], down_ref.at[i], pass_send.at[1], down_recv.at[i], g.me).wait_recv()
                head = g.wrap(g.row + 1) * side + g.wrap(g.col - 2 * i - 1)
                send(down_ref.at[i], dst_ref.at[head], pass_send.at[1], out_recv, g.near(-1, 0)).start()
            when_source(g.row + 1, up)
            when_source(g.row - 1, down)

    def sent(sem, ref):
        send(ref, ref, sem, out_recv, g.me).wait_send()

    for drow in range(side):
        def done(drow=drow):
            sent(x_send.at[drow], src_ref.at[pl.ds(0, g.parts * side - 1)])
            if g.ties:
                sent(fwd_send.at[drow], src_ref.at[pl.ds(0, 2)])
            if drow:
                sent(y_send.at[drow - 1], stage_ref.at[0])
        when_source(g.row + drow, done)
    if g.ties:
        when_source(g.row + 1, lambda: sent(pass_send.at[0], up_ref))
        when_source(g.row - 1, lambda: sent(pass_send.at[1], down_ref))

    @pl.when(g.is_source(g.row))
    def _():
        blocks = src_ref.at[pl.ds(0, n - 1)]
        send(blocks, blocks, y_send.at[0], out_recv, g.me).wait_recv()

    @pl.when(jnp.logical_not(g.is_source(g.row)))
    def _():
        def clear(index, carry):
            dst_ref[index] = jnp.zeros(dst_ref.shape[1:], dst_ref.dtype)
            return carry
        lax.fori_loop(0, heads, clear, 0)


def return_blocks(n, heads, source_rows, collective_id, blocks):
    half, width = blocks.shape[1], blocks.shape[2]
    side, parts = math.isqrt(heads), n // heads
    chunk = lambda *lead: pltpu.VMEM(lead + (half * parts, width), BF16)
    block = lambda *lead: pltpu.VMEM(lead + (half, width), BF16)
    return pl.pallas_call(
        functools.partial(return_kernel, n, heads, source_rows),
        out_shape=shape((heads, half * parts, width), BF16),
        in_specs=vmem(1),
        out_specs=vmem(1)[0],
        scratch_shapes=[chunk(side - 1, side), block(side), block(side), chunk(2), chunk(2),
                        dma(side), dma(side), dma(side - 1), dma(2), dma(side - 1, side), dma(side), dma(side), dma(2), dma(2),
                        pltpu.SemaphoreType.DMA],
        compiler_params=remote(collective_id),
        name='return_blocks',
    )(blocks)


def to_heads_kernel(n, heads, rows_ref, wide_ref, packed_ref, got_ref, swapped_ref, send_sem, recv_sem):
    me = lax.axis_index('seq')
    part = lax.rem(me, n // heads)
    partner, peers = pair_peers(n, heads, me, part)
    packed_ref[...] = pack(rows_ref[...])
    meet(peers)
    start_rows(n, heads, me, part, packed_ref, lambda peer: peer // (n // heads), got_ref, send_sem.at[0], recv_sem.at[0])
    wait_rows(heads, me, got_ref, send_sem.at[0], recv_sem.at[0])
    swap(got_ref, swapped_ref, send_sem.at[1], recv_sem.at[1], partner)
    place(n, heads, part, got_ref, swapped_ref, wide_ref, False)


def to_heads(n, heads, collective_id, rows):
    q_rows, hd = rows.shape[1], rows.shape[2]
    return pl.pallas_call(
        functools.partial(to_heads_kernel, n, heads),
        out_shape=shape((n, q_rows, 2 * hd), BF16),
        in_specs=vmem(1),
        out_specs=vmem(1)[0],
        scratch_shapes=row_scratch(heads, q_rows, hd) + [pltpu.SemaphoreType.DMA((2,)), pltpu.SemaphoreType.DMA((2,))],
        compiler_params=remote(collective_id),
        name='to_heads',
    )(rows)


def to_rows(n, heads, q_rows, me, part, values, packed_ref, got_ref, rows_ref, send_sem, recv_sem):
    packed_ref[...] = pack(values.T.astype(BF16).reshape(n, q_rows, values.shape[0]))
    start_rows(n, heads, me, part, packed_ref, lambda peer: peer, got_ref, send_sem, recv_sem)
    wait_rows(heads, me, got_ref, send_sem, recv_sem)
    rows_ref[...] = unpack(got_ref[...])


def combine_kernel(n, heads, hd, q_rows, mine_ref, rows_ref, out_ref, lse_ref, theirs_ref, packed_ref, got_ref, send_sem, recv_sem):
    me = lax.axis_index('seq')
    part = lax.rem(me, n // heads)
    partner, peers = pair_peers(n, heads, me, part)
    meet(peers)
    swap(mine_ref, theirs_ref, send_sem.at[0], recv_sem.at[0], partner)
    m_a, m_b = mine_ref[hd + 8:hd + 9], theirs_ref[hd + 8:hd + 9]
    top = jnp.maximum(m_a, m_b)
    s_a, s_b = jnp.exp2(m_a - top), jnp.exp2(m_b - top)
    den = mine_ref[hd:hd + 1] * s_a + theirs_ref[hd:hd + 1] * s_b
    out = (mine_ref[:hd] * s_a + theirs_ref[:hd] * s_b) / den
    out_ref[...] = out
    lse_ref[...] = top + jnp.log2(den)
    to_rows(n, heads, q_rows, me, part, out, packed_ref, got_ref, rows_ref, send_sem.at[1], recv_sem.at[1])


def pair_scratch(n, heads, hd, q_rows, mine):
    return [pltpu.VMEM(mine.shape, F32), pltpu.VMEM((n, q_rows // 2, 2 * hd), BF16), pltpu.VMEM((heads, q_rows // 2, 2 * hd), BF16),
            pltpu.SemaphoreType.DMA((2,)), pltpu.SemaphoreType.DMA((2,))]


def combine(n, heads, hd, q_rows, collective_id, mine):
    total_q = mine.shape[1]
    return pl.pallas_call(
        functools.partial(combine_kernel, n, heads, hd, q_rows),
        out_shape=[shape((heads, q_rows, hd), BF16), shape((hd, total_q), F32), shape((1, total_q), F32)],
        in_specs=vmem(1),
        out_specs=vmem(3),
        scratch_shapes=pair_scratch(n, heads, hd, q_rows, mine),
        compiler_params=remote(collective_id),
        name='combine',
    )(mine)


def pair_sum_kernel(n, heads, q_rows, mine_ref, rows_ref, share_ref, theirs_ref, packed_ref, got_ref, send_sem, recv_sem):
    me = lax.axis_index('seq')
    part = lax.rem(me, n // heads)
    partner, peers = pair_peers(n, heads, me, part)
    meet(peers)
    swap(mine_ref, theirs_ref, send_sem.at[0], recv_sem.at[0], partner)
    total = mine_ref[...] + theirs_ref[...]
    width = share_ref.shape[1]
    share_ref[...] = jnp.where(part == 0, total[:, :width], total[:, width:]).astype(BF16)
    to_rows(n, heads, q_rows, me, part, total, packed_ref, got_ref, rows_ref, send_sem.at[1], recv_sem.at[1])


def pair_sum(n, heads, q_rows, collective_id, mine):
    hd, total_q = mine.shape
    return pl.pallas_call(
        functools.partial(pair_sum_kernel, n, heads, q_rows),
        out_shape=[shape((heads, q_rows, hd), BF16), shape((hd, total_q * heads // n), BF16)],
        in_specs=vmem(1),
        out_specs=vmem(2),
        scratch_shapes=pair_scratch(n, heads, hd, q_rows, mine),
        compiler_params=remote(collective_id),
        name='pair_sum',
    )(mine)


def small_sum_kernel(n, mine_ref, total_ref, all_ref, send_sem, recv_sem):
    me = lax.axis_index('seq')
    meet([lax.rem(me + step, n) for step in range(1, n)])
    for step in range(1, n):
        send(mine_ref, all_ref.at[me], send_sem, recv_sem, lax.rem(me + step, n)).start()
    all_ref[me] = mine_ref[...]
    others = all_ref.at[pl.ds(0, n - 1)]
    whole = send(others, others, send_sem, recv_sem, me)
    whole.wait_send()
    whole.wait_recv()
    total_ref[...] = jnp.sum(all_ref[...], axis=0)


def small_sum(n, collective_id, mine):
    return pl.pallas_call(
        functools.partial(small_sum_kernel, n),
        out_shape=shape(mine.shape, F32),
        in_specs=vmem(1),
        out_specs=vmem(1)[0],
        scratch_shapes=[pltpu.VMEM((n,) + mine.shape, F32), pltpu.SemaphoreType.DMA, pltpu.SemaphoreType.DMA],
        compiler_params=remote(collective_id),
        name='small_sum',
    )(mine)


def forward_kernel(scale, hd, q_block, bounds_ref, kv_ref, q_ref, out_ref, qt_ref, top_ref):
    blocks, last_valid = bounds_ref[0], bounds_ref[1]
    rows, total_q = kv_ref.shape[1], q_ref.shape[0]
    groups = [slice(first, first + q_block) for first in range(0, total_q, q_block)]
    base = slice(hd + 8, hd + 9)
    qt_ref[...] = q_ref[...].T

    def masked_scores(scores):
        position = lax.broadcasted_iota(jnp.int32, scores.shape, 0)
        return jnp.where(position < last_valid, scores, NEG)

    def values_of(keys):
        return jnp.concatenate([keys.T[hd:], jnp.ones((16, rows), keys.dtype)], axis=0)

    for cols in groups:
        top = jnp.max(dot(kv_ref[0], qt_ref[:, cols]), axis=0, keepdims=True)
        out_ref[hd + 8:, cols] = jnp.broadcast_to(top * scale, (8, q_block))
        top_ref[:, cols] = jnp.broadcast_to(top, (8, q_block))
    out_ref[:hd + 8, :] = jnp.zeros((hd + 8, total_q), F32)

    def block(index, masked):
        keys = kv_ref[index]
        values = values_of(keys)
        ahead = dot(keys, qt_ref[:, groups[0]])
        for i, cols in enumerate(groups):
            scores = masked_scores(ahead) if masked else ahead
            if i + 1 < len(groups):
                ahead = dot(keys, qt_ref[:, groups[i + 1]])
            top_ref[:, cols] = jnp.maximum(top_ref[:, cols], jnp.max(scores.reshape(rows // 8, 8, q_block), axis=0))
            weights = jnp.exp2(scores * scale - out_ref[base, cols]).astype(keys.dtype)
            out_ref[:hd + 8, cols] += dot(values, weights)[:hd + 8]

    def step(index, carry):
        block(index, False)
        return carry

    lax.fori_loop(0, blocks - 1, step, 0)
    block(blocks - 1, True)

    excess = jnp.max(top_ref[...] * scale - out_ref[hd + 8:, :])

    @pl.when(excess > 16.0)
    def _():
        out_ref[:hd + 8, :] = jnp.zeros((hd + 8, total_q), F32)
        out_ref[hd + 8:, :] = jnp.full((8, total_q), NEG, F32)

        def running(step_index, carry):
            index, group = step_index // len(groups), lax.rem(step_index, len(groups))
            cols = pl.ds(pl.multiple_of(group * q_block, q_block), q_block)
            keys = kv_ref[index]
            limit = jnp.where(index == blocks - 1, last_valid, rows)
            scores = dot(keys, qt_ref[:, cols]) * scale
            position = lax.broadcasted_iota(jnp.int32, scores.shape, 0)
            scores = jnp.where(position < limit, scores, NEG)
            old = out_ref[base, cols]
            new = jnp.maximum(old, jnp.max(scores, axis=0, keepdims=True))
            weights = jnp.exp2(scores - new).astype(keys.dtype)
            out_ref[:hd + 8, cols] = out_ref[:hd + 8, cols] * jnp.exp2(old - new) + dot(values_of(keys), weights)[:hd + 8]
            out_ref[hd + 8:, cols] = jnp.broadcast_to(new, (8, q_block))
            return carry

        lax.fori_loop(0, blocks * len(groups), running, 0)


def attention_forward(scale, hd, sources, bounds, kv, q):
    rows, width = kv.shape[1], kv.shape[2]
    total_q = q.shape[0]
    return pl.pallas_call(
        functools.partial(forward_kernel, scale, hd, min(512, total_q)),
        out_shape=shape((hd + 16, total_q), F32),
        grid=(1,),
        in_specs=[pl.BlockSpec(memory_space=pltpu.SMEM),
                  pl.BlockSpec((sources, rows, width), lambda i: (0, 0, 0), pipeline_mode=pl.Buffered(1)), full(q)],
        out_specs=pl.BlockSpec((hd + 16, total_q), lambda i: (0, 0)),
        scratch_shapes=[pltpu.VMEM((width, total_q), BF16), pltpu.VMEM((8, total_q), F32)],
        compiler_params=plain(),
        cost_estimate=pl.CostEstimate(flops=4 * total_q * sources * rows * hd, bytes_accessed=kv.size * 2,
                                      transcendentals=total_q * sources * rows),
        name='attention_forward',
    )(bounds, kv, q)


def backward_kernel(scale, key_scale, hd, q_block, bounds_ref, kv_ref, q_ref, do_ref, out_ref, lse_ref, dkv_ref, dq_ref,
                    qt_ref, dot_ref, delta_ref):
    blocks, last_valid = bounds_ref[0], bounds_ref[1]
    rows, total_q = kv_ref.shape[1], q_ref.shape[0]
    width = kv_ref.shape[2]
    groups = [slice(first, first + q_block) for first in range(0, total_q, q_block)]
    dq_ref[...] = jnp.zeros_like(dq_ref)
    qt_ref[...] = q_ref[...].T
    do_t = do_ref[...].T
    dot_ref[...] = do_t
    delta_ref[...] = jnp.sum(do_t[hd:].astype(F32) * out_ref[...], axis=0, keepdims=True)

    lane_scale = jnp.where(lax.broadcasted_iota(jnp.int32, (1, width), 1) < hd, key_scale, 1.0)

    def step(index, carry):
        keys = kv_ref[index]
        keys_t = keys.T[:hd]
        limit = jnp.where(index == blocks - 1, last_valid, rows)
        total = jnp.zeros((rows, width), F32)
        ahead = dot(keys, qt_ref[:, groups[0]]), dot(keys, dot_ref[:, groups[0]])
        for i, cols in enumerate(groups):
            scores, grads = ahead
            if i + 1 < len(groups):
                ahead = dot(keys, qt_ref[:, groups[i + 1]]), dot(keys, dot_ref[:, groups[i + 1]])
            position = lax.broadcasted_iota(jnp.int32, scores.shape, 0)
            prob = jnp.exp2(jnp.where(position < limit, scores * scale - lse_ref[:, cols], NEG))
            grad_scores = (prob * (grads - delta_ref[:, cols])).astype(keys.dtype)
            dq_ref[:, cols] += dot(keys_t, grad_scores)
            total += dot(jnp.concatenate([grad_scores, prob.astype(keys.dtype)], axis=1),
                         jnp.concatenate([q_ref[cols, :], do_ref[cols, :]], axis=0))
        dkv_ref[index] = (total * lane_scale).astype(dkv_ref.dtype)
        return carry

    def clear(index, carry):
        dkv_ref[index] = jnp.zeros((rows, width), dkv_ref.dtype)
        return carry

    lax.fori_loop(0, blocks, step, 0)
    lax.fori_loop(blocks, dkv_ref.shape[0], clear, 0)
    dq_ref[...] = dq_ref[...] * key_scale


def attention_backward(scale, key_scale, hd, sources, bounds, kv, q, do, out_t, lse):
    n, rows, width = kv.shape
    total_q = q.shape[0]
    return pl.pallas_call(
        functools.partial(backward_kernel, scale, key_scale, hd, min(256, total_q)),
        out_shape=[shape((n, rows, width), BF16), shape((hd, total_q), F32)],
        grid=(1,),
        in_specs=[pl.BlockSpec(memory_space=pltpu.SMEM),
                  pl.BlockSpec((sources, rows, width), lambda i: (0, 0, 0), pipeline_mode=pl.Buffered(1)),
                  full(q), full(do), full(out_t), full(lse)],
        out_specs=[pl.BlockSpec((n, rows, width), lambda i: (0, 0, 0)),
                   pl.BlockSpec((hd, total_q), lambda i: (0, 0))],
        scratch_shapes=[pltpu.VMEM((width, total_q), BF16), pltpu.VMEM((width, total_q), BF16), pltpu.VMEM((1, total_q), F32)],
        compiler_params=plain(),
        cost_estimate=pl.CostEstimate(flops=10 * total_q * sources * rows * hd, bytes_accessed=kv.size * 4,
                                      transcendentals=total_q * sources * rows),
        name='attention_backward',
    )(bounds, kv, q, do, out_t, lse)


def prepare_kernel(dec_ref, att_ref, wo_ref, gain_ref, n2_ref, n2t_ref):
    hidden = (dec_ref[...].astype(F32) + dot(att_ref[...], wo_ref[...])).astype(BF16)
    normed = rms_norm(hidden.astype(F32), gain_ref[...].astype(F32)).astype(BF16)
    n2_ref[...] = normed
    n2t_ref[...] = normed.T


def prepare(early, late, wo, gain):
    rows, dim = early.shape[0], wo.shape[1]
    chunk = min(512, rows)
    left = pl.BlockSpec((chunk, dim), lambda i: (i, 0))
    return pl.pallas_call(
        prepare_kernel,
        out_shape=[shape((rows, dim), BF16), shape((dim, rows), BF16)],
        grid=(rows // chunk,),
        in_specs=[left, pl.BlockSpec((chunk, wo.shape[0]), lambda i: (i, 0)), full(wo), full(gain)],
        out_specs=[left, pl.BlockSpec((dim, chunk), lambda i: (0, i))],
        compiler_params=plain(),
        cost_estimate=pl.CostEstimate(flops=2 * rows * dim * dim, bytes_accessed=8 * rows * dim, transcendentals=0),
        name='prepare',
    )(early, late, wo, gain)


def mlp_kernel(chunk, n2_ref, n2t_ref, top_ref, w1_ref, w3_ref, w2_ref, g1_ref, g3_ref, g2_ref, d1_ref, d3_ref, act_ref):
    rows = n2_ref.shape[0]
    w1, w3, w2t = w1_ref[...], w3_ref[...], w2_ref[...].T
    for first in range(0, rows, chunk):
        part = slice(first, first + chunk)
        gate = dot(n2_ref[part, :], w1)
        up = dot(n2_ref[part, :], w3)
        grad = dot(top_ref[part, :], w2t)
        sig = jax.nn.sigmoid(gate)
        silu = gate * sig
        act_ref[part, :] = (silu * up).astype(act_ref.dtype)
        d3_ref[part, :] = (grad * silu).astype(d3_ref.dtype)
        d1_ref[part, :] = (grad * up * (sig + silu * (1.0 - sig))).astype(d1_ref.dtype)
    g1_ref[...] = dot(n2t_ref[...], d1_ref[...])
    g3_ref[...] = dot(n2t_ref[...], d3_ref[...])
    g2_ref[...] = dot_tn(act_ref[...], top_ref[...])


def mlp_weight_grads(n2, n2t, early, w_gate, w_up, w_down):
    rows, dim = n2.shape
    ff = w_gate.shape[1]
    tile = 256
    cols = pl.BlockSpec((dim, tile), lambda i: (0, i))
    tall = pl.BlockSpec((tile, dim), lambda i: (i, 0))
    return pl.pallas_call(
        functools.partial(mlp_kernel, min(512, rows)),
        out_shape=[shape((dim, ff), F32), shape((dim, ff), F32), shape((ff, dim), F32)],
        grid=(ff // tile,),
        in_specs=[full(n2), full(n2t), pl.BlockSpec((rows, dim), lambda i: (0, 1), pipeline_mode=pl.Buffered(1)), cols, cols, tall],
        out_specs=[cols, cols, tall],
        scratch_shapes=[pltpu.VMEM((rows, tile), BF16)] * 3,
        compiler_params=plain(),
        cost_estimate=pl.CostEstimate(flops=12 * rows * dim * ff, bytes_accessed=18 * dim * ff, transcendentals=rows * ff),
        name='mlp_weight_grads',
    )(n2, n2t, early, w_gate, w_up, w_down)


def memory_weight_kernel(memory_ref, dkv_ref, gk_ref, gv_ref):
    group, hd = dkv_ref.shape[0], dkv_ref.shape[2] // 2
    for i in range(group):
        both = dot_tn(dkv_ref[i], memory_ref[...])
        gk_ref[i * hd:(i + 1) * hd, :] = both[:hd]
        gv_ref[i * hd:(i + 1) * hd, :] = both[hd:]


def memory_weight_grads(memory, dkv):
    heads, rows, width = dkv.shape
    dim, hd = memory.shape[1], width // 2
    group = 4
    out = pl.BlockSpec((group * hd, dim), lambda i: (i, 0))
    return pl.pallas_call(
        memory_weight_kernel,
        out_shape=[shape((heads * hd, dim), F32)] * 2,
        grid=(heads // group,),
        in_specs=[full(memory), pl.BlockSpec((group, rows, width), lambda i: (i, 0, 0))],
        out_specs=[out, out],
        compiler_params=plain(),
        cost_estimate=pl.CostEstimate(flops=2 * rows * dim * heads * width, bytes_accessed=16 * rows * dim, transcendentals=0),
        name='memory_weight_grads',
    )(memory, dkv)


def memory_grad_kernel(dkv_ref, wk_ref, wv_ref, out_ref):
    group = dkv_ref.shape[0]
    left = jnp.concatenate([dkv_ref[i] for i in range(group)], axis=1)
    right = jnp.concatenate([part[i] for i in range(group) for part in (wk_ref, wv_ref)], axis=0)

    @pl.when(pl.program_id(0) == 0)
    def _():
        out_ref[...] = dot(left, right)

    @pl.when(pl.program_id(0) > 0)
    def _():
        out_ref[...] += dot(left, right)


def memory_grad(dkv, wk_t, wv_t):
    heads, rows, width = dkv.shape
    hd, dim = wk_t.shape[1], wk_t.shape[2]
    group = 4
    weight = pl.BlockSpec((group, hd, dim), lambda i: (i, 0, 0))
    return pl.pallas_call(
        memory_grad_kernel,
        out_shape=shape((rows, dim), F32),
        grid=(heads // group,),
        in_specs=[pl.BlockSpec((group, rows, width), lambda i: (i, 0, 0)), weight, weight],
        out_specs=pl.BlockSpec((rows, dim), lambda i: (0, 0)),
        compiler_params=plain(),
        cost_estimate=pl.CostEstimate(flops=2 * rows * dim * heads * width, bytes_accessed=12 * rows * dim, transcendentals=0),
        name='memory_grad',
    )(dkv, wk_t, wv_t)


def outer_kernel(dec_ref, gain_ref, att_ref, gh_ref, dq_ref, gwo_ref, gwq_ref, n1_ref):
    @pl.when(pl.program_id(0) == 0)
    def _():
        n1_ref[...] = rms_norm(dec_ref[...].astype(F32), gain_ref[...].astype(F32)).astype(BF16)

    group, parts, hd, share = dq_ref.shape
    gwo_ref[...] = dot_tn(att_ref[...], gh_ref[...])
    total = None
    for p in range(parts):
        left = jnp.concatenate([dq_ref[i, p] for i in range(group)], axis=0)
        term = dot(left, n1_ref[p * share:(p + 1) * share, :])
        total = term if total is None else total + term
    gwq_ref[...] = total


def outer_weight_grads(early, late, gain, dq_all):
    heads, parts, hd, share = dq_all.shape
    rows, dim = early.shape[0], gain.shape[1]
    group = 4
    out = pl.BlockSpec((group * hd, dim), lambda i: (i, 0))
    return pl.pallas_call(
        outer_kernel,
        out_shape=[shape((heads * hd, dim), F32)] * 2,
        grid=(heads // group,),
        in_specs=[pl.BlockSpec((rows, dim), lambda i: (0, 0), pipeline_mode=pl.Buffered(1)), full(gain),
                  pl.BlockSpec((rows, group * hd), lambda i: (0, i)),
                  pl.BlockSpec((rows, dim), lambda i: (0, 1), pipeline_mode=pl.Buffered(1)),
                  pl.BlockSpec((group, parts, hd, share), lambda i: (i, 0, 0, 0))],
        out_specs=[out, out],
        scratch_shapes=[pltpu.VMEM((rows, dim), BF16)],
        compiler_params=plain(),
        cost_estimate=pl.CostEstimate(flops=4 * rows * dim * heads * hd, bytes_accessed=16 * rows * dim, transcendentals=0),
        name='outer_weight_grads',
    )(early, gain, late, late, dq_all)


def solution(mesh):
    n = mesh.shape['seq']
    row_spec = P(('data', 'seq'), None)
    weight_spec = P()
    part_vec = P('data')
    part_mat = P('data', None)
    part_cube = P('data', None, None)

    def device_step(dec_in, memory, mem_len, grad_out, norm_attn, wq_cross, wk_cross, wv_cross, wo_cross, norm_mlp, w_gate, w_up, w_down):
        q_rows, dim = dec_in.shape
        m_rows = memory.shape[0]
        heads, hd = wq_cross.shape[1], wq_cross.shape[2]
        parts = n // heads
        half = m_rows // parts
        sources = -(-3 * n // 4)
        total_q = q_rows * n
        key_scale = hd ** -0.5
        scale = key_scale * LOG2E
        me = lax.axis_index('seq')
        part = lax.rem(me, parts)

        reach = mem_len[0] - part * half
        blocks = jnp.minimum((reach + m_rows - 1) // m_rows, sources)
        bounds = jnp.stack([blocks, jnp.minimum(reach - (blocks - 1) * m_rows, half)]).astype(jnp.int32)

        wq_t, wk_t, wv_t = (jnp.transpose(w, (1, 2, 0)) for w in (wq_cross, wk_cross, wv_cross))
        gain_attn, gain_mlp = norm_attn.reshape(1, dim), norm_mlp.reshape(1, dim)
        source_rows = -(-sources // (parts * math.isqrt(heads)))
        kv, q_in = exchange(n, heads, source_rows, 0, memory, dec_in, gain_attn, wk_t, wv_t, wq_t)
        head_q = q_in.reshape(total_q, 2 * hd)

        grad_top = grad_out.astype(BF16)
        early_local, kv = lax.optimization_barrier((jnp.concatenate([dec_in, grad_top], axis=1), kv))
        early = lax.all_gather(early_local, 'seq', axis=0, tiled=True)

        mine = attention_forward(scale, hd, sources, bounds, kv, head_q)
        attended, out_t, lse = combine(n, heads, hd, q_rows, 1, mine)

        x_in = dec_in.astype(F32)
        hidden_f = x_in + jnp.einsum('hqe,hed->qd', attended, wo_cross, preferred_element_type=F32)
        hidden = hidden_f.astype(BF16)
        normed_mlp_f, mlp_norm_pull = jax.vjp(rms_norm, hidden.astype(F32), norm_mlp.astype(F32))
        normed_mlp = normed_mlp_f.astype(BF16)
        gate_pre = jnp.dot(normed_mlp, w_gate, preferred_element_type=F32)
        up_pre = jnp.dot(normed_mlp, w_up, preferred_element_type=F32)
        _, gated_pull = jax.vjp(gated_unit, gate_pre, up_pre)
        grad_act = jnp.einsum('qd,fd->qf', grad_top, w_down, preferred_element_type=F32)
        grad_gate, grad_up = gated_pull(grad_act)
        grad_normed_mlp = (jnp.einsum('qf,df->qd', grad_gate.astype(BF16), w_gate, preferred_element_type=F32)
                           + jnp.einsum('qf,df->qd', grad_up.astype(BF16), w_up, preferred_element_type=F32))
        grad_hidden_norm, g_norm_mlp = mlp_norm_pull(grad_normed_mlp)
        grad_hidden = grad_out + grad_hidden_norm
        grad_hidden_b = grad_hidden.astype(BF16)
        grad_att = jnp.einsum('qd,hed->hqe', grad_hidden_b, wo_cross, preferred_element_type=F32).astype(BF16)
        head_do = to_heads(n, heads, 2, grad_att).reshape(total_q, 2 * hd)

        late_local = jnp.concatenate([attended.transpose(1, 0, 2).reshape(q_rows, heads * hd), grad_hidden_b], axis=1)
        head_do, late_local, early = lax.optimization_barrier((head_do, late_local, early))
        late = lax.all_gather(late_local, 'seq', axis=0, tiled=True)

        dkv, dq_part = attention_backward(scale, key_scale, hd, sources, bounds, kv, head_q, head_do, out_t, lse)
        dq_rows, dq_share = pair_sum(n, heads, q_rows, 3, dq_part)
        dkv, dq_share, late = lax.optimization_barrier((dkv, dq_share, late))
        dq_all = lax.all_gather(dq_share, 'seq', axis=0, tiled=False).reshape(heads, parts, hd, total_q // parts)
        dkv_in = return_blocks(n, heads, source_rows, 4, dkv)
        dkv_in, dq_all, dq_rows = lax.optimization_barrier((dkv_in, dq_all, dq_rows))

        gk_part, gv_part = memory_weight_grads(memory, dkv_in)
        gk_part, gv_part, dkv_in, dq_all, dq_rows, early, late = lax.optimization_barrier(
            (gk_part, gv_part, dkv_in, dq_all, dq_rows, early, late))
        g_wk, g_wv = lax.psum((gk_part, gv_part), 'seq')

        n2_all, n2_all_t = prepare(early, late, wo_cross.reshape(heads * hd, dim), gain_mlp)
        g_gate, g_up, g_down = mlp_weight_grads(n2_all, n2_all_t, early, w_gate, w_up, w_down)
        g_wo, g_wq = outer_weight_grads(early, late, gain_attn, dq_all)

        grad_normed = jnp.einsum('hte,dhe->td', dq_rows, wq_cross, preferred_element_type=F32)
        _, norm_pull = jax.vjp(rms_norm, x_in, norm_attn.astype(F32))
        grad_x_norm, g_norm_attn = norm_pull(grad_normed)
        g_dec = grad_hidden + grad_x_norm
        norms = small_sum(n, 5, jnp.concatenate([g_norm_attn, g_norm_mlp]).reshape(-1, 128)).reshape(2, dim)
        g_mem = memory_grad(dkv_in, wk_t, wv_t)
        cube = lambda g: jnp.transpose(g.reshape(heads, hd, dim), (2, 0, 1))
        return (g_dec, g_mem, norms[0], cube(g_wq), cube(g_wk), cube(g_wv), g_wo.reshape(heads, hd, dim), norms[1], g_gate, g_up, g_down)

    return jax.shard_map(device_step, mesh=mesh,
                         in_specs=(row_spec, row_spec, part_vec, row_spec) + (weight_spec,) * 9,
                         out_specs=(row_spec, row_spec, part_vec, part_cube, part_cube, part_cube, part_cube, part_vec, part_mat, part_mat, part_mat),
                         check_vma=False)
```

```python
import functools
import math

import jax
import jax.numpy as jnp
from jax import lax
from jax.experimental import pallas as pl
from jax.experimental.pallas import tpu as pltpu
from jax.sharding import PartitionSpec as P

LOG2E = 1.4426950408889634
NEG = -1e30
VMEM_LIMIT = 60 * 1024 * 1024
MESH = pl.DeviceIdType.MESH
BF16, F32 = jnp.bfloat16, jnp.float32


def rms_norm(tensor, gain):
    mean_sq = jnp.mean(tensor * tensor, axis=-1, keepdims=True)
    return tensor * lax.rsqrt(mean_sq + 1e-6) * gain


def gated_unit(gate_pre, up_pre):
    return jax.nn.silu(gate_pre) * up_pre


def dot(a, b):
    return jnp.dot(a, b, preferred_element_type=F32)


def dot_nt(a, b):
    return lax.dot_general(a, b, (((1,), (1,)), ((), ())), preferred_element_type=F32)


def dot_tn(a, b):
    return lax.dot_general(a, b, (((0,), (0,)), ((), ())), preferred_element_type=F32)


def full(array):
    return pl.BlockSpec(array.shape, lambda *_: (0,) * array.ndim, pipeline_mode=pl.Buffered(1))


def vmem(count):
    return [pl.BlockSpec(memory_space=pltpu.VMEM)] * count


def plain(mib):
    return pltpu.CompilerParams(vmem_limit_bytes=mib * 1024 * 1024)


def remote(collective_id):
    return pltpu.CompilerParams(collective_id=collective_id, has_side_effects=True, vmem_limit_bytes=VMEM_LIMIT)


def shape(dims, dtype):
    return jax.ShapeDtypeStruct(dims, dtype)


def meet(peers):
    barrier = pltpu.get_barrier_semaphore()
    for peer in peers:
        pl.semaphore_signal(barrier, inc=1, device_id={'seq': peer}, device_id_type=MESH)
    pl.semaphore_wait(barrier, len(peers))


def send(src, dst, send_sem, recv_sem, peer):
    return pltpu.make_async_remote_copy(src_ref=src, dst_ref=dst, send_sem=send_sem, recv_sem=recv_sem,
                                        device_id={'seq': peer}, device_id_type=MESH)


class Grid:
    def __init__(self, n, heads, source_rows):
        self.n, self.heads, self.source_rows = n, heads, source_rows
        self.parts = n // heads
        self.side = math.isqrt(heads)
        self.me = lax.axis_index('seq')
        self.part = lax.rem(self.me, self.parts)
        self.chip = self.me // self.parts
        self.col = lax.rem(self.chip, self.side)
        self.row = self.chip // self.side
        self.partner = self.chip * self.parts + (self.parts - 1 - self.part)
        self.ties = self.side == 4
        self.direct = (1, 3) if self.ties else (1,)

    def wrap(self, value):
        return lax.rem(value + self.side, self.side)

    def device(self, row, col, part):
        return (row * self.side + col) * self.parts + part

    def near(self, drow, dcol, part=None):
        return self.device(self.wrap(self.row + drow), self.wrap(self.col + dcol), self.part if part is None else part)

    def hop(self, offset):
        return 1 if offset == 1 else -1

    def is_source(self, row):
        return self.wrap(row) < self.source_rows

    def row_peers(self):
        return [lax.rem(self.chip + step, self.heads) * self.parts + self.part for step in range(1, self.heads)]

    def peers(self):
        return self.row_peers() + [self.partner] + [self.near(0, self.hop(d), self.parts - 1 - self.part) for d in self.direct]


def pair_peers(n, heads, me, part):
    parts = n // heads
    head = me // parts
    partner = head * parts + (parts - 1 - part)
    return partner, [partner] + [lax.rem(head + step, heads) * parts + part for step in range(1, heads)]


def pack(rows):
    middle = rows.shape[-2] // 2
    return jnp.concatenate([rows[..., :middle, :], rows[..., middle:, :]], axis=-1)


def unpack(packed):
    middle = packed.shape[-1] // 2
    return jnp.concatenate([packed[..., :middle], packed[..., middle:]], axis=-2)


def start_rows(n, heads, me, part, src, src_of, dst_ref, send_sem, recv_sem):
    parts = n // heads
    head = me // parts
    for step in range(1, heads):
        peer = lax.rem(head + step, heads) * parts + part
        send(src.at[src_of(peer)], dst_ref.at[head], send_sem, recv_sem, peer).start()
    dst_ref[head] = src[src_of(me)]


def wait_rows(heads, me, dst_ref, send_sem, recv_sem):
    others = dst_ref.at[pl.ds(0, heads - 1)]
    whole = send(others, others, send_sem, recv_sem, me)
    whole.wait_send()
    whole.wait_recv()


def swap(src, dst, send_sem, recv_sem, partner):
    copy = send(src, dst, send_sem, recv_sem, partner)
    copy.start()
    copy.wait()


def place(n, heads, part, mine_ref, theirs_ref, wide_ref, low):
    parts = n // heads
    for source, index in ((mine_ref, part), (theirs_ref, parts - 1 - part)):
        for head in range(heads):
            rows = unpack(source[head])
            zeros = jnp.zeros_like(rows)
            wide_ref[head * parts + index] = jnp.concatenate([rows, zeros] if low else [zeros, rows], axis=-1)


def exchange_kernel(n, heads, source_rows, memory_ref, dec_ref, gain_ref, wk_ref, wv_ref, wq_ref, kv_out_ref, q_out_ref,
                    kv_ref, stage_ref, up_ref, down_ref, right_ref, left_ref, packed_ref, got_ref, swapped_ref,
                    row_send, row_recv, y_send, pass_send, x_send, fwd_send, stage_recv, up_recv, down_recv, right_recv,
                    left_recv, out_recv):
    g = Grid(n, heads, source_rows)
    side, hd = g.side, wk_ref.shape[1]
    half = kv_out_ref.shape[1]
    chunk_rows = min(256, kv_ref.shape[1])
    barrier = pltpu.get_barrier_semaphore()
    peers = g.peers()
    for peer in peers:
        pl.semaphore_signal(barrier, inc=1, device_id={'seq': peer}, device_id_type=MESH)

    normed = rms_norm(dec_ref[...].astype(F32), gain_ref[...].astype(F32)).astype(BF16)
    for i in range(0, heads, 4):
        queries = dot_nt(normed, jnp.concatenate([wq_ref[i + j] for j in range(4)], axis=0)).astype(BF16)
        for j in range(4):
            packed_ref[i + j] = pack(queries[:, hd * j:hd * (j + 1)])

    def head(drow, dcol):
        return g.wrap(g.row + drow) * side + g.wrap(g.col + dcol)

    def project(drow, dcols):
        weights = jnp.concatenate([ref[head(drow, d)] for d in dcols for ref in (wk_ref, wv_ref)], axis=0)

        def rows(index, carry):
            at = pl.ds(pl.multiple_of(index * chunk_rows, chunk_rows), chunk_rows)
            both = dot_nt(memory_ref[at, :], weights).astype(BF16)
            for i, d in enumerate(dcols):
                kv_ref[head(drow, d), at, :] = both[:, 2 * hd * i:2 * hd * (i + 1)]
            return carry

        lax.fori_loop(0, kv_ref.shape[1] // chunk_rows, rows, 0)

    def along_column(drow, dcol):
        chunk = kv_ref.at[head(drow, dcol)]
        if drow in g.direct:
            send(chunk, stage_ref.at[drow - 1, dcol], y_send.at[drow - 1], stage_recv.at[drow - 1, dcol], g.near(g.hop(drow), 0)).start()
        elif dcol % 2 == 0:
            send(chunk, up_ref.at[dcol // 2], y_send.at[drow - 1], up_recv.at[dcol // 2], g.near(1, 0)).start()
        else:
            send(chunk, down_ref.at[dcol // 2], y_send.at[drow - 1], down_recv.at[dcol // 2], g.near(-1, 0)).start()

    def along_row(o, dcol):
        chunk = kv_ref.at[head(0, dcol)] if o == 0 else stage_ref.at[o - 1, dcol]
        source = g.device(g.wrap(g.row - o), g.col, g.part)
        if dcol == 0:
            kv_out_ref[source] = chunk[pl.ds(pl.multiple_of(g.part * half, half), half), :]
            away = pl.ds(pl.multiple_of((g.parts - 1 - g.part) * half, half), half)
            send(chunk.at[away], kv_out_ref.at[source], x_send.at[o], out_recv, g.partner).start()
        elif dcol in g.direct:
            for part in range(g.parts):
                send(chunk.at[pl.ds(part * half, half)], kv_out_ref.at[source], x_send.at[o], out_recv,
                     g.near(0, g.hop(dcol), part)).start()
        else:
            send(chunk.at[pl.ds(0, half)], right_ref.at[o], x_send.at[o], right_recv.at[o], g.near(0, 1)).start()
            send(chunk.at[pl.ds(half, half)], left_ref.at[o], x_send.at[o], left_recv.at[o], g.near(0, -1)).start()

    def pass_row(o):
        for ref, sem, come in ((right_ref, right_recv, -1), (left_ref, left_recv, 1)):
            source = g.device(g.wrap(g.row - o), g.wrap(g.col + come), g.part)
            send(ref.at[o], ref.at[o], fwd_send.at[o], sem.at[o], g.me).wait_recv()
            send(ref.at[o], kv_out_ref.at[source], fwd_send.at[o], out_recv, g.near(0, -come, 0 if come < 0 else 1)).start()

    def when_source(row, body):
        pl.when(g.is_source(row))(body)

    if g.ties:
        order = [(2, (2, 1)), (2, (3, 0)), (1, (2, 1)), (3, (2, 1)), (0, (2, 1)), (0, (3, 0))]
        last = [(1, (3, 0)), (3, (3, 0))]
    else:
        order, last = [(1, (1, 0)), (0, (1, 0))], []

    def issue(drow, dcols):
        def body():
            for d in dcols:
                along_row(0, d) if drow == 0 else along_column(drow, d)
        when_source(g.row, body)

    waiting = None
    for drow, dcols in order + last:
        project(drow, dcols)
        if waiting is None:
            pl.semaphore_wait(barrier, len(peers))
            start_rows(n, heads, g.me, g.part, packed_ref, lambda peer: peer // g.parts, got_ref, row_send.at[0], row_recv.at[0])
        elif waiting not in last:
            issue(*waiting)
        waiting = (drow, dcols)
    if not last:
        issue(*waiting)

    if g.ties:
        def up(i):
            send(up_ref.at[i], up_ref.at[i], pass_send.at[0], up_recv.at[i], g.me).wait_recv()
            send(up_ref.at[i], stage_ref.at[1, 2 * i], pass_send.at[0], stage_recv.at[1, 2 * i], g.near(1, 0)).start()

        def down(i):
            send(down_ref.at[i], down_ref.at[i], pass_send.at[1], down_recv.at[i], g.me).wait_recv()
            send(down_ref.at[i], stage_ref.at[1, 2 * i + 1], pass_send.at[1], stage_recv.at[1, 2 * i + 1], g.near(-1, 0)).start()

        for i in range(2):
            when_source(g.row - 1, lambda i=i: up(1 - i))
            when_source(g.row + 1, lambda i=i: down(i))
        for drow, dcols in last:
            issue(drow, dcols)
        when_source(g.row, lambda: pass_row(0))

    wait_rows(heads, g.me, got_ref, row_send.at[0], row_recv.at[0])
    swap(got_ref, swapped_ref, row_send.at[1], row_recv.at[1], g.partner)
    place(n, heads, g.part, got_ref, swapped_ref, q_out_ref, True)

    def arrived(o, dcol):
        def body():
            send(stage_ref.at[o - 1, dcol], stage_ref.at[o - 1, dcol], y_send.at[0], stage_recv.at[o - 1, dcol], g.me).wait_recv()
            along_row(o, dcol)
        when_source(g.row - o, body)

    if g.ties:
        for d in (2, 1):
            for o in g.direct:
                arrived(o, d)
        for o in g.direct:
            when_source(g.row - o, lambda o=o: pass_row(o))
        for d in (2, 1, 0, 3):
            arrived(2, d)
        when_source(g.row - 2, lambda: pass_row(2))
        for d in (3, 0):
            for o in g.direct:
                arrived(o, d)
    else:
        for d in (1, 0):
            arrived(1, d)

    def sent(sem, ref):
        send(ref, ref, sem, out_recv, g.me).wait_send()

    def mine():
        for drow in range(1, side):
            sent(y_send.at[drow - 1], stage_ref.at[0])
    when_source(g.row, mine)
    for o in range(side):
        def passed(o=o):
            sent(x_send.at[o], kv_out_ref.at[pl.ds(0, g.parts * side - 1)])
            if g.ties:
                sent(fwd_send.at[o], kv_out_ref.at[pl.ds(0, 2)])
        when_source(g.row - o, passed)
    if g.ties:
        when_source(g.row - 1, lambda: sent(pass_send.at[0], up_ref))
        when_source(g.row + 1, lambda: sent(pass_send.at[1], down_ref))
    blocks = source_rows * side * g.parts
    others = kv_out_ref.at[pl.ds(0, blocks - source_rows)]
    send(others, others, y_send.at[0], out_recv, g.me).wait_recv()


def row_scratch(heads, q_rows, hd):
    return [pltpu.VMEM((heads, q_rows // 2, 2 * hd), BF16)] * 3


def dma(*dims):
    return pltpu.SemaphoreType.DMA(dims)


def exchange(n, heads, source_rows, collective_id, memory, dec_in, gain, wk_t, wv_t, wq_t):
    m_rows, q_rows, hd = memory.shape[0], dec_in.shape[0], wk_t.shape[1]
    side, parts = math.isqrt(heads), n // heads
    half = m_rows // parts
    chunk = lambda *lead: pltpu.VMEM(lead + (m_rows, 2 * hd), BF16)
    block = lambda *lead: pltpu.VMEM(lead + (half, 2 * hd), BF16)
    return pl.pallas_call(
        functools.partial(exchange_kernel, n, heads, source_rows),
        out_shape=[shape((n, half, 2 * hd), BF16), shape((n, q_rows, 2 * hd), BF16)],
        in_specs=vmem(6),
        out_specs=vmem(2),
        scratch_shapes=[chunk(heads), chunk(side - 1, side), chunk(2), chunk(2), block(side), block(side)]
        + row_scratch(heads, q_rows, hd)
        + [dma(2), dma(2), dma(side - 1), dma(2), dma(side), dma(side), dma(side - 1, side), dma(2), dma(2), dma(side), dma(side),
           pltpu.SemaphoreType.DMA],
        compiler_params=remote(collective_id),
        name='exchange',
    )(memory, dec_in, gain, wk_t, wv_t, wq_t)


def return_kernel(n, heads, source_rows, src_ref, dst_ref, stage_ref, right_ref, left_ref, up_ref, down_ref,
                  x_send, fwd_send, y_send, pass_send, stage_recv, right_recv, left_recv, up_recv, down_recv, out_recv):
    g = Grid(n, heads, source_rows)
    side = g.side
    half = src_ref.shape[1]
    meet(g.peers())
    mine = pl.ds(pl.multiple_of(g.part * half, half), half)

    def landing(drow, dcol, head_col):
        if drow == 0:
            return dst_ref.at[g.row * side + head_col, mine], out_recv
        return stage_ref.at[drow - 1, dcol, mine], stage_recv.at[drow - 1, dcol]

    def along_row(drow, dcol):
        row = g.wrap(g.row + drow)
        col = g.wrap(g.col + dcol)
        for part in range(g.parts):
            source = src_ref.at[g.device(row, col, part)]
            if dcol in g.direct:
                dst, sem = landing(drow, dcol, g.col)
                send(source, dst, x_send.at[drow], sem, g.near(0, g.hop(dcol), part)).start()
            elif part == 0:
                send(source, right_ref.at[drow], x_send.at[drow], right_recv.at[drow], g.near(0, 1)).start()
            else:
                send(source, left_ref.at[drow], x_send.at[drow], left_recv.at[drow], g.near(0, -1)).start()

    def own_chip(drow):
        row = g.wrap(g.row + drow)
        away = src_ref.at[g.device(row, g.col, g.parts - 1 - g.part)]
        dst, sem = landing(drow, 0, g.col)
        dst[...] = src_ref[g.device(row, g.col, g.part)]
        send(away, dst, x_send.at[drow], sem, g.partner).start()

    def pass_row(drow):
        for ref, come_sem, come in ((right_ref, right_recv, -1), (left_ref, left_recv, 1)):
            send(ref.at[drow], ref.at[drow], fwd_send.at[drow], come_sem.at[drow], g.me).wait_recv()
            dst, sem = landing(drow, 2, g.wrap(g.col + come))
            send(ref.at[drow], dst, fwd_send.at[drow], sem, g.near(0, -come, 0 if come < 0 else 1)).start()

    def along_column(drow, dcol):
        chunk = stage_ref.at[drow - 1, dcol]
        got = chunk.at[pl.ds(0, half)] if dcol == 0 else chunk
        send(got, got, y_send.at[drow - 1], stage_recv.at[drow - 1, dcol], g.me).wait_recv()
        head = g.row * side + g.wrap(g.col - dcol)
        if drow in g.direct:
            send(chunk, dst_ref.at[head], y_send.at[drow - 1], out_recv, g.near(g.hop(drow), 0)).start()
        elif dcol % 2 == 0:
            send(chunk, up_ref.at[dcol // 2], y_send.at[drow - 1], up_recv.at[dcol // 2], g.near(1, 0)).start()
        else:
            send(chunk, down_ref.at[dcol // 2], y_send.at[drow - 1], down_recv.at[dcol // 2], g.near(-1, 0)).start()

    def when_source(row, body):
        pl.when(g.is_source(row))(body)

    def rows_of(drow):
        def body():
            for d in (2, 1, 3) if g.ties else (1,):
                along_row(drow, d)
        when_source(g.row + drow, body)

    def relay(drow):
        when_source(g.row + drow, lambda: pass_row(drow))

    def column(drow, d):
        when_source(g.row + drow, lambda: along_column(drow, d))

    def up(i):
        def body():
            send(up_ref.at[i], up_ref.at[i], pass_send.at[0], up_recv.at[i], g.me).wait_recv()
            head = g.wrap(g.row - 1) * side + g.wrap(g.col - 2 * i)
            send(up_ref.at[i], dst_ref.at[head], pass_send.at[0], out_recv, g.near(1, 0)).start()
        when_source(g.row + 1, body)

    def down(i):
        def body():
            send(down_ref.at[i], down_ref.at[i], pass_send.at[1], down_recv.at[i], g.me).wait_recv()
            head = g.wrap(g.row + 1) * side + g.wrap(g.col - 2 * i - 1)
            send(down_ref.at[i], dst_ref.at[head], pass_send.at[1], out_recv, g.near(-1, 0)).start()
        when_source(g.row - 1, body)

    for drow in (2, 1, 3, 0) if g.ties else (1, 0):
        when_source(g.row + drow, lambda drow=drow: own_chip(drow))
    if g.ties:
        rows_of(2)
        rows_of(1)
        for drow in (2, 1, 3):
            column(drow, 0)
        relay(2)
        rows_of(3)
        relay(1)
        column(2, 1)
        column(2, 3)
        column(2, 2)
        up(0)
        down(0)
        rows_of(0)
        column(1, 1)
        column(1, 3)
        relay(3)
        column(1, 2)
        up(1)
        down(1)
        relay(0)
        column(3, 1)
        column(3, 3)
        column(3, 2)
    else:
        rows_of(1)
        rows_of(0)
        column(1, 0)
        column(1, 1)

    def sent(sem, ref):
        send(ref, ref, sem, out_recv, g.me).wait_send()

    for drow in range(side):
        def done(drow=drow):
            sent(x_send.at[drow], src_ref.at[pl.ds(0, g.parts * side - 1)])
            if g.ties:
                sent(fwd_send.at[drow], src_ref.at[pl.ds(0, 2)])
            if drow:
                sent(y_send.at[drow - 1], stage_ref.at[0])
        when_source(g.row + drow, done)
    if g.ties:
        when_source(g.row + 1, lambda: sent(pass_send.at[0], up_ref))
        when_source(g.row - 1, lambda: sent(pass_send.at[1], down_ref))

    @pl.when(g.is_source(g.row))
    def _():
        blocks = src_ref.at[pl.ds(0, n - 1)]
        send(blocks, blocks, y_send.at[0], out_recv, g.me).wait_recv()

    @pl.when(jnp.logical_not(g.is_source(g.row)))
    def _():
        def clear(index, carry):
            dst_ref[index] = jnp.zeros(dst_ref.shape[1:], dst_ref.dtype)
            return carry
        lax.fori_loop(0, heads, clear, 0)


def return_blocks(n, heads, source_rows, collective_id, blocks):
    half, width = blocks.shape[1], blocks.shape[2]
    side, parts = math.isqrt(heads), n // heads
    chunk = lambda *lead: pltpu.VMEM(lead + (half * parts, width), BF16)
    block = lambda *lead: pltpu.VMEM(lead + (half, width), BF16)
    return pl.pallas_call(
        functools.partial(return_kernel, n, heads, source_rows),
        out_shape=shape((heads, half * parts, width), BF16),
        in_specs=vmem(1),
        out_specs=vmem(1)[0],
        scratch_shapes=[chunk(side - 1, side), block(side), block(side), chunk(2), chunk(2),
                        dma(side), dma(side), dma(side - 1), dma(2), dma(side - 1, side), dma(side), dma(side), dma(2), dma(2),
                        pltpu.SemaphoreType.DMA],
        compiler_params=remote(collective_id),
        name='return_blocks',
    )(blocks)


def to_heads_kernel(n, heads, rows_ref, wide_ref, packed_ref, got_ref, swapped_ref, send_sem, recv_sem):
    me = lax.axis_index('seq')
    part = lax.rem(me, n // heads)
    partner, peers = pair_peers(n, heads, me, part)
    packed_ref[...] = pack(rows_ref[...])
    meet(peers)
    start_rows(n, heads, me, part, packed_ref, lambda peer: peer // (n // heads), got_ref, send_sem.at[0], recv_sem.at[0])
    wait_rows(heads, me, got_ref, send_sem.at[0], recv_sem.at[0])
    swap(got_ref, swapped_ref, send_sem.at[1], recv_sem.at[1], partner)
    place(n, heads, part, got_ref, swapped_ref, wide_ref, False)


def to_heads(n, heads, collective_id, rows):
    q_rows, hd = rows.shape[1], rows.shape[2]
    return pl.pallas_call(
        functools.partial(to_heads_kernel, n, heads),
        out_shape=shape((n, q_rows, 2 * hd), BF16),
        in_specs=vmem(1),
        out_specs=vmem(1)[0],
        scratch_shapes=row_scratch(heads, q_rows, hd) + [pltpu.SemaphoreType.DMA((2,)), pltpu.SemaphoreType.DMA((2,))],
        compiler_params=remote(collective_id),
        name='to_heads',
    )(rows)


def to_rows(n, heads, q_rows, me, part, values, packed_ref, got_ref, rows_ref, send_sem, recv_sem):
    packed_ref[...] = pack(values.T.astype(BF16).reshape(n, q_rows, values.shape[0]))
    start_rows(n, heads, me, part, packed_ref, lambda peer: peer, got_ref, send_sem, recv_sem)
    wait_rows(heads, me, got_ref, send_sem, recv_sem)
    rows_ref[...] = unpack(got_ref[...])


def combine_kernel(n, heads, hd, q_rows, mine_ref, rows_ref, out_ref, lse_ref, theirs_ref, packed_ref, got_ref, send_sem, recv_sem):
    me = lax.axis_index('seq')
    part = lax.rem(me, n // heads)
    partner, peers = pair_peers(n, heads, me, part)
    meet(peers)
    swap(mine_ref, theirs_ref, send_sem.at[0], recv_sem.at[0], partner)
    m_a, m_b = mine_ref[hd + 8:hd + 9], theirs_ref[hd + 8:hd + 9]
    top = jnp.maximum(m_a, m_b)
    s_a, s_b = jnp.exp2(m_a - top), jnp.exp2(m_b - top)
    den = mine_ref[hd:hd + 1] * s_a + theirs_ref[hd:hd + 1] * s_b
    out = (mine_ref[:hd] * s_a + theirs_ref[:hd] * s_b) / den
    out_ref[...] = out
    lse_ref[...] = top + jnp.log2(den)
    to_rows(n, heads, q_rows, me, part, out, packed_ref, got_ref, rows_ref, send_sem.at[1], recv_sem.at[1])


def pair_scratch(n, heads, hd, q_rows, mine):
    return [pltpu.VMEM(mine.shape, F32), pltpu.VMEM((n, q_rows // 2, 2 * hd), BF16), pltpu.VMEM((heads, q_rows // 2, 2 * hd), BF16),
            pltpu.SemaphoreType.DMA((2,)), pltpu.SemaphoreType.DMA((2,))]


def combine(n, heads, hd, q_rows, collective_id, mine):
    total_q = mine.shape[1]
    return pl.pallas_call(
        functools.partial(combine_kernel, n, heads, hd, q_rows),
        out_shape=[shape((heads, q_rows, hd), BF16), shape((hd, total_q), F32), shape((1, total_q), F32)],
        in_specs=vmem(1),
        out_specs=vmem(3),
        scratch_shapes=pair_scratch(n, heads, hd, q_rows, mine),
        compiler_params=remote(collective_id),
        name='combine',
    )(mine)


def pair_sum_kernel(n, heads, q_rows, mine_ref, rows_ref, share_ref, theirs_ref, packed_ref, got_ref, send_sem, recv_sem):
    me = lax.axis_index('seq')
    part = lax.rem(me, n // heads)
    partner, peers = pair_peers(n, heads, me, part)
    meet(peers)
    swap(mine_ref, theirs_ref, send_sem.at[0], recv_sem.at[0], partner)
    total = mine_ref[...] + theirs_ref[...]
    width = share_ref.shape[1]
    share_ref[...] = jnp.where(part == 0, total[:, :width], total[:, width:]).astype(BF16)
    to_rows(n, heads, q_rows, me, part, total, packed_ref, got_ref, rows_ref, send_sem.at[1], recv_sem.at[1])


def pair_sum(n, heads, q_rows, collective_id, mine):
    hd, total_q = mine.shape
    return pl.pallas_call(
        functools.partial(pair_sum_kernel, n, heads, q_rows),
        out_shape=[shape((heads, q_rows, hd), BF16), shape((hd, total_q * heads // n), BF16)],
        in_specs=vmem(1),
        out_specs=vmem(2),
        scratch_shapes=pair_scratch(n, heads, hd, q_rows, mine),
        compiler_params=remote(collective_id),
        name='pair_sum',
    )(mine)


def small_sum_kernel(n, mine_ref, total_ref, all_ref, send_sem, recv_sem):
    me = lax.axis_index('seq')
    meet([lax.rem(me + step, n) for step in range(1, n)])
    for step in range(1, n):
        send(mine_ref, all_ref.at[me], send_sem, recv_sem, lax.rem(me + step, n)).start()
    all_ref[me] = mine_ref[...]
    others = all_ref.at[pl.ds(0, n - 1)]
    whole = send(others, others, send_sem, recv_sem, me)
    whole.wait_send()
    whole.wait_recv()
    total_ref[...] = jnp.sum(all_ref[...], axis=0)


def small_sum(n, collective_id, mine):
    return pl.pallas_call(
        functools.partial(small_sum_kernel, n),
        out_shape=shape(mine.shape, F32),
        in_specs=vmem(1),
        out_specs=vmem(1)[0],
        scratch_shapes=[pltpu.VMEM((n,) + mine.shape, F32), pltpu.SemaphoreType.DMA, pltpu.SemaphoreType.DMA],
        compiler_params=remote(collective_id),
        name='small_sum',
    )(mine)


def forward_kernel(scale, hd, q_block, bounds_ref, kv_ref, q_ref, out_ref, qt_ref, top_ref):
    blocks, last_valid = bounds_ref[0], bounds_ref[1]
    rows, total_q = kv_ref.shape[1], q_ref.shape[0]
    groups = [slice(first, first + q_block) for first in range(0, total_q, q_block)]
    base = slice(hd + 8, hd + 9)
    qt_ref[...] = q_ref[...].T

    def values_of(keys):
        return jnp.concatenate([keys.T[hd:], jnp.ones((16, rows), keys.dtype)], axis=0)

    def group_of(index):
        return pl.ds(pl.multiple_of(index * q_block, q_block), q_block)

    def first_step(group, carry):
        cols = group_of(group)
        top = jnp.max(dot(kv_ref[0], qt_ref[:, cols]), axis=0, keepdims=True)
        out_ref[hd + 8:, cols] = jnp.broadcast_to(top * scale, (8, q_block))
        top_ref[:, cols] = jnp.broadcast_to(top, (8, q_block))
        return carry

    lax.fori_loop(0, len(groups), first_step, 0)
    out_ref[:hd + 8, :] = jnp.zeros((hd + 8, total_q), F32)

    def finish(values, scores, cols):
        top_ref[:, cols] = jnp.maximum(top_ref[:, cols], jnp.max(scores.reshape(rows // 8, 8, q_block), axis=0))
        weights = jnp.exp2(scores * scale - out_ref[base, cols]).astype(values.dtype)
        out_ref[:hd + 8, cols] += dot(values, weights)[:hd + 8]

    def step(index, carry):
        keys = kv_ref[index]
        values = values_of(keys)
        ahead = dot(keys, qt_ref[:, groups[0]])
        for i, cols in enumerate(groups):
            scores = ahead
            if i + 1 < len(groups):
                ahead = dot(keys, qt_ref[:, groups[i + 1]])
            finish(values, scores, cols)
        return carry

    def last_step(group, carry):
        cols = group_of(group)
        keys = kv_ref[blocks - 1]
        scores = dot(keys, qt_ref[:, cols])
        position = lax.broadcasted_iota(jnp.int32, scores.shape, 0)
        finish(values_of(keys), jnp.where(position < last_valid, scores, NEG), cols)
        return carry

    lax.fori_loop(0, blocks - 1, step, 0)
    lax.fori_loop(0, len(groups), last_step, 0)

    excess = jnp.max(top_ref[...] * scale - out_ref[hd + 8:, :])

    @pl.when(excess > 16.0)
    def _():
        out_ref[:hd + 8, :] = jnp.zeros((hd + 8, total_q), F32)
        out_ref[hd + 8:, :] = jnp.full((8, total_q), NEG, F32)

        def running(step_index, carry):
            index, group = step_index // len(groups), lax.rem(step_index, len(groups))
            cols = group_of(group)
            keys = kv_ref[index]
            limit = jnp.where(index == blocks - 1, last_valid, rows)
            scores = dot(keys, qt_ref[:, cols]) * scale
            position = lax.broadcasted_iota(jnp.int32, scores.shape, 0)
            scores = jnp.where(position < limit, scores, NEG)
            old = out_ref[base, cols]
            new = jnp.maximum(old, jnp.max(scores, axis=0, keepdims=True))
            weights = jnp.exp2(scores - new).astype(keys.dtype)
            out_ref[:hd + 8, cols] = out_ref[:hd + 8, cols] * jnp.exp2(old - new) + dot(values_of(keys), weights)[:hd + 8]
            out_ref[hd + 8:, cols] = jnp.broadcast_to(new, (8, q_block))
            return carry

        lax.fori_loop(0, blocks * len(groups), running, 0)


def attention_forward(scale, hd, sources, bounds, kv, q):
    rows, width = kv.shape[1], kv.shape[2]
    total_q = q.shape[0]
    return pl.pallas_call(
        functools.partial(forward_kernel, scale, hd, min(512, total_q)),
        out_shape=shape((hd + 16, total_q), F32),
        grid=(1,),
        in_specs=[pl.BlockSpec(memory_space=pltpu.SMEM),
                  pl.BlockSpec((sources, rows, width), lambda i: (0, 0, 0), pipeline_mode=pl.Buffered(1)), full(q)],
        out_specs=pl.BlockSpec((hd + 16, total_q), lambda i: (0, 0)),
        scratch_shapes=[pltpu.VMEM((width, total_q), BF16), pltpu.VMEM((8, total_q), F32)],
        compiler_params=plain(12),
        cost_estimate=pl.CostEstimate(flops=4 * total_q * sources * rows * hd, bytes_accessed=kv.size * 2,
                                      transcendentals=total_q * sources * rows),
        name='attention_forward',
    )(bounds, kv, q)


def backward_kernel(scale, key_scale, hd, q_block, bounds_ref, kv_ref, q_ref, do_ref, out_ref, lse_ref, dkv_ref, dq_ref,
                    qt_ref, dot_ref, delta_ref):
    blocks, last_valid = bounds_ref[0], bounds_ref[1]
    rows, total_q = kv_ref.shape[1], q_ref.shape[0]
    width = kv_ref.shape[2]
    groups = [slice(first, first + q_block) for first in range(0, total_q, q_block)]
    dq_ref[...] = jnp.zeros_like(dq_ref)
    qt_ref[...] = q_ref[...].T
    do_t = do_ref[...].T
    dot_ref[...] = do_t
    delta_ref[...] = jnp.sum(do_t[hd:].astype(F32) * out_ref[...], axis=0, keepdims=True)

    lane_scale = jnp.where(lax.broadcasted_iota(jnp.int32, (1, width), 1) < hd, key_scale, 1.0)

    def products(keys, cols):
        return dot(keys, qt_ref[:, cols]), dot(keys, dot_ref[:, cols])

    def finish(keys, keys_t, scores, grads, cols, valid):
        prob = jnp.exp2(scores * scale - lse_ref[:, cols])
        if valid is not None:
            position = lax.broadcasted_iota(jnp.int32, scores.shape, 0)
            prob = jnp.where(position < valid, prob, 0.0)
        grad_scores = (prob * (grads - delta_ref[:, cols])).astype(keys.dtype)
        dq_ref[:, cols] += dot(keys_t, grad_scores)
        return dot(jnp.concatenate([grad_scores, prob.astype(keys.dtype)], axis=1),
                   jnp.concatenate([q_ref[cols, :], do_ref[cols, :]], axis=0))

    def step(index, carry):
        keys = kv_ref[index]
        keys_t = keys.T[:hd]
        total = jnp.zeros((rows, width), F32)
        ahead = products(keys, groups[0])
        for i, cols in enumerate(groups):
            scores, grads = ahead
            if i + 1 < len(groups):
                ahead = products(keys, groups[i + 1])
            total += finish(keys, keys_t, scores, grads, cols, None)
        dkv_ref[index] = (total * lane_scale).astype(dkv_ref.dtype)
        return carry

    def last_step(group, total):
        keys = kv_ref[blocks - 1]
        cols = pl.ds(pl.multiple_of(group * q_block, q_block), q_block)
        scores, grads = products(keys, cols)
        return total + finish(keys, keys.T[:hd], scores, grads, cols, last_valid)

    def clear(index, carry):
        dkv_ref[index] = jnp.zeros((rows, width), dkv_ref.dtype)
        return carry

    lax.fori_loop(0, blocks - 1, step, 0)
    total = lax.fori_loop(0, len(groups), last_step, jnp.zeros((rows, width), F32))
    dkv_ref[blocks - 1] = (total * lane_scale).astype(dkv_ref.dtype)
    lax.fori_loop(blocks, dkv_ref.shape[0], clear, 0)
    dq_ref[...] = dq_ref[...] * key_scale


def attention_backward(scale, key_scale, hd, sources, bounds, kv, q, do, out_t, lse):
    n, rows, width = kv.shape
    total_q = q.shape[0]
    return pl.pallas_call(
        functools.partial(backward_kernel, scale, key_scale, hd, min(256, total_q)),
        out_shape=[shape((n, rows, width), BF16), shape((hd, total_q), F32)],
        grid=(1,),
        in_specs=[pl.BlockSpec(memory_space=pltpu.SMEM),
                  pl.BlockSpec((sources, rows, width), lambda i: (0, 0, 0), pipeline_mode=pl.Buffered(1)),
                  full(q), full(do), full(out_t), full(lse)],
        out_specs=[pl.BlockSpec((n, rows, width), lambda i: (0, 0, 0)),
                   pl.BlockSpec((hd, total_q), lambda i: (0, 0))],
        scratch_shapes=[pltpu.VMEM((width, total_q), BF16), pltpu.VMEM((width, total_q), BF16), pltpu.VMEM((1, total_q), F32)],
        compiler_params=plain(24),
        cost_estimate=pl.CostEstimate(flops=10 * total_q * sources * rows * hd, bytes_accessed=kv.size * 4,
                                      transcendentals=total_q * sources * rows),
        name='attention_backward',
    )(bounds, kv, q, do, out_t, lse)


def prepare_kernel(dec_ref, att_ref, wo_ref, gain_ref, n2_ref, n2t_ref):
    hidden = (dec_ref[...].astype(F32) + dot(att_ref[...], wo_ref[...])).astype(BF16)
    normed = rms_norm(hidden.astype(F32), gain_ref[...].astype(F32)).astype(BF16)
    n2_ref[...] = normed
    n2t_ref[...] = normed.T


def prepare(early, late, wo, gain):
    rows, dim = early.shape[0], wo.shape[1]
    chunk = min(512, rows)
    left = pl.BlockSpec((chunk, dim), lambda i: (i, 0))
    return pl.pallas_call(
        prepare_kernel,
        out_shape=[shape((rows, dim), BF16), shape((dim, rows), BF16)],
        grid=(rows // chunk,),
        in_specs=[left, pl.BlockSpec((chunk, wo.shape[0]), lambda i: (i, 0)), full(wo), full(gain)],
        out_specs=[left, pl.BlockSpec((dim, chunk), lambda i: (0, i))],
        compiler_params=plain(20),
        cost_estimate=pl.CostEstimate(flops=2 * rows * dim * dim, bytes_accessed=8 * rows * dim, transcendentals=0),
        name='prepare',
    )(early, late, wo, gain)


def mlp_kernel(chunk, n2_ref, n2t_ref, top_ref, w1_ref, w3_ref, w2_ref, g1_ref, g3_ref, g2_ref, d1_ref, d3_ref, act_ref):
    rows = n2_ref.shape[0]
    w1, w3, w2t = w1_ref[...], w3_ref[...], w2_ref[...].T
    for first in range(0, rows, chunk):
        part = slice(first, first + chunk)
        gate = dot(n2_ref[part, :], w1)
        up = dot(n2_ref[part, :], w3)
        grad = dot(top_ref[part, :], w2t)
        sig = jax.nn.sigmoid(gate)
        silu = gate * sig
        act_ref[part, :] = (silu * up).astype(act_ref.dtype)
        d3_ref[part, :] = (grad * silu).astype(d3_ref.dtype)
        d1_ref[part, :] = (grad * up * (sig + silu * (1.0 - sig))).astype(d1_ref.dtype)
    g1_ref[...] = dot(n2t_ref[...], d1_ref[...])
    g3_ref[...] = dot(n2t_ref[...], d3_ref[...])
    g2_ref[...] = dot_tn(act_ref[...], top_ref[...])


def mlp_weight_grads(n2, n2t, early, w_gate, w_up, w_down):
    rows, dim = n2.shape
    ff = w_gate.shape[1]
    tile = 256
    cols = pl.BlockSpec((dim, tile), lambda i: (0, i))
    tall = pl.BlockSpec((tile, dim), lambda i: (i, 0))
    return pl.pallas_call(
        functools.partial(mlp_kernel, min(512, rows)),
        out_shape=[shape((dim, ff), F32), shape((dim, ff), F32), shape((ff, dim), F32)],
        grid=(ff // tile,),
        in_specs=[full(n2), full(n2t), pl.BlockSpec((rows, dim), lambda i: (0, 1), pipeline_mode=pl.Buffered(1)), cols, cols, tall],
        out_specs=[cols, cols, tall],
        scratch_shapes=[pltpu.VMEM((rows, tile), BF16)] * 3,
        compiler_params=plain(36),
        cost_estimate=pl.CostEstimate(flops=12 * rows * dim * ff, bytes_accessed=18 * dim * ff, transcendentals=rows * ff),
        name='mlp_weight_grads',
    )(n2, n2t, early, w_gate, w_up, w_down)


def memory_weight_kernel(memory_ref, dkv_ref, gk_ref, gv_ref):
    group, hd = dkv_ref.shape[0], dkv_ref.shape[2] // 2
    for i in range(group):
        both = dot_tn(dkv_ref[i], memory_ref[...])
        gk_ref[i * hd:(i + 1) * hd, :] = both[:hd]
        gv_ref[i * hd:(i + 1) * hd, :] = both[hd:]


def memory_weight_grads(memory, dkv):
    heads, rows, width = dkv.shape
    dim, hd = memory.shape[1], width // 2
    group = 4
    out = pl.BlockSpec((group * hd, dim), lambda i: (i, 0))
    return pl.pallas_call(
        memory_weight_kernel,
        out_shape=[shape((heads * hd, dim), F32)] * 2,
        grid=(heads // group,),
        in_specs=[full(memory), pl.BlockSpec((group, rows, width), lambda i: (i, 0, 0))],
        out_specs=[out, out],
        compiler_params=plain(14),
        cost_estimate=pl.CostEstimate(flops=2 * rows * dim * heads * width, bytes_accessed=16 * rows * dim, transcendentals=0),
        name='memory_weight_grads',
    )(memory, dkv)


def memory_grad_kernel(dkv_ref, wk_ref, wv_ref, out_ref):
    group = dkv_ref.shape[0]
    left = jnp.concatenate([dkv_ref[i] for i in range(group)], axis=1)
    right = jnp.concatenate([part[i] for i in range(group) for part in (wk_ref, wv_ref)], axis=0)

    @pl.when(pl.program_id(0) == 0)
    def _():
        out_ref[...] = dot(left, right)

    @pl.when(pl.program_id(0) > 0)
    def _():
        out_ref[...] += dot(left, right)


def memory_grad(dkv, wk_t, wv_t):
    heads, rows, width = dkv.shape
    hd, dim = wk_t.shape[1], wk_t.shape[2]
    group = 4
    weight = pl.BlockSpec((group, hd, dim), lambda i: (i, 0, 0))
    return pl.pallas_call(
        memory_grad_kernel,
        out_shape=shape((rows, dim), F32),
        grid=(heads // group,),
        in_specs=[pl.BlockSpec((group, rows, width), lambda i: (i, 0, 0)), weight, weight],
        out_specs=pl.BlockSpec((rows, dim), lambda i: (0, 0)),
        compiler_params=plain(18),
        cost_estimate=pl.CostEstimate(flops=2 * rows * dim * heads * width, bytes_accessed=12 * rows * dim, transcendentals=0),
        name='memory_grad',
    )(dkv, wk_t, wv_t)


def outer_kernel(dec_ref, gain_ref, att_ref, gh_ref, dq_ref, gwo_ref, gwq_ref):
    heads, _, hd, chunk = dq_ref.shape
    normed = rms_norm(dec_ref[...].astype(F32), gain_ref[...].astype(F32)).astype(BF16)
    left = dq_ref[...].reshape(heads * hd, chunk)

    @pl.when(pl.program_id(0) == 0)
    def _():
        gwo_ref[...] = jnp.zeros_like(gwo_ref)
        gwq_ref[...] = jnp.zeros_like(gwq_ref)

    gwo_ref[...] += dot_tn(att_ref[...], gh_ref[...])
    gwq_ref[...] += dot(left, normed)


def outer_weight_grads(early, late, gain, dq_all):
    heads, parts, hd, share = dq_all.shape
    rows, dim = early.shape[0], gain.shape[1]
    chunk = min(512, share)
    per = share // chunk
    out = pl.BlockSpec((heads * hd, dim), lambda i: (0, 0))
    return pl.pallas_call(
        outer_kernel,
        out_shape=[shape((heads * hd, dim), F32)] * 2,
        grid=(rows // chunk,),
        in_specs=[pl.BlockSpec((chunk, dim), lambda i: (i, 0)), full(gain), pl.BlockSpec((chunk, heads * hd), lambda i: (i, 0)),
                  pl.BlockSpec((chunk, dim), lambda i: (i, 1)),
                  pl.BlockSpec((heads, 1, hd, chunk), lambda i: (0, i // per, 0, i % per))],
        out_specs=[out, out],
        compiler_params=plain(32),
        cost_estimate=pl.CostEstimate(flops=4 * rows * dim * heads * hd, bytes_accessed=16 * rows * dim, transcendentals=0),
        name='outer_weight_grads',
    )(early, gain, late, late, dq_all)


def solution(mesh):
    n = mesh.shape['seq']
    row_spec = P(('data', 'seq'), None)
    weight_spec = P()
    part_vec = P('data')
    part_mat = P('data', None)
    part_cube = P('data', None, None)

    def device_step(dec_in, memory, mem_len, grad_out, norm_attn, wq_cross, wk_cross, wv_cross, wo_cross, norm_mlp, w_gate, w_up, w_down):
        q_rows, dim = dec_in.shape
        m_rows = memory.shape[0]
        heads, hd = wq_cross.shape[1], wq_cross.shape[2]
        parts = n // heads
        half = m_rows // parts
        sources = -(-3 * n // 4)
        total_q = q_rows * n
        key_scale = hd ** -0.5
        scale = key_scale * LOG2E
        me = lax.axis_index('seq')
        part = lax.rem(me, parts)

        reach = mem_len[0] - part * half
        blocks = jnp.minimum((reach + m_rows - 1) // m_rows, sources)
        bounds = jnp.stack([blocks, jnp.minimum(reach - (blocks - 1) * m_rows, half)]).astype(jnp.int32)

        wq_t, wk_t, wv_t = (jnp.transpose(w, (1, 2, 0)) for w in (wq_cross, wk_cross, wv_cross))
        gain_attn, gain_mlp = norm_attn.reshape(1, dim), norm_mlp.reshape(1, dim)
        source_rows = -(-sources // (parts * math.isqrt(heads)))
        kv, q_in = exchange(n, heads, source_rows, 0, memory, dec_in, gain_attn, wk_t, wv_t, wq_t)
        head_q = q_in.reshape(total_q, 2 * hd)

        grad_top = grad_out.astype(BF16)
        early_local, kv = lax.optimization_barrier((jnp.concatenate([dec_in, grad_top], axis=1), kv))
        early = lax.all_gather(early_local, 'seq', axis=0, tiled=True)

        mine = attention_forward(scale, hd, sources, bounds, kv, head_q)
        attended, out_t, lse = combine(n, heads, hd, q_rows, 1, mine)

        x_in = dec_in.astype(F32)
        hidden_f = x_in + jnp.einsum('hqe,hed->qd', attended, wo_cross, preferred_element_type=F32)
        hidden = hidden_f.astype(BF16)
        normed_mlp_f, mlp_norm_pull = jax.vjp(rms_norm, hidden.astype(F32), norm_mlp.astype(F32))
        normed_mlp = normed_mlp_f.astype(BF16)
        gate_pre = jnp.dot(normed_mlp, w_gate, preferred_element_type=F32)
        up_pre = jnp.dot(normed_mlp, w_up, preferred_element_type=F32)
        _, gated_pull = jax.vjp(gated_unit, gate_pre, up_pre)
        grad_act = jnp.einsum('qd,fd->qf', grad_top, w_down, preferred_element_type=F32)
        grad_gate, grad_up = gated_pull(grad_act)
        grad_normed_mlp = (jnp.einsum('qf,df->qd', grad_gate.astype(BF16), w_gate, preferred_element_type=F32)
                           + jnp.einsum('qf,df->qd', grad_up.astype(BF16), w_up, preferred_element_type=F32))
        grad_hidden_norm, g_norm_mlp = mlp_norm_pull(grad_normed_mlp)
        grad_hidden = grad_out + grad_hidden_norm
        grad_hidden_b = grad_hidden.astype(BF16)
        grad_att = jnp.einsum('qd,hed->hqe', grad_hidden_b, wo_cross, preferred_element_type=F32).astype(BF16)
        head_do = to_heads(n, heads, 2, grad_att).reshape(total_q, 2 * hd)

        late_local = jnp.concatenate([attended.transpose(1, 0, 2).reshape(q_rows, heads * hd), grad_hidden_b], axis=1)
        head_do, late_local, early = lax.optimization_barrier((head_do, late_local, early))
        late = lax.all_gather(late_local, 'seq', axis=0, tiled=True)

        dkv, dq_part = attention_backward(scale, key_scale, hd, sources, bounds, kv, head_q, head_do, out_t, lse)
        dq_rows, dq_share = pair_sum(n, heads, q_rows, 3, dq_part)
        dkv, dq_share, late = lax.optimization_barrier((dkv, dq_share, late))
        dq_all = lax.all_gather(dq_share, 'seq', axis=0, tiled=False).reshape(heads, parts, hd, total_q // parts)
        dkv_in = return_blocks(n, heads, source_rows, 4, dkv)
        dkv_in, dq_all, dq_rows = lax.optimization_barrier((dkv_in, dq_all, dq_rows))

        gk_part, gv_part = memory_weight_grads(memory, dkv_in)
        gk_part, gv_part, dkv_in, dq_all, dq_rows, early, late = lax.optimization_barrier(
            (gk_part, gv_part, dkv_in, dq_all, dq_rows, early, late))
        g_wk, g_wv = lax.psum((gk_part, gv_part), 'seq')

        n2_all, n2_all_t = prepare(early, late, wo_cross.reshape(heads * hd, dim), gain_mlp)
        g_gate, g_up, g_down = mlp_weight_grads(n2_all, n2_all_t, early, w_gate, w_up, w_down)
        g_wo, g_wq = outer_weight_grads(early, late, gain_attn, dq_all)

        grad_normed = jnp.einsum('hte,dhe->td', dq_rows, wq_cross, preferred_element_type=F32)
        _, norm_pull = jax.vjp(rms_norm, x_in, norm_attn.astype(F32))
        grad_x_norm, g_norm_attn = norm_pull(grad_normed)
        g_dec = grad_hidden + grad_x_norm
        norms = small_sum(n, 5, jnp.concatenate([g_norm_attn, g_norm_mlp]).reshape(-1, 128)).reshape(2, dim)
        g_mem = memory_grad(dkv_in, wk_t, wv_t)
        cube = lambda g: jnp.transpose(g.reshape(heads, hd, dim), (2, 0, 1))
        return (g_dec, g_mem, norms[0], cube(g_wq), cube(g_wk), cube(g_wv), g_wo.reshape(heads, hd, dim), norms[1], g_gate, g_up, g_down)

    return jax.shard_map(device_step, mesh=mesh,
                         in_specs=(row_spec, row_spec, part_vec, row_spec) + (weight_spec,) * 9,
                         out_specs=(row_spec, row_spec, part_vec, part_cube, part_cube, part_cube, part_cube, part_vec, part_mat, part_mat, part_mat),
                         check_vma=False)
```

```python
import functools
import math

import jax
import jax.numpy as jnp
from jax import lax
from jax.experimental import pallas as pl
from jax.experimental.pallas import tpu as pltpu
from jax.sharding import PartitionSpec as P

LOG2E = 1.4426950408889634
NEG = -1e30
VMEM_LIMIT = 60 * 1024 * 1024
MESH = pl.DeviceIdType.MESH
BF16, F32 = jnp.bfloat16, jnp.float32


def rms_norm(tensor, gain):
    mean_sq = jnp.mean(tensor * tensor, axis=-1, keepdims=True)
    return tensor * lax.rsqrt(mean_sq + 1e-6) * gain


def gated_unit(gate_pre, up_pre):
    return jax.nn.silu(gate_pre) * up_pre


def dot(a, b):
    return jnp.dot(a, b, preferred_element_type=F32)


def dot_nt(a, b):
    return lax.dot_general(a, b, (((1,), (1,)), ((), ())), preferred_element_type=F32)


def dot_tn(a, b):
    return lax.dot_general(a, b, (((0,), (0,)), ((), ())), preferred_element_type=F32)


def full(array):
    return pl.BlockSpec(array.shape, lambda *_: (0,) * array.ndim, pipeline_mode=pl.Buffered(1))


def vmem(count):
    return [pl.BlockSpec(memory_space=pltpu.VMEM)] * count


def plain():
    return pltpu.CompilerParams(vmem_limit_bytes=VMEM_LIMIT)


def remote(collective_id):
    return pltpu.CompilerParams(collective_id=collective_id, has_side_effects=True, vmem_limit_bytes=VMEM_LIMIT)


def shape(dims, dtype):
    return jax.ShapeDtypeStruct(dims, dtype)


def meet(peers):
    barrier = pltpu.get_barrier_semaphore()
    for peer in peers:
        pl.semaphore_signal(barrier, inc=1, device_id={'seq': peer}, device_id_type=MESH)
    pl.semaphore_wait(barrier, len(peers))


def send(src, dst, send_sem, recv_sem, peer):
    return pltpu.make_async_remote_copy(src_ref=src, dst_ref=dst, send_sem=send_sem, recv_sem=recv_sem,
                                        device_id={'seq': peer}, device_id_type=MESH)


class Grid:
    def __init__(self, n, heads, source_rows):
        self.n, self.heads, self.source_rows = n, heads, source_rows
        self.parts = n // heads
        self.side = math.isqrt(heads)
        self.me = lax.axis_index('seq')
        self.part = lax.rem(self.me, self.parts)
        self.chip = self.me // self.parts
        self.col = lax.rem(self.chip, self.side)
        self.row = self.chip // self.side
        self.partner = self.chip * self.parts + (self.parts - 1 - self.part)
        self.ties = self.side == 4
        self.direct = (1, 3) if self.ties else (1,)

    def wrap(self, value):
        return lax.rem(value + self.side, self.side)

    def device(self, row, col, part):
        return (row * self.side + col) * self.parts + part

    def near(self, drow, dcol, part=None):
        return self.device(self.wrap(self.row + drow), self.wrap(self.col + dcol), self.part if part is None else part)

    def hop(self, offset):
        return 1 if offset == 1 else -1

    def is_source(self, row):
        return self.wrap(row) < self.source_rows

    def row_peers(self):
        return [lax.rem(self.chip + step, self.heads) * self.parts + self.part for step in range(1, self.heads)]

    def peers(self):
        return self.row_peers() + [self.partner] + [self.near(0, self.hop(d), self.parts - 1 - self.part) for d in self.direct]


def pair_peers(n, heads, me, part):
    parts = n // heads
    head = me // parts
    partner = head * parts + (parts - 1 - part)
    return partner, [partner] + [lax.rem(head + step, heads) * parts + part for step in range(1, heads)]


def pack(rows):
    middle = rows.shape[-2] // 2
    return jnp.concatenate([rows[..., :middle, :], rows[..., middle:, :]], axis=-1)


def unpack(packed):
    middle = packed.shape[-1] // 2
    return jnp.concatenate([packed[..., :middle], packed[..., middle:]], axis=-2)


def start_rows(n, heads, me, part, src, src_of, dst_ref, send_sem, recv_sem):
    parts = n // heads
    head = me // parts
    for step in range(1, heads):
        peer = lax.rem(head + step, heads) * parts + part
        send(src.at[src_of(peer)], dst_ref.at[head], send_sem, recv_sem, peer).start()
    dst_ref[head] = src[src_of(me)]


def wait_rows(heads, me, dst_ref, send_sem, recv_sem):
    others = dst_ref.at[pl.ds(0, heads - 1)]
    whole = send(others, others, send_sem, recv_sem, me)
    whole.wait_send()
    whole.wait_recv()


def swap(src, dst, send_sem, recv_sem, partner):
    copy = send(src, dst, send_sem, recv_sem, partner)
    copy.start()
    copy.wait()


def place(n, heads, part, mine_ref, theirs_ref, wide_ref, low):
    parts = n // heads
    for source, index in ((mine_ref, part), (theirs_ref, parts - 1 - part)):
        for head in range(heads):
            rows = unpack(source[head])
            zeros = jnp.zeros_like(rows)
            wide_ref[head * parts + index] = jnp.concatenate([rows, zeros] if low else [zeros, rows], axis=-1)


def exchange_kernel(n, heads, source_rows, memory_ref, dec_ref, gain_ref, wk_ref, wv_ref, wq_ref, kv_out_ref, q_out_ref,
                    kv_ref, stage_ref, up_ref, down_ref, right_ref, left_ref, packed_ref, got_ref, swapped_ref,
                    row_send, row_recv, y_send, pass_send, x_send, fwd_send, stage_recv, up_recv, down_recv, right_recv,
                    left_recv, out_recv):
    g = Grid(n, heads, source_rows)
    side, hd = g.side, wk_ref.shape[1]
    half = kv_out_ref.shape[1]
    chunk_rows = min(256, kv_ref.shape[1])
    barrier = pltpu.get_barrier_semaphore()
    peers = g.peers()
    for peer in peers:
        pl.semaphore_signal(barrier, inc=1, device_id={'seq': peer}, device_id_type=MESH)

    normed = rms_norm(dec_ref[...].astype(F32), gain_ref[...].astype(F32)).astype(BF16)
    for i in range(0, heads, 4):
        queries = dot_nt(normed, jnp.concatenate([wq_ref[i + j] for j in range(4)], axis=0)).astype(BF16)
        for j in range(4):
            packed_ref[i + j] = pack(queries[:, hd * j:hd * (j + 1)])

    def head(drow, dcol):
        return g.wrap(g.row + drow) * side + g.wrap(g.col + dcol)

    def project(drow, dcols):
        weights = jnp.concatenate([ref[head(drow, d)] for d in dcols for ref in (wk_ref, wv_ref)], axis=0)

        def rows(index, carry):
            at = pl.ds(pl.multiple_of(index * chunk_rows, chunk_rows), chunk_rows)
            both = dot_nt(memory_ref[at, :], weights).astype(BF16)
            for i, d in enumerate(dcols):
                kv_ref[head(drow, d), at, :] = both[:, 2 * hd * i:2 * hd * (i + 1)]
            return carry

        lax.fori_loop(0, kv_ref.shape[1] // chunk_rows, rows, 0)

    def along_column(drow, dcol):
        chunk = kv_ref.at[head(drow, dcol)]
        if drow in g.direct:
            send(chunk, stage_ref.at[drow - 1, dcol], y_send.at[drow - 1], stage_recv.at[drow - 1, dcol], g.near(g.hop(drow), 0)).start()
        elif dcol % 2 == 0:
            send(chunk, up_ref.at[dcol // 2], y_send.at[drow - 1], up_recv.at[dcol // 2], g.near(1, 0)).start()
        else:
            send(chunk, down_ref.at[dcol // 2], y_send.at[drow - 1], down_recv.at[dcol // 2], g.near(-1, 0)).start()

    def along_row(o, dcol):
        chunk = kv_ref.at[head(0, dcol)] if o == 0 else stage_ref.at[o - 1, dcol]
        source = g.device(g.wrap(g.row - o), g.col, g.part)
        if dcol == 0:
            kv_out_ref[source] = chunk[pl.ds(pl.multiple_of(g.part * half, half), half), :]
            away = pl.ds(pl.multiple_of((g.parts - 1 - g.part) * half, half), half)
            send(chunk.at[away], kv_out_ref.at[source], x_send.at[o], out_recv, g.partner).start()
        elif dcol in g.direct:
            for part in range(g.parts):
                send(chunk.at[pl.ds(part * half, half)], kv_out_ref.at[source], x_send.at[o], out_recv,
                     g.near(0, g.hop(dcol), part)).start()
        else:
            send(chunk.at[pl.ds(0, half)], right_ref.at[o], x_send.at[o], right_recv.at[o], g.near(0, 1)).start()
            send(chunk.at[pl.ds(half, half)], left_ref.at[o], x_send.at[o], left_recv.at[o], g.near(0, -1)).start()

    def pass_row(o):
        for ref, sem, come in ((right_ref, right_recv, -1), (left_ref, left_recv, 1)):
            source = g.device(g.wrap(g.row - o), g.wrap(g.col + come), g.part)
            send(ref.at[o], ref.at[o], fwd_send.at[o], sem.at[o], g.me).wait_recv()
            send(ref.at[o], kv_out_ref.at[source], fwd_send.at[o], out_recv, g.near(0, -come, 0 if come < 0 else 1)).start()

    def when_source(row, body):
        pl.when(g.is_source(row))(body)

    if g.ties:
        order = [(2, (2, 1)), (2, (3, 0)), (1, (2, 1)), (3, (2, 1)), (0, (2, 1)), (0, (3, 0))]
        last = [(1, (3, 0)), (3, (3, 0))]
    else:
        order, last = [(1, (1, 0)), (0, (1, 0))], []

    def issue(drow, dcols):
        def body():
            for d in dcols:
                along_row(0, d) if drow == 0 else along_column(drow, d)
        when_source(g.row, body)

    waiting = None
    for drow, dcols in order + last:
        project(drow, dcols)
        if waiting is None:
            pl.semaphore_wait(barrier, len(peers))
            start_rows(n, heads, g.me, g.part, packed_ref, lambda peer: peer // g.parts, got_ref, row_send.at[0], row_recv.at[0])
        elif waiting not in last:
            issue(*waiting)
        waiting = (drow, dcols)
    if not last:
        issue(*waiting)

    if g.ties:
        def up(i):
            send(up_ref.at[i], up_ref.at[i], pass_send.at[0], up_recv.at[i], g.me).wait_recv()
            send(up_ref.at[i], stage_ref.at[1, 2 * i], pass_send.at[0], stage_recv.at[1, 2 * i], g.near(1, 0)).start()

        def down(i):
            send(down_ref.at[i], down_ref.at[i], pass_send.at[1], down_recv.at[i], g.me).wait_recv()
            send(down_ref.at[i], stage_ref.at[1, 2 * i + 1], pass_send.at[1], stage_recv.at[1, 2 * i + 1], g.near(-1, 0)).start()

        for i in range(2):
            when_source(g.row - 1, lambda i=i: up(1 - i))
            when_source(g.row + 1, lambda i=i: down(i))
        for drow, dcols in last:
            issue(drow, dcols)
        when_source(g.row, lambda: pass_row(0))

    wait_rows(heads, g.me, got_ref, row_send.at[0], row_recv.at[0])
    swap(got_ref, swapped_ref, row_send.at[1], row_recv.at[1], g.partner)
    place(n, heads, g.part, got_ref, swapped_ref, q_out_ref, True)

    def arrived(o, dcol):
        def body():
            send(stage_ref.at[o - 1, dcol], stage_ref.at[o - 1, dcol], y_send.at[0], stage_recv.at[o - 1, dcol], g.me).wait_recv()
            along_row(o, dcol)
        when_source(g.row - o, body)

    if g.ties:
        for d in (2, 1):
            for o in g.direct:
                arrived(o, d)
        for o in g.direct:
            when_source(g.row - o, lambda o=o: pass_row(o))
        for d in (2, 1, 0, 3):
            arrived(2, d)
        when_source(g.row - 2, lambda: pass_row(2))
        for d in (3, 0):
            for o in g.direct:
                arrived(o, d)
    else:
        for d in (1, 0):
            arrived(1, d)

    def sent(sem, ref):
        send(ref, ref, sem, out_recv, g.me).wait_send()

    def mine():
        for drow in range(1, side):
            sent(y_send.at[drow - 1], stage_ref.at[0])
    when_source(g.row, mine)
    for o in range(side):
        def passed(o=o):
            sent(x_send.at[o], kv_out_ref.at[pl.ds(0, g.parts * side - 1)])
            if g.ties:
                sent(fwd_send.at[o], kv_out_ref.at[pl.ds(0, 2)])
        when_source(g.row - o, passed)
    if g.ties:
        when_source(g.row - 1, lambda: sent(pass_send.at[0], up_ref))
        when_source(g.row + 1, lambda: sent(pass_send.at[1], down_ref))
    blocks = source_rows * side * g.parts
    others = kv_out_ref.at[pl.ds(0, blocks - source_rows)]
    send(others, others, y_send.at[0], out_recv, g.me).wait_recv()


def row_scratch(heads, q_rows, hd):
    return [pltpu.VMEM((heads, q_rows // 2, 2 * hd), BF16)] * 3


def dma(*dims):
    return pltpu.SemaphoreType.DMA(dims)


def exchange(n, heads, source_rows, collective_id, memory, dec_in, gain, wk_t, wv_t, wq_t):
    m_rows, q_rows, hd = memory.shape[0], dec_in.shape[0], wk_t.shape[1]
    side, parts = math.isqrt(heads), n // heads
    half = m_rows // parts
    chunk = lambda *lead: pltpu.VMEM(lead + (m_rows, 2 * hd), BF16)
    block = lambda *lead: pltpu.VMEM(lead + (half, 2 * hd), BF16)
    return pl.pallas_call(
        functools.partial(exchange_kernel, n, heads, source_rows),
        out_shape=[shape((n, half, 2 * hd), BF16), shape((n, q_rows, 2 * hd), BF16)],
        in_specs=vmem(6),
        out_specs=vmem(2),
        scratch_shapes=[chunk(heads), chunk(side - 1, side), chunk(2), chunk(2), block(side), block(side)]
        + row_scratch(heads, q_rows, hd)
        + [dma(2), dma(2), dma(side - 1), dma(2), dma(side), dma(side), dma(side - 1, side), dma(2), dma(2), dma(side), dma(side),
           pltpu.SemaphoreType.DMA],
        compiler_params=remote(collective_id),
        name='exchange',
    )(memory, dec_in, gain, wk_t, wv_t, wq_t)


def return_kernel(n, heads, source_rows, src_ref, dq_ref, dst_ref, rows_ref, stage_ref, right_ref, left_ref, up_ref, down_ref,
                  theirs_ref, packed_ref, got_ref, row_send, row_recv,
                  x_send, fwd_send, y_send, pass_send, stage_recv, right_recv, left_recv, up_recv, down_recv, out_recv):
    g = Grid(n, heads, source_rows)
    side = g.side
    half = src_ref.shape[1]
    meet(g.peers())
    mine = pl.ds(pl.multiple_of(g.part * half, half), half)

    def landing(drow, dcol, head_col):
        if drow == 0:
            return dst_ref.at[g.row * side + head_col, mine], out_recv
        return stage_ref.at[drow - 1, dcol, mine], stage_recv.at[drow - 1, dcol]

    def along_row(drow, dcol):
        row = g.wrap(g.row + drow)
        col = g.wrap(g.col + dcol)
        for part in range(g.parts):
            source = src_ref.at[g.device(row, col, part)]
            if dcol in g.direct:
                dst, sem = landing(drow, dcol, g.col)
                send(source, dst, x_send.at[drow], sem, g.near(0, g.hop(dcol), part)).start()
            elif part == 0:
                send(source, right_ref.at[drow], x_send.at[drow], right_recv.at[drow], g.near(0, 1)).start()
            else:
                send(source, left_ref.at[drow], x_send.at[drow], left_recv.at[drow], g.near(0, -1)).start()

    def own_chip(drow):
        row = g.wrap(g.row + drow)
        away = src_ref.at[g.device(row, g.col, g.parts - 1 - g.part)]
        dst, sem = landing(drow, 0, g.col)
        dst[...] = src_ref[g.device(row, g.col, g.part)]
        send(away, dst, x_send.at[drow], sem, g.partner).start()

    def pass_row(drow):
        for ref, come_sem, come in ((right_ref, right_recv, -1), (left_ref, left_recv, 1)):
            send(ref.at[drow], ref.at[drow], fwd_send.at[drow], come_sem.at[drow], g.me).wait_recv()
            dst, sem = landing(drow, 2, g.wrap(g.col + come))
            send(ref.at[drow], dst, fwd_send.at[drow], sem, g.near(0, -come, 0 if come < 0 else 1)).start()

    def along_column(drow, dcol):
        chunk = stage_ref.at[drow - 1, dcol]
        got = chunk.at[pl.ds(0, half)] if dcol == 0 else chunk
        send(got, got, y_send.at[drow - 1], stage_recv.at[drow - 1, dcol], g.me).wait_recv()
        head = g.row * side + g.wrap(g.col - dcol)
        if drow in g.direct:
            send(chunk, dst_ref.at[head], y_send.at[drow - 1], out_recv, g.near(g.hop(drow), 0)).start()
        elif dcol % 2 == 0:
            send(chunk, up_ref.at[dcol // 2], y_send.at[drow - 1], up_recv.at[dcol // 2], g.near(1, 0)).start()
        else:
            send(chunk, down_ref.at[dcol // 2], y_send.at[drow - 1], down_recv.at[dcol // 2], g.near(-1, 0)).start()

    def when_source(row, body):
        pl.when(g.is_source(row))(body)

    def rows_of(drow):
        def body():
            for d in (2, 1, 3) if g.ties else (1,):
                along_row(drow, d)
        when_source(g.row + drow, body)

    def relay(drow):
        when_source(g.row + drow, lambda: pass_row(drow))

    def column(drow, d):
        when_source(g.row + drow, lambda: along_column(drow, d))

    def up(i):
        def body():
            send(up_ref.at[i], up_ref.at[i], pass_send.at[0], up_recv.at[i], g.me).wait_recv()
            head = g.wrap(g.row - 1) * side + g.wrap(g.col - 2 * i)
            send(up_ref.at[i], dst_ref.at[head], pass_send.at[0], out_recv, g.near(1, 0)).start()
        when_source(g.row + 1, body)

    def down(i):
        def body():
            send(down_ref.at[i], down_ref.at[i], pass_send.at[1], down_recv.at[i], g.me).wait_recv()
            head = g.wrap(g.row + 1) * side + g.wrap(g.col - 2 * i - 1)
            send(down_ref.at[i], dst_ref.at[head], pass_send.at[1], out_recv, g.near(-1, 0)).start()
        when_source(g.row - 1, body)

    def start_dq():
        swap(dq_ref, theirs_ref, row_send.at[0], row_recv.at[0], g.partner)
        total = (dq_ref[...] + theirs_ref[...]).T.astype(BF16)
        packed_ref[...] = pack(total.reshape(n, total.shape[0] // n, total.shape[1]))
        start_rows(n, heads, g.me, g.part, packed_ref, lambda peer: peer, got_ref, row_send.at[1], row_recv.at[1])

    for drow in (2, 1, 3, 0) if g.ties else (1, 0):
        when_source(g.row + drow, lambda drow=drow: own_chip(drow))
    if g.ties:
        rows_of(2)
        rows_of(1)
        start_dq()
        for drow in (2, 1, 3):
            column(drow, 0)
        relay(2)
        rows_of(3)
        relay(1)
        column(2, 1)
        column(2, 3)
        column(2, 2)
        up(0)
        down(0)
        rows_of(0)
        column(1, 1)
        column(1, 3)
        relay(3)
        column(1, 2)
        up(1)
        down(1)
        relay(0)
        column(3, 1)
        column(3, 3)
        column(3, 2)
    else:
        rows_of(1)
        rows_of(0)
        start_dq()
        column(1, 0)
        column(1, 1)
    wait_rows(heads, g.me, got_ref, row_send.at[1], row_recv.at[1])
    rows_ref[...] = unpack(got_ref[...])

    def sent(sem, ref):
        send(ref, ref, sem, out_recv, g.me).wait_send()

    for drow in range(side):
        def done(drow=drow):
            sent(x_send.at[drow], src_ref.at[pl.ds(0, g.parts * side - 1)])
            if g.ties:
                sent(fwd_send.at[drow], src_ref.at[pl.ds(0, 2)])
            if drow:
                sent(y_send.at[drow - 1], stage_ref.at[0])
        when_source(g.row + drow, done)
    if g.ties:
        when_source(g.row + 1, lambda: sent(pass_send.at[0], up_ref))
        when_source(g.row - 1, lambda: sent(pass_send.at[1], down_ref))

    @pl.when(g.is_source(g.row))
    def _():
        blocks = src_ref.at[pl.ds(0, n - 1)]
        send(blocks, blocks, y_send.at[0], out_recv, g.me).wait_recv()

    @pl.when(jnp.logical_not(g.is_source(g.row)))
    def _():
        def clear(index, carry):
            dst_ref[index] = jnp.zeros(dst_ref.shape[1:], dst_ref.dtype)
            return carry
        lax.fori_loop(0, heads, clear, 0)


def return_blocks(n, heads, source_rows, collective_id, blocks, dq):
    half, width = blocks.shape[1], blocks.shape[2]
    hd, total_q = dq.shape
    q_rows = total_q // n
    side, parts = math.isqrt(heads), n // heads
    chunk = lambda *lead: pltpu.VMEM(lead + (half * parts, width), BF16)
    block = lambda *lead: pltpu.VMEM(lead + (half, width), BF16)
    return pl.pallas_call(
        functools.partial(return_kernel, n, heads, source_rows),
        out_shape=[shape((heads, half * parts, width), BF16), shape((heads, q_rows, hd), BF16)],
        in_specs=vmem(2),
        out_specs=vmem(2),
        scratch_shapes=[chunk(side - 1, side), block(side), block(side), chunk(2), chunk(2), pltpu.VMEM(dq.shape, F32),
                        pltpu.VMEM((n, q_rows // 2, 2 * hd), BF16), pltpu.VMEM((heads, q_rows // 2, 2 * hd), BF16), dma(2), dma(2),
                        dma(side), dma(side), dma(side - 1), dma(2), dma(side - 1, side), dma(side), dma(side), dma(2), dma(2),
                        pltpu.SemaphoreType.DMA],
        compiler_params=remote(collective_id),
        name='return_blocks',
    )(blocks, dq)


def to_heads_kernel(n, heads, rows_ref, wide_ref, packed_ref, got_ref, swapped_ref, send_sem, recv_sem):
    me = lax.axis_index('seq')
    part = lax.rem(me, n // heads)
    partner, peers = pair_peers(n, heads, me, part)
    packed_ref[...] = pack(rows_ref[...])
    meet(peers)
    start_rows(n, heads, me, part, packed_ref, lambda peer: peer // (n // heads), got_ref, send_sem.at[0], recv_sem.at[0])
    wait_rows(heads, me, got_ref, send_sem.at[0], recv_sem.at[0])
    swap(got_ref, swapped_ref, send_sem.at[1], recv_sem.at[1], partner)
    place(n, heads, part, got_ref, swapped_ref, wide_ref, False)


def to_heads(n, heads, collective_id, rows):
    q_rows, hd = rows.shape[1], rows.shape[2]
    return pl.pallas_call(
        functools.partial(to_heads_kernel, n, heads),
        out_shape=shape((n, q_rows, 2 * hd), BF16),
        in_specs=vmem(1),
        out_specs=vmem(1)[0],
        scratch_shapes=row_scratch(heads, q_rows, hd) + [pltpu.SemaphoreType.DMA((2,)), pltpu.SemaphoreType.DMA((2,))],
        compiler_params=remote(collective_id),
        name='to_heads',
    )(rows)


def to_rows(n, heads, q_rows, me, part, values, packed_ref, got_ref, rows_ref, send_sem, recv_sem):
    packed_ref[...] = pack(values.T.astype(BF16).reshape(n, q_rows, values.shape[0]))
    start_rows(n, heads, me, part, packed_ref, lambda peer: peer, got_ref, send_sem, recv_sem)
    wait_rows(heads, me, got_ref, send_sem, recv_sem)
    rows_ref[...] = unpack(got_ref[...])


def combine_kernel(n, heads, hd, q_rows, mine_ref, rows_ref, out_ref, lse_ref, theirs_ref, packed_ref, got_ref, send_sem, recv_sem):
    me = lax.axis_index('seq')
    part = lax.rem(me, n // heads)
    partner, peers = pair_peers(n, heads, me, part)
    meet(peers)
    swap(mine_ref, theirs_ref, send_sem.at[0], recv_sem.at[0], partner)
    m_a, m_b = mine_ref[hd + 8:hd + 9], theirs_ref[hd + 8:hd + 9]
    top = jnp.maximum(m_a, m_b)
    s_a, s_b = jnp.exp2(m_a - top), jnp.exp2(m_b - top)
    den = mine_ref[hd:hd + 1] * s_a + theirs_ref[hd:hd + 1] * s_b
    out = (mine_ref[:hd] * s_a + theirs_ref[:hd] * s_b) / den
    out_ref[...] = out
    lse_ref[...] = top + jnp.log2(den)
    to_rows(n, heads, q_rows, me, part, out, packed_ref, got_ref, rows_ref, send_sem.at[1], recv_sem.at[1])


def pair_scratch(n, heads, hd, q_rows, mine):
    return [pltpu.VMEM(mine.shape, F32), pltpu.VMEM((n, q_rows // 2, 2 * hd), BF16), pltpu.VMEM((heads, q_rows // 2, 2 * hd), BF16),
            pltpu.SemaphoreType.DMA((2,)), pltpu.SemaphoreType.DMA((2,))]


def combine(n, heads, hd, q_rows, collective_id, mine):
    total_q = mine.shape[1]
    return pl.pallas_call(
        functools.partial(combine_kernel, n, heads, hd, q_rows),
        out_shape=[shape((heads, q_rows, hd), BF16), shape((hd, total_q), F32), shape((1, total_q), F32)],
        in_specs=vmem(1),
        out_specs=vmem(3),
        scratch_shapes=pair_scratch(n, heads, hd, q_rows, mine),
        compiler_params=remote(collective_id),
        name='combine',
    )(mine)


def small_sum_kernel(n, mine_ref, total_ref, all_ref, send_sem, recv_sem):
    me = lax.axis_index('seq')
    meet([lax.rem(me + step, n) for step in range(1, n)])
    for step in range(1, n):
        send(mine_ref, all_ref.at[me], send_sem, recv_sem, lax.rem(me + step, n)).start()
    all_ref[me] = mine_ref[...]
    others = all_ref.at[pl.ds(0, n - 1)]
    whole = send(others, others, send_sem, recv_sem, me)
    whole.wait_send()
    whole.wait_recv()
    total_ref[...] = jnp.sum(all_ref[...], axis=0)


def small_sum(n, collective_id, mine):
    return pl.pallas_call(
        functools.partial(small_sum_kernel, n),
        out_shape=shape(mine.shape, F32),
        in_specs=vmem(1),
        out_specs=vmem(1)[0],
        scratch_shapes=[pltpu.VMEM((n,) + mine.shape, F32), pltpu.SemaphoreType.DMA, pltpu.SemaphoreType.DMA],
        compiler_params=remote(collective_id),
        name='small_sum',
    )(mine)


def forward_kernel(scale, hd, q_block, bounds_ref, kv_ref, q_ref, out_ref, qt_ref, top_ref):
    blocks, last_valid = bounds_ref[0], bounds_ref[1]
    rows, total_q = kv_ref.shape[1], q_ref.shape[0]
    groups = [slice(first, first + q_block) for first in range(0, total_q, q_block)]
    base = slice(hd + 8, hd + 9)
    qt_ref[...] = q_ref[...].T

    def values_of(keys):
        return jnp.concatenate([keys.T[hd:], jnp.ones((16, rows), keys.dtype)], axis=0)

    def group_of(index):
        return pl.ds(pl.multiple_of(index * q_block, q_block), q_block)

    def first_step(group, carry):
        cols = group_of(group)
        top = jnp.max(dot(kv_ref[0], qt_ref[:, cols]), axis=0, keepdims=True)
        out_ref[hd + 8:, cols] = jnp.broadcast_to(top * scale, (8, q_block))
        top_ref[:, cols] = jnp.broadcast_to(top, (8, q_block))
        return carry

    lax.fori_loop(0, len(groups), first_step, 0)
    out_ref[:hd + 8, :] = jnp.zeros((hd + 8, total_q), F32)

    def finish(values, scores, cols):
        top_ref[:, cols] = jnp.maximum(top_ref[:, cols], jnp.max(scores.reshape(rows // 8, 8, q_block), axis=0))
        weights = jnp.exp2(scores * scale - out_ref[base, cols]).astype(values.dtype)
        out_ref[:hd + 8, cols] += dot(values, weights)[:hd + 8]

    def step(index, carry):
        keys = kv_ref[index]
        values = values_of(keys)
        for cols in groups:
            finish(values, dot(keys, qt_ref[:, cols]), cols)
        return carry

    def last_step(group, carry):
        cols = group_of(group)
        keys = kv_ref[blocks - 1]
        scores = dot(keys, qt_ref[:, cols])
        position = lax.broadcasted_iota(jnp.int32, scores.shape, 0)
        finish(values_of(keys), jnp.where(position < last_valid, scores, NEG), cols)
        return carry

    lax.fori_loop(0, blocks - 1, step, 0)
    lax.fori_loop(0, len(groups), last_step, 0)

    excess = jnp.max(top_ref[...] * scale - out_ref[hd + 8:, :])

    @pl.when(excess > 16.0)
    def _():
        out_ref[:hd + 8, :] = jnp.zeros((hd + 8, total_q), F32)
        out_ref[hd + 8:, :] = jnp.full((8, total_q), NEG, F32)

        def running(step_index, carry):
            index, group = step_index // len(groups), lax.rem(step_index, len(groups))
            cols = group_of(group)
            keys = kv_ref[index]
            limit = jnp.where(index == blocks - 1, last_valid, rows)
            scores = dot(keys, qt_ref[:, cols]) * scale
            position = lax.broadcasted_iota(jnp.int32, scores.shape, 0)
            scores = jnp.where(position < limit, scores, NEG)
            old = out_ref[base, cols]
            new = jnp.maximum(old, jnp.max(scores, axis=0, keepdims=True))
            weights = jnp.exp2(scores - new).astype(keys.dtype)
            out_ref[:hd + 8, cols] = out_ref[:hd + 8, cols] * jnp.exp2(old - new) + dot(values_of(keys), weights)[:hd + 8]
            out_ref[hd + 8:, cols] = jnp.broadcast_to(new, (8, q_block))
            return carry

        lax.fori_loop(0, blocks * len(groups), running, 0)


def attention_forward(scale, hd, sources, bounds, kv, q):
    rows, width = kv.shape[1], kv.shape[2]
    total_q = q.shape[0]
    return pl.pallas_call(
        functools.partial(forward_kernel, scale, hd, min(1024, total_q)),
        out_shape=shape((hd + 16, total_q), F32),
        grid=(1,),
        in_specs=[pl.BlockSpec(memory_space=pltpu.SMEM),
                  pl.BlockSpec((sources, rows, width), lambda i: (0, 0, 0), pipeline_mode=pl.Buffered(1)), full(q)],
        out_specs=pl.BlockSpec((hd + 16, total_q), lambda i: (0, 0)),
        scratch_shapes=[pltpu.VMEM((width, total_q), BF16), pltpu.VMEM((8, total_q), F32)],
        compiler_params=plain(),
        cost_estimate=pl.CostEstimate(flops=4 * total_q * sources * rows * hd, bytes_accessed=kv.size * 2,
                                      transcendentals=total_q * sources * rows),
        name='attention_forward',
    )(bounds, kv, q)


def backward_kernel(scale, key_scale, hd, q_block, bounds_ref, kv_ref, q_ref, do_ref, out_ref, lse_ref, dkv_ref, dq_ref,
                    qt_ref, dot_ref, delta_ref):
    blocks, last_valid = bounds_ref[0], bounds_ref[1]
    rows, total_q = kv_ref.shape[1], q_ref.shape[0]
    width = kv_ref.shape[2]
    groups = [slice(first, first + q_block) for first in range(0, total_q, q_block)]
    dq_ref[...] = jnp.zeros_like(dq_ref)
    qt_ref[...] = q_ref[...].T
    do_t = do_ref[...].T
    dot_ref[...] = do_t
    delta_ref[...] = jnp.sum(do_t[hd:].astype(F32) * out_ref[...], axis=0, keepdims=True)

    lane_scale = jnp.where(lax.broadcasted_iota(jnp.int32, (1, width), 1) < hd, key_scale, 1.0)

    def products(keys, cols):
        return dot(keys, qt_ref[:, cols]), dot(keys, dot_ref[:, cols])

    def finish(keys, keys_t, scores, grads, cols, valid):
        prob = jnp.exp2(scores * scale - lse_ref[:, cols])
        if valid is not None:
            position = lax.broadcasted_iota(jnp.int32, scores.shape, 0)
            prob = jnp.where(position < valid, prob, 0.0)
        grad_scores = (prob * (grads - delta_ref[:, cols])).astype(keys.dtype)
        update = dot(grad_scores, q_ref[cols, :]) + dot(prob.astype(keys.dtype), do_ref[cols, :])
        dq_ref[:, cols] += dot(keys_t, grad_scores)
        return update

    def step(index, carry):
        keys = kv_ref[index]
        keys_t = keys.T[:hd]
        total = jnp.zeros((rows, width), F32)
        for cols in groups:
            scores, grads = products(keys, cols)
            total += finish(keys, keys_t, scores, grads, cols, None)
        dkv_ref[index] = (total * lane_scale).astype(dkv_ref.dtype)
        return carry

    def last_step(group, total):
        keys = kv_ref[blocks - 1]
        cols = pl.ds(pl.multiple_of(group * q_block, q_block), q_block)
        scores, grads = products(keys, cols)
        return total + finish(keys, keys.T[:hd], scores, grads, cols, last_valid)

    def clear(index, carry):
        dkv_ref[index] = jnp.zeros((rows, width), dkv_ref.dtype)
        return carry

    lax.fori_loop(0, blocks - 1, step, 0)
    total = lax.fori_loop(0, len(groups), last_step, jnp.zeros((rows, width), F32))
    dkv_ref[blocks - 1] = (total * lane_scale).astype(dkv_ref.dtype)
    lax.fori_loop(blocks, dkv_ref.shape[0], clear, 0)
    dq_ref[...] = dq_ref[...] * key_scale


def attention_backward(scale, key_scale, hd, sources, bounds, kv, q, do, out_t, lse):
    n, rows, width = kv.shape
    total_q = q.shape[0]
    return pl.pallas_call(
        functools.partial(backward_kernel, scale, key_scale, hd, min(512, total_q)),
        out_shape=[shape((n, rows, width), BF16), shape((hd, total_q), F32)],
        grid=(1,),
        in_specs=[pl.BlockSpec(memory_space=pltpu.SMEM),
                  pl.BlockSpec((sources, rows, width), lambda i: (0, 0, 0), pipeline_mode=pl.Buffered(1)),
                  full(q), full(do), full(out_t), full(lse)],
        out_specs=[pl.BlockSpec((n, rows, width), lambda i: (0, 0, 0)),
                   pl.BlockSpec((hd, total_q), lambda i: (0, 0))],
        scratch_shapes=[pltpu.VMEM((width, total_q), BF16), pltpu.VMEM((width, total_q), BF16), pltpu.VMEM((1, total_q), F32)],
        compiler_params=plain(),
        cost_estimate=pl.CostEstimate(flops=10 * total_q * sources * rows * hd, bytes_accessed=kv.size * 4,
                                      transcendentals=total_q * sources * rows),
        name='attention_backward',
    )(bounds, kv, q, do, out_t, lse)


def prepare_kernel(dec_ref, att_ref, wo_ref, gain_ref, n2_ref, n2t_ref):
    hidden = (dec_ref[...].astype(F32) + dot(att_ref[...], wo_ref[...])).astype(BF16)
    normed = rms_norm(hidden.astype(F32), gain_ref[...].astype(F32)).astype(BF16)
    n2_ref[...] = normed
    n2t_ref[...] = normed.T


def prepare(gathered, wo, gain):
    rows, dim = gathered.shape[0], wo.shape[1]
    chunk = min(512, rows)
    left = pl.BlockSpec((chunk, dim), lambda i: (i, 0))
    return pl.pallas_call(
        prepare_kernel,
        out_shape=[shape((rows, dim), BF16), shape((dim, rows), BF16)],
        grid=(rows // chunk,),
        in_specs=[pl.BlockSpec((chunk, dim), lambda i: (i, 2)), left, full(wo), full(gain)],
        out_specs=[left, pl.BlockSpec((dim, chunk), lambda i: (0, i))],
        compiler_params=plain(),
        cost_estimate=pl.CostEstimate(flops=2 * rows * dim * dim, bytes_accessed=8 * rows * dim, transcendentals=0),
        name='prepare',
    )(gathered, gathered, wo, gain)


def mlp_kernel(chunk, n2_ref, n2t_ref, top_ref, w1_ref, w3_ref, w2_ref, g1_ref, g3_ref, g2_ref, d1_ref, d3_ref, act_ref):
    rows = n2_ref.shape[0]
    w1, w3, w2t = w1_ref[...], w3_ref[...], w2_ref[...].T
    for first in range(0, rows, chunk):
        part = slice(first, first + chunk)
        gate = dot(n2_ref[part, :], w1)
        up = dot(n2_ref[part, :], w3)
        grad = dot(top_ref[part, :], w2t)
        sig = jax.nn.sigmoid(gate)
        silu = gate * sig
        act_ref[part, :] = (silu * up).astype(act_ref.dtype)
        d3_ref[part, :] = (grad * silu).astype(d3_ref.dtype)
        d1_ref[part, :] = (grad * up * (sig + silu * (1.0 - sig))).astype(d1_ref.dtype)
    g1_ref[...] = dot(n2t_ref[...], d1_ref[...])
    g3_ref[...] = dot(n2t_ref[...], d3_ref[...])
    g2_ref[...] = dot_tn(act_ref[...], top_ref[...])


def mlp_weight_grads(n2, n2t, gathered, w_gate, w_up, w_down):
    rows, dim = n2.shape
    ff = w_gate.shape[1]
    tile = 256
    cols = pl.BlockSpec((dim, tile), lambda i: (0, i))
    tall = pl.BlockSpec((tile, dim), lambda i: (i, 0))
    return pl.pallas_call(
        functools.partial(mlp_kernel, min(512, rows)),
        out_shape=[shape((dim, ff), F32), shape((dim, ff), F32), shape((ff, dim), F32)],
        grid=(ff // tile,),
        in_specs=[full(n2), full(n2t), pl.BlockSpec((rows, dim), lambda i: (0, 3), pipeline_mode=pl.Buffered(1)), cols, cols, tall],
        out_specs=[cols, cols, tall],
        scratch_shapes=[pltpu.VMEM((rows, tile), BF16)] * 3,
        compiler_params=plain(),
        cost_estimate=pl.CostEstimate(flops=12 * rows * dim * ff, bytes_accessed=18 * dim * ff, transcendentals=rows * ff),
        name='mlp_weight_grads',
    )(n2, n2t, gathered, w_gate, w_up, w_down)


def memory_weight_kernel(memory_ref, dkv_ref, dec_ref, gain_ref, dq_ref, gk_ref, gv_ref, gq_ref):
    group, hd = dkv_ref.shape[0], dkv_ref.shape[2] // 2
    normed = rms_norm(dec_ref[...].astype(F32), gain_ref[...].astype(F32)).astype(BF16)
    for i in range(group):
        rows = slice(i * hd, (i + 1) * hd)
        both = dot_tn(dkv_ref[i], memory_ref[...])
        gk_ref[rows, :] = both[:hd]
        gv_ref[rows, :] = both[hd:]
        gq_ref[rows, :] = dot_tn(dq_ref[i], normed)


def memory_weight_grads(memory, dkv, dec_in, gain, dq_rows):
    heads, rows, width = dkv.shape
    dim, hd = memory.shape[1], width // 2
    group = 4
    out = pl.BlockSpec((group * hd, dim), lambda i: (i, 0))
    return pl.pallas_call(
        memory_weight_kernel,
        out_shape=[shape((heads * hd, dim), F32)] * 3,
        grid=(heads // group,),
        in_specs=[full(memory), pl.BlockSpec((group, rows, width), lambda i: (i, 0, 0)), full(dec_in), full(gain),
                  pl.BlockSpec((group,) + dq_rows.shape[1:], lambda i: (i, 0, 0))],
        out_specs=[out, out, out],
        compiler_params=plain(),
        cost_estimate=pl.CostEstimate(flops=2 * rows * dim * heads * width, bytes_accessed=16 * rows * dim, transcendentals=0),
        name='memory_weight_grads',
    )(memory, dkv, dec_in, gain, dq_rows)


def memory_grad_kernel(dkv_ref, wk_ref, wv_ref, out_ref):
    group = dkv_ref.shape[0]
    left = jnp.concatenate([dkv_ref[i] for i in range(group)], axis=1)
    right = jnp.concatenate([part[i] for i in range(group) for part in (wk_ref, wv_ref)], axis=0)

    @pl.when(pl.program_id(0) == 0)
    def _():
        out_ref[...] = dot(left, right)

    @pl.when(pl.program_id(0) > 0)
    def _():
        out_ref[...] += dot(left, right)


def memory_grad(dkv, wk_t, wv_t):
    heads, rows, width = dkv.shape
    hd, dim = wk_t.shape[1], wk_t.shape[2]
    group = 4
    weight = pl.BlockSpec((group, hd, dim), lambda i: (i, 0, 0))
    return pl.pallas_call(
        memory_grad_kernel,
        out_shape=shape((rows, dim), F32),
        grid=(heads // group,),
        in_specs=[pl.BlockSpec((group, rows, width), lambda i: (i, 0, 0)), weight, weight],
        out_specs=pl.BlockSpec((rows, dim), lambda i: (0, 0)),
        compiler_params=plain(),
        cost_estimate=pl.CostEstimate(flops=2 * rows * dim * heads * width, bytes_accessed=12 * rows * dim, transcendentals=0),
        name='memory_grad',
    )(dkv, wk_t, wv_t)


def outer_kernel(att_ref, gh_ref, out_ref):
    @pl.when(pl.program_id(0) == 0)
    def _():
        out_ref[...] = jnp.zeros_like(out_ref)

    out_ref[...] += dot_tn(att_ref[...], gh_ref[...])


def outer_weight_grad(gathered, dim):
    rows = gathered.shape[0]
    chunk = min(512, rows)
    return pl.pallas_call(
        outer_kernel,
        out_shape=shape((dim, dim), F32),
        grid=(rows // chunk,),
        in_specs=[pl.BlockSpec((chunk, dim), lambda i: (i, 0)), pl.BlockSpec((chunk, dim), lambda i: (i, 1))],
        out_specs=pl.BlockSpec((dim, dim), lambda i: (0, 0)),
        compiler_params=plain(),
        cost_estimate=pl.CostEstimate(flops=2 * rows * dim * dim, bytes_accessed=8 * rows * dim, transcendentals=0),
        name='outer_weight_grad',
    )(gathered, gathered)


def solution(mesh):
    n = mesh.shape['seq']
    row_spec = P(('data', 'seq'), None)
    weight_spec = P()
    part_vec = P('data')
    part_mat = P('data', None)
    part_cube = P('data', None, None)

    def device_step(dec_in, memory, mem_len, grad_out, norm_attn, wq_cross, wk_cross, wv_cross, wo_cross, norm_mlp, w_gate, w_up, w_down):
        q_rows, dim = dec_in.shape
        m_rows = memory.shape[0]
        heads, hd = wq_cross.shape[1], wq_cross.shape[2]
        parts = n // heads
        half = m_rows // parts
        sources = -(-3 * n // 4)
        total_q = q_rows * n
        key_scale = hd ** -0.5
        scale = key_scale * LOG2E
        me = lax.axis_index('seq')
        part = lax.rem(me, parts)

        reach = mem_len[0] - part * half
        blocks = jnp.minimum((reach + m_rows - 1) // m_rows, sources)
        bounds = jnp.stack([blocks, jnp.minimum(reach - (blocks - 1) * m_rows, half)]).astype(jnp.int32)

        wq_t, wk_t, wv_t = (jnp.transpose(w, (1, 2, 0)) for w in (wq_cross, wk_cross, wv_cross))
        gain_attn, gain_mlp = norm_attn.reshape(1, dim), norm_mlp.reshape(1, dim)
        source_rows = -(-sources // (parts * math.isqrt(heads)))
        kv, q_in = exchange(n, heads, source_rows, 0, memory, dec_in, gain_attn, wk_t, wv_t, wq_t)
        head_q = q_in.reshape(total_q, 2 * hd)

        grad_top = grad_out.astype(BF16)
        mine = attention_forward(scale, hd, sources, bounds, kv, head_q)
        attended, out_t, lse = combine(n, heads, hd, q_rows, 1, mine)

        x_in = dec_in.astype(F32)
        hidden_f = x_in + jnp.einsum('hqe,hed->qd', attended, wo_cross, preferred_element_type=F32)
        hidden = hidden_f.astype(BF16)
        normed_mlp_f, mlp_norm_pull = jax.vjp(rms_norm, hidden.astype(F32), norm_mlp.astype(F32))
        normed_mlp = normed_mlp_f.astype(BF16)
        gate_pre = jnp.dot(normed_mlp, w_gate, preferred_element_type=F32)
        up_pre = jnp.dot(normed_mlp, w_up, preferred_element_type=F32)
        _, gated_pull = jax.vjp(gated_unit, gate_pre, up_pre)
        grad_act = jnp.einsum('qd,fd->qf', grad_top, w_down, preferred_element_type=F32)
        grad_gate, grad_up = gated_pull(grad_act)
        grad_normed_mlp = (jnp.einsum('qf,df->qd', grad_gate.astype(BF16), w_gate, preferred_element_type=F32)
                           + jnp.einsum('qf,df->qd', grad_up.astype(BF16), w_up, preferred_element_type=F32))
        grad_hidden_norm, g_norm_mlp = mlp_norm_pull(grad_normed_mlp)
        grad_hidden = grad_out + grad_hidden_norm
        grad_hidden_b = grad_hidden.astype(BF16)
        grad_att = jnp.einsum('qd,hed->hqe', grad_hidden_b, wo_cross, preferred_element_type=F32).astype(BF16)
        head_do = to_heads(n, heads, 2, grad_att).reshape(total_q, 2 * hd)

        factors = jnp.concatenate([attended.transpose(1, 0, 2).reshape(q_rows, heads * hd), grad_hidden_b, dec_in, grad_top], axis=1)
        head_do, factors = lax.optimization_barrier((head_do, factors))
        gathered = lax.all_gather(factors, 'seq', axis=0, tiled=True)

        dkv, dq_part = attention_backward(scale, key_scale, hd, sources, bounds, kv, head_q, head_do, out_t, lse)
        dkv_in, dq_rows = return_blocks(n, heads, source_rows, 4, dkv, dq_part)
        dkv_in, dq_rows, gathered = lax.optimization_barrier((dkv_in, dq_rows, gathered))

        sums = memory_weight_grads(memory, dkv_in, dec_in, gain_attn, dq_rows)
        *sums, dkv_in, dq_rows, gathered = lax.optimization_barrier((*sums, dkv_in, dq_rows, gathered))
        g_wk, g_wv, g_wq = lax.psum(tuple(sums), 'seq')

        n2_all, n2_all_t = prepare(gathered, wo_cross.reshape(heads * hd, dim), gain_mlp)
        g_gate, g_up, g_down = mlp_weight_grads(n2_all, n2_all_t, gathered, w_gate, w_up, w_down)
        g_wo = outer_weight_grad(gathered, dim)

        grad_normed = jnp.einsum('hte,dhe->td', dq_rows, wq_cross, preferred_element_type=F32)
        _, norm_pull = jax.vjp(rms_norm, x_in, norm_attn.astype(F32))
        grad_x_norm, g_norm_attn = norm_pull(grad_normed)
        g_dec = grad_hidden + grad_x_norm
        norms = small_sum(n, 5, jnp.concatenate([g_norm_attn, g_norm_mlp]).reshape(-1, 128)).reshape(2, dim)
        g_mem = memory_grad(dkv_in, wk_t, wv_t)
        cube = lambda g: jnp.transpose(g.reshape(heads, hd, dim), (2, 0, 1))
        return (g_dec, g_mem, norms[0], cube(g_wq), cube(g_wk), cube(g_wv), g_wo.reshape(heads, hd, dim), norms[1], g_gate, g_up, g_down)

    return jax.shard_map(device_step, mesh=mesh,
                         in_specs=(row_spec, row_spec, part_vec, row_spec) + (weight_spec,) * 9,
                         out_specs=(row_spec, row_spec, part_vec, part_cube, part_cube, part_cube, part_cube, part_vec, part_mat, part_mat, part_mat),
                         check_vma=False)
```

```python
import functools
import math

import jax
import jax.numpy as jnp
from jax import lax
from jax.experimental import pallas as pl
from jax.experimental.pallas import tpu as pltpu
from jax.sharding import PartitionSpec as P

LOG2E = 1.4426950408889634
NEG = -1e30
VMEM_LIMIT = 60 * 1024 * 1024
MESH = pl.DeviceIdType.MESH
BF16, F32 = jnp.bfloat16, jnp.float32


def rms_norm(tensor, gain):
    mean_sq = jnp.mean(tensor * tensor, axis=-1, keepdims=True)
    return tensor * lax.rsqrt(mean_sq + 1e-6) * gain


def dot(a, b):
    return jnp.dot(a, b, preferred_element_type=F32)


def dot_nt(a, b):
    return lax.dot_general(a, b, (((1,), (1,)), ((), ())), preferred_element_type=F32)


def dot_tn(a, b):
    return lax.dot_general(a, b, (((0,), (0,)), ((), ())), preferred_element_type=F32)


def full(array):
    return pl.BlockSpec(array.shape, lambda *_: (0,) * array.ndim, pipeline_mode=pl.Buffered(1))


def vmem(count):
    return [pl.BlockSpec(memory_space=pltpu.VMEM)] * count


def plain():
    return pltpu.CompilerParams(vmem_limit_bytes=VMEM_LIMIT)


def remote(collective_id):
    return pltpu.CompilerParams(collective_id=collective_id, has_side_effects=True, vmem_limit_bytes=VMEM_LIMIT)


def shape(dims, dtype):
    return jax.ShapeDtypeStruct(dims, dtype)


def meet(peers):
    barrier = pltpu.get_barrier_semaphore()
    for peer in peers:
        pl.semaphore_signal(barrier, inc=1, device_id={'seq': peer}, device_id_type=MESH)
    pl.semaphore_wait(barrier, len(peers))


def send(src, dst, send_sem, recv_sem, peer):
    return pltpu.make_async_remote_copy(src_ref=src, dst_ref=dst, send_sem=send_sem, recv_sem=recv_sem,
                                        device_id={'seq': peer}, device_id_type=MESH)


class Grid:
    def __init__(self, n, heads, source_rows):
        self.n, self.heads, self.source_rows = n, heads, source_rows
        self.parts = n // heads
        self.side = math.isqrt(heads)
        self.me = lax.axis_index('seq')
        self.part = lax.rem(self.me, self.parts)
        self.chip = self.me // self.parts
        self.col = lax.rem(self.chip, self.side)
        self.row = self.chip // self.side
        self.partner = self.chip * self.parts + (self.parts - 1 - self.part)
        self.ties = self.side == 4
        self.direct = (1, 3) if self.ties else (1,)

    def wrap(self, value):
        return lax.rem(value + self.side, self.side)

    def device(self, row, col, part):
        return (row * self.side + col) * self.parts + part

    def near(self, drow, dcol, part=None):
        return self.device(self.wrap(self.row + drow), self.wrap(self.col + dcol), self.part if part is None else part)

    def hop(self, offset):
        return 1 if offset == 1 else -1

    def is_source(self, row):
        return self.wrap(row) < self.source_rows

    def row_peers(self):
        return [lax.rem(self.chip + step, self.heads) * self.parts + self.part for step in range(1, self.heads)]

    def peers(self):
        return self.row_peers() + [self.partner] + [self.near(0, self.hop(d), self.parts - 1 - self.part) for d in self.direct]


def pair_peers(n, heads, me, part):
    parts = n // heads
    head = me // parts
    partner = head * parts + (parts - 1 - part)
    return partner, [partner] + [lax.rem(head + step, heads) * parts + part for step in range(1, heads)]


def pack(rows):
    middle = rows.shape[-2] // 2
    return jnp.concatenate([rows[..., :middle, :], rows[..., middle:, :]], axis=-1)


def unpack(packed):
    middle = packed.shape[-1] // 2
    return jnp.concatenate([packed[..., :middle], packed[..., middle:]], axis=-2)


def start_rows(n, heads, me, part, src, src_of, dst_ref, send_sem, recv_sem):
    parts = n // heads
    head = me // parts
    for step in range(1, heads):
        peer = lax.rem(head + step, heads) * parts + part
        send(src.at[src_of(peer)], dst_ref.at[head], send_sem, recv_sem, peer).start()
    dst_ref[head] = src[src_of(me)]


def wait_rows(heads, me, dst_ref, send_sem, recv_sem):
    others = dst_ref.at[pl.ds(0, heads - 1)]
    whole = send(others, others, send_sem, recv_sem, me)
    whole.wait_send()
    whole.wait_recv()


def swap(src, dst, send_sem, recv_sem, partner):
    copy = send(src, dst, send_sem, recv_sem, partner)
    copy.start()
    copy.wait()


def place(n, heads, part, mine_ref, theirs_ref, wide_ref, low):
    parts = n // heads
    for source, index in ((mine_ref, part), (theirs_ref, parts - 1 - part)):
        for head in range(heads):
            rows = unpack(source[head])
            zeros = jnp.zeros_like(rows)
            wide_ref[head * parts + index] = jnp.concatenate([rows, zeros] if low else [zeros, rows], axis=-1)


def exchange_kernel(n, heads, source_rows, memory_ref, dec_ref, gain_ref, wk_ref, wv_ref, wq_ref, kv_out_ref, q_out_ref,
                    kv_ref, stage_ref, up_ref, down_ref, right_ref, left_ref, packed_ref, got_ref, swapped_ref,
                    row_send, row_recv, y_send, pass_send, x_send, fwd_send, stage_recv, up_recv, down_recv, right_recv,
                    left_recv, out_recv):
    g = Grid(n, heads, source_rows)
    side, hd = g.side, wk_ref.shape[1]
    half = kv_out_ref.shape[1]
    chunk_rows = min(256, kv_ref.shape[1])
    barrier = pltpu.get_barrier_semaphore()
    peers = g.peers()
    for peer in peers:
        pl.semaphore_signal(barrier, inc=1, device_id={'seq': peer}, device_id_type=MESH)

    normed = rms_norm(dec_ref[...].astype(F32), gain_ref[...].astype(F32)).astype(BF16)
    for i in range(0, heads, 4):
        queries = dot_nt(normed, jnp.concatenate([wq_ref[i + j] for j in range(4)], axis=0)).astype(BF16)
        for j in range(4):
            packed_ref[i + j] = pack(queries[:, hd * j:hd * (j + 1)])

    def head(drow, dcol):
        return g.wrap(g.row + drow) * side + g.wrap(g.col + dcol)

    def project(drow, dcols):
        weights = jnp.concatenate([ref[head(drow, d)] for d in dcols for ref in (wk_ref, wv_ref)], axis=0)

        def rows(index, carry):
            at = pl.ds(pl.multiple_of(index * chunk_rows, chunk_rows), chunk_rows)
            both = dot_nt(memory_ref[at, :], weights).astype(BF16)
            for i, d in enumerate(dcols):
                kv_ref[head(drow, d), at, :] = both[:, 2 * hd * i:2 * hd * (i + 1)]
            return carry

        lax.fori_loop(0, kv_ref.shape[1] // chunk_rows, rows, 0)

    def along_column(drow, dcol):
        chunk = kv_ref.at[head(drow, dcol)]
        if drow in g.direct:
            send(chunk, stage_ref.at[drow - 1, dcol], y_send.at[drow - 1], stage_recv.at[drow - 1, dcol], g.near(g.hop(drow), 0)).start()
        elif dcol % 2 == 0:
            send(chunk, up_ref.at[dcol // 2], y_send.at[drow - 1], up_recv.at[dcol // 2], g.near(1, 0)).start()
        else:
            send(chunk, down_ref.at[dcol // 2], y_send.at[drow - 1], down_recv.at[dcol // 2], g.near(-1, 0)).start()

    def along_row(o, dcol):
        chunk = kv_ref.at[head(0, dcol)] if o == 0 else stage_ref.at[o - 1, dcol]
        source = g.device(g.wrap(g.row - o), g.col, g.part)
        if dcol == 0:
            kv_out_ref[source] = chunk[pl.ds(pl.multiple_of(g.part * half, half), half), :]
            away = pl.ds(pl.multiple_of((g.parts - 1 - g.part) * half, half), half)
            send(chunk.at[away], kv_out_ref.at[source], x_send.at[o], out_recv, g.partner).start()
        elif dcol in g.direct:
            for part in range(g.parts):
                send(chunk.at[pl.ds(part * half, half)], kv_out_ref.at[source], x_send.at[o], out_recv,
                     g.near(0, g.hop(dcol), part)).start()
        else:
            send(chunk.at[pl.ds(0, half)], right_ref.at[o], x_send.at[o], right_recv.at[o], g.near(0, 1)).start()
            send(chunk.at[pl.ds(half, half)], left_ref.at[o], x_send.at[o], left_recv.at[o], g.near(0, -1)).start()

    def pass_row(o):
        for ref, sem, come in ((right_ref, right_recv, -1), (left_ref, left_recv, 1)):
            source = g.device(g.wrap(g.row - o), g.wrap(g.col + come), g.part)
            send(ref.at[o], ref.at[o], fwd_send.at[o], sem.at[o], g.me).wait_recv()
            send(ref.at[o], kv_out_ref.at[source], fwd_send.at[o], out_recv, g.near(0, -come, 0 if come < 0 else 1)).start()

    def when_source(row, body):
        pl.when(g.is_source(row))(body)

    if g.ties:
        order = [(2, (2, 1)), (2, (3, 0)), (1, (2, 1)), (3, (2, 1)), (0, (2, 1)), (0, (3, 0))]
        last = [(1, (3, 0)), (3, (3, 0))]
    else:
        order, last = [(1, (1, 0)), (0, (1, 0))], []

    def issue(drow, dcols):
        def body():
            for d in dcols:
                along_row(0, d) if drow == 0 else along_column(drow, d)
        when_source(g.row, body)

    waiting = None
    for drow, dcols in order + last:
        project(drow, dcols)
        if waiting is None:
            pl.semaphore_wait(barrier, len(peers))
            start_rows(n, heads, g.me, g.part, packed_ref, lambda peer: peer // g.parts, got_ref, row_send.at[0], row_recv.at[0])
        elif waiting not in last:
            issue(*waiting)
        waiting = (drow, dcols)
    if not last:
        issue(*waiting)

    if g.ties:
        def up(i):
            send(up_ref.at[i], up_ref.at[i], pass_send.at[0], up_recv.at[i], g.me).wait_recv()
            send(up_ref.at[i], stage_ref.at[1, 2 * i], pass_send.at[0], stage_recv.at[1, 2 * i], g.near(1, 0)).start()

        def down(i):
            send(down_ref.at[i], down_ref.at[i], pass_send.at[1], down_recv.at[i], g.me).wait_recv()
            send(down_ref.at[i], stage_ref.at[1, 2 * i + 1], pass_send.at[1], stage_recv.at[1, 2 * i + 1], g.near(-1, 0)).start()

        for i in range(2):
            when_source(g.row - 1, lambda i=i: up(1 - i))
            when_source(g.row + 1, lambda i=i: down(i))
        for drow, dcols in last:
            issue(drow, dcols)
        when_source(g.row, lambda: pass_row(0))

    wait_rows(heads, g.me, got_ref, row_send.at[0], row_recv.at[0])
    swap(got_ref, swapped_ref, row_send.at[1], row_recv.at[1], g.partner)
    place(n, heads, g.part, got_ref, swapped_ref, q_out_ref, True)

    def arrived(o, dcol):
        def body():
            send(stage_ref.at[o - 1, dcol], stage_ref.at[o - 1, dcol], y_send.at[0], stage_recv.at[o - 1, dcol], g.me).wait_recv()
            along_row(o, dcol)
        when_source(g.row - o, body)

    if g.ties:
        for d in (2, 1):
            for o in g.direct:
                arrived(o, d)
        for o in g.direct:
            when_source(g.row - o, lambda o=o: pass_row(o))
        for d in (2, 1, 0, 3):
            arrived(2, d)
        when_source(g.row - 2, lambda: pass_row(2))
        for d in (3, 0):
            for o in g.direct:
                arrived(o, d)
    else:
        for d in (1, 0):
            arrived(1, d)

    def sent(sem, ref):
        send(ref, ref, sem, out_recv, g.me).wait_send()

    def mine():
        for drow in range(1, side):
            sent(y_send.at[drow - 1], stage_ref.at[0])
    when_source(g.row, mine)
    for o in range(side):
        def passed(o=o):
            sent(x_send.at[o], kv_out_ref.at[pl.ds(0, g.parts * side - 1)])
            if g.ties:
                sent(fwd_send.at[o], kv_out_ref.at[pl.ds(0, 2)])
        when_source(g.row - o, passed)
    if g.ties:
        when_source(g.row - 1, lambda: sent(pass_send.at[0], up_ref))
        when_source(g.row + 1, lambda: sent(pass_send.at[1], down_ref))
    blocks = source_rows * side * g.parts
    others = kv_out_ref.at[pl.ds(0, blocks - source_rows)]
    send(others, others, y_send.at[0], out_recv, g.me).wait_recv()


def row_scratch(heads, q_rows, hd):
    return [pltpu.VMEM((heads, q_rows // 2, 2 * hd), BF16)] * 3


def dma(*dims):
    return pltpu.SemaphoreType.DMA(dims)


def exchange(n, heads, source_rows, collective_id, memory, dec_in, gain, wk_t, wv_t, wq_t):
    m_rows, q_rows, hd = memory.shape[0], dec_in.shape[0], wk_t.shape[1]
    side, parts = math.isqrt(heads), n // heads
    half = m_rows // parts
    chunk = lambda *lead: pltpu.VMEM(lead + (m_rows, 2 * hd), BF16)
    block = lambda *lead: pltpu.VMEM(lead + (half, 2 * hd), BF16)
    return pl.pallas_call(
        functools.partial(exchange_kernel, n, heads, source_rows),
        out_shape=[shape((n, half, 2 * hd), BF16), shape((n, q_rows, 2 * hd), BF16)],
        in_specs=vmem(6),
        out_specs=vmem(2),
        scratch_shapes=[chunk(heads), chunk(side - 1, side), chunk(2), chunk(2), block(side), block(side)]
        + row_scratch(heads, q_rows, hd)
        + [dma(2), dma(2), dma(side - 1), dma(2), dma(side), dma(side), dma(side - 1, side), dma(2), dma(2), dma(side), dma(side),
           pltpu.SemaphoreType.DMA],
        compiler_params=remote(collective_id),
        name='exchange',
    )(memory, dec_in, gain, wk_t, wv_t, wq_t)


def return_kernel(n, heads, source_rows, src_ref, dq_ref, dst_ref, rows_ref, stage_ref, right_ref, left_ref, up_ref, down_ref,
                  theirs_ref, packed_ref, got_ref, row_send, row_recv,
                  x_send, fwd_send, y_send, pass_send, stage_recv, right_recv, left_recv, up_recv, down_recv, out_recv):
    g = Grid(n, heads, source_rows)
    side = g.side
    half = src_ref.shape[1]
    meet(g.peers())
    mine = pl.ds(pl.multiple_of(g.part * half, half), half)

    def landing(drow, dcol, head_col):
        if drow == 0:
            return dst_ref.at[g.row * side + head_col, mine], out_recv
        return stage_ref.at[drow - 1, dcol, mine], stage_recv.at[drow - 1, dcol]

    def along_row(drow, dcol):
        row = g.wrap(g.row + drow)
        col = g.wrap(g.col + dcol)
        for part in range(g.parts):
            source = src_ref.at[g.device(row, col, part)]
            if dcol in g.direct:
                dst, sem = landing(drow, dcol, g.col)
                send(source, dst, x_send.at[drow], sem, g.near(0, g.hop(dcol), part)).start()
            elif part == 0:
                send(source, right_ref.at[drow], x_send.at[drow], right_recv.at[drow], g.near(0, 1)).start()
            else:
                send(source, left_ref.at[drow], x_send.at[drow], left_recv.at[drow], g.near(0, -1)).start()

    def own_chip(drow):
        row = g.wrap(g.row + drow)
        away = src_ref.at[g.device(row, g.col, g.parts - 1 - g.part)]
        dst, sem = landing(drow, 0, g.col)
        dst[...] = src_ref[g.device(row, g.col, g.part)]
        send(away, dst, x_send.at[drow], sem, g.partner).start()

    def pass_row(drow):
        for ref, come_sem, come in ((right_ref, right_recv, -1), (left_ref, left_recv, 1)):
            send(ref.at[drow], ref.at[drow], fwd_send.at[drow], come_sem.at[drow], g.me).wait_recv()
            dst, sem = landing(drow, 2, g.wrap(g.col + come))
            send(ref.at[drow], dst, fwd_send.at[drow], sem, g.near(0, -come, 0 if come < 0 else 1)).start()

    def along_column(drow, dcol):
        chunk = stage_ref.at[drow - 1, dcol]
        got = chunk.at[pl.ds(0, half)] if dcol == 0 else chunk
        send(got, got, y_send.at[drow - 1], stage_recv.at[drow - 1, dcol], g.me).wait_recv()
        head = g.row * side + g.wrap(g.col - dcol)
        if drow in g.direct:
            send(chunk, dst_ref.at[head], y_send.at[drow - 1], out_recv, g.near(g.hop(drow), 0)).start()
        elif dcol % 2 == 0:
            send(chunk, up_ref.at[dcol // 2], y_send.at[drow - 1], up_recv.at[dcol // 2], g.near(1, 0)).start()
        else:
            send(chunk, down_ref.at[dcol // 2], y_send.at[drow - 1], down_recv.at[dcol // 2], g.near(-1, 0)).start()

    def when_source(row, body):
        pl.when(g.is_source(row))(body)

    def rows_of(drow):
        def body():
            for d in (2, 1, 3) if g.ties else (1,):
                along_row(drow, d)
        when_source(g.row + drow, body)

    def relay(drow):
        when_source(g.row + drow, lambda: pass_row(drow))

    def column(drow, d):
        when_source(g.row + drow, lambda: along_column(drow, d))

    def up(i):
        def body():
            send(up_ref.at[i], up_ref.at[i], pass_send.at[0], up_recv.at[i], g.me).wait_recv()
            head = g.wrap(g.row - 1) * side + g.wrap(g.col - 2 * i)
            send(up_ref.at[i], dst_ref.at[head], pass_send.at[0], out_recv, g.near(1, 0)).start()
        when_source(g.row + 1, body)

    def down(i):
        def body():
            send(down_ref.at[i], down_ref.at[i], pass_send.at[1], down_recv.at[i], g.me).wait_recv()
            head = g.wrap(g.row + 1) * side + g.wrap(g.col - 2 * i - 1)
            send(down_ref.at[i], dst_ref.at[head], pass_send.at[1], out_recv, g.near(-1, 0)).start()
        when_source(g.row - 1, body)

    def start_dq():
        swap(dq_ref, theirs_ref, row_send.at[0], row_recv.at[0], g.partner)
        total = (dq_ref[...] + theirs_ref[...]).T.astype(BF16)
        packed_ref[...] = pack(total.reshape(n, total.shape[0] // n, total.shape[1]))
        start_rows(n, heads, g.me, g.part, packed_ref, lambda peer: peer, got_ref, row_send.at[1], row_recv.at[1])

    for drow in (2, 1, 3, 0) if g.ties else (1, 0):
        when_source(g.row + drow, lambda drow=drow: own_chip(drow))
    if g.ties:
        rows_of(2)
        rows_of(1)
        start_dq()
        for drow in (2, 1, 3):
            column(drow, 0)
        relay(2)
        rows_of(3)
        relay(1)
        column(2, 1)
        column(2, 3)
        column(2, 2)
        up(0)
        down(0)
        rows_of(0)
        column(1, 1)
        column(1, 3)
        relay(3)
        column(1, 2)
        up(1)
        down(1)
        relay(0)
        column(3, 1)
        column(3, 3)
        column(3, 2)
    else:
        rows_of(1)
        rows_of(0)
        start_dq()
        column(1, 0)
        column(1, 1)
    wait_rows(heads, g.me, got_ref, row_send.at[1], row_recv.at[1])
    rows_ref[...] = unpack(got_ref[...])

    def sent(sem, ref):
        send(ref, ref, sem, out_recv, g.me).wait_send()

    for drow in range(side):
        def done(drow=drow):
            sent(x_send.at[drow], src_ref.at[pl.ds(0, g.parts * side - 1)])
            if g.ties:
                sent(fwd_send.at[drow], src_ref.at[pl.ds(0, 2)])
            if drow:
                sent(y_send.at[drow - 1], stage_ref.at[0])
        when_source(g.row + drow, done)
    if g.ties:
        when_source(g.row + 1, lambda: sent(pass_send.at[0], up_ref))
        when_source(g.row - 1, lambda: sent(pass_send.at[1], down_ref))

    @pl.when(g.is_source(g.row))
    def _():
        blocks = src_ref.at[pl.ds(0, n - 1)]
        send(blocks, blocks, y_send.at[0], out_recv, g.me).wait_recv()

    @pl.when(jnp.logical_not(g.is_source(g.row)))
    def _():
        def clear(index, carry):
            dst_ref[index] = jnp.zeros(dst_ref.shape[1:], dst_ref.dtype)
            return carry
        lax.fori_loop(0, heads, clear, 0)


def return_blocks(n, heads, source_rows, collective_id, blocks, dq):
    half, width = blocks.shape[1], blocks.shape[2]
    hd, total_q = dq.shape
    q_rows = total_q // n
    side, parts = math.isqrt(heads), n // heads
    chunk = lambda *lead: pltpu.VMEM(lead + (half * parts, width), BF16)
    block = lambda *lead: pltpu.VMEM(lead + (half, width), BF16)
    return pl.pallas_call(
        functools.partial(return_kernel, n, heads, source_rows),
        out_shape=[shape((heads, half * parts, width), BF16), shape((heads, q_rows, hd), BF16)],
        in_specs=vmem(2),
        out_specs=vmem(2),
        scratch_shapes=[chunk(side - 1, side), block(side), block(side), chunk(2), chunk(2), pltpu.VMEM(dq.shape, F32),
                        pltpu.VMEM((n, q_rows // 2, 2 * hd), BF16), pltpu.VMEM((heads, q_rows // 2, 2 * hd), BF16), dma(2), dma(2),
                        dma(side), dma(side), dma(side - 1), dma(2), dma(side - 1, side), dma(side), dma(side), dma(2), dma(2),
                        pltpu.SemaphoreType.DMA],
        compiler_params=remote(collective_id),
        name='return_blocks',
    )(blocks, dq)


def decoder_kernel(n, heads, mine_ref, dec_ref, gout_ref, gain_ref, wo_hbm, wg_hbm, wu_hbm, wd_hbm,
                   out_ref, lse_ref, do_ref, factors_ref, gh_ref, gnorm_ref,
                   theirs_ref, packed_ref, got_ref, sent_ref, back_ref, swapped_ref, wo_ref, wg_ref, wu_ref, wd_ref,
                   load_sem, send_sem, recv_sem):
    me = lax.axis_index('seq')
    part = lax.rem(me, n // heads)
    partner, peers = pair_peers(n, heads, me, part)
    q_rows, dim = dec_ref.shape
    hd = out_ref.shape[0]
    loads = [pltpu.make_async_copy(src, dst, load_sem.at[i]) for i, (src, dst) in enumerate(
        ((wd_hbm, wd_ref), (wo_hbm, wo_ref), (wg_hbm, wg_ref), (wu_hbm, wu_ref)))]
    for load in loads:
        load.start()
    meet(peers)

    swap(mine_ref, theirs_ref, send_sem.at[0], recv_sem.at[0], partner)
    m_a, m_b = mine_ref[hd + 8:hd + 9], theirs_ref[hd + 8:hd + 9]
    top = jnp.maximum(m_a, m_b)
    s_a, s_b = jnp.exp2(m_a - top), jnp.exp2(m_b - top)
    den = mine_ref[hd:hd + 1] * s_a + theirs_ref[hd:hd + 1] * s_b
    out = (mine_ref[:hd] * s_a + theirs_ref[:hd] * s_b) / den
    packed_ref[...] = pack(out.T.astype(BF16).reshape(n, q_rows, hd))
    start_rows(n, heads, me, part, packed_ref, lambda peer: peer, got_ref, send_sem.at[1], recv_sem.at[1])
    out_ref[...] = out
    lse_ref[...] = top + jnp.log2(den)

    loads[0].wait()
    grad_act = dot_nt(gout_ref[...].astype(BF16), wd_ref[...])
    wait_rows(heads, me, got_ref, send_sem.at[1], recv_sem.at[1])

    attended = jnp.concatenate([unpack(got_ref[h]) for h in range(heads)], axis=1)
    loads[1].wait()
    hidden = (dec_ref[...].astype(F32) + dot(attended, wo_ref[...])).astype(BF16).astype(F32)
    gain = gain_ref[...].astype(F32)
    inverse = lax.rsqrt(jnp.mean(hidden * hidden, axis=-1, keepdims=True) + 1e-6)
    scaled = hidden * inverse
    normed = (scaled * gain).astype(BF16)
    loads[2].wait()
    gate = dot(normed, wg_ref[...])
    loads[3].wait()
    up = dot(normed, wu_ref[...])
    sig = jax.nn.sigmoid(gate)
    silu = gate * sig
    grad_gate = (grad_act * up * (sig + silu * (1.0 - sig))).astype(BF16)
    grad_up = (grad_act * silu).astype(BF16)
    grad_normed = (dot_nt(wg_ref[...], grad_gate) + dot_nt(wu_ref[...], grad_up)).T
    gnorm_ref[...] = jnp.sum(grad_normed * scaled, axis=0, keepdims=True)
    inner = grad_normed * gain
    grad_hidden = gout_ref[...] + inverse * (inner - scaled * jnp.mean(inner * scaled, axis=-1, keepdims=True))
    rounded = grad_hidden.astype(BF16)
    grad_att = dot_nt(wo_ref[...], rounded).T.astype(BF16)
    for h in range(heads):
        sent_ref[h] = pack(grad_att[:, hd * h:hd * (h + 1)])
    factors_ref[:, :dim] = attended
    factors_ref[:, dim:] = rounded
    gh_ref[...] = grad_hidden

    start_rows(n, heads, me, part, sent_ref, lambda peer: peer // (n // heads), back_ref, send_sem.at[2], recv_sem.at[2])
    wait_rows(heads, me, back_ref, send_sem.at[2], recv_sem.at[2])
    swap(back_ref, swapped_ref, send_sem.at[3], recv_sem.at[3], partner)
    place(n, heads, part, back_ref, swapped_ref, do_ref, False)


def decoder_rows(n, heads, collective_id, mine, dec_in, grad_out, gain, wo, w_gate, w_up, w_down):
    q_rows, dim = dec_in.shape
    hd, total_q = wo.shape[0] // heads, mine.shape[1]
    hbm = pl.BlockSpec(memory_space=pl.ANY)
    return pl.pallas_call(
        functools.partial(decoder_kernel, n, heads),
        out_shape=[shape((hd, total_q), F32), shape((1, total_q), F32), shape((n, q_rows, 2 * hd), BF16),
                   shape((q_rows, 2 * dim), BF16), shape((q_rows, dim), F32), shape((1, dim), F32)],
        in_specs=vmem(4) + [hbm] * 4,
        out_specs=vmem(6),
        scratch_shapes=[pltpu.VMEM(mine.shape, F32), pltpu.VMEM((n, q_rows // 2, 2 * hd), BF16)]
        + [pltpu.VMEM((heads, q_rows // 2, 2 * hd), BF16)] * 4
        + [pltpu.VMEM(w.shape, BF16) for w in (wo, w_gate, w_up, w_down)] + [dma(4), dma(4), dma(4)],
        compiler_params=remote(collective_id),
        name='decoder_rows',
    )(mine, dec_in, grad_out, gain, wo, w_gate, w_up, w_down)


def small_sum_kernel(n, mine_ref, total_ref, all_ref, send_sem, recv_sem):
    me = lax.axis_index('seq')
    meet([lax.rem(me + step, n) for step in range(1, n)])
    for step in range(1, n):
        send(mine_ref, all_ref.at[me], send_sem, recv_sem, lax.rem(me + step, n)).start()
    all_ref[me] = mine_ref[...]
    others = all_ref.at[pl.ds(0, n - 1)]
    whole = send(others, others, send_sem, recv_sem, me)
    whole.wait_send()
    whole.wait_recv()
    total_ref[...] = jnp.sum(all_ref[...], axis=0)


def small_sum(n, collective_id, mine):
    return pl.pallas_call(
        functools.partial(small_sum_kernel, n),
        out_shape=shape(mine.shape, F32),
        in_specs=vmem(1),
        out_specs=vmem(1)[0],
        scratch_shapes=[pltpu.VMEM((n,) + mine.shape, F32), pltpu.SemaphoreType.DMA, pltpu.SemaphoreType.DMA],
        compiler_params=remote(collective_id),
        name='small_sum',
    )(mine)


def forward_kernel(scale, hd, q_block, bounds_ref, kv_ref, q_ref, out_ref, qt_ref, top_ref):
    blocks, last_valid = bounds_ref[0], bounds_ref[1]
    rows, total_q = kv_ref.shape[1], q_ref.shape[0]
    groups = [slice(first, first + q_block) for first in range(0, total_q, q_block)]
    base = slice(hd + 8, hd + 9)
    qt_ref[...] = q_ref[...].T

    def values_of(keys):
        return jnp.concatenate([keys.T[hd:], jnp.ones((16, rows), keys.dtype)], axis=0)

    def group_of(index):
        return pl.ds(pl.multiple_of(index * q_block, q_block), q_block)

    def first_step(group, carry):
        cols = group_of(group)
        top = jnp.max(dot(kv_ref[0], qt_ref[:, cols]), axis=0, keepdims=True)
        out_ref[hd + 8:, cols] = jnp.broadcast_to(top * scale, (8, q_block))
        top_ref[:, cols] = jnp.broadcast_to(top, (8, q_block))
        return carry

    lax.fori_loop(0, len(groups), first_step, 0)
    out_ref[:hd + 8, :] = jnp.zeros((hd + 8, total_q), F32)

    def finish(values, scores, cols):
        top_ref[:, cols] = jnp.maximum(top_ref[:, cols], jnp.max(scores.reshape(rows // 8, 8, q_block), axis=0))
        weights = jnp.exp2(scores * scale - out_ref[base, cols]).astype(values.dtype)
        out_ref[:hd + 8, cols] += dot(values, weights)[:hd + 8]

    def step(index, carry):
        keys = kv_ref[index]
        values = values_of(keys)
        for cols in groups:
            finish(values, dot(keys, qt_ref[:, cols]), cols)
        return carry

    def last_step(group, carry):
        cols = group_of(group)
        keys = kv_ref[blocks - 1]
        scores = dot(keys, qt_ref[:, cols])
        position = lax.broadcasted_iota(jnp.int32, scores.shape, 0)
        finish(values_of(keys), jnp.where(position < last_valid, scores, NEG), cols)
        return carry

    lax.fori_loop(0, blocks - 1, step, 0)
    lax.fori_loop(0, len(groups), last_step, 0)

    excess = jnp.max(top_ref[...] * scale - out_ref[hd + 8:, :])

    @pl.when(excess > 16.0)
    def _():
        out_ref[:hd + 8, :] = jnp.zeros((hd + 8, total_q), F32)
        out_ref[hd + 8:, :] = jnp.full((8, total_q), NEG, F32)

        def running(step_index, carry):
            index, group = step_index // len(groups), lax.rem(step_index, len(groups))
            cols = group_of(group)
            keys = kv_ref[index]
            limit = jnp.where(index == blocks - 1, last_valid, rows)
            scores = dot(keys, qt_ref[:, cols]) * scale
            position = lax.broadcasted_iota(jnp.int32, scores.shape, 0)
            scores = jnp.where(position < limit, scores, NEG)
            old = out_ref[base, cols]
            new = jnp.maximum(old, jnp.max(scores, axis=0, keepdims=True))
            weights = jnp.exp2(scores - new).astype(keys.dtype)
            out_ref[:hd + 8, cols] = out_ref[:hd + 8, cols] * jnp.exp2(old - new) + dot(values_of(keys), weights)[:hd + 8]
            out_ref[hd + 8:, cols] = jnp.broadcast_to(new, (8, q_block))
            return carry

        lax.fori_loop(0, blocks * len(groups), running, 0)


def attention_forward(scale, hd, sources, bounds, kv, q):
    rows, width = kv.shape[1], kv.shape[2]
    total_q = q.shape[0]
    return pl.pallas_call(
        functools.partial(forward_kernel, scale, hd, min(1024, total_q)),
        out_shape=shape((hd + 16, total_q), F32),
        grid=(1,),
        in_specs=[pl.BlockSpec(memory_space=pltpu.SMEM),
                  pl.BlockSpec((sources, rows, width), lambda i: (0, 0, 0), pipeline_mode=pl.Buffered(1)), full(q)],
        out_specs=pl.BlockSpec((hd + 16, total_q), lambda i: (0, 0)),
        scratch_shapes=[pltpu.VMEM((width, total_q), BF16), pltpu.VMEM((8, total_q), F32)],
        compiler_params=plain(),
        cost_estimate=pl.CostEstimate(flops=4 * total_q * sources * rows * hd, bytes_accessed=kv.size * 2,
                                      transcendentals=total_q * sources * rows),
        name='attention_forward',
    )(bounds, kv, q)


def backward_kernel(scale, key_scale, hd, q_block, bounds_ref, kv_ref, q_ref, do_ref, out_ref, lse_ref, dkv_ref, dq_ref,
                    qt_ref, dot_ref, delta_ref):
    blocks, last_valid = bounds_ref[0], bounds_ref[1]
    rows, total_q = kv_ref.shape[1], q_ref.shape[0]
    width = kv_ref.shape[2]
    groups = [slice(first, first + q_block) for first in range(0, total_q, q_block)]
    dq_ref[...] = jnp.zeros_like(dq_ref)
    qt_ref[...] = q_ref[...].T
    do_t = do_ref[...].T
    dot_ref[...] = do_t
    delta_ref[...] = jnp.sum(do_t[hd:].astype(F32) * out_ref[...], axis=0, keepdims=True)

    lane_scale = jnp.where(lax.broadcasted_iota(jnp.int32, (1, width), 1) < hd, key_scale, 1.0)

    def products(keys, cols):
        return dot(keys, qt_ref[:, cols]), dot(keys, dot_ref[:, cols])

    def finish(keys, keys_t, scores, grads, cols, valid):
        prob = jnp.exp2(scores * scale - lse_ref[:, cols])
        if valid is not None:
            position = lax.broadcasted_iota(jnp.int32, scores.shape, 0)
            prob = jnp.where(position < valid, prob, 0.0)
        grad_scores = (prob * (grads - delta_ref[:, cols])).astype(keys.dtype)
        update = dot(grad_scores, q_ref[cols, :]) + dot(prob.astype(keys.dtype), do_ref[cols, :])
        dq_ref[:, cols] += dot(keys_t, grad_scores)
        return update

    def step(index, carry):
        keys = kv_ref[index]
        keys_t = keys.T[:hd]
        total = jnp.zeros((rows, width), F32)
        for cols in groups:
            scores, grads = products(keys, cols)
            total += finish(keys, keys_t, scores, grads, cols, None)
        dkv_ref[index] = (total * lane_scale).astype(dkv_ref.dtype)
        return carry

    def last_step(group, total):
        keys = kv_ref[blocks - 1]
        cols = pl.ds(pl.multiple_of(group * q_block, q_block), q_block)
        scores, grads = products(keys, cols)
        return total + finish(keys, keys.T[:hd], scores, grads, cols, last_valid)

    def clear(index, carry):
        dkv_ref[index] = jnp.zeros((rows, width), dkv_ref.dtype)
        return carry

    lax.fori_loop(0, blocks - 1, step, 0)
    total = lax.fori_loop(0, len(groups), last_step, jnp.zeros((rows, width), F32))
    dkv_ref[blocks - 1] = (total * lane_scale).astype(dkv_ref.dtype)
    lax.fori_loop(blocks, dkv_ref.shape[0], clear, 0)
    dq_ref[...] = dq_ref[...] * key_scale


def attention_backward(scale, key_scale, hd, sources, bounds, kv, q, do, out_t, lse):
    n, rows, width = kv.shape
    total_q = q.shape[0]
    return pl.pallas_call(
        functools.partial(backward_kernel, scale, key_scale, hd, min(512, total_q)),
        out_shape=[shape((n, rows, width), BF16), shape((hd, total_q), F32)],
        grid=(1,),
        in_specs=[pl.BlockSpec(memory_space=pltpu.SMEM),
                  pl.BlockSpec((sources, rows, width), lambda i: (0, 0, 0), pipeline_mode=pl.Buffered(1)),
                  full(q), full(do), full(out_t), full(lse)],
        out_specs=[pl.BlockSpec((n, rows, width), lambda i: (0, 0, 0)),
                   pl.BlockSpec((hd, total_q), lambda i: (0, 0))],
        scratch_shapes=[pltpu.VMEM((width, total_q), BF16), pltpu.VMEM((width, total_q), BF16), pltpu.VMEM((1, total_q), F32)],
        compiler_params=plain(),
        cost_estimate=pl.CostEstimate(flops=10 * total_q * sources * rows * hd, bytes_accessed=kv.size * 4,
                                      transcendentals=total_q * sources * rows),
        name='attention_backward',
    )(bounds, kv, q, do, out_t, lse)


def prepare_kernel(dec_ref, att_ref, wo_ref, gain_ref, n2_ref, n2t_ref):
    hidden = (dec_ref[...].astype(F32) + dot(att_ref[...], wo_ref[...])).astype(BF16)
    normed = rms_norm(hidden.astype(F32), gain_ref[...].astype(F32)).astype(BF16)
    n2_ref[...] = normed
    n2t_ref[...] = normed.T


def prepare(early, late, wo, gain):
    rows, dim = early.shape[0], wo.shape[1]
    chunk = min(512, rows)
    left = pl.BlockSpec((chunk, dim), lambda i: (i, 0))
    return pl.pallas_call(
        prepare_kernel,
        out_shape=[shape((rows, dim), BF16), shape((dim, rows), BF16)],
        grid=(rows // chunk,),
        in_specs=[left, left, full(wo), full(gain)],
        out_specs=[left, pl.BlockSpec((dim, chunk), lambda i: (0, i))],
        compiler_params=plain(),
        cost_estimate=pl.CostEstimate(flops=2 * rows * dim * dim, bytes_accessed=8 * rows * dim, transcendentals=0),
        name='prepare',
    )(early, late, wo, gain)


def mlp_kernel(chunk, n2_ref, n2t_ref, top_ref, w1_ref, w3_ref, w2_ref, g1_ref, g3_ref, g2_ref, d1_ref, d3_ref, act_ref):
    rows = n2_ref.shape[0]
    w1, w3, w2t = w1_ref[...], w3_ref[...], w2_ref[...].T
    for first in range(0, rows, chunk):
        part = slice(first, first + chunk)
        gate = dot(n2_ref[part, :], w1)
        up = dot(n2_ref[part, :], w3)
        grad = dot(top_ref[part, :], w2t)
        sig = jax.nn.sigmoid(gate)
        silu = gate * sig
        act_ref[part, :] = (silu * up).astype(act_ref.dtype)
        d3_ref[part, :] = (grad * silu).astype(d3_ref.dtype)
        d1_ref[part, :] = (grad * up * (sig + silu * (1.0 - sig))).astype(d1_ref.dtype)
    g1_ref[...] = dot(n2t_ref[...], d1_ref[...])
    g3_ref[...] = dot(n2t_ref[...], d3_ref[...])
    g2_ref[...] = dot_tn(act_ref[...], top_ref[...])


def mlp_weight_grads(n2, n2t, early, w_gate, w_up, w_down):
    rows, dim = n2.shape
    ff = w_gate.shape[1]
    tile = 256
    cols = pl.BlockSpec((dim, tile), lambda i: (0, i))
    tall = pl.BlockSpec((tile, dim), lambda i: (i, 0))
    return pl.pallas_call(
        functools.partial(mlp_kernel, min(512, rows)),
        out_shape=[shape((dim, ff), F32), shape((dim, ff), F32), shape((ff, dim), F32)],
        grid=(ff // tile,),
        in_specs=[full(n2), full(n2t), pl.BlockSpec((rows, dim), lambda i: (0, 1), pipeline_mode=pl.Buffered(1)), cols, cols, tall],
        out_specs=[cols, cols, tall],
        scratch_shapes=[pltpu.VMEM((rows, tile), BF16)] * 3,
        compiler_params=plain(),
        cost_estimate=pl.CostEstimate(flops=12 * rows * dim * ff, bytes_accessed=18 * dim * ff, transcendentals=rows * ff),
        name='mlp_weight_grads',
    )(n2, n2t, early, w_gate, w_up, w_down)


def memory_weight_kernel(memory_ref, dkv_ref, dec_ref, gain_ref, dq_ref, gk_ref, gv_ref, gq_ref):
    group, hd = dkv_ref.shape[0], dkv_ref.shape[2] // 2
    normed = rms_norm(dec_ref[...].astype(F32), gain_ref[...].astype(F32)).astype(BF16)
    for i in range(group):
        rows = slice(i * hd, (i + 1) * hd)
        both = dot_tn(dkv_ref[i], memory_ref[...])
        gk_ref[rows, :] = both[:hd]
        gv_ref[rows, :] = both[hd:]
        gq_ref[rows, :] = dot_tn(dq_ref[i], normed)


def memory_weight_grads(memory, dkv, dec_in, gain, dq_rows):
    heads, rows, width = dkv.shape
    dim, hd = memory.shape[1], width // 2
    group = 4
    out = pl.BlockSpec((group * hd, dim), lambda i: (i, 0))
    return pl.pallas_call(
        memory_weight_kernel,
        out_shape=[shape((heads * hd, dim), F32)] * 3,
        grid=(heads // group,),
        in_specs=[full(memory), pl.BlockSpec((group, rows, width), lambda i: (i, 0, 0)), full(dec_in), full(gain),
                  pl.BlockSpec((group,) + dq_rows.shape[1:], lambda i: (i, 0, 0))],
        out_specs=[out, out, out],
        compiler_params=plain(),
        cost_estimate=pl.CostEstimate(flops=2 * rows * dim * heads * width, bytes_accessed=16 * rows * dim, transcendentals=0),
        name='memory_weight_grads',
    )(memory, dkv, dec_in, gain, dq_rows)


def memory_grad_kernel(dkv_ref, wk_ref, wv_ref, out_ref):
    group = dkv_ref.shape[0]
    left = jnp.concatenate([dkv_ref[i] for i in range(group)], axis=1)
    right = jnp.concatenate([part[i] for i in range(group) for part in (wk_ref, wv_ref)], axis=0)

    @pl.when(pl.program_id(0) == 0)
    def _():
        out_ref[...] = dot(left, right)

    @pl.when(pl.program_id(0) > 0)
    def _():
        out_ref[...] += dot(left, right)


def memory_grad(dkv, wk_t, wv_t):
    heads, rows, width = dkv.shape
    hd, dim = wk_t.shape[1], wk_t.shape[2]
    group = 4
    weight = pl.BlockSpec((group, hd, dim), lambda i: (i, 0, 0))
    return pl.pallas_call(
        memory_grad_kernel,
        out_shape=shape((rows, dim), F32),
        grid=(heads // group,),
        in_specs=[pl.BlockSpec((group, rows, width), lambda i: (i, 0, 0)), weight, weight],
        out_specs=pl.BlockSpec((rows, dim), lambda i: (0, 0)),
        compiler_params=plain(),
        cost_estimate=pl.CostEstimate(flops=2 * rows * dim * heads * width, bytes_accessed=12 * rows * dim, transcendentals=0),
        name='memory_grad',
    )(dkv, wk_t, wv_t)


def outer_kernel(att_ref, gh_ref, out_ref):
    @pl.when(pl.program_id(0) == 0)
    def _():
        out_ref[...] = jnp.zeros_like(out_ref)

    out_ref[...] += dot_tn(att_ref[...], gh_ref[...])


def outer_weight_grad(late, dim):
    rows = late.shape[0]
    chunk = min(512, rows)
    return pl.pallas_call(
        outer_kernel,
        out_shape=shape((dim, dim), F32),
        grid=(rows // chunk,),
        in_specs=[pl.BlockSpec((chunk, dim), lambda i: (i, 0)), pl.BlockSpec((chunk, dim), lambda i: (i, 1))],
        out_specs=pl.BlockSpec((dim, dim), lambda i: (0, 0)),
        compiler_params=plain(),
        cost_estimate=pl.CostEstimate(flops=2 * rows * dim * dim, bytes_accessed=8 * rows * dim, transcendentals=0),
        name='outer_weight_grad',
    )(late, late)


def solution(mesh):
    n = mesh.shape['seq']
    row_spec = P(('data', 'seq'), None)
    weight_spec = P()
    part_vec = P('data')
    part_mat = P('data', None)
    part_cube = P('data', None, None)

    def device_step(dec_in, memory, mem_len, grad_out, norm_attn, wq_cross, wk_cross, wv_cross, wo_cross, norm_mlp, w_gate, w_up, w_down):
        q_rows, dim = dec_in.shape
        m_rows = memory.shape[0]
        heads, hd = wq_cross.shape[1], wq_cross.shape[2]
        parts = n // heads
        half = m_rows // parts
        sources = -(-3 * n // 4)
        total_q = q_rows * n
        key_scale = hd ** -0.5
        scale = key_scale * LOG2E
        me = lax.axis_index('seq')
        part = lax.rem(me, parts)

        reach = mem_len[0] - part * half
        blocks = jnp.minimum((reach + m_rows - 1) // m_rows, sources)
        bounds = jnp.stack([blocks, jnp.minimum(reach - (blocks - 1) * m_rows, half)]).astype(jnp.int32)

        wq_t, wk_t, wv_t = (jnp.transpose(w, (1, 2, 0)) for w in (wq_cross, wk_cross, wv_cross))
        gain_attn, gain_mlp = norm_attn.reshape(1, dim), norm_mlp.reshape(1, dim)
        source_rows = -(-sources // (parts * math.isqrt(heads)))
        kv, q_in = exchange(n, heads, source_rows, 0, memory, dec_in, gain_attn, wk_t, wv_t, wq_t)
        head_q = q_in.reshape(total_q, 2 * hd)

        early_local, kv = lax.optimization_barrier((jnp.concatenate([dec_in, grad_out.astype(BF16)], axis=1), kv))
        early = lax.all_gather(early_local, 'seq', axis=0, tiled=True)

        wo = wo_cross.reshape(heads * hd, dim)
        mine = attention_forward(scale, hd, sources, bounds, kv, head_q)
        out_t, lse, do_in, factors, grad_hidden, g_norm_mlp = decoder_rows(
            n, heads, 1, mine, dec_in, grad_out, gain_mlp, wo, w_gate, w_up, w_down)
        do_in, factors, early = lax.optimization_barrier((do_in, factors, early))
        late = lax.all_gather(factors, 'seq', axis=0, tiled=True)

        dkv, dq_part = attention_backward(scale, key_scale, hd, sources, bounds, kv, head_q, do_in.reshape(total_q, 2 * hd), out_t, lse)
        dkv_in, dq_rows = return_blocks(n, heads, source_rows, 4, dkv, dq_part)
        dkv_in, dq_rows, late = lax.optimization_barrier((dkv_in, dq_rows, late))

        sums = memory_weight_grads(memory, dkv_in, dec_in, gain_attn, dq_rows)
        *sums, dkv_in, dq_rows, early, late = lax.optimization_barrier((*sums, dkv_in, dq_rows, early, late))
        g_wk, g_wv, g_wq = lax.psum(tuple(sums), 'seq')

        n2_all, n2_all_t = prepare(early, late, wo, gain_mlp)
        g_gate, g_up, g_down = mlp_weight_grads(n2_all, n2_all_t, early, w_gate, w_up, w_down)
        g_wo = outer_weight_grad(late, dim)

        grad_normed = jnp.einsum('hte,dhe->td', dq_rows, wq_cross, preferred_element_type=F32)
        _, norm_pull = jax.vjp(rms_norm, dec_in.astype(F32), norm_attn.astype(F32))
        grad_x_norm, g_norm_attn = norm_pull(grad_normed)
        g_dec = grad_hidden + grad_x_norm
        norms = small_sum(n, 5, jnp.concatenate([g_norm_attn, g_norm_mlp[0]]).reshape(-1, 128)).reshape(2, dim)
        g_mem = memory_grad(dkv_in, wk_t, wv_t)
        cube = lambda g: jnp.transpose(g.reshape(heads, hd, dim), (2, 0, 1))
        return (g_dec, g_mem, norms[0], cube(g_wq), cube(g_wk), cube(g_wv), g_wo.reshape(heads, hd, dim), norms[1], g_gate, g_up, g_down)

    return jax.shard_map(device_step, mesh=mesh,
                         in_specs=(row_spec, row_spec, part_vec, row_spec) + (weight_spec,) * 9,
                         out_specs=(row_spec, row_spec, part_vec, part_cube, part_cube, part_cube, part_cube, part_vec, part_mat, part_mat, part_mat),
                         check_vma=False)
```

```python
import functools
import math

import jax
import jax.numpy as jnp
from jax import lax
from jax.experimental import pallas as pl
from jax.experimental.pallas import tpu as pltpu
from jax.sharding import PartitionSpec as P

LOG2E = 1.4426950408889634
NEG = -1e30
VMEM_LIMIT = 60 * 1024 * 1024
MESH = pl.DeviceIdType.MESH
BF16, F32 = jnp.bfloat16, jnp.float32


def rms_norm(tensor, gain):
    mean_sq = jnp.mean(tensor * tensor, axis=-1, keepdims=True)
    return tensor * lax.rsqrt(mean_sq + 1e-6) * gain


def dot(a, b):
    return jnp.dot(a, b, preferred_element_type=F32)


def dot_nt(a, b):
    return lax.dot_general(a, b, (((1,), (1,)), ((), ())), preferred_element_type=F32)


def dot_tn(a, b):
    return lax.dot_general(a, b, (((0,), (0,)), ((), ())), preferred_element_type=F32)


def full(array):
    return pl.BlockSpec(array.shape, lambda *_: (0,) * array.ndim, pipeline_mode=pl.Buffered(1))


def vmem(count):
    return [pl.BlockSpec(memory_space=pltpu.VMEM)] * count


def plain():
    return pltpu.CompilerParams(vmem_limit_bytes=VMEM_LIMIT)


def remote(collective_id):
    return pltpu.CompilerParams(collective_id=collective_id, has_side_effects=True, vmem_limit_bytes=VMEM_LIMIT)


def shape(dims, dtype):
    return jax.ShapeDtypeStruct(dims, dtype)


def meet(peers):
    barrier = pltpu.get_barrier_semaphore()
    for peer in peers:
        pl.semaphore_signal(barrier, inc=1, device_id={'seq': peer}, device_id_type=MESH)
    pl.semaphore_wait(barrier, len(peers))


def send(src, dst, send_sem, recv_sem, peer):
    return pltpu.make_async_remote_copy(src_ref=src, dst_ref=dst, send_sem=send_sem, recv_sem=recv_sem,
                                        device_id={'seq': peer}, device_id_type=MESH)


class Grid:
    def __init__(self, n, heads, source_rows):
        self.n, self.heads, self.source_rows = n, heads, source_rows
        self.parts = n // heads
        self.side = math.isqrt(heads)
        self.me = lax.axis_index('seq')
        self.part = lax.rem(self.me, self.parts)
        self.chip = self.me // self.parts
        self.col = lax.rem(self.chip, self.side)
        self.row = self.chip // self.side
        self.partner = self.chip * self.parts + (self.parts - 1 - self.part)
        self.ties = self.side == 4
        self.direct = (1, 3) if self.ties else (1,)

    def wrap(self, value):
        return lax.rem(value + self.side, self.side)

    def device(self, row, col, part):
        return (row * self.side + col) * self.parts + part

    def near(self, drow, dcol, part=None):
        return self.device(self.wrap(self.row + drow), self.wrap(self.col + dcol), self.part if part is None else part)

    def hop(self, offset):
        return 1 if offset == 1 else -1

    def is_source(self, row):
        return self.wrap(row) < self.source_rows

    def row_peers(self):
        return [lax.rem(self.chip + step, self.heads) * self.parts + self.part for step in range(1, self.heads)]

    def peers(self):
        return self.row_peers() + [self.partner] + [self.near(0, self.hop(d), self.parts - 1 - self.part) for d in self.direct]


def pair_peers(n, heads, me, part):
    parts = n // heads
    head = me // parts
    partner = head * parts + (parts - 1 - part)
    return partner, [partner] + [lax.rem(head + step, heads) * parts + part for step in range(1, heads)]


def pack(rows):
    middle = rows.shape[-2] // 2
    return jnp.concatenate([rows[..., :middle, :], rows[..., middle:, :]], axis=-1)


def unpack(packed):
    middle = packed.shape[-1] // 2
    return jnp.concatenate([packed[..., :middle], packed[..., middle:]], axis=-2)


def start_rows(n, heads, me, part, src, src_of, dst_ref, send_sem, recv_sem):
    parts = n // heads
    head = me // parts
    for step in range(1, heads):
        peer = lax.rem(head + step, heads) * parts + part
        send(src.at[src_of(peer)], dst_ref.at[head], send_sem, recv_sem, peer).start()
    dst_ref[head] = src[src_of(me)]


def wait_rows(heads, me, dst_ref, send_sem, recv_sem):
    others = dst_ref.at[pl.ds(0, heads - 1)]
    whole = send(others, others, send_sem, recv_sem, me)
    whole.wait_send()
    whole.wait_recv()


def swap(src, dst, send_sem, recv_sem, partner):
    copy = send(src, dst, send_sem, recv_sem, partner)
    copy.start()
    copy.wait()


def place(n, heads, part, mine_ref, theirs_ref, wide_ref, low):
    parts = n // heads
    for source, index in ((mine_ref, part), (theirs_ref, parts - 1 - part)):
        for head in range(heads):
            rows = unpack(source[head])
            zeros = jnp.zeros_like(rows)
            wide_ref[head * parts + index] = jnp.concatenate([rows, zeros] if low else [zeros, rows], axis=-1)


def exchange_kernel(n, heads, source_rows, memory_ref, dec_ref, gout_ref, gain_ref, wk_ref, wv_ref, wq_ref, kv_out_ref, q_out_ref, early_ref,
                    kv_ref, stage_ref, up_ref, down_ref, right_ref, left_ref, packed_ref, got_ref, swapped_ref,
                    row_send, row_recv, y_send, pass_send, x_send, fwd_send, stage_recv, up_recv, down_recv, right_recv,
                    left_recv, out_recv):
    g = Grid(n, heads, source_rows)
    side, hd = g.side, wk_ref.shape[1]
    half = kv_out_ref.shape[1]
    chunk_rows = min(256, kv_ref.shape[1])
    barrier = pltpu.get_barrier_semaphore()
    peers = g.peers()
    for peer in peers:
        pl.semaphore_signal(barrier, inc=1, device_id={'seq': peer}, device_id_type=MESH)

    dim = dec_ref.shape[1]
    early_ref[:, :dim] = dec_ref[...]
    early_ref[:, dim:] = gout_ref[...].astype(BF16)
    normed = rms_norm(dec_ref[...].astype(F32), gain_ref[...].astype(F32)).astype(BF16)
    for i in range(0, heads, 4):
        queries = dot_nt(normed, jnp.concatenate([wq_ref[i + j] for j in range(4)], axis=0)).astype(BF16)
        for j in range(4):
            packed_ref[i + j] = pack(queries[:, hd * j:hd * (j + 1)])

    def head(drow, dcol):
        return g.wrap(g.row + drow) * side + g.wrap(g.col + dcol)

    def project(drow, dcols):
        weights = jnp.concatenate([ref[head(drow, d)] for d in dcols for ref in (wk_ref, wv_ref)], axis=0)

        def rows(index, carry):
            at = pl.ds(pl.multiple_of(index * chunk_rows, chunk_rows), chunk_rows)
            both = dot_nt(memory_ref[at, :], weights).astype(BF16)
            for i, d in enumerate(dcols):
                kv_ref[head(drow, d), at, :] = both[:, 2 * hd * i:2 * hd * (i + 1)]
            return carry

        lax.fori_loop(0, kv_ref.shape[1] // chunk_rows, rows, 0)

    def along_column(drow, dcol):
        chunk = kv_ref.at[head(drow, dcol)]
        if drow in g.direct:
            send(chunk, stage_ref.at[drow - 1, dcol], y_send.at[drow - 1], stage_recv.at[drow - 1, dcol], g.near(g.hop(drow), 0)).start()
        elif dcol % 2 == 0:
            send(chunk, up_ref.at[dcol // 2], y_send.at[drow - 1], up_recv.at[dcol // 2], g.near(1, 0)).start()
        else:
            send(chunk, down_ref.at[dcol // 2], y_send.at[drow - 1], down_recv.at[dcol // 2], g.near(-1, 0)).start()

    def along_row(o, dcol):
        chunk = kv_ref.at[head(0, dcol)] if o == 0 else stage_ref.at[o - 1, dcol]
        source = g.device(g.wrap(g.row - o), g.col, g.part)
        if dcol == 0:
            kv_out_ref[source] = chunk[pl.ds(pl.multiple_of(g.part * half, half), half), :]
            away = pl.ds(pl.multiple_of((g.parts - 1 - g.part) * half, half), half)
            send(chunk.at[away], kv_out_ref.at[source], x_send.at[o], out_recv, g.partner).start()
        elif dcol in g.direct:
            for part in range(g.parts):
                send(chunk.at[pl.ds(part * half, half)], kv_out_ref.at[source], x_send.at[o], out_recv,
                     g.near(0, g.hop(dcol), part)).start()
        else:
            send(chunk.at[pl.ds(0, half)], right_ref.at[o], x_send.at[o], right_recv.at[o], g.near(0, 1)).start()
            send(chunk.at[pl.ds(half, half)], left_ref.at[o], x_send.at[o], left_recv.at[o], g.near(0, -1)).start()

    def pass_row(o):
        for ref, sem, come in ((right_ref, right_recv, -1), (left_ref, left_recv, 1)):
            source = g.device(g.wrap(g.row - o), g.wrap(g.col + come), g.part)
            send(ref.at[o], ref.at[o], fwd_send.at[o], sem.at[o], g.me).wait_recv()
            send(ref.at[o], kv_out_ref.at[source], fwd_send.at[o], out_recv, g.near(0, -come, 0 if come < 0 else 1)).start()

    def when_source(row, body):
        pl.when(g.is_source(row))(body)

    if g.ties:
        order = [(2, (2, 1)), (2, (3, 0)), (1, (2, 1)), (3, (2, 3)), (0, (2, 1)), (0, (3, 0))]
        last = [(1, (3, 0)), (3, (1, 0))]
    else:
        order, last = [(1, (1, 0)), (0, (1, 0))], []

    def issue(drow, dcols):
        def body():
            for d in dcols:
                along_row(0, d) if drow == 0 else along_column(drow, d)
        when_source(g.row, body)

    waiting = None
    for drow, dcols in order + last:
        project(drow, dcols)
        if waiting is None:
            pl.semaphore_wait(barrier, len(peers))
            start_rows(n, heads, g.me, g.part, packed_ref, lambda peer: peer // g.parts, got_ref, row_send.at[0], row_recv.at[0])
        elif waiting not in last:
            issue(*waiting)
        waiting = (drow, dcols)
    if not last:
        issue(*waiting)

    if g.ties:
        def up(i):
            send(up_ref.at[i], up_ref.at[i], pass_send.at[0], up_recv.at[i], g.me).wait_recv()
            send(up_ref.at[i], stage_ref.at[1, 2 * i], pass_send.at[0], stage_recv.at[1, 2 * i], g.near(1, 0)).start()

        def down(i):
            send(down_ref.at[i], down_ref.at[i], pass_send.at[1], down_recv.at[i], g.me).wait_recv()
            send(down_ref.at[i], stage_ref.at[1, 2 * i + 1], pass_send.at[1], stage_recv.at[1, 2 * i + 1], g.near(-1, 0)).start()

        for i in range(2):
            when_source(g.row - 1, lambda i=i: up(1 - i))
            when_source(g.row + 1, lambda i=i: down(i))
        for drow, dcols in last:
            issue(drow, dcols)
        when_source(g.row, lambda: pass_row(0))

    wait_rows(heads, g.me, got_ref, row_send.at[0], row_recv.at[0])
    swap(got_ref, swapped_ref, row_send.at[1], row_recv.at[1], g.partner)
    place(n, heads, g.part, got_ref, swapped_ref, q_out_ref, True)

    def arrived(o, dcol):
        def body():
            send(stage_ref.at[o - 1, dcol], stage_ref.at[o - 1, dcol], y_send.at[0], stage_recv.at[o - 1, dcol], g.me).wait_recv()
            along_row(o, dcol)
        when_source(g.row - o, body)

    if g.ties:
        for o, d in ((1, 2), (3, 2), (1, 1), (3, 3)):
            arrived(o, d)
        for o in g.direct:
            when_source(g.row - o, lambda o=o: pass_row(o))
        for d in (2, 1, 0, 3):
            arrived(2, d)
        when_source(g.row - 2, lambda: pass_row(2))
        for o, d in ((1, 3), (3, 1), (1, 0), (3, 0)):
            arrived(o, d)
    else:
        for d in (1, 0):
            arrived(1, d)

    def sent(sem, ref):
        send(ref, ref, sem, out_recv, g.me).wait_send()

    def mine():
        for drow in range(1, side):
            sent(y_send.at[drow - 1], stage_ref.at[0])
    when_source(g.row, mine)
    for o in range(side):
        def passed(o=o):
            sent(x_send.at[o], kv_out_ref.at[pl.ds(0, g.parts * side - 1)])
            if g.ties:
                sent(fwd_send.at[o], kv_out_ref.at[pl.ds(0, 2)])
        when_source(g.row - o, passed)
    if g.ties:
        when_source(g.row - 1, lambda: sent(pass_send.at[0], up_ref))
        when_source(g.row + 1, lambda: sent(pass_send.at[1], down_ref))
    blocks = source_rows * side * g.parts
    others = kv_out_ref.at[pl.ds(0, blocks - source_rows)]
    send(others, others, y_send.at[0], out_recv, g.me).wait_recv()


def row_scratch(heads, q_rows, hd):
    return [pltpu.VMEM((heads, q_rows // 2, 2 * hd), BF16)] * 3


def dma(*dims):
    return pltpu.SemaphoreType.DMA(dims)


def exchange(n, heads, source_rows, collective_id, memory, dec_in, grad_out, gain, wk_t, wv_t, wq_t):
    m_rows, q_rows, hd = memory.shape[0], dec_in.shape[0], wk_t.shape[1]
    side, parts = math.isqrt(heads), n // heads
    half = m_rows // parts
    chunk = lambda *lead: pltpu.VMEM(lead + (m_rows, 2 * hd), BF16)
    block = lambda *lead: pltpu.VMEM(lead + (half, 2 * hd), BF16)
    return pl.pallas_call(
        functools.partial(exchange_kernel, n, heads, source_rows),
        out_shape=[shape((n, half, 2 * hd), BF16), shape((n, q_rows, 2 * hd), BF16), shape((q_rows, 2 * dec_in.shape[1]), BF16)],
        in_specs=vmem(7),
        out_specs=vmem(3),
        scratch_shapes=[chunk(heads), chunk(side - 1, side), chunk(2), chunk(2), block(side), block(side)]
        + row_scratch(heads, q_rows, hd)
        + [dma(2), dma(2), dma(side - 1), dma(2), dma(side), dma(side), dma(side - 1, side), dma(2), dma(2), dma(side), dma(side),
           pltpu.SemaphoreType.DMA],
        compiler_params=remote(collective_id),
        name='exchange',
    )(memory, dec_in, grad_out, gain, wk_t, wv_t, wq_t)


def return_kernel(n, heads, source_rows, src_ref, dq_ref, dst_ref, rows_ref, stage_ref, right_ref, left_ref, up_ref, down_ref,
                  theirs_ref, packed_ref, got_ref, row_send, row_recv,
                  x_send, fwd_send, y_send, pass_send, stage_recv, right_recv, left_recv, up_recv, down_recv, out_recv):
    g = Grid(n, heads, source_rows)
    side = g.side
    half = src_ref.shape[1]
    meet(g.peers())
    mine = pl.ds(pl.multiple_of(g.part * half, half), half)

    def landing(drow, dcol, head_col):
        if drow == 0:
            return dst_ref.at[g.row * side + head_col, mine], out_recv
        return stage_ref.at[drow - 1, dcol, mine], stage_recv.at[drow - 1, dcol]

    def along_row(drow, dcol):
        row = g.wrap(g.row + drow)
        col = g.wrap(g.col + dcol)
        for part in range(g.parts):
            source = src_ref.at[g.device(row, col, part)]
            if dcol in g.direct:
                dst, sem = landing(drow, dcol, g.col)
                send(source, dst, x_send.at[drow], sem, g.near(0, g.hop(dcol), part)).start()
            elif part == 0:
                send(source, right_ref.at[drow], x_send.at[drow], right_recv.at[drow], g.near(0, 1)).start()
            else:
                send(source, left_ref.at[drow], x_send.at[drow], left_recv.at[drow], g.near(0, -1)).start()

    def own_chip(drow):
        row = g.wrap(g.row + drow)
        away = src_ref.at[g.device(row, g.col, g.parts - 1 - g.part)]
        dst, sem = landing(drow, 0, g.col)
        dst[...] = src_ref[g.device(row, g.col, g.part)]
        send(away, dst, x_send.at[drow], sem, g.partner).start()

    def pass_row(drow):
        for ref, come_sem, come in ((right_ref, right_recv, -1), (left_ref, left_recv, 1)):
            send(ref.at[drow], ref.at[drow], fwd_send.at[drow], come_sem.at[drow], g.me).wait_recv()
            dst, sem = landing(drow, 2, g.wrap(g.col + come))
            send(ref.at[drow], dst, fwd_send.at[drow], sem, g.near(0, -come, 0 if come < 0 else 1)).start()

    def along_column(drow, dcol):
        chunk = stage_ref.at[drow - 1, dcol]
        got = chunk.at[pl.ds(0, half)] if dcol == 0 else chunk
        send(got, got, y_send.at[drow - 1], stage_recv.at[drow - 1, dcol], g.me).wait_recv()
        head = g.row * side + g.wrap(g.col - dcol)
        if drow in g.direct:
            send(chunk, dst_ref.at[head], y_send.at[drow - 1], out_recv, g.near(g.hop(drow), 0)).start()
        elif dcol % 2 == 0:
            send(chunk, up_ref.at[dcol // 2], y_send.at[drow - 1], up_recv.at[dcol // 2], g.near(1, 0)).start()
        else:
            send(chunk, down_ref.at[dcol // 2], y_send.at[drow - 1], down_recv.at[dcol // 2], g.near(-1, 0)).start()

    def when_source(row, body):
        pl.when(g.is_source(row))(body)

    def rows_of(drow):
        def body():
            for d in (2, 1, 3) if g.ties else (1,):
                along_row(drow, d)
        when_source(g.row + drow, body)

    def relay(drow):
        when_source(g.row + drow, lambda: pass_row(drow))

    def column(drow, d):
        when_source(g.row + drow, lambda: along_column(drow, d))

    def up(i):
        def body():
            send(up_ref.at[i], up_ref.at[i], pass_send.at[0], up_recv.at[i], g.me).wait_recv()
            head = g.wrap(g.row - 1) * side + g.wrap(g.col - 2 * i)
            send(up_ref.at[i], dst_ref.at[head], pass_send.at[0], out_recv, g.near(1, 0)).start()
        when_source(g.row + 1, body)

    def down(i):
        def body():
            send(down_ref.at[i], down_ref.at[i], pass_send.at[1], down_recv.at[i], g.me).wait_recv()
            head = g.wrap(g.row + 1) * side + g.wrap(g.col - 2 * i - 1)
            send(down_ref.at[i], dst_ref.at[head], pass_send.at[1], out_recv, g.near(-1, 0)).start()
        when_source(g.row - 1, body)

    def start_dq():
        swap(dq_ref, theirs_ref, row_send.at[0], row_recv.at[0], g.partner)
        total = (dq_ref[...] + theirs_ref[...]).T.astype(BF16)
        packed_ref[...] = pack(total.reshape(n, total.shape[0] // n, total.shape[1]))
        start_rows(n, heads, g.me, g.part, packed_ref, lambda peer: peer, got_ref, row_send.at[1], row_recv.at[1])

    for drow in (2, 1, 3, 0) if g.ties else (1, 0):
        when_source(g.row + drow, lambda drow=drow: own_chip(drow))
    if g.ties:
        rows_of(2)
        rows_of(1)
        for drow in (2, 1, 3):
            column(drow, 0)
        start_dq()
        relay(2)
        rows_of(3)
        relay(1)
        column(2, 1)
        column(2, 3)
        column(2, 2)
        up(0)
        down(0)
        rows_of(0)
        column(1, 1)
        column(1, 3)
        relay(3)
        column(1, 2)
        up(1)
        down(1)
        relay(0)
        column(3, 1)
        column(3, 3)
        column(3, 2)
    else:
        rows_of(1)
        rows_of(0)
        start_dq()
        column(1, 0)
        column(1, 1)
    wait_rows(heads, g.me, got_ref, row_send.at[1], row_recv.at[1])
    rows_ref[...] = unpack(got_ref[...])

    def sent(sem, ref):
        send(ref, ref, sem, out_recv, g.me).wait_send()

    for drow in range(side):
        def done(drow=drow):
            sent(x_send.at[drow], src_ref.at[pl.ds(0, g.parts * side - 1)])
            if g.ties:
                sent(fwd_send.at[drow], src_ref.at[pl.ds(0, 2)])
            if drow:
                sent(y_send.at[drow - 1], stage_ref.at[0])
        when_source(g.row + drow, done)
    if g.ties:
        when_source(g.row + 1, lambda: sent(pass_send.at[0], up_ref))
        when_source(g.row - 1, lambda: sent(pass_send.at[1], down_ref))

    @pl.when(g.is_source(g.row))
    def _():
        blocks = src_ref.at[pl.ds(0, n - 1)]
        send(blocks, blocks, y_send.at[0], out_recv, g.me).wait_recv()

    @pl.when(jnp.logical_not(g.is_source(g.row)))
    def _():
        def clear(index, carry):
            dst_ref[index] = jnp.zeros(dst_ref.shape[1:], dst_ref.dtype)
            return carry
        lax.fori_loop(0, heads, clear, 0)


def return_blocks(n, heads, source_rows, collective_id, blocks, dq):
    half, width = blocks.shape[1], blocks.shape[2]
    hd, total_q = dq.shape
    q_rows = total_q // n
    side, parts = math.isqrt(heads), n // heads
    chunk = lambda *lead: pltpu.VMEM(lead + (half * parts, width), BF16)
    block = lambda *lead: pltpu.VMEM(lead + (half, width), BF16)
    return pl.pallas_call(
        functools.partial(return_kernel, n, heads, source_rows),
        out_shape=[shape((heads, half * parts, width), BF16), shape((heads, q_rows, hd), BF16)],
        in_specs=vmem(2),
        out_specs=vmem(2),
        scratch_shapes=[chunk(side - 1, side), block(side), block(side), chunk(2), chunk(2), pltpu.VMEM(dq.shape, F32),
                        pltpu.VMEM((n, q_rows // 2, 2 * hd), BF16), pltpu.VMEM((heads, q_rows // 2, 2 * hd), BF16), dma(2), dma(2),
                        dma(side), dma(side), dma(side - 1), dma(2), dma(side - 1, side), dma(side), dma(side), dma(2), dma(2),
                        pltpu.SemaphoreType.DMA],
        compiler_params=remote(collective_id),
        name='return_blocks',
    )(blocks, dq)


def decoder_kernel(n, heads, mine_ref, dec_ref, gout_ref, gain_ref, wo_hbm, wg_hbm, wu_hbm, wd_hbm,
                   out_ref, lse_ref, do_ref, factors_ref, gh_ref, gnorm_ref,
                   theirs_ref, packed_ref, got_ref, sent_ref, back_ref, swapped_ref, wo_ref, wg_ref, wu_ref, wd_ref,
                   load_sem, send_sem, recv_sem):
    me = lax.axis_index('seq')
    part = lax.rem(me, n // heads)
    partner, peers = pair_peers(n, heads, me, part)
    q_rows, dim = dec_ref.shape
    hd = out_ref.shape[0]
    loads = [pltpu.make_async_copy(src, dst, load_sem.at[i]) for i, (src, dst) in enumerate(
        ((wd_hbm, wd_ref), (wo_hbm, wo_ref), (wg_hbm, wg_ref), (wu_hbm, wu_ref)))]
    for load in loads:
        load.start()
    meet(peers)

    swap(mine_ref, theirs_ref, send_sem.at[0], recv_sem.at[0], partner)
    m_a, m_b = mine_ref[hd + 8:hd + 9], theirs_ref[hd + 8:hd + 9]
    top = jnp.maximum(m_a, m_b)
    s_a, s_b = jnp.exp2(m_a - top), jnp.exp2(m_b - top)
    den = mine_ref[hd:hd + 1] * s_a + theirs_ref[hd:hd + 1] * s_b
    out = (mine_ref[:hd] * s_a + theirs_ref[:hd] * s_b) / den
    packed_ref[...] = pack(out.T.astype(BF16).reshape(n, q_rows, hd))
    start_rows(n, heads, me, part, packed_ref, lambda peer: peer, got_ref, send_sem.at[1], recv_sem.at[1])
    out_ref[...] = out
    lse_ref[...] = top + jnp.log2(den)

    loads[0].wait()
    grad_act = dot_nt(gout_ref[...].astype(BF16), wd_ref[...])
    wait_rows(heads, me, got_ref, send_sem.at[1], recv_sem.at[1])

    attended = jnp.concatenate([unpack(got_ref[h]) for h in range(heads)], axis=1)
    loads[1].wait()
    hidden = (dec_ref[...].astype(F32) + dot(attended, wo_ref[...])).astype(BF16).astype(F32)
    gain = gain_ref[...].astype(F32)
    inverse = lax.rsqrt(jnp.mean(hidden * hidden, axis=-1, keepdims=True) + 1e-6)
    scaled = hidden * inverse
    normed = (scaled * gain).astype(BF16)
    loads[2].wait()
    gate = dot(normed, wg_ref[...])
    loads[3].wait()
    up = dot(normed, wu_ref[...])
    sig = jax.nn.sigmoid(gate)
    silu = gate * sig
    grad_gate = (grad_act * up * (sig + silu * (1.0 - sig))).astype(BF16)
    grad_up = (grad_act * silu).astype(BF16)
    grad_normed = (dot_nt(wg_ref[...], grad_gate) + dot_nt(wu_ref[...], grad_up)).T
    gnorm_ref[...] = jnp.sum(grad_normed * scaled, axis=0, keepdims=True)
    inner = grad_normed * gain
    grad_hidden = gout_ref[...] + inverse * (inner - scaled * jnp.mean(inner * scaled, axis=-1, keepdims=True))
    rounded = grad_hidden.astype(BF16)
    grad_att = dot_nt(wo_ref[...], rounded).T.astype(BF16)
    for h in range(heads):
        sent_ref[h] = pack(grad_att[:, hd * h:hd * (h + 1)])
    factors_ref[:, :dim] = attended
    factors_ref[:, dim:] = rounded
    gh_ref[...] = grad_hidden

    start_rows(n, heads, me, part, sent_ref, lambda peer: peer // (n // heads), back_ref, send_sem.at[2], recv_sem.at[2])
    wait_rows(heads, me, back_ref, send_sem.at[2], recv_sem.at[2])
    swap(back_ref, swapped_ref, send_sem.at[3], recv_sem.at[3], partner)
    place(n, heads, part, back_ref, swapped_ref, do_ref, False)


def decoder_rows(n, heads, collective_id, mine, dec_in, grad_out, gain, wo, w_gate, w_up, w_down):
    q_rows, dim = dec_in.shape
    hd, total_q = wo.shape[0] // heads, mine.shape[1]
    hbm = pl.BlockSpec(memory_space=pl.ANY)
    return pl.pallas_call(
        functools.partial(decoder_kernel, n, heads),
        out_shape=[shape((hd, total_q), F32), shape((1, total_q), F32), shape((n, q_rows, 2 * hd), BF16),
                   shape((q_rows, 2 * dim), BF16), shape((q_rows, dim), F32), shape((1, dim), F32)],
        in_specs=vmem(4) + [hbm] * 4,
        out_specs=vmem(6),
        scratch_shapes=[pltpu.VMEM(mine.shape, F32), pltpu.VMEM((n, q_rows // 2, 2 * hd), BF16)]
        + [pltpu.VMEM((heads, q_rows // 2, 2 * hd), BF16)] * 4
        + [pltpu.VMEM(w.shape, BF16) for w in (wo, w_gate, w_up, w_down)] + [dma(4), dma(4), dma(4)],
        compiler_params=remote(collective_id),
        name='decoder_rows',
    )(mine, dec_in, grad_out, gain, wo, w_gate, w_up, w_down)


def small_sum_kernel(n, mine_ref, total_ref, all_ref, send_sem, recv_sem):
    me = lax.axis_index('seq')
    meet([lax.rem(me + step, n) for step in range(1, n)])
    for step in range(1, n):
        send(mine_ref, all_ref.at[me], send_sem, recv_sem, lax.rem(me + step, n)).start()
    all_ref[me] = mine_ref[...]
    others = all_ref.at[pl.ds(0, n - 1)]
    whole = send(others, others, send_sem, recv_sem, me)
    whole.wait_send()
    whole.wait_recv()
    total_ref[...] = jnp.sum(all_ref[...], axis=0)


def small_sum(n, collective_id, mine):
    return pl.pallas_call(
        functools.partial(small_sum_kernel, n),
        out_shape=shape(mine.shape, F32),
        in_specs=vmem(1),
        out_specs=vmem(1)[0],
        scratch_shapes=[pltpu.VMEM((n,) + mine.shape, F32), pltpu.SemaphoreType.DMA, pltpu.SemaphoreType.DMA],
        compiler_params=remote(collective_id),
        name='small_sum',
    )(mine)


def valid_blocks(mem_len, rows, parts, sources):
    reach = mem_len - lax.rem(lax.axis_index('seq'), parts) * rows
    blocks = jnp.minimum((reach + parts * rows - 1) // (parts * rows), sources)
    return blocks, jnp.minimum(reach - (blocks - 1) * parts * rows, rows)


def forward_kernel(scale, hd, parts, q_block, len_ref, kv_ref, q_ref, out_ref, qt_ref, top_ref):
    rows, total_q = kv_ref.shape[1], q_ref.shape[0]
    blocks, last_valid = valid_blocks(len_ref[0], rows, parts, kv_ref.shape[0])
    groups = [slice(first, first + q_block) for first in range(0, total_q, q_block)]
    base = slice(hd + 8, hd + 9)
    qt_ref[...] = q_ref[...].T

    def values_of(keys):
        return jnp.concatenate([keys.T[hd:], jnp.ones((16, rows), keys.dtype)], axis=0)

    def group_of(index):
        return pl.ds(pl.multiple_of(index * q_block, q_block), q_block)

    def first_step(group, carry):
        cols = group_of(group)
        top = jnp.max(dot(kv_ref[0], qt_ref[:, cols]), axis=0, keepdims=True)
        out_ref[hd + 8:, cols] = jnp.broadcast_to(top * scale, (8, q_block))
        top_ref[:, cols] = jnp.broadcast_to(top, (8, q_block))
        return carry

    lax.fori_loop(0, len(groups), first_step, 0)
    out_ref[:hd + 8, :] = jnp.zeros((hd + 8, total_q), F32)

    def finish(values, scores, cols):
        top_ref[:, cols] = jnp.maximum(top_ref[:, cols], jnp.max(scores.reshape(rows // 8, 8, q_block), axis=0))
        weights = jnp.exp2(scores * scale - out_ref[base, cols]).astype(values.dtype)
        out_ref[:hd + 8, cols] += dot(values, weights)[:hd + 8]

    def step(index, carry):
        keys = kv_ref[index]
        values = values_of(keys)
        for cols in groups:
            finish(values, dot(keys, qt_ref[:, cols]), cols)
        return carry

    def last_step(group, carry):
        cols = group_of(group)
        keys = kv_ref[blocks - 1]
        scores = dot(keys, qt_ref[:, cols])
        position = lax.broadcasted_iota(jnp.int32, scores.shape, 0)
        finish(values_of(keys), jnp.where(position < last_valid, scores, NEG), cols)
        return carry

    lax.fori_loop(0, blocks - 1, step, 0)
    lax.fori_loop(0, len(groups), last_step, 0)

    excess = jnp.max(top_ref[...] * scale - out_ref[hd + 8:, :])

    @pl.when(excess > 16.0)
    def _():
        out_ref[:hd + 8, :] = jnp.zeros((hd + 8, total_q), F32)
        out_ref[hd + 8:, :] = jnp.full((8, total_q), NEG, F32)

        def running(step_index, carry):
            index, group = step_index // len(groups), lax.rem(step_index, len(groups))
            cols = group_of(group)
            keys = kv_ref[index]
            limit = jnp.where(index == blocks - 1, last_valid, rows)
            scores = dot(keys, qt_ref[:, cols]) * scale
            position = lax.broadcasted_iota(jnp.int32, scores.shape, 0)
            scores = jnp.where(position < limit, scores, NEG)
            old = out_ref[base, cols]
            new = jnp.maximum(old, jnp.max(scores, axis=0, keepdims=True))
            weights = jnp.exp2(scores - new).astype(keys.dtype)
            out_ref[:hd + 8, cols] = out_ref[:hd + 8, cols] * jnp.exp2(old - new) + dot(values_of(keys), weights)[:hd + 8]
            out_ref[hd + 8:, cols] = jnp.broadcast_to(new, (8, q_block))
            return carry

        lax.fori_loop(0, blocks * len(groups), running, 0)


def attention_forward(scale, hd, parts, sources, mem_len, kv, q):
    rows, width = kv.shape[1], kv.shape[2]
    total_q = q.shape[0]
    return pl.pallas_call(
        functools.partial(forward_kernel, scale, hd, parts, min(1024, total_q)),
        out_shape=shape((hd + 16, total_q), F32),
        grid=(1,),
        in_specs=[pl.BlockSpec(memory_space=pltpu.SMEM),
                  pl.BlockSpec((sources, rows, width), lambda i: (0, 0, 0), pipeline_mode=pl.Buffered(1)), full(q)],
        out_specs=pl.BlockSpec((hd + 16, total_q), lambda i: (0, 0)),
        scratch_shapes=[pltpu.VMEM((width, total_q), BF16), pltpu.VMEM((8, total_q), F32)],
        compiler_params=plain(),
        cost_estimate=pl.CostEstimate(flops=4 * total_q * sources * rows * hd, bytes_accessed=kv.size * 2,
                                      transcendentals=total_q * sources * rows),
        name='attention_forward',
    )(mem_len, kv, q)


def backward_kernel(scale, key_scale, hd, parts, q_block, len_ref, kv_ref, q_ref, do_ref, out_ref, lse_ref, dkv_ref, dq_ref,
                    qt_ref, dot_ref, delta_ref):
    rows, total_q = kv_ref.shape[1], q_ref.shape[0]
    blocks, last_valid = valid_blocks(len_ref[0], rows, parts, kv_ref.shape[0])
    width = kv_ref.shape[2]
    groups = [slice(first, first + q_block) for first in range(0, total_q, q_block)]
    dq_ref[...] = jnp.zeros_like(dq_ref)
    qt_ref[...] = q_ref[...].T
    do_t = do_ref[...].T
    dot_ref[...] = do_t
    delta_ref[...] = jnp.sum(do_t[hd:].astype(F32) * out_ref[...], axis=0, keepdims=True)

    lane_scale = jnp.where(lax.broadcasted_iota(jnp.int32, (1, width), 1) < hd, key_scale, 1.0)

    def products(keys, cols):
        return dot(keys, qt_ref[:, cols]), dot(keys, dot_ref[:, cols])

    def finish(keys, keys_t, scores, grads, cols, valid):
        prob = jnp.exp2(scores * scale - lse_ref[:, cols])
        if valid is not None:
            position = lax.broadcasted_iota(jnp.int32, scores.shape, 0)
            prob = jnp.where(position < valid, prob, 0.0)
        grad_scores = (prob * (grads - delta_ref[:, cols])).astype(keys.dtype)
        update = dot(grad_scores, q_ref[cols, :]) + dot(prob.astype(keys.dtype), do_ref[cols, :])
        dq_ref[:, cols] += dot(keys_t, grad_scores)
        return update

    def step(index, carry):
        keys = kv_ref[index]
        keys_t = keys.T[:hd]
        total = jnp.zeros((rows, width), F32)
        for cols in groups:
            scores, grads = products(keys, cols)
            total += finish(keys, keys_t, scores, grads, cols, None)
        dkv_ref[index] = (total * lane_scale).astype(dkv_ref.dtype)
        return carry

    def last_step(group, total):
        keys = kv_ref[blocks - 1]
        cols = pl.ds(pl.multiple_of(group * q_block, q_block), q_block)
        scores, grads = products(keys, cols)
        return total + finish(keys, keys.T[:hd], scores, grads, cols, last_valid)

    def clear(index, carry):
        dkv_ref[index] = jnp.zeros((rows, width), dkv_ref.dtype)
        return carry

    lax.fori_loop(0, blocks - 1, step, 0)
    total = lax.fori_loop(0, len(groups), last_step, jnp.zeros((rows, width), F32))
    dkv_ref[blocks - 1] = (total * lane_scale).astype(dkv_ref.dtype)
    lax.fori_loop(blocks, dkv_ref.shape[0], clear, 0)
    dq_ref[...] = dq_ref[...] * key_scale


def attention_backward(scale, key_scale, hd, parts, sources, mem_len, kv, q, do, out_t, lse):
    n, rows, width = kv.shape
    total_q = q.shape[0]
    return pl.pallas_call(
        functools.partial(backward_kernel, scale, key_scale, hd, parts, min(512, total_q)),
        out_shape=[shape((n, rows, width), BF16), shape((hd, total_q), F32)],
        grid=(1,),
        in_specs=[pl.BlockSpec(memory_space=pltpu.SMEM),
                  pl.BlockSpec((sources, rows, width), lambda i: (0, 0, 0), pipeline_mode=pl.Buffered(1)),
                  full(q), full(do), full(out_t), full(lse)],
        out_specs=[pl.BlockSpec((n, rows, width), lambda i: (0, 0, 0)),
                   pl.BlockSpec((hd, total_q), lambda i: (0, 0))],
        scratch_shapes=[pltpu.VMEM((width, total_q), BF16), pltpu.VMEM((width, total_q), BF16), pltpu.VMEM((1, total_q), F32)],
        compiler_params=plain(),
        cost_estimate=pl.CostEstimate(flops=10 * total_q * sources * rows * hd, bytes_accessed=kv.size * 4,
                                      transcendentals=total_q * sources * rows),
        name='attention_backward',
    )(mem_len, kv, q, do, out_t, lse)


def prepare_kernel(dec_ref, att_ref, wo_ref, gain_ref, n2_ref, n2t_ref):
    hidden = (dec_ref[...].astype(F32) + dot(att_ref[...], wo_ref[...])).astype(BF16)
    normed = rms_norm(hidden.astype(F32), gain_ref[...].astype(F32)).astype(BF16)
    n2_ref[...] = normed
    n2t_ref[...] = normed.T


def prepare(early, late, wo, gain):
    rows, dim = early.shape[0], wo.shape[1]
    chunk = min(512, rows)
    left = pl.BlockSpec((chunk, dim), lambda i: (i, 0))
    return pl.pallas_call(
        prepare_kernel,
        out_shape=[shape((rows, dim), BF16), shape((dim, rows), BF16)],
        grid=(rows // chunk,),
        in_specs=[left, left, full(wo), full(gain)],
        out_specs=[left, pl.BlockSpec((dim, chunk), lambda i: (0, i))],
        compiler_params=plain(),
        cost_estimate=pl.CostEstimate(flops=2 * rows * dim * dim, bytes_accessed=8 * rows * dim, transcendentals=0),
        name='prepare',
    )(early, late, wo, gain)


def mlp_kernel(chunk, n2_ref, n2t_ref, top_ref, w1_ref, w3_ref, w2_ref, g1_ref, g3_ref, g2_ref, d1_ref, d3_ref, act_ref):
    rows = n2_ref.shape[0]
    w1, w3, w2t = w1_ref[...], w3_ref[...], w2_ref[...].T
    for first in range(0, rows, chunk):
        part = slice(first, first + chunk)
        gate = dot(n2_ref[part, :], w1)
        up = dot(n2_ref[part, :], w3)
        grad = dot(top_ref[part, :], w2t)
        sig = jax.nn.sigmoid(gate)
        silu = gate * sig
        act_ref[part, :] = (silu * up).astype(act_ref.dtype)
        d3_ref[part, :] = (grad * silu).astype(d3_ref.dtype)
        d1_ref[part, :] = (grad * up * (sig + silu * (1.0 - sig))).astype(d1_ref.dtype)
    g1_ref[...] = dot(n2t_ref[...], d1_ref[...])
    g3_ref[...] = dot(n2t_ref[...], d3_ref[...])
    g2_ref[...] = dot_tn(act_ref[...], top_ref[...])


def mlp_weight_grads(n2, n2t, early, w_gate, w_up, w_down):
    rows, dim = n2.shape
    ff = w_gate.shape[1]
    tile = 256
    cols = pl.BlockSpec((dim, tile), lambda i: (0, i))
    tall = pl.BlockSpec((tile, dim), lambda i: (i, 0))
    return pl.pallas_call(
        functools.partial(mlp_kernel, min(512, rows)),
        out_shape=[shape((dim, ff), F32), shape((dim, ff), F32), shape((ff, dim), F32)],
        grid=(ff // tile,),
        in_specs=[full(n2), full(n2t), pl.BlockSpec((rows, dim), lambda i: (0, 1), pipeline_mode=pl.Buffered(1)), cols, cols, tall],
        out_specs=[cols, cols, tall],
        scratch_shapes=[pltpu.VMEM((rows, tile), BF16)] * 3,
        compiler_params=plain(),
        cost_estimate=pl.CostEstimate(flops=12 * rows * dim * ff, bytes_accessed=18 * dim * ff, transcendentals=rows * ff),
        name='mlp_weight_grads',
    )(n2, n2t, early, w_gate, w_up, w_down)


def memory_weight_kernel(memory_ref, dkv_ref, dec_ref, gain_ref, dq_ref, gk_ref, gv_ref, gq_ref):
    group, hd = dkv_ref.shape[0], dkv_ref.shape[2] // 2
    normed = rms_norm(dec_ref[...].astype(F32), gain_ref[...].astype(F32)).astype(BF16)
    for i in range(group):
        rows = slice(i * hd, (i + 1) * hd)
        both = dot_tn(dkv_ref[i], memory_ref[...])
        gk_ref[rows, :] = both[:hd]
        gv_ref[rows, :] = both[hd:]
        gq_ref[rows, :] = dot_tn(dq_ref[i], normed)


def memory_weight_grads(memory, dkv, dec_in, gain, dq_rows):
    heads, rows, width = dkv.shape
    dim, hd = memory.shape[1], width // 2
    group = 2
    out = pl.BlockSpec((group * hd, dim), lambda i: (i, 0))
    return pl.pallas_call(
        memory_weight_kernel,
        out_shape=[shape((heads * hd, dim), F32)] * 3,
        grid=(heads // group,),
        in_specs=[full(memory), pl.BlockSpec((group, rows, width), lambda i: (i, 0, 0)), full(dec_in), full(gain),
                  pl.BlockSpec((group,) + dq_rows.shape[1:], lambda i: (i, 0, 0))],
        out_specs=[out, out, out],
        compiler_params=plain(),
        cost_estimate=pl.CostEstimate(flops=2 * rows * dim * heads * width, bytes_accessed=16 * rows * dim, transcendentals=0),
        name='memory_weight_grads',
    )(memory, dkv, dec_in, gain, dq_rows)


def memory_grad_kernel(dkv_ref, wk_ref, wv_ref, out_ref):
    group = dkv_ref.shape[0]
    left = jnp.concatenate([dkv_ref[i] for i in range(group)], axis=1)
    right = jnp.concatenate([part[i] for i in range(group) for part in (wk_ref, wv_ref)], axis=0)

    @pl.when(pl.program_id(0) == 0)
    def _():
        out_ref[...] = dot(left, right)

    @pl.when(pl.program_id(0) > 0)
    def _():
        out_ref[...] += dot(left, right)


def memory_grad(dkv, wk_t, wv_t):
    heads, rows, width = dkv.shape
    hd, dim = wk_t.shape[1], wk_t.shape[2]
    group = 4
    weight = pl.BlockSpec((group, hd, dim), lambda i: (i, 0, 0))
    return pl.pallas_call(
        memory_grad_kernel,
        out_shape=shape((rows, dim), F32),
        grid=(heads // group,),
        in_specs=[pl.BlockSpec((group, rows, width), lambda i: (i, 0, 0)), weight, weight],
        out_specs=pl.BlockSpec((rows, dim), lambda i: (0, 0)),
        compiler_params=plain(),
        cost_estimate=pl.CostEstimate(flops=2 * rows * dim * heads * width, bytes_accessed=12 * rows * dim, transcendentals=0),
        name='memory_grad',
    )(dkv, wk_t, wv_t)


def outer_kernel(att_ref, gh_ref, out_ref):
    @pl.when(pl.program_id(0) == 0)
    def _():
        out_ref[...] = jnp.zeros_like(out_ref)

    out_ref[...] += dot_tn(att_ref[...], gh_ref[...])


def outer_weight_grad(late, dim):
    rows = late.shape[0]
    chunk = min(512, rows)
    return pl.pallas_call(
        outer_kernel,
        out_shape=shape((dim, dim), F32),
        grid=(rows // chunk,),
        in_specs=[pl.BlockSpec((chunk, dim), lambda i: (i, 0)), pl.BlockSpec((chunk, dim), lambda i: (i, 1))],
        out_specs=pl.BlockSpec((dim, dim), lambda i: (0, 0)),
        compiler_params=plain(),
        cost_estimate=pl.CostEstimate(flops=2 * rows * dim * dim, bytes_accessed=8 * rows * dim, transcendentals=0),
        name='outer_weight_grad',
    )(late, late)


def solution(mesh):
    n = mesh.shape['seq']
    row_spec = P(('data', 'seq'), None)
    weight_spec = P()
    part_vec = P('data')
    part_mat = P('data', None)
    part_cube = P('data', None, None)

    def device_step(dec_in, memory, mem_len, grad_out, norm_attn, wq_cross, wk_cross, wv_cross, wo_cross, norm_mlp, w_gate, w_up, w_down):
        q_rows, dim = dec_in.shape
        heads, hd = wq_cross.shape[1], wq_cross.shape[2]
        parts = n // heads
        sources = -(-3 * n // 4)
        total_q = q_rows * n
        key_scale = hd ** -0.5
        scale = key_scale * LOG2E
        wq_t, wk_t, wv_t = (jnp.transpose(w, (1, 2, 0)) for w in (wq_cross, wk_cross, wv_cross))
        source_rows = -(-sources // (parts * math.isqrt(heads)))
        kv, q_in, early_local = exchange(n, heads, source_rows, 0, memory, dec_in, grad_out, norm_attn, wk_t, wv_t, wq_t)
        head_q = q_in.reshape(total_q, 2 * hd)

        early = lax.all_gather(early_local, 'seq', axis=0, tiled=True)

        wo = wo_cross.reshape(heads * hd, dim)
        mine = attention_forward(scale, hd, parts, sources, mem_len, kv, head_q)
        out_t, lse, do_in, factors, grad_hidden, g_norm_mlp = decoder_rows(
            n, heads, 1, mine, dec_in, grad_out, norm_mlp, wo, w_gate, w_up, w_down)
        do_in, factors, early = lax.optimization_barrier((do_in, factors, early))
        late = lax.all_gather(factors, 'seq', axis=0, tiled=True)

        dkv, dq_part = attention_backward(scale, key_scale, hd, parts, sources, mem_len, kv, head_q, do_in.reshape(total_q, 2 * hd), out_t, lse)
        dkv_in, dq_rows = return_blocks(n, heads, source_rows, 4, dkv, dq_part)
        dkv_in, dq_rows, late = lax.optimization_barrier((dkv_in, dq_rows, late))

        sums = memory_weight_grads(memory, dkv_in, dec_in, norm_attn, dq_rows)
        *sums, dkv_in, dq_rows, early, late = lax.optimization_barrier((*sums, dkv_in, dq_rows, early, late))
        g_wk, g_wv, g_wq = lax.psum(tuple(sums), 'seq')

        n2_all, n2_all_t = prepare(early, late, wo, norm_mlp)
        g_gate, g_up, g_down = mlp_weight_grads(n2_all, n2_all_t, early, w_gate, w_up, w_down)
        g_wo = outer_weight_grad(late, dim)

        grad_normed = jnp.einsum('hte,dhe->td', dq_rows, wq_cross, preferred_element_type=F32)
        _, norm_pull = jax.vjp(rms_norm, dec_in.astype(F32), norm_attn.astype(F32))
        grad_x_norm, g_norm_attn = norm_pull(grad_normed)
        g_dec = grad_hidden + grad_x_norm
        norms = small_sum(n, 5, jnp.concatenate([g_norm_attn, g_norm_mlp[0]]).reshape(-1, 128)).reshape(2, dim)
        g_mem = memory_grad(dkv_in, wk_t, wv_t)
        cube = lambda g: jnp.transpose(g.reshape(heads, hd, dim), (2, 0, 1))
        return (g_dec, g_mem, norms[0], cube(g_wq), cube(g_wk), cube(g_wv), g_wo.reshape(heads, hd, dim), norms[1], g_gate, g_up, g_down)

    return jax.shard_map(device_step, mesh=mesh,
                         in_specs=(row_spec, row_spec, part_vec, row_spec) + (weight_spec,) * 9,
                         out_specs=(row_spec, row_spec, part_vec, part_cube, part_cube, part_cube, part_cube, part_vec, part_mat, part_mat, part_mat),
                         check_vma=False)
```

```python
import functools
import math

import jax
import jax.numpy as jnp
from jax import lax
from jax.experimental import pallas as pl
from jax.experimental.pallas import tpu as pltpu
from jax.sharding import PartitionSpec as P

LOG2E = 1.4426950408889634
NEG = -1e30
VMEM_LIMIT = 60 * 1024 * 1024
MESH = pl.DeviceIdType.MESH
BF16, F32 = jnp.bfloat16, jnp.float32


def rms_norm(tensor, gain):
    mean_sq = jnp.mean(tensor * tensor, axis=-1, keepdims=True)
    return tensor * lax.rsqrt(mean_sq + 1e-6) * gain


def dot(a, b):
    return jnp.dot(a, b, preferred_element_type=F32)


def dot_nt(a, b):
    return lax.dot_general(a, b, (((1,), (1,)), ((), ())), preferred_element_type=F32)


def dot_tn(a, b):
    return lax.dot_general(a, b, (((0,), (0,)), ((), ())), preferred_element_type=F32)


def full(array):
    return pl.BlockSpec(array.shape, lambda *_: (0,) * array.ndim, pipeline_mode=pl.Buffered(1))


def vmem(count):
    return [pl.BlockSpec(memory_space=pltpu.VMEM)] * count


def plain():
    return pltpu.CompilerParams(vmem_limit_bytes=VMEM_LIMIT)


def remote(collective_id):
    return pltpu.CompilerParams(collective_id=collective_id, has_side_effects=True, vmem_limit_bytes=VMEM_LIMIT)


def shape(dims, dtype):
    return jax.ShapeDtypeStruct(dims, dtype)


def meet(peers):
    barrier = pltpu.get_barrier_semaphore()
    for peer in peers:
        pl.semaphore_signal(barrier, inc=1, device_id={'seq': peer}, device_id_type=MESH)
    pl.semaphore_wait(barrier, len(peers))


def send(src, dst, send_sem, recv_sem, peer):
    return pltpu.make_async_remote_copy(src_ref=src, dst_ref=dst, send_sem=send_sem, recv_sem=recv_sem,
                                        device_id={'seq': peer}, device_id_type=MESH)


class Grid:
    def __init__(self, n, heads, source_rows):
        self.n, self.heads, self.source_rows = n, heads, source_rows
        self.parts = n // heads
        self.side = math.isqrt(heads)
        self.me = lax.axis_index('seq')
        self.part = lax.rem(self.me, self.parts)
        self.chip = self.me // self.parts
        self.col = lax.rem(self.chip, self.side)
        self.row = self.chip // self.side
        self.partner = self.chip * self.parts + (self.parts - 1 - self.part)
        self.ties = self.side == 4
        self.direct = (1, 3) if self.ties else (1,)

    def wrap(self, value):
        return lax.rem(value + self.side, self.side)

    def device(self, row, col, part):
        return (row * self.side + col) * self.parts + part

    def near(self, drow, dcol, part=None):
        return self.device(self.wrap(self.row + drow), self.wrap(self.col + dcol), self.part if part is None else part)

    def hop(self, offset):
        return 1 if offset == 1 else -1

    def is_source(self, row):
        return self.wrap(row) < self.source_rows

    def row_peers(self):
        return [lax.rem(self.chip + step, self.heads) * self.parts + self.part for step in range(1, self.heads)]

    def peers(self):
        return self.row_peers() + [self.partner] + [self.near(0, self.hop(d), self.parts - 1 - self.part) for d in self.direct]


def pair_peers(n, heads, me, part):
    parts = n // heads
    head = me // parts
    partner = head * parts + (parts - 1 - part)
    return partner, [partner] + [lax.rem(head + step, heads) * parts + part for step in range(1, heads)]


def pack(rows):
    middle = rows.shape[-2] // 2
    return jnp.concatenate([rows[..., :middle, :], rows[..., middle:, :]], axis=-1)


def unpack(packed):
    middle = packed.shape[-1] // 2
    return jnp.concatenate([packed[..., :middle], packed[..., middle:]], axis=-2)


def start_rows(n, heads, me, part, src, src_of, dst_ref, send_sem, recv_sem):
    parts = n // heads
    head = me // parts
    for step in range(1, heads):
        peer = lax.rem(head + step, heads) * parts + part
        send(src.at[src_of(peer)], dst_ref.at[head], send_sem, recv_sem, peer).start()
    dst_ref[head] = src[src_of(me)]


def wait_rows(heads, me, dst_ref, send_sem, recv_sem):
    others = dst_ref.at[pl.ds(0, heads - 1)]
    whole = send(others, others, send_sem, recv_sem, me)
    whole.wait_send()
    whole.wait_recv()


def swap(src, dst, send_sem, recv_sem, partner):
    copy = send(src, dst, send_sem, recv_sem, partner)
    copy.start()
    copy.wait()


def place(n, heads, part, mine_ref, theirs_ref, wide_ref, low):
    parts = n // heads
    for source, index in ((mine_ref, part), (theirs_ref, parts - 1 - part)):
        for head in range(heads):
            rows = unpack(source[head])
            zeros = jnp.zeros_like(rows)
            wide_ref[head * parts + index] = jnp.concatenate([rows, zeros] if low else [zeros, rows], axis=-1)


def exchange_kernel(n, heads, source_rows, memory_ref, dec_ref, gout_ref, gain_ref, wk_ref, wv_ref, wq_ref, kv_out_ref, q_out_ref, early_ref,
                    kv_ref, stage_ref, up_ref, down_ref, right_ref, left_ref, packed_ref, got_ref, swapped_ref,
                    row_send, row_recv, y_send, pass_send, x_send, fwd_send, stage_recv, up_recv, down_recv, right_recv,
                    left_recv, out_recv):
    g = Grid(n, heads, source_rows)
    side, hd = g.side, wk_ref.shape[1]
    half = kv_out_ref.shape[1]
    chunk_rows = min(256, kv_ref.shape[1])
    barrier = pltpu.get_barrier_semaphore()
    peers = g.peers()
    for peer in peers:
        pl.semaphore_signal(barrier, inc=1, device_id={'seq': peer}, device_id_type=MESH)

    dim = dec_ref.shape[1]
    early_ref[:, :dim] = dec_ref[...]
    early_ref[:, dim:] = gout_ref[...].astype(BF16)
    normed = rms_norm(dec_ref[...].astype(F32), gain_ref[...].astype(F32)).astype(BF16)
    for i in range(0, heads, 4):
        queries = dot_nt(normed, jnp.concatenate([wq_ref[i + j] for j in range(4)], axis=0)).astype(BF16)
        for j in range(4):
            packed_ref[i + j] = pack(queries[:, hd * j:hd * (j + 1)])

    def head(drow, dcol):
        return g.wrap(g.row + drow) * side + g.wrap(g.col + dcol)

    def project(drow, dcols):
        weights = jnp.concatenate([ref[head(drow, d)] for d in dcols for ref in (wk_ref, wv_ref)], axis=0)

        def rows(index, carry):
            at = pl.ds(pl.multiple_of(index * chunk_rows, chunk_rows), chunk_rows)
            both = dot_nt(memory_ref[at, :], weights).astype(BF16)
            for i, d in enumerate(dcols):
                kv_ref[head(drow, d), at, :] = both[:, 2 * hd * i:2 * hd * (i + 1)]
            return carry

        lax.fori_loop(0, kv_ref.shape[1] // chunk_rows, rows, 0)

    def along_column(drow, dcol):
        chunk = kv_ref.at[head(drow, dcol)]
        if drow in g.direct:
            send(chunk, stage_ref.at[drow - 1, dcol], y_send.at[drow - 1], stage_recv.at[drow - 1, dcol], g.near(g.hop(drow), 0)).start()
        elif dcol % 2 == 0:
            send(chunk, up_ref.at[dcol // 2], y_send.at[drow - 1], up_recv.at[dcol // 2], g.near(1, 0)).start()
        else:
            send(chunk, down_ref.at[dcol // 2], y_send.at[drow - 1], down_recv.at[dcol // 2], g.near(-1, 0)).start()

    def along_row(o, dcol):
        chunk = kv_ref.at[head(0, dcol)] if o == 0 else stage_ref.at[o - 1, dcol]
        source = g.device(g.wrap(g.row - o), g.col, g.part)
        if dcol == 0:
            kv_out_ref[source] = chunk[pl.ds(pl.multiple_of(g.part * half, half), half), :]
            away = pl.ds(pl.multiple_of((g.parts - 1 - g.part) * half, half), half)
            send(chunk.at[away], kv_out_ref.at[source], x_send.at[o], out_recv, g.partner).start()
        elif dcol in g.direct:
            for part in range(g.parts):
                send(chunk.at[pl.ds(part * half, half)], kv_out_ref.at[source], x_send.at[o], out_recv,
                     g.near(0, g.hop(dcol), part)).start()
        else:
            send(chunk.at[pl.ds(0, half)], right_ref.at[o], x_send.at[o], right_recv.at[o], g.near(0, 1)).start()
            send(chunk.at[pl.ds(half, half)], left_ref.at[o], x_send.at[o], left_recv.at[o], g.near(0, -1)).start()

    def pass_row(o):
        for ref, sem, come in ((right_ref, right_recv, -1), (left_ref, left_recv, 1)):
            source = g.device(g.wrap(g.row - o), g.wrap(g.col + come), g.part)
            send(ref.at[o], ref.at[o], fwd_send.at[o], sem.at[o], g.me).wait_recv()
            send(ref.at[o], kv_out_ref.at[source], fwd_send.at[o], out_recv, g.near(0, -come, 0 if come < 0 else 1)).start()

    def when_source(row, body):
        pl.when(g.is_source(row))(body)

    if g.ties:
        order = [(2, (2, 1)), (2, (3, 0)), (1, (2, 1)), (3, (2, 3)), (0, (2, 1)), (0, (3, 0))]
        last = [(1, (3, 0)), (3, (1, 0))]
    else:
        order, last = [(1, (1, 0)), (0, (1, 0))], []

    def issue(drow, dcols):
        def body():
            for d in dcols:
                along_row(0, d) if drow == 0 else along_column(drow, d)
        when_source(g.row, body)

    waiting = None
    for drow, dcols in order + last:
        project(drow, dcols)
        if waiting is None:
            pl.semaphore_wait(barrier, len(peers))
            start_rows(n, heads, g.me, g.part, packed_ref, lambda peer: peer // g.parts, got_ref, row_send.at[0], row_recv.at[0])
        elif waiting not in last:
            issue(*waiting)
        waiting = (drow, dcols)
    if not last:
        issue(*waiting)

    if g.ties:
        def up(i):
            send(up_ref.at[i], up_ref.at[i], pass_send.at[0], up_recv.at[i], g.me).wait_recv()
            send(up_ref.at[i], stage_ref.at[1, 2 * i], pass_send.at[0], stage_recv.at[1, 2 * i], g.near(1, 0)).start()

        def down(i):
            send(down_ref.at[i], down_ref.at[i], pass_send.at[1], down_recv.at[i], g.me).wait_recv()
            send(down_ref.at[i], stage_ref.at[1, 2 * i + 1], pass_send.at[1], stage_recv.at[1, 2 * i + 1], g.near(-1, 0)).start()

        for i in range(2):
            when_source(g.row - 1, lambda i=i: up(1 - i))
            when_source(g.row + 1, lambda i=i: down(i))
        for drow, dcols in last:
            issue(drow, dcols)
        when_source(g.row, lambda: pass_row(0))

    wait_rows(heads, g.me, got_ref, row_send.at[0], row_recv.at[0])
    swap(got_ref, swapped_ref, row_send.at[1], row_recv.at[1], g.partner)
    place(n, heads, g.part, got_ref, swapped_ref, q_out_ref, True)

    def arrived(o, dcol):
        def body():
            send(stage_ref.at[o - 1, dcol], stage_ref.at[o - 1, dcol], y_send.at[0], stage_recv.at[o - 1, dcol], g.me).wait_recv()
            along_row(o, dcol)
        when_source(g.row - o, body)

    if g.ties:
        for o, d in ((1, 2), (3, 2), (1, 1), (3, 3)):
            arrived(o, d)
        for o in g.direct:
            when_source(g.row - o, lambda o=o: pass_row(o))
        for d in (2, 1, 0, 3):
            arrived(2, d)
        when_source(g.row - 2, lambda: pass_row(2))
        for o, d in ((1, 3), (3, 1), (1, 0), (3, 0)):
            arrived(o, d)
    else:
        for d in (1, 0):
            arrived(1, d)

    def sent(sem, ref):
        send(ref, ref, sem, out_recv, g.me).wait_send()

    def mine():
        for drow in range(1, side):
            sent(y_send.at[drow - 1], stage_ref.at[0])
    when_source(g.row, mine)
    for o in range(side):
        def passed(o=o):
            sent(x_send.at[o], kv_out_ref.at[pl.ds(0, g.parts * side - 1)])
            if g.ties:
                sent(fwd_send.at[o], kv_out_ref.at[pl.ds(0, 2)])
        when_source(g.row - o, passed)
    if g.ties:
        when_source(g.row - 1, lambda: sent(pass_send.at[0], up_ref))
        when_source(g.row + 1, lambda: sent(pass_send.at[1], down_ref))
    blocks = source_rows * side * g.parts
    others = kv_out_ref.at[pl.ds(0, blocks - source_rows)]
    send(others, others, y_send.at[0], out_recv, g.me).wait_recv()


def row_scratch(heads, q_rows, hd):
    return [pltpu.VMEM((heads, q_rows // 2, 2 * hd), BF16)] * 3


def dma(*dims):
    return pltpu.SemaphoreType.DMA(dims)


def exchange(n, heads, source_rows, collective_id, memory, dec_in, grad_out, gain, wk_t, wv_t, wq_t):
    m_rows, q_rows, hd = memory.shape[0], dec_in.shape[0], wk_t.shape[1]
    side, parts = math.isqrt(heads), n // heads
    half = m_rows // parts
    chunk = lambda *lead: pltpu.VMEM(lead + (m_rows, 2 * hd), BF16)
    block = lambda *lead: pltpu.VMEM(lead + (half, 2 * hd), BF16)
    return pl.pallas_call(
        functools.partial(exchange_kernel, n, heads, source_rows),
        out_shape=[shape((n, half, 2 * hd), BF16), shape((n, q_rows, 2 * hd), BF16), shape((q_rows, 2 * dec_in.shape[1]), BF16)],
        in_specs=vmem(7),
        out_specs=vmem(3),
        scratch_shapes=[chunk(heads), chunk(side - 1, side), chunk(2), chunk(2), block(side), block(side)]
        + row_scratch(heads, q_rows, hd)
        + [dma(2), dma(2), dma(side - 1), dma(2), dma(side), dma(side), dma(side - 1, side), dma(2), dma(2), dma(side), dma(side),
           pltpu.SemaphoreType.DMA],
        compiler_params=remote(collective_id),
        name='exchange',
    )(memory, dec_in, grad_out, gain, wk_t, wv_t, wq_t)


def return_kernel(n, heads, source_rows, src_ref, dq_ref, dst_ref, rows_ref, dqt_ref, stage_ref, right_ref, left_ref, up_ref, down_ref,
                  theirs_ref, packed_ref, got_ref, row_send, row_recv,
                  x_send, fwd_send, y_send, pass_send, stage_recv, right_recv, left_recv, up_recv, down_recv, out_recv):
    g = Grid(n, heads, source_rows)
    side = g.side
    half = src_ref.shape[1]
    meet(g.peers())
    mine = pl.ds(pl.multiple_of(g.part * half, half), half)

    def landing(drow, dcol, head_col):
        if drow == 0:
            return dst_ref.at[g.row * side + head_col, mine], out_recv
        return stage_ref.at[drow - 1, dcol, mine], stage_recv.at[drow - 1, dcol]

    def along_row(drow, dcol):
        row = g.wrap(g.row + drow)
        col = g.wrap(g.col + dcol)
        for part in range(g.parts):
            source = src_ref.at[g.device(row, col, part)]
            if dcol in g.direct:
                dst, sem = landing(drow, dcol, g.col)
                send(source, dst, x_send.at[drow], sem, g.near(0, g.hop(dcol), part)).start()
            elif part == 0:
                send(source, right_ref.at[drow], x_send.at[drow], right_recv.at[drow], g.near(0, 1)).start()
            else:
                send(source, left_ref.at[drow], x_send.at[drow], left_recv.at[drow], g.near(0, -1)).start()

    def own_chip(drow):
        row = g.wrap(g.row + drow)
        away = src_ref.at[g.device(row, g.col, g.parts - 1 - g.part)]
        dst, sem = landing(drow, 0, g.col)
        dst[...] = src_ref[g.device(row, g.col, g.part)]
        send(away, dst, x_send.at[drow], sem, g.partner).start()

    def pass_row(drow):
        for ref, come_sem, come in ((right_ref, right_recv, -1), (left_ref, left_recv, 1)):
            send(ref.at[drow], ref.at[drow], fwd_send.at[drow], come_sem.at[drow], g.me).wait_recv()
            dst, sem = landing(drow, 2, g.wrap(g.col + come))
            send(ref.at[drow], dst, fwd_send.at[drow], sem, g.near(0, -come, 0 if come < 0 else 1)).start()

    def along_column(drow, dcol):
        chunk = stage_ref.at[drow - 1, dcol]
        got = chunk.at[pl.ds(0, half)] if dcol == 0 else chunk
        send(got, got, y_send.at[drow - 1], stage_recv.at[drow - 1, dcol], g.me).wait_recv()
        head = g.row * side + g.wrap(g.col - dcol)
        if drow in g.direct:
            send(chunk, dst_ref.at[head], y_send.at[drow - 1], out_recv, g.near(g.hop(drow), 0)).start()
        elif dcol % 2 == 0:
            send(chunk, up_ref.at[dcol // 2], y_send.at[drow - 1], up_recv.at[dcol // 2], g.near(1, 0)).start()
        else:
            send(chunk, down_ref.at[dcol // 2], y_send.at[drow - 1], down_recv.at[dcol // 2], g.near(-1, 0)).start()

    def when_source(row, body):
        pl.when(g.is_source(row))(body)

    def rows_of(drow):
        def body():
            for d in (2, 1, 3) if g.ties else (1,):
                along_row(drow, d)
        when_source(g.row + drow, body)

    def relay(drow):
        when_source(g.row + drow, lambda: pass_row(drow))

    def column(drow, d):
        when_source(g.row + drow, lambda: along_column(drow, d))

    def up(i):
        def body():
            send(up_ref.at[i], up_ref.at[i], pass_send.at[0], up_recv.at[i], g.me).wait_recv()
            head = g.wrap(g.row - 1) * side + g.wrap(g.col - 2 * i)
            send(up_ref.at[i], dst_ref.at[head], pass_send.at[0], out_recv, g.near(1, 0)).start()
        when_source(g.row + 1, body)

    def down(i):
        def body():
            send(down_ref.at[i], down_ref.at[i], pass_send.at[1], down_recv.at[i], g.me).wait_recv()
            head = g.wrap(g.row + 1) * side + g.wrap(g.col - 2 * i - 1)
            send(down_ref.at[i], dst_ref.at[head], pass_send.at[1], out_recv, g.near(-1, 0)).start()
        when_source(g.row - 1, body)

    def start_dq():
        swap(dq_ref, theirs_ref, row_send.at[0], row_recv.at[0], g.partner)
        both = (dq_ref[...] + theirs_ref[...]).astype(BF16)
        share = dqt_ref.shape[0]
        dqt_ref[...] = jnp.where(g.part == 0, both[:share], both[share:])
        total = both.T
        packed_ref[...] = pack(total.reshape(n, total.shape[0] // n, total.shape[1]))
        start_rows(n, heads, g.me, g.part, packed_ref, lambda peer: peer, got_ref, row_send.at[1], row_recv.at[1])

    for drow in (2, 1, 3, 0) if g.ties else (1, 0):
        when_source(g.row + drow, lambda drow=drow: own_chip(drow))
    if g.ties:
        rows_of(2)
        rows_of(1)
        for drow in (2, 1, 3):
            column(drow, 0)
        start_dq()
        relay(2)
        rows_of(3)
        relay(1)
        column(2, 1)
        column(2, 3)
        column(2, 2)
        up(0)
        down(0)
        rows_of(0)
        column(1, 1)
        column(1, 3)
        relay(3)
        column(1, 2)
        up(1)
        down(1)
        relay(0)
        column(3, 1)
        column(3, 3)
        column(3, 2)
    else:
        rows_of(1)
        rows_of(0)
        start_dq()
        column(1, 0)
        column(1, 1)
    wait_rows(heads, g.me, got_ref, row_send.at[1], row_recv.at[1])
    rows_ref[...] = unpack(got_ref[...])

    def sent(sem, ref):
        send(ref, ref, sem, out_recv, g.me).wait_send()

    for drow in range(side):
        def done(drow=drow):
            sent(x_send.at[drow], src_ref.at[pl.ds(0, g.parts * side - 1)])
            if g.ties:
                sent(fwd_send.at[drow], src_ref.at[pl.ds(0, 2)])
            if drow:
                sent(y_send.at[drow - 1], stage_ref.at[0])
        when_source(g.row + drow, done)
    if g.ties:
        when_source(g.row + 1, lambda: sent(pass_send.at[0], up_ref))
        when_source(g.row - 1, lambda: sent(pass_send.at[1], down_ref))

    @pl.when(g.is_source(g.row))
    def _():
        blocks = src_ref.at[pl.ds(0, n - 1)]
        send(blocks, blocks, y_send.at[0], out_recv, g.me).wait_recv()

    @pl.when(jnp.logical_not(g.is_source(g.row)))
    def _():
        def clear(index, carry):
            dst_ref[index] = jnp.zeros(dst_ref.shape[1:], dst_ref.dtype)
            return carry
        lax.fori_loop(0, heads, clear, 0)


def return_blocks(n, heads, source_rows, collective_id, blocks, dq):
    half, width = blocks.shape[1], blocks.shape[2]
    hd, total_q = dq.shape
    q_rows = total_q // n
    side, parts = math.isqrt(heads), n // heads
    chunk = lambda *lead: pltpu.VMEM(lead + (half * parts, width), BF16)
    block = lambda *lead: pltpu.VMEM(lead + (half, width), BF16)
    return pl.pallas_call(
        functools.partial(return_kernel, n, heads, source_rows),
        out_shape=[shape((heads, half * parts, width), BF16), shape((heads, q_rows, hd), BF16), shape((hd // parts, total_q), BF16)],
        in_specs=vmem(2),
        out_specs=vmem(3),
        scratch_shapes=[chunk(side - 1, side), block(side), block(side), chunk(2), chunk(2), pltpu.VMEM(dq.shape, F32),
                        pltpu.VMEM((n, q_rows // 2, 2 * hd), BF16), pltpu.VMEM((heads, q_rows // 2, 2 * hd), BF16), dma(2), dma(2),
                        dma(side), dma(side), dma(side - 1), dma(2), dma(side - 1, side), dma(side), dma(side), dma(2), dma(2),
                        pltpu.SemaphoreType.DMA],
        compiler_params=remote(collective_id),
        name='return_blocks',
    )(blocks, dq)


def decoder_kernel(n, heads, mine_ref, dec_ref, gout_ref, gain_ref, wo_hbm, wg_hbm, wu_hbm, wd_hbm,
                   out_ref, lse_ref, do_ref, factors_ref, gh_ref, gnorm_ref,
                   theirs_ref, packed_ref, got_ref, sent_ref, back_ref, swapped_ref, wo_ref, wg_ref, wu_ref, wd_ref,
                   load_sem, send_sem, recv_sem):
    me = lax.axis_index('seq')
    part = lax.rem(me, n // heads)
    partner, peers = pair_peers(n, heads, me, part)
    q_rows, dim = dec_ref.shape
    hd = out_ref.shape[0]
    loads = [pltpu.make_async_copy(src, dst, load_sem.at[i]) for i, (src, dst) in enumerate(
        ((wd_hbm, wd_ref), (wo_hbm, wo_ref), (wg_hbm, wg_ref), (wu_hbm, wu_ref)))]
    for load in loads:
        load.start()
    meet(peers)

    swap(mine_ref, theirs_ref, send_sem.at[0], recv_sem.at[0], partner)
    m_a, m_b = mine_ref[hd + 8:hd + 9], theirs_ref[hd + 8:hd + 9]
    top = jnp.maximum(m_a, m_b)
    s_a, s_b = jnp.exp2(m_a - top), jnp.exp2(m_b - top)
    den = mine_ref[hd:hd + 1] * s_a + theirs_ref[hd:hd + 1] * s_b
    out = (mine_ref[:hd] * s_a + theirs_ref[:hd] * s_b) / den
    packed_ref[...] = pack(out.T.astype(BF16).reshape(n, q_rows, hd))
    start_rows(n, heads, me, part, packed_ref, lambda peer: peer, got_ref, send_sem.at[1], recv_sem.at[1])
    out_ref[...] = out
    lse_ref[...] = top + jnp.log2(den)

    loads[0].wait()
    grad_act = dot_nt(gout_ref[...].astype(BF16), wd_ref[...])
    wait_rows(heads, me, got_ref, send_sem.at[1], recv_sem.at[1])

    attended = jnp.concatenate([unpack(got_ref[h]) for h in range(heads)], axis=1)
    loads[1].wait()
    hidden = (dec_ref[...].astype(F32) + dot(attended, wo_ref[...])).astype(BF16).astype(F32)
    gain = gain_ref[...].astype(F32)
    inverse = lax.rsqrt(jnp.mean(hidden * hidden, axis=-1, keepdims=True) + 1e-6)
    scaled = hidden * inverse
    normed = (scaled * gain).astype(BF16)
    loads[2].wait()
    gate = dot(normed, wg_ref[...])
    loads[3].wait()
    up = dot(normed, wu_ref[...])
    sig = jax.nn.sigmoid(gate)
    silu = gate * sig
    grad_gate = (grad_act * up * (sig + silu * (1.0 - sig))).astype(BF16)
    grad_up = (grad_act * silu).astype(BF16)
    grad_normed = (dot_nt(wg_ref[...], grad_gate) + dot_nt(wu_ref[...], grad_up)).T
    gnorm_ref[...] = jnp.sum(grad_normed * scaled, axis=0, keepdims=True)
    inner = grad_normed * gain
    grad_hidden = gout_ref[...] + inverse * (inner - scaled * jnp.mean(inner * scaled, axis=-1, keepdims=True))
    rounded = grad_hidden.astype(BF16)
    grad_att = dot_nt(wo_ref[...], rounded).T.astype(BF16)
    for h in range(heads):
        sent_ref[h] = pack(grad_att[:, hd * h:hd * (h + 1)])
    factors_ref[:, :dim] = attended
    factors_ref[:, dim:] = rounded
    gh_ref[...] = grad_hidden

    start_rows(n, heads, me, part, sent_ref, lambda peer: peer // (n // heads), back_ref, send_sem.at[2], recv_sem.at[2])
    wait_rows(heads, me, back_ref, send_sem.at[2], recv_sem.at[2])
    swap(back_ref, swapped_ref, send_sem.at[3], recv_sem.at[3], partner)
    place(n, heads, part, back_ref, swapped_ref, do_ref, False)


def decoder_rows(n, heads, collective_id, mine, dec_in, grad_out, gain, wo, w_gate, w_up, w_down):
    q_rows, dim = dec_in.shape
    hd, total_q = wo.shape[0] // heads, mine.shape[1]
    hbm = pl.BlockSpec(memory_space=pl.ANY)
    return pl.pallas_call(
        functools.partial(decoder_kernel, n, heads),
        out_shape=[shape((hd, total_q), F32), shape((1, total_q), F32), shape((n, q_rows, 2 * hd), BF16),
                   shape((q_rows, 2 * dim), BF16), shape((q_rows, dim), F32), shape((1, dim), F32)],
        in_specs=vmem(4) + [hbm] * 4,
        out_specs=vmem(6),
        scratch_shapes=[pltpu.VMEM(mine.shape, F32), pltpu.VMEM((n, q_rows // 2, 2 * hd), BF16)]
        + [pltpu.VMEM((heads, q_rows // 2, 2 * hd), BF16)] * 4
        + [pltpu.VMEM(w.shape, BF16) for w in (wo, w_gate, w_up, w_down)] + [dma(4), dma(4), dma(4)],
        compiler_params=remote(collective_id),
        name='decoder_rows',
    )(mine, dec_in, grad_out, gain, wo, w_gate, w_up, w_down)


def valid_blocks(mem_len, rows, parts, sources):
    reach = mem_len - lax.rem(lax.axis_index('seq'), parts) * rows
    blocks = jnp.minimum((reach + parts * rows - 1) // (parts * rows), sources)
    return blocks, jnp.minimum(reach - (blocks - 1) * parts * rows, rows)


def forward_kernel(scale, hd, parts, q_block, len_ref, kv_ref, q_ref, out_ref, qt_ref, top_ref):
    rows, total_q = kv_ref.shape[1], q_ref.shape[0]
    blocks, last_valid = valid_blocks(len_ref[0], rows, parts, kv_ref.shape[0])
    groups = [slice(first, first + q_block) for first in range(0, total_q, q_block)]
    base = slice(hd + 8, hd + 9)
    qt_ref[...] = q_ref[...].T

    def values_of(keys):
        return jnp.concatenate([keys.T[hd:], jnp.ones((16, rows), keys.dtype)], axis=0)

    def group_of(index):
        return pl.ds(pl.multiple_of(index * q_block, q_block), q_block)

    def first_step(group, carry):
        cols = group_of(group)
        top = jnp.max(dot(kv_ref[0], qt_ref[:, cols]), axis=0, keepdims=True)
        out_ref[hd + 8:, cols] = jnp.broadcast_to(top * scale, (8, q_block))
        top_ref[:, cols] = jnp.broadcast_to(top, (8, q_block))
        return carry

    lax.fori_loop(0, len(groups), first_step, 0)
    out_ref[:hd + 8, :] = jnp.zeros((hd + 8, total_q), F32)

    def finish(values, scores, cols):
        top_ref[:, cols] = jnp.maximum(top_ref[:, cols], jnp.max(scores.reshape(rows // 8, 8, q_block), axis=0))
        weights = jnp.exp2(scores * scale - out_ref[base, cols]).astype(values.dtype)
        out_ref[:hd + 8, cols] += dot(values, weights)[:hd + 8]

    def step(index, carry):
        keys = kv_ref[index]
        values = values_of(keys)
        for cols in groups:
            finish(values, dot(keys, qt_ref[:, cols]), cols)
        return carry

    def last_step(group, carry):
        cols = group_of(group)
        keys = kv_ref[blocks - 1]
        scores = dot(keys, qt_ref[:, cols])
        position = lax.broadcasted_iota(jnp.int32, scores.shape, 0)
        finish(values_of(keys), jnp.where(position < last_valid, scores, NEG), cols)
        return carry

    lax.fori_loop(0, blocks - 1, step, 0)
    lax.fori_loop(0, len(groups), last_step, 0)

    excess = jnp.max(top_ref[...] * scale - out_ref[hd + 8:, :])

    @pl.when(excess > 16.0)
    def _():
        out_ref[:hd + 8, :] = jnp.zeros((hd + 8, total_q), F32)
        out_ref[hd + 8:, :] = jnp.full((8, total_q), NEG, F32)

        def running(step_index, carry):
            index, group = step_index // len(groups), lax.rem(step_index, len(groups))
            cols = group_of(group)
            keys = kv_ref[index]
            limit = jnp.where(index == blocks - 1, last_valid, rows)
            scores = dot(keys, qt_ref[:, cols]) * scale
            position = lax.broadcasted_iota(jnp.int32, scores.shape, 0)
            scores = jnp.where(position < limit, scores, NEG)
            old = out_ref[base, cols]
            new = jnp.maximum(old, jnp.max(scores, axis=0, keepdims=True))
            weights = jnp.exp2(scores - new).astype(keys.dtype)
            out_ref[:hd + 8, cols] = out_ref[:hd + 8, cols] * jnp.exp2(old - new) + dot(values_of(keys), weights)[:hd + 8]
            out_ref[hd + 8:, cols] = jnp.broadcast_to(new, (8, q_block))
            return carry

        lax.fori_loop(0, blocks * len(groups), running, 0)


def attention_forward(scale, hd, parts, sources, mem_len, kv, q):
    rows, width = kv.shape[1], kv.shape[2]
    total_q = q.shape[0]
    return pl.pallas_call(
        functools.partial(forward_kernel, scale, hd, parts, min(1024, total_q)),
        out_shape=shape((hd + 16, total_q), F32),
        grid=(1,),
        in_specs=[pl.BlockSpec(memory_space=pltpu.SMEM),
                  pl.BlockSpec((sources, rows, width), lambda i: (0, 0, 0), pipeline_mode=pl.Buffered(1)), full(q)],
        out_specs=pl.BlockSpec((hd + 16, total_q), lambda i: (0, 0)),
        scratch_shapes=[pltpu.VMEM((width, total_q), BF16), pltpu.VMEM((8, total_q), F32)],
        compiler_params=plain(),
        cost_estimate=pl.CostEstimate(flops=4 * total_q * sources * rows * hd, bytes_accessed=kv.size * 2,
                                      transcendentals=total_q * sources * rows),
        name='attention_forward',
    )(mem_len, kv, q)


def backward_kernel(scale, key_scale, hd, parts, q_block, len_ref, kv_ref, q_ref, do_ref, out_ref, lse_ref, dkv_ref, dq_ref,
                    qt_ref, dot_ref, delta_ref):
    rows, total_q = kv_ref.shape[1], q_ref.shape[0]
    blocks, last_valid = valid_blocks(len_ref[0], rows, parts, kv_ref.shape[0])
    width = kv_ref.shape[2]
    groups = [slice(first, first + q_block) for first in range(0, total_q, q_block)]
    dq_ref[...] = jnp.zeros_like(dq_ref)
    qt_ref[...] = q_ref[...].T
    do_t = do_ref[...].T
    dot_ref[...] = do_t
    delta_ref[...] = jnp.sum(do_t[hd:].astype(F32) * out_ref[...], axis=0, keepdims=True)

    lane_scale = jnp.where(lax.broadcasted_iota(jnp.int32, (1, width), 1) < hd, key_scale, 1.0)

    def products(keys, cols):
        return dot(keys, qt_ref[:, cols]), dot(keys, dot_ref[:, cols])

    def finish(keys, keys_t, scores, grads, cols, valid):
        prob = jnp.exp2(scores * scale - lse_ref[:, cols])
        if valid is not None:
            position = lax.broadcasted_iota(jnp.int32, scores.shape, 0)
            prob = jnp.where(position < valid, prob, 0.0)
        grad_scores = (prob * (grads - delta_ref[:, cols])).astype(keys.dtype)
        update = dot(grad_scores, q_ref[cols, :]) + dot(prob.astype(keys.dtype), do_ref[cols, :])
        dq_ref[:, cols] += dot(keys_t, grad_scores)
        return update

    def step(index, carry):
        keys = kv_ref[index]
        keys_t = keys.T[:hd]
        total = jnp.zeros((rows, width), F32)
        for cols in groups:
            scores, grads = products(keys, cols)
            total += finish(keys, keys_t, scores, grads, cols, None)
        dkv_ref[index] = (total * lane_scale).astype(dkv_ref.dtype)
        return carry

    def last_step(group, total):
        keys = kv_ref[blocks - 1]
        cols = pl.ds(pl.multiple_of(group * q_block, q_block), q_block)
        scores, grads = products(keys, cols)
        return total + finish(keys, keys.T[:hd], scores, grads, cols, last_valid)

    def clear(index, carry):
        dkv_ref[index] = jnp.zeros((rows, width), dkv_ref.dtype)
        return carry

    lax.fori_loop(0, blocks - 1, step, 0)
    total = lax.fori_loop(0, len(groups), last_step, jnp.zeros((rows, width), F32))
    dkv_ref[blocks - 1] = (total * lane_scale).astype(dkv_ref.dtype)
    lax.fori_loop(blocks, dkv_ref.shape[0], clear, 0)
    dq_ref[...] = dq_ref[...] * key_scale


def attention_backward(scale, key_scale, hd, parts, sources, mem_len, kv, q, do, out_t, lse):
    n, rows, width = kv.shape
    total_q = q.shape[0]
    return pl.pallas_call(
        functools.partial(backward_kernel, scale, key_scale, hd, parts, min(512, total_q)),
        out_shape=[shape((n, rows, width), BF16), shape((hd, total_q), F32)],
        grid=(1,),
        in_specs=[pl.BlockSpec(memory_space=pltpu.SMEM),
                  pl.BlockSpec((sources, rows, width), lambda i: (0, 0, 0), pipeline_mode=pl.Buffered(1)),
                  full(q), full(do), full(out_t), full(lse)],
        out_specs=[pl.BlockSpec((n, rows, width), lambda i: (0, 0, 0)),
                   pl.BlockSpec((hd, total_q), lambda i: (0, 0))],
        scratch_shapes=[pltpu.VMEM((width, total_q), BF16), pltpu.VMEM((width, total_q), BF16), pltpu.VMEM((1, total_q), F32)],
        compiler_params=plain(),
        cost_estimate=pl.CostEstimate(flops=10 * total_q * sources * rows * hd, bytes_accessed=kv.size * 4,
                                      transcendentals=total_q * sources * rows),
        name='attention_backward',
    )(mem_len, kv, q, do, out_t, lse)


def reduce_kernel(n, heads, tile, chunk, gk_hbm, gv_hbm, early_hbm, late_hbm, w1_hbm, w3_hbm, w2_hbm, wo_ref, wq_ref, gain1_ref,
                  gain2_ref, dqt_ref, dqr_ref, dec_ref, gh_ref, gnorm_ref,
                  sums_ref, gdec_ref, norms_ref, n2_hbm, d1_hbm, d3_hbm, act_hbm,
                  acc_ref, pair_ref, far_ref, near_ref, n2_ref, top_ref, att_ref, decs_ref, w1_ref, w3_ref, w2_ref,
                  d1_ref, d3_ref, act_ref, mine_ref, all_ref,
                  own_sem, pair_send, pair_recv, far_send, far_recv, near_send, near_recv, rows_sem, top_sem, w_sem, out_sem, n2_sem,
                  norm_send, norm_recv):
    g = Grid(n, heads, 0)
    side = g.side
    rows, dim = n2_ref.shape
    tiles = d1_hbm.shape[1] // tile
    part_rows = acc_ref.shape[1]
    hd = part_rows

    def start_rows_of(index):
        slot = lax.rem(index, 2)
        at = pl.ds(pl.multiple_of(index * chunk, chunk), chunk)
        for i, (src, dst) in enumerate(((late_hbm, att_ref), (early_hbm, decs_ref))):
            pltpu.make_async_copy(src.at[at, pl.ds(0, dim)], dst.at[slot], rows_sem.at[slot, i]).start()

    def tile_at(index):
        return pl.ds(pl.multiple_of(index * tile, tile), tile)

    def weights(index):
        slot = lax.rem(index, 2)
        at = tile_at(index)
        return [pltpu.make_async_copy(src, dst.at[slot], w_sem.at[slot, i]) for i, (src, dst) in enumerate(
            ((w1_hbm.at[:, at], w1_ref), (w3_hbm.at[:, at], w3_ref), (w2_hbm.at[at, :], w2_ref)))]

    def results(index):
        slot = lax.rem(index, 2)
        return [pltpu.make_async_copy(src.at[slot], dst.at[:, tile_at(index)], out_sem.at[slot, i]) for i, (src, dst) in enumerate(
            ((d1_ref, d1_hbm), (d3_ref, d3_hbm), (act_ref, act_hbm)))]

    start_rows_of(0)
    top_load = pltpu.make_async_copy(early_hbm.at[:, pl.ds(dim, dim)], top_ref, top_sem)
    top_load.start()
    for copy in weights(0):
        copy.start()

    def summand(c, core):
        source = gk_hbm if c < heads // g.parts else gv_hbm
        first = ((g.parts * c) % heads + core) * part_rows
        return source.at[pl.ds(pl.multiple_of(first, part_rows), part_rows), :]

    owns = [pltpu.make_async_copy(summand(c, g.part), acc_ref.at[c], own_sem.at[c]) for c in range(heads)]
    for copy in owns:
        copy.start()

    grad_query = jnp.concatenate([dqr_ref[h] for h in range(heads)], axis=1)
    grad_normed = dot(grad_query, wq_ref[...])
    x = dec_ref[...].astype(F32)
    inverse = lax.rsqrt(jnp.mean(x * x, axis=-1, keepdims=True) + 1e-6)
    scaled = x * inverse
    inner = grad_normed * gain1_ref[...].astype(F32)
    gdec_ref[...] = gh_ref[...] + inverse * (inner - scaled * jnp.mean(inner * scaled, axis=-1, keepdims=True))
    mine_ref[0:1, :] = jnp.sum(grad_normed * scaled, axis=0, keepdims=True)
    mine_ref[1:2, :] = gnorm_ref[...]

    meet([lax.rem(g.me + step, n) for step in range(1, n)])
    for c in range(heads):
        send(summand(c, g.parts - 1 - g.part), pair_ref.at[c], pair_send, pair_recv, g.partner).start()
    for step in range(1, n):
        send(mine_ref, all_ref.at[g.me], norm_send, norm_recv, lax.rem(g.me + step, n)).start()
    all_ref[g.me] = mine_ref[...]

    sums_ref[part_rows:, :] = jnp.zeros((sums_ref.shape[0] - part_rows, dim), F32)

    def prepare(index, carry):
        slot = lax.rem(index, 2)
        at = pl.ds(pl.multiple_of(index * chunk, chunk), chunk)
        for i, (src, dst) in enumerate(((late_hbm, att_ref), (early_hbm, decs_ref))):
            pltpu.make_async_copy(src.at[at, pl.ds(0, dim)], dst.at[slot], rows_sem.at[slot, i]).wait()

        @pl.when(index + 1 < rows // chunk)
        def _():
            start_rows_of(index + 1)

        dec = decs_ref[slot].astype(F32)
        hidden = (dec + dot(att_ref[slot], wo_ref[...])).astype(BF16).astype(F32)
        n2_ref[at, :] = rms_norm(hidden, gain2_ref[...].astype(F32)).astype(BF16)
        first = rms_norm(dec, gain1_ref[...].astype(F32)).astype(BF16)
        sums_ref[part_rows:, :] += dot(dqt_ref[:, at], first)
        return carry

    lax.fori_loop(0, rows // chunk, prepare, 0)
    top_load.wait()
    n2_store = pltpu.make_async_copy(n2_ref, n2_hbm, n2_sem)
    n2_store.start()

    quarter = part_rows // 4
    streams = [(axis, way, pl.ds((2 * axis + (way < 0)) * quarter, quarter)) for axis in (0, 1) for way in (1, -1)]

    def place_of(axis, line, other):
        return other * side + line if axis == 0 else line * side + other

    def pieces(stage, axis, line):
        position = g.row if axis == 0 else g.col
        return [place_of(axis, line, o) for o in range(side)] if stage == 0 else [place_of(axis, line, position)]

    def ring(stage, stream, step):
        axis, way, part = streams[stream]
        axis = axis if stage == 0 else 1 - axis
        here = g.col if axis == 0 else g.row
        ref, sends, recvs = (far_ref, far_send, far_recv) if stage == 0 else (near_ref, near_send, near_recv)
        to = g.near(0, way) if axis == 0 else g.near(way, 0)
        return axis, way, part, here, ref.at[stream, step - 1], sends.at[stream, step - 1], recvs.at[stream, step - 1], to

    def line_of(here, way, step):
        return lax.rem(here - way * step + 2 * side, side)

    def start_step(stage, step):
        for stream in range(4):
            axis, way, part, here, buffer, sem, recv, to = ring(stage, stream, step)
            for i, c in enumerate(pieces(stage, axis, line_of(here, way, step))):
                send(acc_ref.at[c, part], buffer.at[i], sem, recv, to).start()

    def end_step(stage, step):
        for stream in range(4):
            axis, way, part, here, buffer, sem, recv, to = ring(stage, stream, step)
            whole = send(buffer, buffer, sem, recv, g.me)
            whole.wait_recv()
            for i, c in enumerate(pieces(stage, axis, line_of(here, way, step + 1))):
                acc_ref[c, part, :] = acc_ref[c, part, :] + buffer[i]
            whole.wait_send()

    def add_pair():
        for copy in owns:
            copy.wait()
        whole = send(pair_ref, pair_ref, pair_send, pair_recv, g.me)
        whole.wait_recv()

        def add(c, carry):
            acc_ref[c] = acc_ref[c] + pair_ref[c]
            return carry

        lax.fori_loop(0, heads, add, 0)
        whole.wait_send()

    def first():
        add_pair()
        start_step(0, 1)

    def turn():
        end_step(0, side - 1)
        start_step(1, 1)

    def between(stage, step):
        def body():
            end_step(stage, step)
            start_step(stage, step + 1)
        return body

    events = ([first] + [between(0, t) for t in range(1, side - 1)] + [turn] + [between(1, t) for t in range(1, side - 1)]
              + [lambda: end_step(1, side - 1)])
    at_tile = (0, 2, 4, 6, 7, 8, 9)
    inside = tiles > at_tile[-1] and len(events) == len(at_tile)

    def activations(index, carry):
        slot = lax.rem(index, 2)
        for copy in weights(index):
            copy.wait()

        @pl.when(index + 1 < tiles)
        def _():
            for copy in weights(index + 1):
                copy.start()

        @pl.when(index >= 2)
        def _():
            for copy in results(index - 2):
                copy.wait()

        if inside:
            for event, when in zip(events, at_tile):
                pl.when(index == when)(event)

        w1, w3, w2t = w1_ref[slot], w3_ref[slot], w2_ref[slot].T
        for first_row in range(0, rows, chunk):
            part = slice(first_row, first_row + chunk)
            gate = dot(n2_ref[part, :], w1)
            up = dot(n2_ref[part, :], w3)
            grad = dot(top_ref[part, :], w2t)
            sig = jax.nn.sigmoid(gate)
            silu = gate * sig
            act_ref[slot, part, :] = (silu * up).astype(BF16)
            d3_ref[slot, part, :] = (grad * silu).astype(BF16)
            d1_ref[slot, part, :] = (grad * up * (sig + silu * (1.0 - sig))).astype(BF16)
        for copy in results(index):
            copy.start()
        return carry

    lax.fori_loop(0, tiles, activations, 0)
    if not inside:
        for event in events:
            event()
    sums_ref[:part_rows, :] = acc_ref[g.chip]

    others = all_ref.at[pl.ds(0, n - 1)]
    whole = send(others, others, norm_send, norm_recv, g.me)
    whole.wait_send()
    whole.wait_recv()
    norms_ref[...] = jnp.sum(all_ref[...], axis=0)
    n2_store.wait()
    for index in range(max(tiles - 2, 0), tiles):
        for copy in results(index):
            copy.wait()


def reduce_sums(n, heads, collective_id, gk, gv, early, late, w_gate, w_up, w_down, wo, wq, gain1, gain2, dqt, dq_rows, dec_in, gh, gnorm):
    rows, dim = early.shape[0], gk.shape[1]
    ff, tile, chunk = w_gate.shape[1], 256, min(512, early.shape[0])
    part_rows = 2 * gk.shape[0] // n
    side = math.isqrt(heads)
    hbm = pl.BlockSpec(memory_space=pl.ANY)
    return pl.pallas_call(
        functools.partial(reduce_kernel, n, heads, tile, chunk),
        out_shape=[shape((part_rows + dqt.shape[0], dim), F32), shape(gh.shape, F32), shape((2, dim), F32), shape((rows, dim), BF16)]
        + [shape((rows, ff), BF16)] * 3,
        in_specs=[hbm] * 7 + vmem(9),
        out_specs=vmem(3) + [hbm] * 4,
        scratch_shapes=[pltpu.VMEM((heads, part_rows, dim), F32)] * 2
        + [pltpu.VMEM((4, side - 1, side, part_rows // 4, dim), F32), pltpu.VMEM((4, side - 1, 1, part_rows // 4, dim), F32)]
        + [pltpu.VMEM((rows, dim), BF16)] * 2 + [pltpu.VMEM((2, chunk, dim), BF16)] * 2
        + [pltpu.VMEM((2, dim, tile), BF16)] * 2 + [pltpu.VMEM((2, tile, dim), BF16)] + [pltpu.VMEM((2, rows, tile), BF16)] * 3
        + [pltpu.VMEM((2, dim), F32), pltpu.VMEM((n, 2, dim), F32)]
        + [dma(heads), pltpu.SemaphoreType.DMA, pltpu.SemaphoreType.DMA, dma(4, side - 1), dma(4, side - 1), dma(4, side - 1),
           dma(4, side - 1), dma(2, 2), pltpu.SemaphoreType.DMA, dma(2, 3), dma(2, 3), pltpu.SemaphoreType.DMA,
           pltpu.SemaphoreType.DMA, pltpu.SemaphoreType.DMA],
        compiler_params=remote(collective_id),
        cost_estimate=pl.CostEstimate(flops=6 * rows * dim * ff, bytes_accessed=12 * rows * ff, transcendentals=rows * ff),
        name='reduce_sums',
    )(gk, gv, early, late, w_gate, w_up, w_down, wo, wq, gain1, gain2, dqt, dq_rows, dec_in, gh, gnorm)


def mlp_kernel(n2_ref, top_ref, d1_ref, d3_ref, act_ref, g1_ref, g3_ref, g2_ref, n2t_ref):
    @pl.when(pl.program_id(0) == 0)
    def _():
        n2t_ref[...] = n2_ref[...].T

    g1_ref[...] = dot(n2t_ref[...], d1_ref[...])
    g3_ref[...] = dot(n2t_ref[...], d3_ref[...])
    g2_ref[...] = dot_tn(act_ref[...], top_ref[...])


def mlp_weight_grads(n2, early, d1, d3, act):
    rows, dim = n2.shape
    ff = d1.shape[1]
    tile = 256
    cols = pl.BlockSpec((dim, tile), lambda i: (0, i))
    tall = pl.BlockSpec((tile, dim), lambda i: (i, 0))
    part = pl.BlockSpec((rows, tile), lambda i: (0, i))
    return pl.pallas_call(
        mlp_kernel,
        out_shape=[shape((dim, ff), F32), shape((dim, ff), F32), shape((ff, dim), F32)],
        grid=(ff // tile,),
        in_specs=[full(n2), pl.BlockSpec((rows, dim), lambda i: (0, 1), pipeline_mode=pl.Buffered(1)), part, part, part],
        out_specs=[cols, cols, tall],
        scratch_shapes=[pltpu.VMEM((dim, rows), BF16)],
        compiler_params=plain(),
        cost_estimate=pl.CostEstimate(flops=6 * rows * dim * ff, bytes_accessed=18 * dim * ff, transcendentals=0),
        name='mlp_weight_grads',
    )(n2, early, d1, d3, act)


def memory_weight_kernel(memory_ref, dkv_ref, gk_ref, gv_ref):
    group, hd = dkv_ref.shape[0], dkv_ref.shape[2] // 2
    for i in range(group):
        both = dot_tn(dkv_ref[i], memory_ref[...])
        gk_ref[i * hd:(i + 1) * hd, :] = both[:hd]
        gv_ref[i * hd:(i + 1) * hd, :] = both[hd:]


def memory_weight_grads(memory, dkv):
    heads, rows, width = dkv.shape
    dim, hd = memory.shape[1], width // 2
    group = 4
    out = pl.BlockSpec((group * hd, dim), lambda i: (i, 0))
    return pl.pallas_call(
        memory_weight_kernel,
        out_shape=[shape((heads * hd, dim), F32)] * 2,
        grid=(heads // group,),
        in_specs=[full(memory), pl.BlockSpec((group, rows, width), lambda i: (i, 0, 0))],
        out_specs=[out, out],
        compiler_params=plain(),
        cost_estimate=pl.CostEstimate(flops=2 * rows * dim * heads * width, bytes_accessed=16 * rows * dim, transcendentals=0),
        name='memory_weight_grads',
    )(memory, dkv)


def memory_grad_kernel(dkv_ref, wk_ref, wv_ref, out_ref):
    group = dkv_ref.shape[0]
    left = jnp.concatenate([dkv_ref[i] for i in range(group)], axis=1)
    right = jnp.concatenate([part[i] for i in range(group) for part in (wk_ref, wv_ref)], axis=0)

    @pl.when(pl.program_id(0) == 0)
    def _():
        out_ref[...] = dot(left, right)

    @pl.when(pl.program_id(0) > 0)
    def _():
        out_ref[...] += dot(left, right)


def memory_grad(dkv, wk_t, wv_t):
    heads, rows, width = dkv.shape
    hd, dim = wk_t.shape[1], wk_t.shape[2]
    group = 4
    weight = pl.BlockSpec((group, hd, dim), lambda i: (i, 0, 0))
    return pl.pallas_call(
        memory_grad_kernel,
        out_shape=shape((rows, dim), F32),
        grid=(heads // group,),
        in_specs=[pl.BlockSpec((group, rows, width), lambda i: (i, 0, 0)), weight, weight],
        out_specs=pl.BlockSpec((rows, dim), lambda i: (0, 0)),
        compiler_params=plain(),
        cost_estimate=pl.CostEstimate(flops=2 * rows * dim * heads * width, bytes_accessed=12 * rows * dim, transcendentals=0),
        name='memory_grad',
    )(dkv, wk_t, wv_t)


def outer_kernel(att_ref, gh_ref, out_ref):
    @pl.when(pl.program_id(0) == 0)
    def _():
        out_ref[...] = jnp.zeros_like(out_ref)

    out_ref[...] += dot_tn(att_ref[...], gh_ref[...])


def outer_weight_grad(late, dim):
    rows = late.shape[0]
    chunk = min(512, rows)
    return pl.pallas_call(
        outer_kernel,
        out_shape=shape((dim, dim), F32),
        grid=(rows // chunk,),
        in_specs=[pl.BlockSpec((chunk, dim), lambda i: (i, 0)), pl.BlockSpec((chunk, dim), lambda i: (i, 1))],
        out_specs=pl.BlockSpec((dim, dim), lambda i: (0, 0)),
        compiler_params=plain(),
        cost_estimate=pl.CostEstimate(flops=2 * rows * dim * dim, bytes_accessed=8 * rows * dim, transcendentals=0),
        name='outer_weight_grad',
    )(late, late)


def solution(mesh):
    n = mesh.shape['seq']
    row_spec = P(('data', 'seq'), None)
    weight_spec = P()
    part_vec = P('data')
    part_mat = P('data', None)
    part_cube = P('data', None, None)

    def device_step(dec_in, memory, mem_len, grad_out, norm_attn, wq_cross, wk_cross, wv_cross, wo_cross, norm_mlp, w_gate, w_up, w_down):
        q_rows, dim = dec_in.shape
        heads, hd = wq_cross.shape[1], wq_cross.shape[2]
        parts = n // heads
        sources = -(-3 * n // 4)
        total_q = q_rows * n
        key_scale = hd ** -0.5
        scale = key_scale * LOG2E
        wq_t, wk_t, wv_t = (jnp.transpose(w, (1, 2, 0)) for w in (wq_cross, wk_cross, wv_cross))
        source_rows = -(-sources // (parts * math.isqrt(heads)))
        kv, q_in, early_local = exchange(n, heads, source_rows, 0, memory, dec_in, grad_out, norm_attn, wk_t, wv_t, wq_t)
        head_q = q_in.reshape(total_q, 2 * hd)

        early = lax.all_gather(early_local, 'seq', axis=0, tiled=True)

        wo = wo_cross.reshape(heads * hd, dim)
        mine = attention_forward(scale, hd, parts, sources, mem_len, kv, head_q)
        out_t, lse, do_in, factors, grad_hidden, g_norm_mlp = decoder_rows(
            n, heads, 1, mine, dec_in, grad_out, norm_mlp, wo, w_gate, w_up, w_down)
        do_in, factors, early = lax.optimization_barrier((do_in, factors, early))
        late = lax.all_gather(factors, 'seq', axis=0, tiled=True)

        dkv, dq_part = attention_backward(scale, key_scale, hd, parts, sources, mem_len, kv, head_q, do_in.reshape(total_q, 2 * hd), out_t, lse)
        dkv_in, dq_rows, dq_t = return_blocks(n, heads, source_rows, 4, dkv, dq_part)
        dkv_in, dq_rows, late = lax.optimization_barrier((dkv_in, dq_rows, late))

        gk_part, gv_part = memory_weight_grads(memory, dkv_in)
        sums, g_dec, norms, n2_all, d1, d3, act = reduce_sums(
            n, heads, 5, gk_part, gv_part, early, late, w_gate, w_up, w_down, wo, wq_t.reshape(heads * hd, dim), norm_attn, norm_mlp,
            dq_t, dq_rows, dec_in, grad_hidden, g_norm_mlp)
        sums, n2_all, d1, d3, act, dkv_in, late, early = lax.optimization_barrier((sums, n2_all, d1, d3, act, dkv_in, late, early))
        total = lax.all_gather(sums, 'seq', axis=0, tiled=False)
        g_gate, g_up, g_down = mlp_weight_grads(n2_all, early, d1, d3, act)
        g_wo = outer_weight_grad(late, dim)
        g_mem = memory_grad(dkv_in, wk_t, wv_t)

        rows = 2 * heads * hd // n
        cube = lambda g: jnp.transpose(g.reshape(heads, hd, dim), (2, 0, 1))
        g_wk, g_wv, g_wq = total[:n // 2, :rows], total[n // 2:, :rows], total[:, rows:]
        return (g_dec, g_mem, norms[0], cube(g_wq), cube(g_wk), cube(g_wv), g_wo.reshape(heads, hd, dim), norms[1], g_gate, g_up, g_down)

    return jax.shard_map(device_step, mesh=mesh,
                         in_specs=(row_spec, row_spec, part_vec, row_spec) + (weight_spec,) * 9,
                         out_specs=(row_spec, row_spec, part_vec, part_cube, part_cube, part_cube, part_cube, part_vec, part_mat, part_mat, part_mat),
                         check_vma=False)
```

```python
import functools
import math

import jax
import jax.numpy as jnp
from jax import lax
from jax.experimental import pallas as pl
from jax.experimental.pallas import tpu as pltpu
from jax.sharding import PartitionSpec as P

LOG2E = 1.4426950408889634
NEG = -1e30
VMEM_LIMIT = 60 * 1024 * 1024
MESH = pl.DeviceIdType.MESH
BF16, F32 = jnp.bfloat16, jnp.float32


def rms_norm(tensor, gain):
    mean_sq = jnp.mean(tensor * tensor, axis=-1, keepdims=True)
    return tensor * lax.rsqrt(mean_sq + 1e-6) * gain


def dot(a, b):
    return jnp.dot(a, b, preferred_element_type=F32)


def dot_nt(a, b):
    return lax.dot_general(a, b, (((1,), (1,)), ((), ())), preferred_element_type=F32)


def dot_tn(a, b):
    return lax.dot_general(a, b, (((0,), (0,)), ((), ())), preferred_element_type=F32)


def full(array):
    return pl.BlockSpec(array.shape, lambda *_: (0,) * array.ndim, pipeline_mode=pl.Buffered(1))


def vmem(count):
    return [pl.BlockSpec(memory_space=pltpu.VMEM)] * count


def plain():
    return pltpu.CompilerParams(vmem_limit_bytes=VMEM_LIMIT)


def remote(collective_id):
    return pltpu.CompilerParams(collective_id=collective_id, has_side_effects=True, vmem_limit_bytes=VMEM_LIMIT)


def shape(dims, dtype):
    return jax.ShapeDtypeStruct(dims, dtype)


def meet(peers):
    barrier = pltpu.get_barrier_semaphore()
    for peer in peers:
        pl.semaphore_signal(barrier, inc=1, device_id={'seq': peer}, device_id_type=MESH)
    pl.semaphore_wait(barrier, len(peers))


def send(src, dst, send_sem, recv_sem, peer):
    return pltpu.make_async_remote_copy(src_ref=src, dst_ref=dst, send_sem=send_sem, recv_sem=recv_sem,
                                        device_id={'seq': peer}, device_id_type=MESH)


class Grid:
    def __init__(self, n, heads, source_rows):
        self.n, self.heads, self.source_rows = n, heads, source_rows
        self.parts = n // heads
        self.side = math.isqrt(heads)
        self.me = lax.axis_index('seq')
        self.part = lax.rem(self.me, self.parts)
        self.chip = self.me // self.parts
        self.col = lax.rem(self.chip, self.side)
        self.row = self.chip // self.side
        self.partner = self.chip * self.parts + (self.parts - 1 - self.part)
        self.ties = self.side == 4
        self.direct = (1, 3) if self.ties else (1,)

    def wrap(self, value):
        return lax.rem(value + self.side, self.side)

    def device(self, row, col, part):
        return (row * self.side + col) * self.parts + part

    def near(self, drow, dcol, part=None):
        return self.device(self.wrap(self.row + drow), self.wrap(self.col + dcol), self.part if part is None else part)

    def hop(self, offset):
        return 1 if offset == 1 else -1

    def is_source(self, row):
        return self.wrap(row) < self.source_rows

    def row_peers(self):
        return [lax.rem(self.chip + step, self.heads) * self.parts + self.part for step in range(1, self.heads)]

    def peers(self):
        return self.row_peers() + [self.partner] + [self.near(0, self.hop(d), self.parts - 1 - self.part) for d in self.direct]


def pair_peers(n, heads, me, part):
    parts = n // heads
    head = me // parts
    partner = head * parts + (parts - 1 - part)
    return partner, [partner] + [lax.rem(head + step, heads) * parts + part for step in range(1, heads)]


def pack(rows):
    middle = rows.shape[-2] // 2
    return jnp.concatenate([rows[..., :middle, :], rows[..., middle:, :]], axis=-1)


def unpack(packed):
    middle = packed.shape[-1] // 2
    return jnp.concatenate([packed[..., :middle], packed[..., middle:]], axis=-2)


def start_rows(n, heads, me, part, src, src_of, dst_ref, send_sem, recv_sem):
    parts = n // heads
    head = me // parts
    for step in range(1, heads):
        peer = lax.rem(head + step, heads) * parts + part
        send(src.at[src_of(peer)], dst_ref.at[head], send_sem, recv_sem, peer).start()
    dst_ref[head] = src[src_of(me)]


def wait_rows(heads, me, dst_ref, send_sem, recv_sem):
    others = dst_ref.at[pl.ds(0, heads - 1)]
    whole = send(others, others, send_sem, recv_sem, me)
    whole.wait_send()
    whole.wait_recv()


def swap(src, dst, send_sem, recv_sem, partner):
    copy = send(src, dst, send_sem, recv_sem, partner)
    copy.start()
    copy.wait()


def place(n, heads, part, mine_ref, theirs_ref, wide_ref, low):
    parts = n // heads
    for source, index in ((mine_ref, part), (theirs_ref, parts - 1 - part)):
        for head in range(heads):
            rows = unpack(source[head])
            zeros = jnp.zeros_like(rows)
            wide_ref[head * parts + index] = jnp.concatenate([rows, zeros] if low else [zeros, rows], axis=-1)


def exchange_kernel(n, heads, source_rows, memory_ref, dec_ref, gout_ref, gain_ref, wk_ref, wv_ref, wq_ref, kv_out_ref, q_out_ref, early_ref,
                    kv_ref, stage_ref, up_ref, down_ref, right_ref, left_ref, packed_ref, got_ref, swapped_ref,
                    row_send, row_recv, y_send, pass_send, x_send, fwd_send, stage_recv, up_recv, down_recv, right_recv,
                    left_recv, out_recv):
    g = Grid(n, heads, source_rows)
    side, hd = g.side, wk_ref.shape[1]
    half = kv_out_ref.shape[1]
    chunk_rows = min(256, kv_ref.shape[1])
    barrier = pltpu.get_barrier_semaphore()
    peers = g.peers()
    for peer in peers:
        pl.semaphore_signal(barrier, inc=1, device_id={'seq': peer}, device_id_type=MESH)

    dim = dec_ref.shape[1]
    early_ref[:, :dim] = dec_ref[...]
    early_ref[:, dim:] = gout_ref[...].astype(BF16)
    normed = rms_norm(dec_ref[...].astype(F32), gain_ref[...].astype(F32)).astype(BF16)
    for i in range(0, heads, 4):
        queries = dot_nt(normed, jnp.concatenate([wq_ref[i + j] for j in range(4)], axis=0)).astype(BF16)
        for j in range(4):
            packed_ref[i + j] = pack(queries[:, hd * j:hd * (j + 1)])

    def head(drow, dcol):
        return g.wrap(g.row + drow) * side + g.wrap(g.col + dcol)

    def project(drow, dcols):
        weights = jnp.concatenate([ref[head(drow, d)] for d in dcols for ref in (wk_ref, wv_ref)], axis=0)

        def rows(index, carry):
            at = pl.ds(pl.multiple_of(index * chunk_rows, chunk_rows), chunk_rows)
            both = dot_nt(memory_ref[at, :], weights).astype(BF16)
            for i, d in enumerate(dcols):
                kv_ref[head(drow, d), at, :] = both[:, 2 * hd * i:2 * hd * (i + 1)]
            return carry

        lax.fori_loop(0, kv_ref.shape[1] // chunk_rows, rows, 0)

    def along_column(drow, dcol):
        chunk = kv_ref.at[head(drow, dcol)]
        if drow in g.direct:
            send(chunk, stage_ref.at[drow - 1, dcol], y_send.at[drow - 1], stage_recv.at[drow - 1, dcol], g.near(g.hop(drow), 0)).start()
        elif dcol % 2 == 0:
            send(chunk, up_ref.at[dcol // 2], y_send.at[drow - 1], up_recv.at[dcol // 2], g.near(1, 0)).start()
        else:
            send(chunk, down_ref.at[dcol // 2], y_send.at[drow - 1], down_recv.at[dcol // 2], g.near(-1, 0)).start()

    def along_row(o, dcol):
        chunk = kv_ref.at[head(0, dcol)] if o == 0 else stage_ref.at[o - 1, dcol]
        source = g.device(g.wrap(g.row - o), g.col, g.part)
        if dcol == 0:
            kv_out_ref[source] = chunk[pl.ds(pl.multiple_of(g.part * half, half), half), :]
            away = pl.ds(pl.multiple_of((g.parts - 1 - g.part) * half, half), half)
            send(chunk.at[away], kv_out_ref.at[source], x_send.at[o], out_recv, g.partner).start()
        elif dcol in g.direct:
            for part in range(g.parts):
                send(chunk.at[pl.ds(part * half, half)], kv_out_ref.at[source], x_send.at[o], out_recv,
                     g.near(0, g.hop(dcol), part)).start()
        else:
            send(chunk.at[pl.ds(0, half)], right_ref.at[o], x_send.at[o], right_recv.at[o], g.near(0, 1)).start()
            send(chunk.at[pl.ds(half, half)], left_ref.at[o], x_send.at[o], left_recv.at[o], g.near(0, -1)).start()

    def pass_row(o):
        for ref, sem, come in ((right_ref, right_recv, -1), (left_ref, left_recv, 1)):
            source = g.device(g.wrap(g.row - o), g.wrap(g.col + come), g.part)
            send(ref.at[o], ref.at[o], fwd_send.at[o], sem.at[o], g.me).wait_recv()
            send(ref.at[o], kv_out_ref.at[source], fwd_send.at[o], out_recv, g.near(0, -come, 0 if come < 0 else 1)).start()

    def when_source(row, body):
        pl.when(g.is_source(row))(body)

    if g.ties:
        order = [(2, (2, 1)), (2, (3, 0)), (1, (2, 1)), (3, (2, 3)), (0, (2, 1)), (0, (3, 0))]
        last = [(1, (3, 0)), (3, (1, 0))]
    else:
        order, last = [(1, (1, 0)), (0, (1, 0))], []

    def issue(drow, dcols):
        def body():
            for d in dcols:
                along_row(0, d) if drow == 0 else along_column(drow, d)
        when_source(g.row, body)

    waiting = None
    for drow, dcols in order + last:
        project(drow, dcols)
        if waiting is None:
            pl.semaphore_wait(barrier, len(peers))
            start_rows(n, heads, g.me, g.part, packed_ref, lambda peer: peer // g.parts, got_ref, row_send.at[0], row_recv.at[0])
        elif waiting not in last:
            issue(*waiting)
        waiting = (drow, dcols)
    if not last:
        issue(*waiting)

    if g.ties:
        def up(i):
            send(up_ref.at[i], up_ref.at[i], pass_send.at[0], up_recv.at[i], g.me).wait_recv()
            send(up_ref.at[i], stage_ref.at[1, 2 * i], pass_send.at[0], stage_recv.at[1, 2 * i], g.near(1, 0)).start()

        def down(i):
            send(down_ref.at[i], down_ref.at[i], pass_send.at[1], down_recv.at[i], g.me).wait_recv()
            send(down_ref.at[i], stage_ref.at[1, 2 * i + 1], pass_send.at[1], stage_recv.at[1, 2 * i + 1], g.near(-1, 0)).start()

        for i in range(2):
            when_source(g.row - 1, lambda i=i: up(1 - i))
            when_source(g.row + 1, lambda i=i: down(i))
        for drow, dcols in last:
            issue(drow, dcols)
        when_source(g.row, lambda: pass_row(0))

    wait_rows(heads, g.me, got_ref, row_send.at[0], row_recv.at[0])
    swap(got_ref, swapped_ref, row_send.at[1], row_recv.at[1], g.partner)
    place(n, heads, g.part, got_ref, swapped_ref, q_out_ref, True)

    def arrived(o, dcol):
        def body():
            send(stage_ref.at[o - 1, dcol], stage_ref.at[o - 1, dcol], y_send.at[0], stage_recv.at[o - 1, dcol], g.me).wait_recv()
            along_row(o, dcol)
        when_source(g.row - o, body)

    if g.ties:
        for o, d in ((1, 2), (3, 2), (1, 1), (3, 3)):
            arrived(o, d)
        for o in g.direct:
            when_source(g.row - o, lambda o=o: pass_row(o))
        for d in (2, 1, 0, 3):
            arrived(2, d)
        when_source(g.row - 2, lambda: pass_row(2))
        for o, d in ((1, 3), (3, 1), (1, 0), (3, 0)):
            arrived(o, d)
    else:
        for d in (1, 0):
            arrived(1, d)

    def sent(sem, ref):
        send(ref, ref, sem, out_recv, g.me).wait_send()

    def mine():
        for drow in range(1, side):
            sent(y_send.at[drow - 1], stage_ref.at[0])
    when_source(g.row, mine)
    for o in range(side):
        def passed(o=o):
            sent(x_send.at[o], kv_out_ref.at[pl.ds(0, g.parts * side - 1)])
            if g.ties:
                sent(fwd_send.at[o], kv_out_ref.at[pl.ds(0, 2)])
        when_source(g.row - o, passed)
    if g.ties:
        when_source(g.row - 1, lambda: sent(pass_send.at[0], up_ref))
        when_source(g.row + 1, lambda: sent(pass_send.at[1], down_ref))
    blocks = source_rows * side * g.parts
    others = kv_out_ref.at[pl.ds(0, blocks - source_rows)]
    send(others, others, y_send.at[0], out_recv, g.me).wait_recv()


def row_scratch(heads, q_rows, hd):
    return [pltpu.VMEM((heads, q_rows // 2, 2 * hd), BF16)] * 3


def dma(*dims):
    return pltpu.SemaphoreType.DMA(dims)


def exchange(n, heads, source_rows, collective_id, memory, dec_in, grad_out, gain, wk_t, wv_t, wq_t):
    m_rows, q_rows, hd = memory.shape[0], dec_in.shape[0], wk_t.shape[1]
    side, parts = math.isqrt(heads), n // heads
    half = m_rows // parts
    chunk = lambda *lead: pltpu.VMEM(lead + (m_rows, 2 * hd), BF16)
    block = lambda *lead: pltpu.VMEM(lead + (half, 2 * hd), BF16)
    return pl.pallas_call(
        functools.partial(exchange_kernel, n, heads, source_rows),
        out_shape=[shape((n, half, 2 * hd), BF16), shape((n, q_rows, 2 * hd), BF16), shape((q_rows, 2 * dec_in.shape[1]), BF16)],
        in_specs=vmem(7),
        out_specs=vmem(3),
        scratch_shapes=[chunk(heads), chunk(side - 1, side), chunk(2), chunk(2), block(side), block(side)]
        + row_scratch(heads, q_rows, hd)
        + [dma(2), dma(2), dma(side - 1), dma(2), dma(side), dma(side), dma(side - 1, side), dma(2), dma(2), dma(side), dma(side),
           pltpu.SemaphoreType.DMA],
        compiler_params=remote(collective_id),
        name='exchange',
    )(memory, dec_in, grad_out, gain, wk_t, wv_t, wq_t)


def return_kernel(n, heads, source_rows, src_ref, dq_ref, dst_ref, rows_ref, dqt_ref, stage_ref, right_ref, left_ref, up_ref, down_ref,
                  theirs_ref, packed_ref, got_ref, row_send, row_recv,
                  x_send, fwd_send, y_send, pass_send, stage_recv, right_recv, left_recv, up_recv, down_recv, out_recv):
    g = Grid(n, heads, source_rows)
    side = g.side
    half = src_ref.shape[1]
    meet(g.peers())
    mine = pl.ds(pl.multiple_of(g.part * half, half), half)

    def landing(drow, dcol, head_col):
        if drow == 0:
            return dst_ref.at[g.row * side + head_col, mine], out_recv
        return stage_ref.at[drow - 1, dcol, mine], stage_recv.at[drow - 1, dcol]

    def along_row(drow, dcol):
        row = g.wrap(g.row + drow)
        col = g.wrap(g.col + dcol)
        for part in range(g.parts):
            source = src_ref.at[g.device(row, col, part)]
            if dcol in g.direct:
                dst, sem = landing(drow, dcol, g.col)
                send(source, dst, x_send.at[drow], sem, g.near(0, g.hop(dcol), part)).start()
            elif part == 0:
                send(source, right_ref.at[drow], x_send.at[drow], right_recv.at[drow], g.near(0, 1)).start()
            else:
                send(source, left_ref.at[drow], x_send.at[drow], left_recv.at[drow], g.near(0, -1)).start()

    def own_chip(drow):
        row = g.wrap(g.row + drow)
        away = src_ref.at[g.device(row, g.col, g.parts - 1 - g.part)]
        dst, sem = landing(drow, 0, g.col)
        dst[...] = src_ref[g.device(row, g.col, g.part)]
        send(away, dst, x_send.at[drow], sem, g.partner).start()

    def pass_row(drow):
        for ref, come_sem, come in ((right_ref, right_recv, -1), (left_ref, left_recv, 1)):
            send(ref.at[drow], ref.at[drow], fwd_send.at[drow], come_sem.at[drow], g.me).wait_recv()
            dst, sem = landing(drow, 2, g.wrap(g.col + come))
            send(ref.at[drow], dst, fwd_send.at[drow], sem, g.near(0, -come, 0 if come < 0 else 1)).start()

    def along_column(drow, dcol):
        chunk = stage_ref.at[drow - 1, dcol]
        got = chunk.at[pl.ds(0, half)] if dcol == 0 else chunk
        send(got, got, y_send.at[drow - 1], stage_recv.at[drow - 1, dcol], g.me).wait_recv()
        head = g.row * side + g.wrap(g.col - dcol)
        if drow in g.direct:
            send(chunk, dst_ref.at[head], y_send.at[drow - 1], out_recv, g.near(g.hop(drow), 0)).start()
        elif dcol % 2 == 0:
            send(chunk, up_ref.at[dcol // 2], y_send.at[drow - 1], up_recv.at[dcol // 2], g.near(1, 0)).start()
        else:
            send(chunk, down_ref.at[dcol // 2], y_send.at[drow - 1], down_recv.at[dcol // 2], g.near(-1, 0)).start()

    def when_source(row, body):
        pl.when(g.is_source(row))(body)

    def rows_of(drow):
        def body():
            for d in (2, 1, 3) if g.ties else (1,):
                along_row(drow, d)
        when_source(g.row + drow, body)

    def relay(drow):
        when_source(g.row + drow, lambda: pass_row(drow))

    def column(drow, d):
        when_source(g.row + drow, lambda: along_column(drow, d))

    def up(i):
        def body():
            send(up_ref.at[i], up_ref.at[i], pass_send.at[0], up_recv.at[i], g.me).wait_recv()
            head = g.wrap(g.row - 1) * side + g.wrap(g.col - 2 * i)
            send(up_ref.at[i], dst_ref.at[head], pass_send.at[0], out_recv, g.near(1, 0)).start()
        when_source(g.row + 1, body)

    def down(i):
        def body():
            send(down_ref.at[i], down_ref.at[i], pass_send.at[1], down_recv.at[i], g.me).wait_recv()
            head = g.wrap(g.row + 1) * side + g.wrap(g.col - 2 * i - 1)
            send(down_ref.at[i], dst_ref.at[head], pass_send.at[1], out_recv, g.near(-1, 0)).start()
        when_source(g.row - 1, body)

    def start_dq():
        swap(dq_ref, theirs_ref, row_send.at[0], row_recv.at[0], g.partner)
        both = (dq_ref[...] + theirs_ref[...]).astype(BF16)
        share = dqt_ref.shape[0]
        dqt_ref[...] = jnp.where(g.part == 0, both[:share], both[share:])
        total = both.T
        packed_ref[...] = pack(total.reshape(n, total.shape[0] // n, total.shape[1]))
        start_rows(n, heads, g.me, g.part, packed_ref, lambda peer: peer, got_ref, row_send.at[1], row_recv.at[1])

    for drow in (2, 1, 3, 0) if g.ties else (1, 0):
        when_source(g.row + drow, lambda drow=drow: own_chip(drow))
    if g.ties:
        rows_of(2)
        rows_of(1)
        for drow in (2, 1, 3):
            column(drow, 0)
        start_dq()
        relay(2)
        rows_of(3)
        relay(1)
        column(2, 1)
        column(2, 3)
        column(2, 2)
        up(0)
        down(0)
        rows_of(0)
        column(1, 1)
        column(1, 3)
        relay(3)
        column(1, 2)
        up(1)
        down(1)
        relay(0)
        column(3, 1)
        column(3, 3)
        column(3, 2)
    else:
        rows_of(1)
        rows_of(0)
        start_dq()
        column(1, 0)
        column(1, 1)
    wait_rows(heads, g.me, got_ref, row_send.at[1], row_recv.at[1])
    rows_ref[...] = unpack(got_ref[...])

    def sent(sem, ref):
        send(ref, ref, sem, out_recv, g.me).wait_send()

    for drow in range(side):
        def done(drow=drow):
            sent(x_send.at[drow], src_ref.at[pl.ds(0, g.parts * side - 1)])
            if g.ties:
                sent(fwd_send.at[drow], src_ref.at[pl.ds(0, 2)])
            if drow:
                sent(y_send.at[drow - 1], stage_ref.at[0])
        when_source(g.row + drow, done)
    if g.ties:
        when_source(g.row + 1, lambda: sent(pass_send.at[0], up_ref))
        when_source(g.row - 1, lambda: sent(pass_send.at[1], down_ref))

    @pl.when(g.is_source(g.row))
    def _():
        blocks = src_ref.at[pl.ds(0, n - 1)]
        send(blocks, blocks, y_send.at[0], out_recv, g.me).wait_recv()

    @pl.when(jnp.logical_not(g.is_source(g.row)))
    def _():
        def clear(index, carry):
            dst_ref[index] = jnp.zeros(dst_ref.shape[1:], dst_ref.dtype)
            return carry
        lax.fori_loop(0, heads, clear, 0)


def return_blocks(n, heads, source_rows, collective_id, blocks, dq):
    half, width = blocks.shape[1], blocks.shape[2]
    hd, total_q = dq.shape
    q_rows = total_q // n
    side, parts = math.isqrt(heads), n // heads
    chunk = lambda *lead: pltpu.VMEM(lead + (half * parts, width), BF16)
    block = lambda *lead: pltpu.VMEM(lead + (half, width), BF16)
    return pl.pallas_call(
        functools.partial(return_kernel, n, heads, source_rows),
        out_shape=[shape((heads, half * parts, width), BF16), shape((heads, q_rows, hd), BF16), shape((hd // parts, total_q), BF16)],
        in_specs=vmem(2),
        out_specs=vmem(3),
        scratch_shapes=[chunk(side - 1, side), block(side), block(side), chunk(2), chunk(2), pltpu.VMEM(dq.shape, F32),
                        pltpu.VMEM((n, q_rows // 2, 2 * hd), BF16), pltpu.VMEM((heads, q_rows // 2, 2 * hd), BF16), dma(2), dma(2),
                        dma(side), dma(side), dma(side - 1), dma(2), dma(side - 1, side), dma(side), dma(side), dma(2), dma(2),
                        pltpu.SemaphoreType.DMA],
        compiler_params=remote(collective_id),
        name='return_blocks',
    )(blocks, dq)


def decoder_kernel(n, heads, mine_ref, dec_ref, gout_ref, gain_ref, wo_hbm, wg_hbm, wu_hbm, wd_hbm,
                   out_ref, lse_ref, do_ref, factors_ref, gh_ref, gnorm_ref,
                   theirs_ref, packed_ref, got_ref, sent_ref, back_ref, swapped_ref, wo_ref, wg_ref, wu_ref, wd_ref,
                   load_sem, send_sem, recv_sem):
    me = lax.axis_index('seq')
    part = lax.rem(me, n // heads)
    partner, peers = pair_peers(n, heads, me, part)
    q_rows, dim = dec_ref.shape
    hd = out_ref.shape[0]
    loads = [pltpu.make_async_copy(src, dst, load_sem.at[i]) for i, (src, dst) in enumerate(
        ((wd_hbm, wd_ref), (wo_hbm, wo_ref), (wg_hbm, wg_ref), (wu_hbm, wu_ref)))]
    for load in loads:
        load.start()
    meet(peers)

    swap(mine_ref, theirs_ref, send_sem.at[0], recv_sem.at[0], partner)
    m_a, m_b = mine_ref[hd + 8:hd + 9], theirs_ref[hd + 8:hd + 9]
    top = jnp.maximum(m_a, m_b)
    s_a, s_b = jnp.exp2(m_a - top), jnp.exp2(m_b - top)
    den = mine_ref[hd:hd + 1] * s_a + theirs_ref[hd:hd + 1] * s_b
    out = (mine_ref[:hd] * s_a + theirs_ref[:hd] * s_b) / den
    packed_ref[...] = pack(out.T.astype(BF16).reshape(n, q_rows, hd))
    start_rows(n, heads, me, part, packed_ref, lambda peer: peer, got_ref, send_sem.at[1], recv_sem.at[1])
    out_ref[...] = out
    lse_ref[...] = top + jnp.log2(den)

    loads[0].wait()
    grad_act = dot_nt(gout_ref[...].astype(BF16), wd_ref[...])
    wait_rows(heads, me, got_ref, send_sem.at[1], recv_sem.at[1])

    attended = jnp.concatenate([unpack(got_ref[h]) for h in range(heads)], axis=1)
    loads[1].wait()
    hidden = (dec_ref[...].astype(F32) + dot(attended, wo_ref[...])).astype(BF16).astype(F32)
    gain = gain_ref[...].astype(F32)
    inverse = lax.rsqrt(jnp.mean(hidden * hidden, axis=-1, keepdims=True) + 1e-6)
    scaled = hidden * inverse
    normed = (scaled * gain).astype(BF16)
    loads[2].wait()
    gate = dot(normed, wg_ref[...])
    loads[3].wait()
    up = dot(normed, wu_ref[...])
    sig = jax.nn.sigmoid(gate)
    silu = gate * sig
    grad_gate = (grad_act * up * (sig + silu * (1.0 - sig))).astype(BF16)
    grad_up = (grad_act * silu).astype(BF16)
    grad_normed = (dot_nt(wg_ref[...], grad_gate) + dot_nt(wu_ref[...], grad_up)).T
    gnorm_ref[...] = jnp.sum(grad_normed * scaled, axis=0, keepdims=True)
    inner = grad_normed * gain
    grad_hidden = gout_ref[...] + inverse * (inner - scaled * jnp.mean(inner * scaled, axis=-1, keepdims=True))
    rounded = grad_hidden.astype(BF16)
    grad_att = dot_nt(wo_ref[...], rounded).T.astype(BF16)
    for h in range(heads):
        sent_ref[h] = pack(grad_att[:, hd * h:hd * (h + 1)])
    factors_ref[:, :dim] = attended
    factors_ref[:, dim:] = rounded
    gh_ref[...] = grad_hidden

    start_rows(n, heads, me, part, sent_ref, lambda peer: peer // (n // heads), back_ref, send_sem.at[2], recv_sem.at[2])
    wait_rows(heads, me, back_ref, send_sem.at[2], recv_sem.at[2])
    swap(back_ref, swapped_ref, send_sem.at[3], recv_sem.at[3], partner)
    place(n, heads, part, back_ref, swapped_ref, do_ref, False)


def decoder_rows(n, heads, collective_id, mine, dec_in, grad_out, gain, wo, w_gate, w_up, w_down):
    q_rows, dim = dec_in.shape
    hd, total_q = wo.shape[0] // heads, mine.shape[1]
    hbm = pl.BlockSpec(memory_space=pl.ANY)
    return pl.pallas_call(
        functools.partial(decoder_kernel, n, heads),
        out_shape=[shape((hd, total_q), F32), shape((1, total_q), F32), shape((n, q_rows, 2 * hd), BF16),
                   shape((q_rows, 2 * dim), BF16), shape((q_rows, dim), F32), shape((1, dim), F32)],
        in_specs=vmem(4) + [hbm] * 4,
        out_specs=vmem(6),
        scratch_shapes=[pltpu.VMEM(mine.shape, F32), pltpu.VMEM((n, q_rows // 2, 2 * hd), BF16)]
        + [pltpu.VMEM((heads, q_rows // 2, 2 * hd), BF16)] * 4
        + [pltpu.VMEM(w.shape, BF16) for w in (wo, w_gate, w_up, w_down)] + [dma(4), dma(4), dma(4)],
        compiler_params=remote(collective_id),
        name='decoder_rows',
    )(mine, dec_in, grad_out, gain, wo, w_gate, w_up, w_down)


def valid_blocks(mem_len, rows, parts, sources):
    reach = mem_len - lax.rem(lax.axis_index('seq'), parts) * rows
    blocks = jnp.minimum((reach + parts * rows - 1) // (parts * rows), sources)
    return blocks, jnp.minimum(reach - (blocks - 1) * parts * rows, rows)


def forward_kernel(scale, hd, parts, q_block, len_ref, kv_ref, q_ref, out_ref, qt_ref, top_ref):
    rows, total_q = kv_ref.shape[1], q_ref.shape[0]
    blocks, last_valid = valid_blocks(len_ref[0], rows, parts, kv_ref.shape[0])
    groups = [slice(first, first + q_block) for first in range(0, total_q, q_block)]
    base = slice(hd + 8, hd + 9)
    qt_ref[...] = q_ref[...].T

    def values_of(keys):
        return jnp.concatenate([keys.T[hd:], jnp.ones((16, rows), keys.dtype)], axis=0)

    def group_of(index):
        return pl.ds(pl.multiple_of(index * q_block, q_block), q_block)

    def first_step(group, carry):
        cols = group_of(group)
        top = jnp.max(dot(kv_ref[0], qt_ref[:, cols]), axis=0, keepdims=True)
        out_ref[hd + 8:, cols] = jnp.broadcast_to(top * scale, (8, q_block))
        top_ref[:, cols] = jnp.broadcast_to(top, (8, q_block))
        return carry

    lax.fori_loop(0, len(groups), first_step, 0)
    out_ref[:hd + 8, :] = jnp.zeros((hd + 8, total_q), F32)

    def finish(values, scores, cols):
        top_ref[:, cols] = jnp.maximum(top_ref[:, cols], jnp.max(scores.reshape(rows // 8, 8, q_block), axis=0))
        weights = jnp.exp2(scores * scale - out_ref[base, cols]).astype(values.dtype)
        out_ref[:hd + 8, cols] += dot(values, weights)[:hd + 8]

    def step(index, carry):
        keys = kv_ref[index]
        values = values_of(keys)
        for cols in groups:
            finish(values, dot(keys, qt_ref[:, cols]), cols)
        return carry

    def last_step(group, carry):
        cols = group_of(group)
        keys = kv_ref[blocks - 1]
        scores = dot(keys, qt_ref[:, cols])
        position = lax.broadcasted_iota(jnp.int32, scores.shape, 0)
        finish(values_of(keys), jnp.where(position < last_valid, scores, NEG), cols)
        return carry

    lax.fori_loop(0, blocks - 1, step, 0)
    lax.fori_loop(0, len(groups), last_step, 0)

    excess = jnp.max(top_ref[...] * scale - out_ref[hd + 8:, :])

    @pl.when(excess > 16.0)
    def _():
        out_ref[:hd + 8, :] = jnp.zeros((hd + 8, total_q), F32)
        out_ref[hd + 8:, :] = jnp.full((8, total_q), NEG, F32)

        def running(step_index, carry):
            index, group = step_index // len(groups), lax.rem(step_index, len(groups))
            cols = group_of(group)
            keys = kv_ref[index]
            limit = jnp.where(index == blocks - 1, last_valid, rows)
            scores = dot(keys, qt_ref[:, cols]) * scale
            position = lax.broadcasted_iota(jnp.int32, scores.shape, 0)
            scores = jnp.where(position < limit, scores, NEG)
            old = out_ref[base, cols]
            new = jnp.maximum(old, jnp.max(scores, axis=0, keepdims=True))
            weights = jnp.exp2(scores - new).astype(keys.dtype)
            out_ref[:hd + 8, cols] = out_ref[:hd + 8, cols] * jnp.exp2(old - new) + dot(values_of(keys), weights)[:hd + 8]
            out_ref[hd + 8:, cols] = jnp.broadcast_to(new, (8, q_block))
            return carry

        lax.fori_loop(0, blocks * len(groups), running, 0)


def attention_forward(scale, hd, parts, sources, mem_len, kv, q):
    rows, width = kv.shape[1], kv.shape[2]
    total_q = q.shape[0]
    return pl.pallas_call(
        functools.partial(forward_kernel, scale, hd, parts, min(1024, total_q)),
        out_shape=shape((hd + 16, total_q), F32),
        grid=(1,),
        in_specs=[pl.BlockSpec(memory_space=pltpu.SMEM),
                  pl.BlockSpec((sources, rows, width), lambda i: (0, 0, 0), pipeline_mode=pl.Buffered(1)), full(q)],
        out_specs=pl.BlockSpec((hd + 16, total_q), lambda i: (0, 0)),
        scratch_shapes=[pltpu.VMEM((width, total_q), BF16), pltpu.VMEM((8, total_q), F32)],
        compiler_params=plain(),
        cost_estimate=pl.CostEstimate(flops=4 * total_q * sources * rows * hd, bytes_accessed=kv.size * 2,
                                      transcendentals=total_q * sources * rows),
        name='attention_forward',
    )(mem_len, kv, q)


def backward_kernel(scale, key_scale, hd, parts, q_block, len_ref, kv_ref, q_ref, do_ref, out_ref, lse_ref, dkv_ref, dq_ref,
                    qt_ref, dot_ref, delta_ref):
    rows, total_q = kv_ref.shape[1], q_ref.shape[0]
    blocks, last_valid = valid_blocks(len_ref[0], rows, parts, kv_ref.shape[0])
    width = kv_ref.shape[2]
    groups = [slice(first, first + q_block) for first in range(0, total_q, q_block)]
    dq_ref[...] = jnp.zeros_like(dq_ref)
    qt_ref[...] = q_ref[...].T
    do_t = do_ref[...].T
    dot_ref[...] = do_t
    delta_ref[...] = jnp.sum(do_t[hd:].astype(F32) * out_ref[...], axis=0, keepdims=True)

    lane_scale = jnp.where(lax.broadcasted_iota(jnp.int32, (1, width), 1) < hd, key_scale, 1.0)

    def products(keys, cols):
        return dot(keys, qt_ref[:, cols]), dot(keys, dot_ref[:, cols])

    def finish(keys, keys_t, scores, grads, cols, valid):
        prob = jnp.exp2(scores * scale - lse_ref[:, cols])
        if valid is not None:
            position = lax.broadcasted_iota(jnp.int32, scores.shape, 0)
            prob = jnp.where(position < valid, prob, 0.0)
        grad_scores = (prob * (grads - delta_ref[:, cols])).astype(keys.dtype)
        update = dot(grad_scores, q_ref[cols, :]) + dot(prob.astype(keys.dtype), do_ref[cols, :])
        dq_ref[:, cols] += dot(keys_t, grad_scores)
        return update

    def step(index, carry):
        keys = kv_ref[index]
        keys_t = keys.T[:hd]
        total = jnp.zeros((rows, width), F32)
        for cols in groups:
            scores, grads = products(keys, cols)
            total += finish(keys, keys_t, scores, grads, cols, None)
        dkv_ref[index] = (total * lane_scale).astype(dkv_ref.dtype)
        return carry

    def last_step(group, total):
        keys = kv_ref[blocks - 1]
        cols = pl.ds(pl.multiple_of(group * q_block, q_block), q_block)
        scores, grads = products(keys, cols)
        return total + finish(keys, keys.T[:hd], scores, grads, cols, last_valid)

    def clear(index, carry):
        dkv_ref[index] = jnp.zeros((rows, width), dkv_ref.dtype)
        return carry

    lax.fori_loop(0, blocks - 1, step, 0)
    total = lax.fori_loop(0, len(groups), last_step, jnp.zeros((rows, width), F32))
    dkv_ref[blocks - 1] = (total * lane_scale).astype(dkv_ref.dtype)
    lax.fori_loop(blocks, dkv_ref.shape[0], clear, 0)
    dq_ref[...] = dq_ref[...] * key_scale


def attention_backward(scale, key_scale, hd, parts, sources, mem_len, kv, q, do, out_t, lse):
    n, rows, width = kv.shape
    total_q = q.shape[0]
    return pl.pallas_call(
        functools.partial(backward_kernel, scale, key_scale, hd, parts, min(512, total_q)),
        out_shape=[shape((n, rows, width), BF16), shape((hd, total_q), F32)],
        grid=(1,),
        in_specs=[pl.BlockSpec(memory_space=pltpu.SMEM),
                  pl.BlockSpec((sources, rows, width), lambda i: (0, 0, 0), pipeline_mode=pl.Buffered(1)),
                  full(q), full(do), full(out_t), full(lse)],
        out_specs=[pl.BlockSpec((n, rows, width), lambda i: (0, 0, 0)),
                   pl.BlockSpec((hd, total_q), lambda i: (0, 0))],
        scratch_shapes=[pltpu.VMEM((width, total_q), BF16), pltpu.VMEM((width, total_q), BF16), pltpu.VMEM((1, total_q), F32)],
        compiler_params=plain(),
        cost_estimate=pl.CostEstimate(flops=10 * total_q * sources * rows * hd, bytes_accessed=kv.size * 4,
                                      transcendentals=total_q * sources * rows),
        name='attention_backward',
    )(mem_len, kv, q, do, out_t, lse)


def reduce_kernel(n, heads, tile, chunk, gk_hbm, gv_hbm, early_hbm, late_hbm, w1_hbm, w3_hbm, w2_hbm, wo_ref, wq_ref, gain1_ref,
                  gain2_ref, dqt_ref, dqr_ref, dec_ref, gh_ref, gnorm_ref,
                  sums_ref, gdec_ref, norms_ref, n2_hbm, d1_hbm, d3_hbm, act_hbm,
                  acc_ref, pair_ref, far_ref, near_ref, n2_ref, top_ref, att_ref, decs_ref, w1_ref, w3_ref, w2_ref,
                  d1_ref, d3_ref, act_ref, mine_ref, all_ref,
                  own_sem, share_send, share_recv, pair_send, pair_recv, far_send, far_recv, near_send, near_recv, rows_sem, top_sem, w_sem, out_sem, n2_sem,
                  norm_send, norm_recv):
    g = Grid(n, heads, 0)
    side = g.side
    rows, dim = n2_ref.shape
    tiles = d1_hbm.shape[0]
    own_tiles = (tiles + g.parts - 1 - g.part) // g.parts
    part_rows = acc_ref.shape[1]
    hd = part_rows

    def start_rows_of(index):
        slot = lax.rem(index, 2)
        at = pl.ds(pl.multiple_of(index * chunk, chunk), chunk)
        for i, (src, dst) in enumerate(((late_hbm, att_ref), (early_hbm, decs_ref))):
            pltpu.make_async_copy(src.at[at, pl.ds(0, dim)], dst.at[slot], rows_sem.at[slot, i]).start()

    def tile_at(index):
        return pl.ds(pl.multiple_of(index * tile, tile), tile)

    def weights(index):
        slot = lax.rem(index, 2)
        at = tile_at(index * g.parts + g.part)
        return [pltpu.make_async_copy(src, dst.at[slot], w_sem.at[slot, i]) for i, (src, dst) in enumerate(
            ((w1_hbm.at[:, at], w1_ref), (w3_hbm.at[:, at], w3_ref), (w2_hbm.at[at, :], w2_ref)))]

    def results(index):
        slot, number = lax.rem(index, 2), index * g.parts + g.part
        pairs = ((d1_ref, d1_hbm), (d3_ref, d3_hbm), (act_ref, act_hbm))
        return ([pltpu.make_async_copy(src.at[slot], dst.at[number], out_sem.at[slot, i]) for i, (src, dst) in enumerate(pairs)],
                [send(src.at[slot], dst.at[number], share_send.at[slot, i], share_recv.at[i], g.partner)
                 for i, (src, dst) in enumerate(pairs)])

    start_rows_of(0)
    top_load = pltpu.make_async_copy(early_hbm.at[:, pl.ds(dim, dim)], top_ref, top_sem)
    top_load.start()
    for copy in weights(0):
        copy.start()

    def summand(c, core):
        source = gk_hbm if c < heads // g.parts else gv_hbm
        first = ((g.parts * c) % heads + core) * part_rows
        return source.at[pl.ds(pl.multiple_of(first, part_rows), part_rows), :]

    owns = [pltpu.make_async_copy(summand(c, g.part), acc_ref.at[c], own_sem.at[c]) for c in range(heads)]
    for copy in owns:
        copy.start()

    grad_query = jnp.concatenate([dqr_ref[h] for h in range(heads)], axis=1)
    grad_normed = dot(grad_query, wq_ref[...])
    x = dec_ref[...].astype(F32)
    inverse = lax.rsqrt(jnp.mean(x * x, axis=-1, keepdims=True) + 1e-6)
    scaled = x * inverse
    inner = grad_normed * gain1_ref[...].astype(F32)
    gdec_ref[...] = gh_ref[...] + inverse * (inner - scaled * jnp.mean(inner * scaled, axis=-1, keepdims=True))
    mine_ref[0:1, :] = jnp.sum(grad_normed * scaled, axis=0, keepdims=True)
    mine_ref[1:2, :] = gnorm_ref[...]

    meet([lax.rem(g.me + step, n) for step in range(1, n)])
    for c in range(heads):
        send(summand(c, g.parts - 1 - g.part), pair_ref.at[c], pair_send, pair_recv, g.partner).start()
    for step in range(1, n):
        send(mine_ref, all_ref.at[g.me], norm_send, norm_recv, lax.rem(g.me + step, n)).start()
    all_ref[g.me] = mine_ref[...]

    sums_ref[part_rows:, :] = jnp.zeros((sums_ref.shape[0] - part_rows, dim), F32)

    def prepare(index, carry):
        slot = lax.rem(index, 2)
        at = pl.ds(pl.multiple_of(index * chunk, chunk), chunk)
        for i, (src, dst) in enumerate(((late_hbm, att_ref), (early_hbm, decs_ref))):
            pltpu.make_async_copy(src.at[at, pl.ds(0, dim)], dst.at[slot], rows_sem.at[slot, i]).wait()

        @pl.when(index + 1 < rows // chunk)
        def _():
            start_rows_of(index + 1)

        dec = decs_ref[slot].astype(F32)
        hidden = (dec + dot(att_ref[slot], wo_ref[...])).astype(BF16).astype(F32)
        n2_ref[at, :] = rms_norm(hidden, gain2_ref[...].astype(F32)).astype(BF16)
        first = rms_norm(dec, gain1_ref[...].astype(F32)).astype(BF16)
        sums_ref[part_rows:, :] += dot(dqt_ref[:, at], first)
        return carry

    lax.fori_loop(0, rows // chunk, prepare, 0)
    top_load.wait()
    n2_store = pltpu.make_async_copy(n2_ref, n2_hbm, n2_sem)
    n2_store.start()

    quarter = part_rows // 4
    streams = [(axis, way, pl.ds((2 * axis + (way < 0)) * quarter, quarter)) for axis in (0, 1) for way in (1, -1)]

    def place_of(axis, line, other):
        return other * side + line if axis == 0 else line * side + other

    def pieces(stage, axis, line):
        position = g.row if axis == 0 else g.col
        return [place_of(axis, line, o) for o in range(side)] if stage == 0 else [place_of(axis, line, position)]

    def ring(stage, stream, step):
        axis, way, part = streams[stream]
        axis = axis if stage == 0 else 1 - axis
        here = g.col if axis == 0 else g.row
        ref, sends, recvs = (far_ref, far_send, far_recv) if stage == 0 else (near_ref, near_send, near_recv)
        to = g.near(0, way) if axis == 0 else g.near(way, 0)
        return axis, way, part, here, ref.at[stream, step - 1], sends.at[stream, step - 1], recvs.at[stream, step - 1], to

    def line_of(here, way, step):
        return lax.rem(here - way * step + 2 * side, side)

    def start_step(stage, step):
        for stream in range(4):
            axis, way, part, here, buffer, sem, recv, to = ring(stage, stream, step)
            for i, c in enumerate(pieces(stage, axis, line_of(here, way, step))):
                send(acc_ref.at[c, part], buffer.at[i], sem, recv, to).start()

    def end_step(stage, step):
        for stream in range(4):
            axis, way, part, here, buffer, sem, recv, to = ring(stage, stream, step)
            whole = send(buffer, buffer, sem, recv, g.me)
            whole.wait_recv()
            for i, c in enumerate(pieces(stage, axis, line_of(here, way, step + 1))):
                acc_ref[c, part, :] = acc_ref[c, part, :] + buffer[i]
            whole.wait_send()

    def add_pair():
        for copy in owns:
            copy.wait()
        whole = send(pair_ref, pair_ref, pair_send, pair_recv, g.me)
        whole.wait_recv()

        def add(c, carry):
            acc_ref[c] = acc_ref[c] + pair_ref[c]
            return carry

        lax.fori_loop(0, heads, add, 0)
        whole.wait_send()

    def first():
        add_pair()
        start_step(0, 1)

    def turn():
        end_step(0, side - 1)
        start_step(1, 1)

    def between(stage, step):
        def body():
            end_step(stage, step)
            start_step(stage, step + 1)
        return body

    events = ([first] + [between(0, t) for t in range(1, side - 1)] + [turn] + [between(1, t) for t in range(1, side - 1)]
              + [lambda: end_step(1, side - 1)])
    at_tile = (0, 1, 2, 4)
    inside = tiles // 2 > at_tile[-1] and len(events) > len(at_tile)

    def finish_results(index):
        stores, shares = results(index)
        for copy in stores:
            copy.wait()
        for copy in shares:
            copy.wait_send()

    def activations(index, carry):
        slot = lax.rem(index, 2)
        for copy in weights(index):
            copy.wait()

        @pl.when(index + 1 < own_tiles)
        def _():
            for copy in weights(index + 1):
                copy.start()

        @pl.when(index >= 2)
        def _():
            finish_results(index - 2)

        if inside:
            for event, when in zip(events, at_tile):
                pl.when(index == when)(event)

        w1, w3, w2t = w1_ref[slot], w3_ref[slot], w2_ref[slot].T
        for first_row in range(0, rows, chunk):
            part = slice(first_row, first_row + chunk)
            gate = dot(n2_ref[part, :], w1)
            up = dot(n2_ref[part, :], w3)
            grad = dot(top_ref[part, :], w2t)
            sig = jax.nn.sigmoid(gate)
            silu = gate * sig
            act_ref[slot, part, :] = (silu * up).astype(BF16)
            d3_ref[slot, part, :] = (grad * silu).astype(BF16)
            d1_ref[slot, part, :] = (grad * up * (sig + silu * (1.0 - sig))).astype(BF16)
        for copies in results(index):
            for copy in copies:
                copy.start()
        return carry

    lax.fori_loop(0, own_tiles, activations, 0)
    for event in events[len(at_tile):] if inside else events:
        event()
    sums_ref[:part_rows, :] = acc_ref[g.chip]

    others = all_ref.at[pl.ds(0, n - 1)]
    whole = send(others, others, norm_send, norm_recv, g.me)
    whole.wait_send()
    whole.wait_recv()
    norms_ref[...] = jnp.sum(all_ref[...], axis=0)
    n2_store.wait()
    @pl.when(own_tiles >= 2)
    def _():
        finish_results(own_tiles - 2)

    finish_results(own_tiles - 1)
    for core in range(g.parts):
        others_tiles = (tiles + core) // g.parts

        @pl.when(g.part == core)
        def _(others_tiles=others_tiles):
            for i, ref in enumerate((d1_hbm, d3_hbm, act_hbm)):
                come = ref.at[pl.ds(0, others_tiles)]
                send(come, come, share_send.at[0, i], share_recv.at[i], g.me).wait_recv()


def reduce_sums(n, heads, collective_id, gk, gv, early, late, w_gate, w_up, w_down, wo, wq, gain1, gain2, dqt, dq_rows, dec_in, gh, gnorm):
    rows, dim = early.shape[0], gk.shape[1]
    ff, tile, chunk = w_gate.shape[1], 256, min(512, early.shape[0])
    part_rows = 2 * gk.shape[0] // n
    side = math.isqrt(heads)
    hbm = pl.BlockSpec(memory_space=pl.ANY)
    return pl.pallas_call(
        functools.partial(reduce_kernel, n, heads, tile, chunk),
        out_shape=[shape((part_rows + dqt.shape[0], dim), F32), shape(gh.shape, F32), shape((2, dim), F32), shape((rows, dim), BF16)]
        + [shape((ff // tile, rows, tile), BF16)] * 3,
        in_specs=[hbm] * 7 + vmem(9),
        out_specs=vmem(3) + [hbm] * 4,
        scratch_shapes=[pltpu.VMEM((heads, part_rows, dim), F32)] * 2
        + [pltpu.VMEM((4, side - 1, side, part_rows // 4, dim), F32), pltpu.VMEM((4, side - 1, 1, part_rows // 4, dim), F32)]
        + [pltpu.VMEM((rows, dim), BF16)] * 2 + [pltpu.VMEM((2, chunk, dim), BF16)] * 2
        + [pltpu.VMEM((2, dim, tile), BF16)] * 2 + [pltpu.VMEM((2, tile, dim), BF16)] + [pltpu.VMEM((2, rows, tile), BF16)] * 3
        + [pltpu.VMEM((2, dim), F32), pltpu.VMEM((n, 2, dim), F32)]
        + [dma(heads), dma(2, 3), dma(3), pltpu.SemaphoreType.DMA, pltpu.SemaphoreType.DMA, dma(4, side - 1), dma(4, side - 1), dma(4, side - 1),
           dma(4, side - 1), dma(2, 2), pltpu.SemaphoreType.DMA, dma(2, 3), dma(2, 3), pltpu.SemaphoreType.DMA,
           pltpu.SemaphoreType.DMA, pltpu.SemaphoreType.DMA],
        compiler_params=remote(collective_id),
        cost_estimate=pl.CostEstimate(flops=6 * rows * dim * ff, bytes_accessed=12 * rows * ff, transcendentals=rows * ff),
        name='reduce_sums',
    )(gk, gv, early, late, w_gate, w_up, w_down, wo, wq, gain1, gain2, dqt, dq_rows, dec_in, gh, gnorm)


def mlp_kernel(n2_ref, top_ref, d1_ref, d3_ref, act_ref, g1_ref, g3_ref, g2_ref, n2t_ref):
    @pl.when(pl.program_id(0) == 0)
    def _():
        n2t_ref[...] = n2_ref[...].T

    g1_ref[...] = dot(n2t_ref[...], d1_ref[...])
    g3_ref[...] = dot(n2t_ref[...], d3_ref[...])
    g2_ref[...] = dot_tn(act_ref[...], top_ref[...])


def mlp_weight_grads(n2, early, d1, d3, act):
    rows, dim = n2.shape
    tile = d1.shape[2]
    ff = d1.shape[0] * tile
    cols = pl.BlockSpec((dim, tile), lambda i: (0, i))
    tall = pl.BlockSpec((tile, dim), lambda i: (i, 0))
    part = pl.BlockSpec((pl.Squeezed(), rows, tile), lambda i: (i, 0, 0))
    return pl.pallas_call(
        mlp_kernel,
        out_shape=[shape((dim, ff), F32), shape((dim, ff), F32), shape((ff, dim), F32)],
        grid=(ff // tile,),
        in_specs=[full(n2), pl.BlockSpec((rows, dim), lambda i: (0, 1), pipeline_mode=pl.Buffered(1)), part, part, part],
        out_specs=[cols, cols, tall],
        scratch_shapes=[pltpu.VMEM((dim, rows), BF16)],
        compiler_params=plain(),
        cost_estimate=pl.CostEstimate(flops=6 * rows * dim * ff, bytes_accessed=18 * dim * ff, transcendentals=0),
        name='mlp_weight_grads',
    )(n2, early, d1, d3, act)


def memory_weight_kernel(memory_ref, dkv_ref, gk_ref, gv_ref):
    group, hd = dkv_ref.shape[0], dkv_ref.shape[2] // 2
    for i in range(group):
        both = dot_tn(dkv_ref[i], memory_ref[...])
        gk_ref[i * hd:(i + 1) * hd, :] = both[:hd]
        gv_ref[i * hd:(i + 1) * hd, :] = both[hd:]


def memory_weight_grads(memory, dkv):
    heads, rows, width = dkv.shape
    dim, hd = memory.shape[1], width // 2
    group = 4
    out = pl.BlockSpec((group * hd, dim), lambda i: (i, 0))
    return pl.pallas_call(
        memory_weight_kernel,
        out_shape=[shape((heads * hd, dim), F32)] * 2,
        grid=(heads // group,),
        in_specs=[full(memory), pl.BlockSpec((group, rows, width), lambda i: (i, 0, 0))],
        out_specs=[out, out],
        compiler_params=plain(),
        cost_estimate=pl.CostEstimate(flops=2 * rows * dim * heads * width, bytes_accessed=16 * rows * dim, transcendentals=0),
        name='memory_weight_grads',
    )(memory, dkv)


def memory_grad_kernel(dkv_ref, wk_ref, wv_ref, out_ref):
    group = dkv_ref.shape[0]
    left = jnp.concatenate([dkv_ref[i] for i in range(group)], axis=1)
    right = jnp.concatenate([part[i] for i in range(group) for part in (wk_ref, wv_ref)], axis=0)

    @pl.when(pl.program_id(0) == 0)
    def _():
        out_ref[...] = dot(left, right)

    @pl.when(pl.program_id(0) > 0)
    def _():
        out_ref[...] += dot(left, right)


def memory_grad(dkv, wk_t, wv_t):
    heads, rows, width = dkv.shape
    hd, dim = wk_t.shape[1], wk_t.shape[2]
    group = 4
    weight = pl.BlockSpec((group, hd, dim), lambda i: (i, 0, 0))
    return pl.pallas_call(
        memory_grad_kernel,
        out_shape=shape((rows, dim), F32),
        grid=(heads // group,),
        in_specs=[pl.BlockSpec((group, rows, width), lambda i: (i, 0, 0)), weight, weight],
        out_specs=pl.BlockSpec((rows, dim), lambda i: (0, 0)),
        compiler_params=plain(),
        cost_estimate=pl.CostEstimate(flops=2 * rows * dim * heads * width, bytes_accessed=12 * rows * dim, transcendentals=0),
        name='memory_grad',
    )(dkv, wk_t, wv_t)


def outer_kernel(att_ref, gh_ref, out_ref):
    @pl.when(pl.program_id(0) == 0)
    def _():
        out_ref[...] = jnp.zeros_like(out_ref)

    out_ref[...] += dot_tn(att_ref[...], gh_ref[...])


def outer_weight_grad(late, dim):
    rows = late.shape[0]
    chunk = min(512, rows)
    return pl.pallas_call(
        outer_kernel,
        out_shape=shape((dim, dim), F32),
        grid=(rows // chunk,),
        in_specs=[pl.BlockSpec((chunk, dim), lambda i: (i, 0)), pl.BlockSpec((chunk, dim), lambda i: (i, 1))],
        out_specs=pl.BlockSpec((dim, dim), lambda i: (0, 0)),
        compiler_params=plain(),
        cost_estimate=pl.CostEstimate(flops=2 * rows * dim * dim, bytes_accessed=8 * rows * dim, transcendentals=0),
        name='outer_weight_grad',
    )(late, late)


def unpack_kernel(gk_ref, gv_ref, gq_ref, k_ref, v_ref, q_ref):
    k_ref[...] = gk_ref[...].reshape(k_ref.shape)
    v_ref[...] = gv_ref[...].reshape(v_ref.shape)
    q_ref[...] = gq_ref[...].reshape(q_ref.shape)


def unpack_sums(total, rows):
    n, both, dim = total.shape
    more = both - rows
    step = 2
    per = rows // more
    out = pl.BlockSpec((step * rows, dim), lambda i: (i, 0))
    return pl.pallas_call(
        unpack_kernel,
        out_shape=[shape((n // 2 * rows, dim), F32)] * 3,
        grid=(n // 2 // step,),
        in_specs=[pl.BlockSpec((step, rows, dim), lambda i: (i, 0, 0)),
                  pl.BlockSpec((step, rows, dim), lambda i: (i + n // 2 // step, 0, 0)),
                  pl.BlockSpec((step * per, more, dim), lambda i: (i, per, 0))],
        out_specs=[out, out, out],
        compiler_params=plain(),
        cost_estimate=pl.CostEstimate(flops=total.size, bytes_accessed=8 * total.size, transcendentals=0),
        name='unpack_sums',
    )(total, total, total)


def solution(mesh):
    n = mesh.shape['seq']
    row_spec = P(('data', 'seq'), None)
    weight_spec = P()
    part_vec = P('data')
    part_mat = P('data', None)
    part_cube = P('data', None, None)

    def device_step(dec_in, memory, mem_len, grad_out, norm_attn, wq_cross, wk_cross, wv_cross, wo_cross, norm_mlp, w_gate, w_up, w_down):
        q_rows, dim = dec_in.shape
        heads, hd = wq_cross.shape[1], wq_cross.shape[2]
        parts = n // heads
        sources = -(-3 * n // 4)
        total_q = q_rows * n
        key_scale = hd ** -0.5
        scale = key_scale * LOG2E
        wq_t, wk_t, wv_t = (jnp.transpose(w, (1, 2, 0)) for w in (wq_cross, wk_cross, wv_cross))
        source_rows = -(-sources // (parts * math.isqrt(heads)))
        kv, q_in, early_local = exchange(n, heads, source_rows, 0, memory, dec_in, grad_out, norm_attn, wk_t, wv_t, wq_t)
        head_q = q_in.reshape(total_q, 2 * hd)

        early = lax.all_gather(early_local, 'seq', axis=0, tiled=True)

        wo = wo_cross.reshape(heads * hd, dim)
        mine = attention_forward(scale, hd, parts, sources, mem_len, kv, head_q)
        out_t, lse, do_in, factors, grad_hidden, g_norm_mlp = decoder_rows(
            n, heads, 1, mine, dec_in, grad_out, norm_mlp, wo, w_gate, w_up, w_down)
        do_in, factors, early = lax.optimization_barrier((do_in, factors, early))
        late = lax.all_gather(factors, 'seq', axis=0, tiled=True)

        dkv, dq_part = attention_backward(scale, key_scale, hd, parts, sources, mem_len, kv, head_q, do_in.reshape(total_q, 2 * hd), out_t, lse)
        dkv_in, dq_rows, dq_t = return_blocks(n, heads, source_rows, 4, dkv, dq_part)
        dkv_in, dq_rows, late = lax.optimization_barrier((dkv_in, dq_rows, late))

        gk_part, gv_part = memory_weight_grads(memory, dkv_in)
        sums, g_dec, norms, n2_all, d1, d3, act = reduce_sums(
            n, heads, 5, gk_part, gv_part, early, late, w_gate, w_up, w_down, wo, wq_t.reshape(heads * hd, dim), norm_attn, norm_mlp,
            dq_t, dq_rows, dec_in, grad_hidden, g_norm_mlp)
        sums, n2_all, d1, d3, act, dkv_in, late, early = lax.optimization_barrier((sums, n2_all, d1, d3, act, dkv_in, late, early))
        total = lax.all_gather(sums, 'seq', axis=0, tiled=False)
        g_gate, g_up, g_down = mlp_weight_grads(n2_all, early, d1, d3, act)
        g_wo = outer_weight_grad(late, dim)
        g_mem = memory_grad(dkv_in, wk_t, wv_t)

        rows = 2 * heads * hd // n
        cube = lambda g: jnp.transpose(g.reshape(heads, hd, dim), (2, 0, 1))
        g_wk, g_wv, g_wq = unpack_sums(total, rows)
        return (g_dec, g_mem, norms[0], cube(g_wq), cube(g_wk), cube(g_wv), g_wo.reshape(heads, hd, dim), norms[1], g_gate, g_up, g_down)

    return jax.shard_map(device_step, mesh=mesh,
                         in_specs=(row_spec, row_spec, part_vec, row_spec) + (weight_spec,) * 9,
                         out_specs=(row_spec, row_spec, part_vec, part_cube, part_cube, part_cube, part_cube, part_vec, part_mat, part_mat, part_mat),
                         check_vma=False)
```

```python
import functools
import math

import jax
import jax.numpy as jnp
from jax import lax
from jax.experimental import pallas as pl
from jax.experimental.pallas import tpu as pltpu
from jax.sharding import PartitionSpec as P

LOG2E = 1.4426950408889634
NEG = -1e30
VMEM_LIMIT = 60 * 1024 * 1024
MESH = pl.DeviceIdType.MESH
BF16, F32 = jnp.bfloat16, jnp.float32


def rms_norm(tensor, gain):
    mean_sq = jnp.mean(tensor * tensor, axis=-1, keepdims=True)
    return tensor * lax.rsqrt(mean_sq + 1e-6) * gain


def dot(a, b):
    return jnp.dot(a, b, preferred_element_type=F32)


def dot_nt(a, b):
    return lax.dot_general(a, b, (((1,), (1,)), ((), ())), preferred_element_type=F32)


def dot_tn(a, b):
    return lax.dot_general(a, b, (((0,), (0,)), ((), ())), preferred_element_type=F32)


def full(array):
    return pl.BlockSpec(array.shape, lambda *_: (0,) * array.ndim, pipeline_mode=pl.Buffered(1))


def vmem(count):
    return [pl.BlockSpec(memory_space=pltpu.VMEM)] * count


def plain():
    return pltpu.CompilerParams(vmem_limit_bytes=VMEM_LIMIT)


def remote(collective_id):
    return pltpu.CompilerParams(collective_id=collective_id, has_side_effects=True, vmem_limit_bytes=VMEM_LIMIT)


def shape(dims, dtype):
    return jax.ShapeDtypeStruct(dims, dtype)


def meet(peers):
    barrier = pltpu.get_barrier_semaphore()
    for peer in peers:
        pl.semaphore_signal(barrier, inc=1, device_id={'seq': peer}, device_id_type=MESH)
    pl.semaphore_wait(barrier, len(peers))


def send(src, dst, send_sem, recv_sem, peer):
    return pltpu.make_async_remote_copy(src_ref=src, dst_ref=dst, send_sem=send_sem, recv_sem=recv_sem,
                                        device_id={'seq': peer}, device_id_type=MESH)


class Grid:
    def __init__(self, n, heads, source_rows):
        self.n, self.heads, self.source_rows = n, heads, source_rows
        self.parts = n // heads
        self.side = math.isqrt(heads)
        self.me = lax.axis_index('seq')
        self.part = lax.rem(self.me, self.parts)
        self.chip = self.me // self.parts
        self.col = lax.rem(self.chip, self.side)
        self.row = self.chip // self.side
        self.partner = self.chip * self.parts + (self.parts - 1 - self.part)
        self.ties = self.side == 4
        self.direct = (1, 3) if self.ties else (1,)

    def wrap(self, value):
        return lax.rem(value + self.side, self.side)

    def device(self, row, col, part):
        return (row * self.side + col) * self.parts + part

    def near(self, drow, dcol, part=None):
        return self.device(self.wrap(self.row + drow), self.wrap(self.col + dcol), self.part if part is None else part)

    def hop(self, offset):
        return 1 if offset == 1 else -1

    def is_source(self, row):
        return self.wrap(row) < self.source_rows

    def row_peers(self):
        return [lax.rem(self.chip + step, self.heads) * self.parts + self.part for step in range(1, self.heads)]

    def peers(self):
        return self.row_peers() + [self.partner] + [self.near(0, self.hop(d), self.parts - 1 - self.part) for d in self.direct]


def pair_peers(n, heads, me, part):
    parts = n // heads
    head = me // parts
    partner = head * parts + (parts - 1 - part)
    return partner, [partner] + [lax.rem(head + step, heads) * parts + part for step in range(1, heads)]


def pack(rows):
    middle = rows.shape[-2] // 2
    return jnp.concatenate([rows[..., :middle, :], rows[..., middle:, :]], axis=-1)


def unpack(packed):
    middle = packed.shape[-1] // 2
    return jnp.concatenate([packed[..., :middle], packed[..., middle:]], axis=-2)


def start_rows(n, heads, me, part, src, src_of, dst_ref, send_sem, recv_sem):
    parts = n // heads
    head = me // parts
    for step in range(1, heads):
        peer = lax.rem(head + step, heads) * parts + part
        send(src.at[src_of(peer)], dst_ref.at[head], send_sem, recv_sem, peer).start()
    dst_ref[head] = src[src_of(me)]


def wait_rows(heads, me, dst_ref, send_sem, recv_sem):
    others = dst_ref.at[pl.ds(0, heads - 1)]
    whole = send(others, others, send_sem, recv_sem, me)
    whole.wait_send()
    whole.wait_recv()


def swap(src, dst, send_sem, recv_sem, partner):
    copy = send(src, dst, send_sem, recv_sem, partner)
    copy.start()
    copy.wait()


def place(n, heads, part, mine_ref, theirs_ref, wide_ref, low):
    parts = n // heads
    for source, index in ((mine_ref, part), (theirs_ref, parts - 1 - part)):
        for head in range(heads):
            rows = unpack(source[head])
            zeros = jnp.zeros_like(rows)
            wide_ref[head * parts + index] = jnp.concatenate([rows, zeros] if low else [zeros, rows], axis=-1)


def exchange_kernel(n, heads, source_rows, memory_ref, dec_ref, gout_ref, gain_ref, wk_ref, wv_ref, wq_ref, kv_out_ref, q_out_ref, early_ref,
                    kv_ref, stage_ref, up_ref, down_ref, right_ref, left_ref, packed_ref, got_ref, swapped_ref,
                    row_send, row_recv, y_send, pass_send, x_send, fwd_send, stage_recv, up_recv, down_recv, right_recv,
                    left_recv, out_recv):
    g = Grid(n, heads, source_rows)
    side, hd = g.side, wk_ref.shape[1]
    half = kv_out_ref.shape[1]
    chunk_rows = min(256, kv_ref.shape[1])
    barrier = pltpu.get_barrier_semaphore()
    peers = g.peers()
    for peer in peers:
        pl.semaphore_signal(barrier, inc=1, device_id={'seq': peer}, device_id_type=MESH)

    dim = dec_ref.shape[1]
    early_ref[:, :dim] = dec_ref[...]
    early_ref[:, dim:] = gout_ref[...].astype(BF16)
    normed = rms_norm(dec_ref[...].astype(F32), gain_ref[...].astype(F32)).astype(BF16)

    def some_heads(index, carry):
        queries = dot_nt(normed, jnp.concatenate([wq_ref[4 * index + j] for j in range(4)], axis=0)).astype(BF16)
        for j in range(4):
            packed_ref[4 * index + j] = pack(queries[:, hd * j:hd * (j + 1)])
        return carry

    lax.fori_loop(0, heads // 4, some_heads, 0)

    def head(drow, dcol):
        return g.wrap(g.row + drow) * side + g.wrap(g.col + dcol)

    def project(drow, dcols):
        weights = jnp.concatenate([ref[head(drow, d)] for d in dcols for ref in (wk_ref, wv_ref)], axis=0)

        def rows(index, carry):
            at = pl.ds(pl.multiple_of(index * chunk_rows, chunk_rows), chunk_rows)
            both = dot_nt(memory_ref[at, :], weights).astype(BF16)
            for i, d in enumerate(dcols):
                kv_ref[head(drow, d), at, :] = both[:, 2 * hd * i:2 * hd * (i + 1)]
            return carry

        lax.fori_loop(0, kv_ref.shape[1] // chunk_rows, rows, 0)

    def along_column(drow, dcol):
        chunk = kv_ref.at[head(drow, dcol)]
        if drow in g.direct:
            send(chunk, stage_ref.at[drow - 1, dcol], y_send.at[drow - 1], stage_recv.at[drow - 1, dcol], g.near(g.hop(drow), 0)).start()
        elif dcol % 2 == 0:
            send(chunk, up_ref.at[dcol // 2], y_send.at[drow - 1], up_recv.at[dcol // 2], g.near(1, 0)).start()
        else:
            send(chunk, down_ref.at[dcol // 2], y_send.at[drow - 1], down_recv.at[dcol // 2], g.near(-1, 0)).start()

    def along_row(o, dcol):
        chunk = kv_ref.at[head(0, dcol)] if o == 0 else stage_ref.at[o - 1, dcol]
        source = g.device(g.wrap(g.row - o), g.col, g.part)
        if dcol == 0:
            kv_out_ref[source] = chunk[pl.ds(pl.multiple_of(g.part * half, half), half), :]
            away = pl.ds(pl.multiple_of((g.parts - 1 - g.part) * half, half), half)
            send(chunk.at[away], kv_out_ref.at[source], x_send.at[o], out_recv, g.partner).start()
        elif dcol in g.direct:
            for part in range(g.parts):
                send(chunk.at[pl.ds(part * half, half)], kv_out_ref.at[source], x_send.at[o], out_recv,
                     g.near(0, g.hop(dcol), part)).start()
        else:
            send(chunk.at[pl.ds(0, half)], right_ref.at[o], x_send.at[o], right_recv.at[o], g.near(0, 1)).start()
            send(chunk.at[pl.ds(half, half)], left_ref.at[o], x_send.at[o], left_recv.at[o], g.near(0, -1)).start()

    def pass_row(o):
        for ref, sem, come in ((right_ref, right_recv, -1), (left_ref, left_recv, 1)):
            source = g.device(g.wrap(g.row - o), g.wrap(g.col + come), g.part)
            send(ref.at[o], ref.at[o], fwd_send.at[o], sem.at[o], g.me).wait_recv()
            send(ref.at[o], kv_out_ref.at[source], fwd_send.at[o], out_recv, g.near(0, -come, 0 if come < 0 else 1)).start()

    def when_source(row, body):
        pl.when(g.is_source(row))(body)

    if g.ties:
        order = [(2, (2, 1)), (2, (3, 0)), (1, (2, 1)), (3, (2, 3)), (0, (2, 1)), (0, (3, 0))]
        last = [(1, (3, 0)), (3, (1, 0))]
    else:
        order, last = [(1, (1, 0)), (0, (1, 0))], []

    def issue(drow, dcols):
        def body():
            for d in dcols:
                along_row(0, d) if drow == 0 else along_column(drow, d)
        when_source(g.row, body)

    waiting = None
    for drow, dcols in order + last:
        project(drow, dcols)
        if waiting is None:
            pl.semaphore_wait(barrier, len(peers))
            start_rows(n, heads, g.me, g.part, packed_ref, lambda peer: peer // g.parts, got_ref, row_send.at[0], row_recv.at[0])
        elif waiting not in last:
            issue(*waiting)
        waiting = (drow, dcols)
    if not last:
        issue(*waiting)

    if g.ties:
        def up(i):
            send(up_ref.at[i], up_ref.at[i], pass_send.at[0], up_recv.at[i], g.me).wait_recv()
            send(up_ref.at[i], stage_ref.at[1, 2 * i], pass_send.at[0], stage_recv.at[1, 2 * i], g.near(1, 0)).start()

        def down(i):
            send(down_ref.at[i], down_ref.at[i], pass_send.at[1], down_recv.at[i], g.me).wait_recv()
            send(down_ref.at[i], stage_ref.at[1, 2 * i + 1], pass_send.at[1], stage_recv.at[1, 2 * i + 1], g.near(-1, 0)).start()

        for i in range(2):
            when_source(g.row - 1, lambda i=i: up(1 - i))
            when_source(g.row + 1, lambda i=i: down(i))
        for drow, dcols in last:
            issue(drow, dcols)
        when_source(g.row, lambda: pass_row(0))

    wait_rows(heads, g.me, got_ref, row_send.at[0], row_recv.at[0])
    swap(got_ref, swapped_ref, row_send.at[1], row_recv.at[1], g.partner)
    place(n, heads, g.part, got_ref, swapped_ref, q_out_ref, True)

    def arrived(o, dcol):
        def body():
            send(stage_ref.at[o - 1, dcol], stage_ref.at[o - 1, dcol], y_send.at[0], stage_recv.at[o - 1, dcol], g.me).wait_recv()
            along_row(o, dcol)
        when_source(g.row - o, body)

    if g.ties:
        for o, d in ((1, 2), (3, 2), (1, 1), (3, 3)):
            arrived(o, d)
        for o in g.direct:
            when_source(g.row - o, lambda o=o: pass_row(o))
        for d in (2, 1, 0, 3):
            arrived(2, d)
        when_source(g.row - 2, lambda: pass_row(2))
        for o, d in ((1, 3), (3, 1), (1, 0), (3, 0)):
            arrived(o, d)
    else:
        for d in (1, 0):
            arrived(1, d)

    def sent(sem, ref):
        send(ref, ref, sem, out_recv, g.me).wait_send()

    def mine():
        for drow in range(1, side):
            sent(y_send.at[drow - 1], stage_ref.at[0])
    when_source(g.row, mine)
    for o in range(side):
        def passed(o=o):
            sent(x_send.at[o], kv_out_ref.at[pl.ds(0, g.parts * side - 1)])
            if g.ties:
                sent(fwd_send.at[o], kv_out_ref.at[pl.ds(0, 2)])
        when_source(g.row - o, passed)
    if g.ties:
        when_source(g.row - 1, lambda: sent(pass_send.at[0], up_ref))
        when_source(g.row + 1, lambda: sent(pass_send.at[1], down_ref))
    blocks = source_rows * side * g.parts
    others = kv_out_ref.at[pl.ds(0, blocks - source_rows)]
    send(others, others, y_send.at[0], out_recv, g.me).wait_recv()


def row_scratch(heads, q_rows, hd):
    return [pltpu.VMEM((heads, q_rows // 2, 2 * hd), BF16)] * 3


def dma(*dims):
    return pltpu.SemaphoreType.DMA(dims)


def exchange(n, heads, source_rows, collective_id, memory, dec_in, grad_out, gain, wk_t, wv_t, wq_t):
    m_rows, q_rows, hd = memory.shape[0], dec_in.shape[0], wk_t.shape[1]
    side, parts = math.isqrt(heads), n // heads
    half = m_rows // parts
    chunk = lambda *lead: pltpu.VMEM(lead + (m_rows, 2 * hd), BF16)
    block = lambda *lead: pltpu.VMEM(lead + (half, 2 * hd), BF16)
    return pl.pallas_call(
        functools.partial(exchange_kernel, n, heads, source_rows),
        out_shape=[shape((n, half, 2 * hd), BF16), shape((n, q_rows, 2 * hd), BF16), shape((q_rows, 2 * dec_in.shape[1]), BF16)],
        in_specs=vmem(7),
        out_specs=vmem(3),
        scratch_shapes=[chunk(heads), chunk(side - 1, side), chunk(2), chunk(2), block(side), block(side)]
        + row_scratch(heads, q_rows, hd)
        + [dma(2), dma(2), dma(side - 1), dma(2), dma(side), dma(side), dma(side - 1, side), dma(2), dma(2), dma(side), dma(side),
           pltpu.SemaphoreType.DMA],
        compiler_params=remote(collective_id),
        name='exchange',
    )(memory, dec_in, grad_out, gain, wk_t, wv_t, wq_t)


def return_kernel(n, heads, source_rows, chunk, src_ref, dq_ref, gain_ref, early_hbm, dst_ref, rows_ref, gq_ref, stage_ref, right_ref,
                  left_ref, up_ref, down_ref, theirs_ref, packed_ref, got_ref, dqt_ref, decs_ref, dec_sem, row_send, row_recv,
                  x_send, fwd_send, y_send, pass_send, stage_recv, right_recv, left_recv, up_recv, down_recv, out_recv):
    g = Grid(n, heads, source_rows)
    side = g.side
    half = src_ref.shape[1]
    total_rows, dim = dqt_ref.shape[1], gq_ref.shape[1]

    def dec_load(index, slot):
        at = pl.ds(pl.multiple_of(index * chunk, chunk), chunk)
        return pltpu.make_async_copy(early_hbm.at[at, pl.ds(0, dim)], decs_ref.at[slot], dec_sem.at[slot])

    dec_load(0, 0).start()
    meet(g.peers())
    mine = pl.ds(pl.multiple_of(g.part * half, half), half)

    def landing(drow, dcol, head_col):
        if drow == 0:
            return dst_ref.at[g.row * side + head_col, mine], out_recv
        return stage_ref.at[drow - 1, dcol, mine], stage_recv.at[drow - 1, dcol]

    def along_row(drow, dcol):
        row = g.wrap(g.row + drow)
        col = g.wrap(g.col + dcol)
        for part in range(g.parts):
            source = src_ref.at[g.device(row, col, part)]
            if dcol in g.direct:
                dst, sem = landing(drow, dcol, g.col)
                send(source, dst, x_send.at[drow], sem, g.near(0, g.hop(dcol), part)).start()
            elif part == 0:
                send(source, right_ref.at[drow], x_send.at[drow], right_recv.at[drow], g.near(0, 1)).start()
            else:
                send(source, left_ref.at[drow], x_send.at[drow], left_recv.at[drow], g.near(0, -1)).start()

    def own_chip(drow):
        row = g.wrap(g.row + drow)
        away = src_ref.at[g.device(row, g.col, g.parts - 1 - g.part)]
        dst, sem = landing(drow, 0, g.col)
        dst[...] = src_ref[g.device(row, g.col, g.part)]
        send(away, dst, x_send.at[drow], sem, g.partner).start()

    def pass_row(drow):
        for ref, come_sem, come in ((right_ref, right_recv, -1), (left_ref, left_recv, 1)):
            send(ref.at[drow], ref.at[drow], fwd_send.at[drow], come_sem.at[drow], g.me).wait_recv()
            dst, sem = landing(drow, 2, g.wrap(g.col + come))
            send(ref.at[drow], dst, fwd_send.at[drow], sem, g.near(0, -come, 0 if come < 0 else 1)).start()

    def along_column(drow, dcol):
        chunk = stage_ref.at[drow - 1, dcol]
        got = chunk.at[pl.ds(0, half)] if dcol == 0 else chunk
        send(got, got, y_send.at[drow - 1], stage_recv.at[drow - 1, dcol], g.me).wait_recv()
        head = g.row * side + g.wrap(g.col - dcol)
        if drow in g.direct:
            send(chunk, dst_ref.at[head], y_send.at[drow - 1], out_recv, g.near(g.hop(drow), 0)).start()
        elif dcol % 2 == 0:
            send(chunk, up_ref.at[dcol // 2], y_send.at[drow - 1], up_recv.at[dcol // 2], g.near(1, 0)).start()
        else:
            send(chunk, down_ref.at[dcol // 2], y_send.at[drow - 1], down_recv.at[dcol // 2], g.near(-1, 0)).start()

    def when_source(row, body):
        pl.when(g.is_source(row))(body)

    def rows_of(drow):
        def body():
            for d in (2, 1, 3) if g.ties else (1,):
                along_row(drow, d)
        when_source(g.row + drow, body)

    def relay(drow):
        when_source(g.row + drow, lambda: pass_row(drow))

    def column(drow, d):
        when_source(g.row + drow, lambda: along_column(drow, d))

    def up(i):
        def body():
            send(up_ref.at[i], up_ref.at[i], pass_send.at[0], up_recv.at[i], g.me).wait_recv()
            head = g.wrap(g.row - 1) * side + g.wrap(g.col - 2 * i)
            send(up_ref.at[i], dst_ref.at[head], pass_send.at[0], out_recv, g.near(1, 0)).start()
        when_source(g.row + 1, body)

    def down(i):
        def body():
            send(down_ref.at[i], down_ref.at[i], pass_send.at[1], down_recv.at[i], g.me).wait_recv()
            head = g.wrap(g.row + 1) * side + g.wrap(g.col - 2 * i - 1)
            send(down_ref.at[i], dst_ref.at[head], pass_send.at[1], out_recv, g.near(-1, 0)).start()
        when_source(g.row - 1, body)

    def start_dq():
        swap(dq_ref, theirs_ref, row_send.at[0], row_recv.at[0], g.partner)
        both = (dq_ref[...] + theirs_ref[...]).astype(BF16)
        share = dqt_ref.shape[0]
        dqt_ref[...] = jnp.where(g.part == 0, both[:share], both[share:])
        total = both.T
        packed_ref[...] = pack(total.reshape(n, total.shape[0] // n, total.shape[1]))
        start_rows(n, heads, g.me, g.part, packed_ref, lambda peer: peer, got_ref, row_send.at[1], row_recv.at[1])

    def query_weight(index, carry):
        slot = lax.rem(index, 2)
        dec_load(index, slot).wait()

        @pl.when(index + 1 < chunks)
        def _():
            dec_load(index + 1, 1 - slot).start()

        normed = rms_norm(decs_ref[slot].astype(F32), gain_ref[...].astype(F32)).astype(BF16)
        gq_ref[...] += dot(dqt_ref[:, pl.ds(pl.multiple_of(index * chunk, chunk), chunk)], normed)
        return carry

    chunks = total_rows // chunk
    for drow in (2, 1, 3, 0) if g.ties else (1, 0):
        when_source(g.row + drow, lambda drow=drow: own_chip(drow))
    if g.ties:
        rows_of(2)
        for drow in (2, 1, 3):
            column(drow, 0)
        relay(2)
        rows_of(1)
        column(2, 1)
        column(2, 3)
        column(2, 2)
        relay(1)
        rows_of(3)
        start_dq()
        up(0)
        down(0)
        column(1, 1)
        column(1, 3)
        column(1, 2)
        relay(3)
        rows_of(0)
        up(1)
        down(1)
        column(3, 1)
        column(3, 3)
        column(3, 2)
        relay(0)
    else:
        rows_of(1)
        rows_of(0)
        start_dq()
        column(1, 0)
        column(1, 1)
    gq_ref[...] = jnp.zeros_like(gq_ref)
    lax.fori_loop(0, chunks, query_weight, 0)
    wait_rows(heads, g.me, got_ref, row_send.at[1], row_recv.at[1])
    rows_ref[...] = unpack(got_ref[...])

    def sent(sem, ref):
        send(ref, ref, sem, out_recv, g.me).wait_send()

    for drow in range(side):
        def done(drow=drow):
            sent(x_send.at[drow], src_ref.at[pl.ds(0, g.parts * side - 1)])
            if g.ties:
                sent(fwd_send.at[drow], src_ref.at[pl.ds(0, 2)])
            if drow:
                sent(y_send.at[drow - 1], stage_ref.at[0])
        when_source(g.row + drow, done)
    if g.ties:
        when_source(g.row + 1, lambda: sent(pass_send.at[0], up_ref))
        when_source(g.row - 1, lambda: sent(pass_send.at[1], down_ref))

    @pl.when(g.is_source(g.row))
    def _():
        blocks = src_ref.at[pl.ds(0, n - 1)]
        send(blocks, blocks, y_send.at[0], out_recv, g.me).wait_recv()

    @pl.when(jnp.logical_not(g.is_source(g.row)))
    def _():
        def clear(index, carry):
            dst_ref[index] = jnp.zeros(dst_ref.shape[1:], dst_ref.dtype)
            return carry
        lax.fori_loop(0, heads, clear, 0)


def return_blocks(n, heads, source_rows, collective_id, blocks, dq, gain, early):
    half, width = blocks.shape[1], blocks.shape[2]
    hd, total_q = dq.shape
    q_rows = total_q // n
    side, parts = math.isqrt(heads), n // heads
    chunk = lambda *lead: pltpu.VMEM(lead + (half * parts, width), BF16)
    block = lambda *lead: pltpu.VMEM(lead + (half, width), BF16)
    piece, dim = min(512, total_q), early.shape[1] // 2
    return pl.pallas_call(
        functools.partial(return_kernel, n, heads, source_rows, piece),
        out_shape=[shape((heads, half * parts, width), BF16), shape((heads, q_rows, hd), BF16), shape((hd // parts, dim), F32)],
        in_specs=vmem(3) + [pl.BlockSpec(memory_space=pl.ANY)],
        out_specs=vmem(3),
        scratch_shapes=[chunk(side - 1, side), block(side), block(side), chunk(2), chunk(2), pltpu.VMEM(dq.shape, F32),
                        pltpu.VMEM((n, q_rows // 2, 2 * hd), BF16), pltpu.VMEM((heads, q_rows // 2, 2 * hd), BF16),
                        pltpu.VMEM((hd // parts, total_q), BF16), pltpu.VMEM((2, piece, dim), BF16), dma(2), dma(2), dma(2),
                        dma(side), dma(side), dma(side - 1), dma(2), dma(side - 1, side), dma(side), dma(side), dma(2), dma(2),
                        pltpu.SemaphoreType.DMA],
        compiler_params=remote(collective_id),
        name='return_blocks',
    )(blocks, dq, gain, early)


def decoder_kernel(n, heads, mine_ref, dec_ref, gout_ref, gain_ref, wo_hbm, wg_hbm, wu_hbm, wd_hbm,
                   out_ref, lse_ref, do_ref, factors_ref, gh_ref, gnorm_ref,
                   theirs_ref, packed_ref, got_ref, sent_ref, back_ref, swapped_ref, wo_ref, wg_ref, wu_ref, wd_ref, gact_ref,
                   load_sem, send_sem, recv_sem):
    me = lax.axis_index('seq')
    part = lax.rem(me, n // heads)
    partner, peers = pair_peers(n, heads, me, part)
    q_rows, dim = dec_ref.shape
    hd = out_ref.shape[0]
    loads = [pltpu.make_async_copy(src, dst, load_sem.at[i]) for i, (src, dst) in enumerate(
        ((wd_hbm, wd_ref), (wo_hbm, wo_ref), (wg_hbm, wg_ref), (wu_hbm, wu_ref)))]
    for load in loads:
        load.start()
    meet(peers)

    swap(mine_ref, theirs_ref, send_sem.at[0], recv_sem.at[0], partner)
    m_a, m_b = mine_ref[hd + 8:hd + 9], theirs_ref[hd + 8:hd + 9]
    top = jnp.maximum(m_a, m_b)
    s_a, s_b = jnp.exp2(m_a - top), jnp.exp2(m_b - top)
    den = mine_ref[hd:hd + 1] * s_a + theirs_ref[hd:hd + 1] * s_b
    out = (mine_ref[:hd] * s_a + theirs_ref[:hd] * s_b) / den
    packed_ref[...] = pack(out.T.astype(BF16).reshape(n, q_rows, hd))
    start_rows(n, heads, me, part, packed_ref, lambda peer: peer, got_ref, send_sem.at[1], recv_sem.at[1])
    out_ref[...] = out
    lse_ref[...] = top + jnp.log2(den)

    loads[0].wait()
    top_rows = gout_ref[...].astype(BF16)
    tile = 256

    def act_tile(index, carry):
        at = pl.ds(pl.multiple_of(index * tile, tile), tile)
        gact_ref[:, at] = dot_nt(top_rows, wd_ref[at, :])
        return carry

    lax.fori_loop(0, wd_ref.shape[0] // tile, act_tile, 0)
    wait_rows(heads, me, got_ref, send_sem.at[1], recv_sem.at[1])

    attended = jnp.concatenate([unpack(got_ref[h]) for h in range(heads)], axis=1)
    loads[1].wait()
    hidden = (dec_ref[...].astype(F32) + dot(attended, wo_ref[...])).astype(BF16).astype(F32)
    gain = gain_ref[...].astype(F32)
    inverse = lax.rsqrt(jnp.mean(hidden * hidden, axis=-1, keepdims=True) + 1e-6)
    scaled = hidden * inverse
    normed = (scaled * gain).astype(BF16)
    loads[2].wait()
    gate = dot(normed, wg_ref[...])
    loads[3].wait()
    up = dot(normed, wu_ref[...])
    sig = jax.nn.sigmoid(gate)
    silu = gate * sig
    grad_act = gact_ref[...]
    grad_gate = (grad_act * up * (sig + silu * (1.0 - sig))).astype(BF16)
    grad_up = (grad_act * silu).astype(BF16)
    grad_normed = (dot_nt(wg_ref[...], grad_gate) + dot_nt(wu_ref[...], grad_up)).T
    gnorm_ref[...] = jnp.sum(grad_normed * scaled, axis=0, keepdims=True)
    inner = grad_normed * gain
    grad_hidden = gout_ref[...] + inverse * (inner - scaled * jnp.mean(inner * scaled, axis=-1, keepdims=True))
    rounded = grad_hidden.astype(BF16)
    grad_att = dot_nt(wo_ref[...], rounded).T.astype(BF16)
    for h in range(heads):
        sent_ref[h] = pack(grad_att[:, hd * h:hd * (h + 1)])
    factors_ref[:, :dim] = attended
    factors_ref[:, dim:] = rounded
    gh_ref[...] = grad_hidden

    start_rows(n, heads, me, part, sent_ref, lambda peer: peer // (n // heads), back_ref, send_sem.at[2], recv_sem.at[2])
    wait_rows(heads, me, back_ref, send_sem.at[2], recv_sem.at[2])
    swap(back_ref, swapped_ref, send_sem.at[3], recv_sem.at[3], partner)
    place(n, heads, part, back_ref, swapped_ref, do_ref, False)


def decoder_rows(n, heads, collective_id, mine, dec_in, grad_out, gain, wo, w_gate, w_up, w_down):
    q_rows, dim = dec_in.shape
    hd, total_q = wo.shape[0] // heads, mine.shape[1]
    hbm = pl.BlockSpec(memory_space=pl.ANY)
    return pl.pallas_call(
        functools.partial(decoder_kernel, n, heads),
        out_shape=[shape((hd, total_q), F32), shape((1, total_q), F32), shape((n, q_rows, 2 * hd), BF16),
                   shape((q_rows, 2 * dim), BF16), shape((q_rows, dim), F32), shape((1, dim), F32)],
        in_specs=vmem(4) + [hbm] * 4,
        out_specs=vmem(6),
        scratch_shapes=[pltpu.VMEM(mine.shape, F32), pltpu.VMEM((n, q_rows // 2, 2 * hd), BF16)]
        + [pltpu.VMEM((heads, q_rows // 2, 2 * hd), BF16)] * 4
        + [pltpu.VMEM(w.shape, BF16) for w in (wo, w_gate, w_up, w_down)] + [pltpu.VMEM((q_rows, w_down.shape[0]), F32), dma(4), dma(4), dma(4)],
        compiler_params=remote(collective_id),
        name='decoder_rows',
    )(mine, dec_in, grad_out, gain, wo, w_gate, w_up, w_down)


def valid_blocks(mem_len, rows, parts, sources):
    reach = mem_len - lax.rem(lax.axis_index('seq'), parts) * rows
    blocks = jnp.minimum((reach + parts * rows - 1) // (parts * rows), sources)
    return blocks, jnp.minimum(reach - (blocks - 1) * parts * rows, rows)


def forward_kernel(scale, hd, parts, q_block, len_ref, kv_ref, q_ref, out_ref, qt_ref, top_ref):
    rows, total_q = kv_ref.shape[1], q_ref.shape[0]
    blocks, last_valid = valid_blocks(len_ref[0], rows, parts, kv_ref.shape[0])
    groups = [slice(first, first + q_block) for first in range(0, total_q, q_block)]
    base = slice(hd + 8, hd + 9)
    qt_ref[...] = q_ref[...].T

    def values_of(keys):
        return jnp.concatenate([keys.T[hd:], jnp.ones((16, rows), keys.dtype)], axis=0)

    def group_of(index):
        return pl.ds(pl.multiple_of(index * q_block, q_block), q_block)

    def first_step(group, carry):
        cols = group_of(group)
        top = jnp.max(dot(kv_ref[0], qt_ref[:, cols]), axis=0, keepdims=True)
        out_ref[hd + 8:, cols] = jnp.broadcast_to(top * scale, (8, q_block))
        top_ref[:, cols] = jnp.broadcast_to(top, (8, q_block))
        return carry

    lax.fori_loop(0, len(groups), first_step, 0)
    out_ref[:hd + 8, :] = jnp.zeros((hd + 8, total_q), F32)

    def finish(values, scores, cols):
        top_ref[:, cols] = jnp.maximum(top_ref[:, cols], jnp.max(scores.reshape(rows // 8, 8, q_block), axis=0))
        weights = jnp.exp2(scores * scale - out_ref[base, cols]).astype(values.dtype)
        out_ref[:hd + 8, cols] += dot(values, weights)[:hd + 8]

    def step(index, carry):
        keys = kv_ref[index]
        values = values_of(keys)
        for cols in groups:
            finish(values, dot(keys, qt_ref[:, cols]), cols)
        return carry

    def last_step(group, carry):
        cols = group_of(group)
        keys = kv_ref[blocks - 1]
        scores = dot(keys, qt_ref[:, cols])
        position = lax.broadcasted_iota(jnp.int32, scores.shape, 0)
        finish(values_of(keys), jnp.where(position < last_valid, scores, NEG), cols)
        return carry

    lax.fori_loop(0, blocks - 1, step, 0)
    lax.fori_loop(0, len(groups), last_step, 0)

    excess = jnp.max(top_ref[...] * scale - out_ref[hd + 8:, :])

    @pl.when(excess > 16.0)
    def _():
        out_ref[:hd + 8, :] = jnp.zeros((hd + 8, total_q), F32)
        out_ref[hd + 8:, :] = jnp.full((8, total_q), NEG, F32)

        def running(step_index, carry):
            index, group = step_index // len(groups), lax.rem(step_index, len(groups))
            cols = group_of(group)
            keys = kv_ref[index]
            limit = jnp.where(index == blocks - 1, last_valid, rows)
            scores = dot(keys, qt_ref[:, cols]) * scale
            position = lax.broadcasted_iota(jnp.int32, scores.shape, 0)
            scores = jnp.where(position < limit, scores, NEG)
            old = out_ref[base, cols]
            new = jnp.maximum(old, jnp.max(scores, axis=0, keepdims=True))
            weights = jnp.exp2(scores - new).astype(keys.dtype)
            out_ref[:hd + 8, cols] = out_ref[:hd + 8, cols] * jnp.exp2(old - new) + dot(values_of(keys), weights)[:hd + 8]
            out_ref[hd + 8:, cols] = jnp.broadcast_to(new, (8, q_block))
            return carry

        lax.fori_loop(0, blocks * len(groups), running, 0)


def attention_forward(scale, hd, parts, sources, mem_len, kv, q):
    rows, width = kv.shape[1], kv.shape[2]
    total_q = q.shape[0]
    return pl.pallas_call(
        functools.partial(forward_kernel, scale, hd, parts, min(1024, total_q)),
        out_shape=shape((hd + 16, total_q), F32),
        grid=(1,),
        in_specs=[pl.BlockSpec(memory_space=pltpu.SMEM),
                  pl.BlockSpec((sources, rows, width), lambda i: (0, 0, 0), pipeline_mode=pl.Buffered(1)), full(q)],
        out_specs=pl.BlockSpec((hd + 16, total_q), lambda i: (0, 0)),
        scratch_shapes=[pltpu.VMEM((width, total_q), BF16), pltpu.VMEM((8, total_q), F32)],
        compiler_params=plain(),
        cost_estimate=pl.CostEstimate(flops=4 * total_q * sources * rows * hd, bytes_accessed=kv.size * 2,
                                      transcendentals=total_q * sources * rows),
        name='attention_forward',
    )(mem_len, kv, q)


def backward_kernel(scale, key_scale, hd, parts, q_block, len_ref, kv_ref, q_ref, do_ref, out_ref, lse_ref, dkv_ref, dq_ref,
                    qt_ref, dot_ref, delta_ref):
    rows, total_q = kv_ref.shape[1], q_ref.shape[0]
    blocks, last_valid = valid_blocks(len_ref[0], rows, parts, kv_ref.shape[0])
    width = kv_ref.shape[2]
    groups = [slice(first, first + q_block) for first in range(0, total_q, q_block)]
    dq_ref[...] = jnp.zeros_like(dq_ref)
    qt_ref[...] = q_ref[...].T
    do_t = do_ref[...].T
    dot_ref[...] = do_t
    delta_ref[...] = jnp.sum(do_t[hd:].astype(F32) * out_ref[...], axis=0, keepdims=True)

    lane_scale = jnp.where(lax.broadcasted_iota(jnp.int32, (1, width), 1) < hd, key_scale, 1.0)

    def products(keys, cols):
        return dot(keys, qt_ref[:, cols]), dot(keys, dot_ref[:, cols])

    def finish(keys, keys_t, scores, grads, cols, valid):
        prob = jnp.exp2(scores * scale - lse_ref[:, cols])
        if valid is not None:
            position = lax.broadcasted_iota(jnp.int32, scores.shape, 0)
            prob = jnp.where(position < valid, prob, 0.0)
        grad_scores = (prob * (grads - delta_ref[:, cols])).astype(keys.dtype)
        update = dot(grad_scores, q_ref[cols, :]) + dot(prob.astype(keys.dtype), do_ref[cols, :])
        dq_ref[:, cols] += dot(keys_t, grad_scores)
        return update

    def step(index, carry):
        keys = kv_ref[index]
        keys_t = keys.T[:hd]
        total = jnp.zeros((rows, width), F32)
        for cols in groups:
            scores, grads = products(keys, cols)
            total += finish(keys, keys_t, scores, grads, cols, None)
        dkv_ref[index] = (total * lane_scale).astype(dkv_ref.dtype)
        return carry

    def last_step(group, total):
        keys = kv_ref[blocks - 1]
        cols = pl.ds(pl.multiple_of(group * q_block, q_block), q_block)
        scores, grads = products(keys, cols)
        return total + finish(keys, keys.T[:hd], scores, grads, cols, last_valid)

    def clear(index, carry):
        dkv_ref[index] = jnp.zeros((rows, width), dkv_ref.dtype)
        return carry

    lax.fori_loop(0, blocks - 1, step, 0)
    total = lax.fori_loop(0, len(groups), last_step, jnp.zeros((rows, width), F32))
    dkv_ref[blocks - 1] = (total * lane_scale).astype(dkv_ref.dtype)
    lax.fori_loop(blocks, dkv_ref.shape[0], clear, 0)
    dq_ref[...] = dq_ref[...] * key_scale


def attention_backward(scale, key_scale, hd, parts, sources, mem_len, kv, q, do, out_t, lse):
    n, rows, width = kv.shape
    total_q = q.shape[0]
    return pl.pallas_call(
        functools.partial(backward_kernel, scale, key_scale, hd, parts, min(512, total_q)),
        out_shape=[shape((n, rows, width), BF16), shape((hd, total_q), F32)],
        grid=(1,),
        in_specs=[pl.BlockSpec(memory_space=pltpu.SMEM),
                  pl.BlockSpec((sources, rows, width), lambda i: (0, 0, 0), pipeline_mode=pl.Buffered(1)),
                  full(q), full(do), full(out_t), full(lse)],
        out_specs=[pl.BlockSpec((n, rows, width), lambda i: (0, 0, 0)),
                   pl.BlockSpec((hd, total_q), lambda i: (0, 0))],
        scratch_shapes=[pltpu.VMEM((width, total_q), BF16), pltpu.VMEM((width, total_q), BF16), pltpu.VMEM((1, total_q), F32)],
        compiler_params=plain(),
        cost_estimate=pl.CostEstimate(flops=10 * total_q * sources * rows * hd, bytes_accessed=kv.size * 4,
                                      transcendentals=total_q * sources * rows),
        name='attention_backward',
    )(mem_len, kv, q, do, out_t, lse)


def reduce_kernel(n, heads, tile, chunk, gk_hbm, gv_hbm, early_hbm, late_hbm, w1_hbm, w3_hbm, w2_hbm, wo_ref, wq_ref, gain1_ref,
                  gain2_ref, dqr_ref, dec_ref, gh_ref, gnorm_ref,
                  sums_ref, gdec_ref, norms_ref, n2_hbm, d1_hbm, d3_hbm, act_hbm,
                  acc_ref, pair_ref, far_ref, near_ref, n2_ref, top_ref, att_ref, decs_ref, w1_ref, w3_ref, w2_ref, w2t_ref,
                  d1_ref, d3_ref, act_ref, mine_ref, all_ref,
                  own_sem, share_send, share_recv, pair_send, pair_recv, far_send, far_recv, near_send, near_recv, rows_sem, top_sem, w_sem, out_sem, n2_sem,
                  norm_send, norm_recv):
    g = Grid(n, heads, 0)
    side = g.side
    rows, dim = n2_ref.shape
    tiles = d1_hbm.shape[0]
    own_tiles = (tiles + g.parts - 1 - g.part) // g.parts
    part_rows = acc_ref.shape[1]

    def start_rows_of(index):
        slot = lax.rem(index, 2)
        at = pl.ds(pl.multiple_of(index * chunk, chunk), chunk)
        for i, (src, dst) in enumerate(((late_hbm, att_ref), (early_hbm, decs_ref))):
            pltpu.make_async_copy(src.at[at, pl.ds(0, dim)], dst.at[slot], rows_sem.at[slot, i]).start()

    def tile_at(index):
        return pl.ds(pl.multiple_of(index * tile, tile), tile)

    def weights(index):
        slot = lax.rem(index, 2)
        at = tile_at(index * g.parts + g.part)
        return [pltpu.make_async_copy(src, dst.at[slot], w_sem.at[slot, i]) for i, (src, dst) in enumerate(
            ((w1_hbm.at[:, at], w1_ref), (w3_hbm.at[:, at], w3_ref), (w2_hbm.at[at, :], w2_ref)))]

    def results(index):
        slot, number = lax.rem(index, 2), index * g.parts + g.part
        pairs = ((d1_ref, d1_hbm), (d3_ref, d3_hbm), (act_ref, act_hbm))
        return ([pltpu.make_async_copy(src.at[slot], dst.at[number], out_sem.at[slot, i]) for i, (src, dst) in enumerate(pairs)],
                [send(src.at[slot], dst.at[number], share_send.at[slot, i], share_recv.at[i], g.partner)
                 for i, (src, dst) in enumerate(pairs)])

    start_rows_of(0)
    top_load = pltpu.make_async_copy(early_hbm.at[:, pl.ds(dim, dim)], top_ref, top_sem)
    top_load.start()
    for copy in weights(0):
        copy.start()

    def summand(c, core):
        source = gk_hbm if c < heads // g.parts else gv_hbm
        first = ((g.parts * c) % heads + core) * part_rows
        return source.at[pl.ds(pl.multiple_of(first, part_rows), part_rows), :]

    owns = [pltpu.make_async_copy(summand(c, g.part), acc_ref.at[c], own_sem.at[c]) for c in range(heads)]
    for copy in owns:
        copy.start()

    meet([lax.rem(g.me + step, n) for step in range(1, n)])
    for c in range(heads):
        send(summand(c, g.parts - 1 - g.part), pair_ref.at[c], pair_send, pair_recv, g.partner).start()

    grad_query = jnp.concatenate([dqr_ref[h] for h in range(heads)], axis=1)
    grad_normed = dot(grad_query, wq_ref[...])
    x = dec_ref[...].astype(F32)
    inverse = lax.rsqrt(jnp.mean(x * x, axis=-1, keepdims=True) + 1e-6)
    scaled = x * inverse
    inner = grad_normed * gain1_ref[...].astype(F32)
    gdec_ref[...] = gh_ref[...] + inverse * (inner - scaled * jnp.mean(inner * scaled, axis=-1, keepdims=True))
    mine_ref[0:1, :] = jnp.sum(grad_normed * scaled, axis=0, keepdims=True)
    mine_ref[1:2, :] = gnorm_ref[...]

    for step in range(1, n):
        send(mine_ref, all_ref.at[g.me], norm_send, norm_recv, lax.rem(g.me + step, n)).start()
    all_ref[g.me] = mine_ref[...]

    quarter = part_rows // 4
    streams = [(axis, way, pl.ds((2 * axis + (way < 0)) * quarter, quarter)) for axis in (0, 1) for way in (1, -1)]

    def place_of(axis, line, other):
        return other * side + line if axis == 0 else line * side + other

    def pieces(stage, axis, line):
        position = g.row if axis == 0 else g.col
        return [place_of(axis, line, o) for o in range(side)] if stage == 0 else [place_of(axis, line, position)]

    def ring(stage, stream, step):
        axis, way, part = streams[stream]
        axis = axis if stage == 0 else 1 - axis
        here = g.col if axis == 0 else g.row
        ref, sends, recvs = (far_ref, far_send, far_recv) if stage == 0 else (near_ref, near_send, near_recv)
        to = g.near(0, way) if axis == 0 else g.near(way, 0)
        return axis, way, part, here, ref.at[stream, step - 1], sends.at[stream, step - 1], recvs.at[stream, step - 1], to

    def line_of(here, way, step):
        return lax.rem(here - way * step + 2 * side, side)

    def start_step(stage, step):
        for stream in range(4):
            axis, way, part, here, buffer, sem, recv, to = ring(stage, stream, step)
            for i, c in enumerate(pieces(stage, axis, line_of(here, way, step))):
                send(acc_ref.at[c, part], buffer.at[i], sem, recv, to).start()

    def end_step(stage, step):
        for stream in range(4):
            axis, way, part, here, buffer, sem, recv, to = ring(stage, stream, step)
            whole = send(buffer, buffer, sem, recv, g.me)
            whole.wait_recv()
            for i, c in enumerate(pieces(stage, axis, line_of(here, way, step + 1))):
                acc_ref[c, part, :] = acc_ref[c, part, :] + buffer[i]
            whole.wait_send()

    def add_pair():
        for copy in owns:
            copy.wait()
        whole = send(pair_ref, pair_ref, pair_send, pair_recv, g.me)
        whole.wait_recv()

        def add(c, carry):
            acc_ref[c] = acc_ref[c] + pair_ref[c]
            return carry

        lax.fori_loop(0, heads, add, 0)
        whole.wait_send()

    def first():
        add_pair()
        start_step(0, 1)

    def turn():
        end_step(0, side - 1)
        start_step(1, 1)

    def between(stage, step):
        def body():
            end_step(stage, step)
            start_step(stage, step + 1)
        return body

    def prepare(index, carry):
        slot = lax.rem(index, 2)
        at = pl.ds(pl.multiple_of(index * chunk, chunk), chunk)
        for i, (src, dst) in enumerate(((late_hbm, att_ref), (early_hbm, decs_ref))):
            pltpu.make_async_copy(src.at[at, pl.ds(0, dim)], dst.at[slot], rows_sem.at[slot, i]).wait()

        @pl.when(index + 1 < rows // chunk)
        def _():
            start_rows_of(index + 1)

        pl.when(index == rows // chunk // 2)(first)
        dec = decs_ref[slot].astype(F32)
        hidden = (dec + dot(att_ref[slot], wo_ref[...])).astype(BF16).astype(F32)
        n2_ref[at, :] = rms_norm(hidden, gain2_ref[...].astype(F32)).astype(BF16)
        return carry

    lax.fori_loop(0, rows // chunk, prepare, 0)
    top_load.wait()
    n2_store = pltpu.make_async_copy(n2_ref, n2_hbm, n2_sem)
    n2_store.start()

    events = ([between(0, t) for t in range(1, side - 1)] + [turn] + [between(1, t) for t in range(1, side - 1)]
              + [lambda: end_step(1, side - 1)])
    at_tile = (1, 3)
    inside = tiles // 2 > at_tile[-1] and len(events) > len(at_tile)

    def finish_results(index):
        stores, shares = results(index)
        for copy in stores:
            copy.wait()
        for copy in shares:
            copy.wait_send()

    def activations(index, carry):
        slot = lax.rem(index, 2)
        for copy in weights(index):
            copy.wait()

        @pl.when(index + 1 < own_tiles)
        def _():
            for copy in weights(index + 1):
                copy.start()

        @pl.when(index >= 2)
        def _():
            finish_results(index - 2)

        if inside:
            for event, when in zip(events, at_tile):
                pl.when(index == when)(event)

        w2t_ref[...] = w2_ref[slot].T

        def some_rows(block, carry):
            for i in range(2):
                part = pl.ds(pl.multiple_of((2 * block + i) * chunk, chunk), chunk)
                gate = dot(n2_ref[part, :], w1_ref[slot])
                up = dot(n2_ref[part, :], w3_ref[slot])
                grad = dot(top_ref[part, :], w2t_ref[...])
                sig = jax.nn.sigmoid(gate)
                silu = gate * sig
                act_ref[slot, part, :] = (silu * up).astype(BF16)
                d3_ref[slot, part, :] = (grad * silu).astype(BF16)
                d1_ref[slot, part, :] = (grad * up * (sig + silu * (1.0 - sig))).astype(BF16)
            return carry

        lax.fori_loop(0, rows // chunk // 2, some_rows, 0)
        for copies in results(index):
            for copy in copies:
                copy.start()
        return carry

    lax.fori_loop(0, own_tiles, activations, 0)
    for event in events[len(at_tile):] if inside else events:
        event()
    sums_ref[...] = acc_ref[g.chip]

    others = all_ref.at[pl.ds(0, n - 1)]
    whole = send(others, others, norm_send, norm_recv, g.me)
    whole.wait_send()
    whole.wait_recv()
    norms_ref[...] = jnp.sum(all_ref[...], axis=0)
    n2_store.wait()
    @pl.when(own_tiles >= 2)
    def _():
        finish_results(own_tiles - 2)

    finish_results(own_tiles - 1)
    for core in range(g.parts):
        others_tiles = (tiles + core) // g.parts

        @pl.when(g.part == core)
        def _(others_tiles=others_tiles):
            for i, ref in enumerate((d1_hbm, d3_hbm, act_hbm)):
                come = ref.at[pl.ds(0, others_tiles)]
                send(come, come, share_send.at[0, i], share_recv.at[i], g.me).wait_recv()


def reduce_sums(n, heads, collective_id, gk, gv, early, late, w_gate, w_up, w_down, wo, wq, gain1, gain2, dq_rows, dec_in, gh, gnorm):
    rows, dim = early.shape[0], gk.shape[1]
    ff, tile, chunk = w_gate.shape[1], 256, min(512, early.shape[0] // 2)
    part_rows = 2 * gk.shape[0] // n
    side = math.isqrt(heads)
    hbm = pl.BlockSpec(memory_space=pl.ANY)
    return pl.pallas_call(
        functools.partial(reduce_kernel, n, heads, tile, chunk),
        out_shape=[shape((part_rows, dim), F32), shape(gh.shape, F32), shape((2, dim), F32), shape((rows, dim), BF16)]
        + [shape((ff // tile, rows, tile), BF16)] * 3,
        in_specs=[hbm] * 7 + vmem(8),
        out_specs=vmem(3) + [hbm] * 4,
        scratch_shapes=[pltpu.VMEM((heads, part_rows, dim), F32)] * 2
        + [pltpu.VMEM((4, side - 1, side, part_rows // 4, dim), F32), pltpu.VMEM((4, side - 1, 1, part_rows // 4, dim), F32)]
        + [pltpu.VMEM((rows, dim), BF16)] * 2 + [pltpu.VMEM((2, chunk, dim), BF16)] * 2
        + [pltpu.VMEM((2, dim, tile), BF16)] * 2 + [pltpu.VMEM((2, tile, dim), BF16), pltpu.VMEM((dim, tile), BF16)] + [pltpu.VMEM((2, rows, tile), BF16)] * 3
        + [pltpu.VMEM((2, dim), F32), pltpu.VMEM((n, 2, dim), F32)]
        + [dma(heads), dma(2, 3), dma(3), pltpu.SemaphoreType.DMA, pltpu.SemaphoreType.DMA, dma(4, side - 1), dma(4, side - 1), dma(4, side - 1),
           dma(4, side - 1), dma(2, 2), pltpu.SemaphoreType.DMA, dma(2, 3), dma(2, 3), pltpu.SemaphoreType.DMA,
           pltpu.SemaphoreType.DMA, pltpu.SemaphoreType.DMA],
        compiler_params=remote(collective_id),
        cost_estimate=pl.CostEstimate(flops=6 * rows * dim * ff, bytes_accessed=12 * rows * ff, transcendentals=rows * ff),
        name='reduce_sums',
    )(gk, gv, early, late, w_gate, w_up, w_down, wo, wq, gain1, gain2, dq_rows, dec_in, gh, gnorm)


def gate_up_kernel(n2_ref, d1_ref, d3_ref, g1_ref, g3_ref, n2t_ref):
    @pl.when(pl.program_id(0) == 0)
    def _():
        n2t_ref[...] = n2_ref[...].T

    g1_ref[...] = dot(n2t_ref[...], d1_ref[...])
    g3_ref[...] = dot(n2t_ref[...], d3_ref[...])


def gate_up_grads(n2, d1, d3):
    rows, dim = n2.shape
    tiles, _, tile = d1.shape
    cols = pl.BlockSpec((dim, tile), lambda i: (0, i))
    part = pl.BlockSpec((pl.Squeezed(), rows, tile), lambda i: (i, 0, 0))
    return pl.pallas_call(
        gate_up_kernel,
        out_shape=[shape((dim, tiles * tile), F32)] * 2,
        grid=(tiles,),
        in_specs=[full(n2), part, part],
        out_specs=[cols, cols],
        scratch_shapes=[pltpu.VMEM((dim, rows), BF16)],
        compiler_params=plain(),
        cost_estimate=pl.CostEstimate(flops=4 * rows * dim * tiles * tile, bytes_accessed=12 * dim * tiles * tile, transcendentals=0),
        name='gate_up_grads',
    )(n2, d1, d3)


def down_kernel(top_ref, act_ref, k_in_ref, v_in_ref, g2_ref, k_ref, v_ref):
    g2_ref[...] = dot_tn(act_ref[...], top_ref[...])
    k_ref[...] = k_in_ref[...]
    v_ref[...] = v_in_ref[...]


def down_grad(early, act, total):
    rows, dim = early.shape[0], early.shape[1] // 2
    tiles, _, tile = act.shape
    blocks = 1 << (tiles.bit_length() - 1)
    height = total.shape[0] // 2 // blocks
    block = lambda first: pl.BlockSpec((height, dim), lambda i: (jnp.minimum(i, blocks - 1) + first, 0))
    return pl.pallas_call(
        down_kernel,
        out_shape=[shape((tiles * tile, dim), F32)] + [shape((total.shape[0] // 2, dim), F32)] * 2,
        grid=(tiles,),
        in_specs=[pl.BlockSpec((rows, dim), lambda i: (0, 1), pipeline_mode=pl.Buffered(1)),
                  pl.BlockSpec((pl.Squeezed(), rows, tile), lambda i: (i, 0, 0)), block(0), block(blocks)],
        out_specs=[pl.BlockSpec((tile, dim), lambda i: (i, 0)), block(0), block(0)],
        compiler_params=plain(),
        cost_estimate=pl.CostEstimate(flops=2 * rows * dim * tiles * tile, bytes_accessed=12 * dim * tiles * tile, transcendentals=0),
        name='down_grad',
    )(early, act, total, total)


def memory_weight_kernel(memory_ref, dkv_ref, gk_ref, gv_ref):
    group, hd = dkv_ref.shape[0], dkv_ref.shape[2] // 2
    for i in range(group):
        both = dot_tn(dkv_ref[i], memory_ref[...])
        gk_ref[i * hd:(i + 1) * hd, :] = both[:hd]
        gv_ref[i * hd:(i + 1) * hd, :] = both[hd:]


def memory_weight_grads(memory, dkv):
    heads, rows, width = dkv.shape
    dim, hd = memory.shape[1], width // 2
    group = 4
    out = pl.BlockSpec((group * hd, dim), lambda i: (i, 0))
    return pl.pallas_call(
        memory_weight_kernel,
        out_shape=[shape((heads * hd, dim), F32)] * 2,
        grid=(heads // group,),
        in_specs=[full(memory), pl.BlockSpec((group, rows, width), lambda i: (i, 0, 0))],
        out_specs=[out, out],
        compiler_params=plain(),
        cost_estimate=pl.CostEstimate(flops=2 * rows * dim * heads * width, bytes_accessed=16 * rows * dim, transcendentals=0),
        name='memory_weight_grads',
    )(memory, dkv)


def memory_grad_kernel(dkv_ref, wk_ref, wv_ref, out_ref):
    group = dkv_ref.shape[0]
    left = jnp.concatenate([dkv_ref[i] for i in range(group)], axis=1)
    right = jnp.concatenate([part[i] for i in range(group) for part in (wk_ref, wv_ref)], axis=0)

    @pl.when(pl.program_id(0) == 0)
    def _():
        out_ref[...] = dot(left, right)

    @pl.when(pl.program_id(0) > 0)
    def _():
        out_ref[...] += dot(left, right)


def memory_grad(dkv, wk_t, wv_t):
    heads, rows, width = dkv.shape
    hd, dim = wk_t.shape[1], wk_t.shape[2]
    group = 4
    weight = pl.BlockSpec((group, hd, dim), lambda i: (i, 0, 0))
    return pl.pallas_call(
        memory_grad_kernel,
        out_shape=shape((rows, dim), F32),
        grid=(heads // group,),
        in_specs=[pl.BlockSpec((group, rows, width), lambda i: (i, 0, 0)), weight, weight],
        out_specs=pl.BlockSpec((rows, dim), lambda i: (0, 0)),
        compiler_params=plain(),
        cost_estimate=pl.CostEstimate(flops=2 * rows * dim * heads * width, bytes_accessed=12 * rows * dim, transcendentals=0),
        name='memory_grad',
    )(dkv, wk_t, wv_t)


def outer_kernel(att_ref, gh_ref, out_ref):
    @pl.when(pl.program_id(0) == 0)
    def _():
        out_ref[...] = jnp.zeros_like(out_ref)

    out_ref[...] += dot_tn(att_ref[...], gh_ref[...])


def outer_weight_grad(late, dim):
    rows = late.shape[0]
    chunk = min(512, rows)
    return pl.pallas_call(
        outer_kernel,
        out_shape=shape((dim, dim), F32),
        grid=(rows // chunk,),
        in_specs=[pl.BlockSpec((chunk, dim), lambda i: (i, 0)), pl.BlockSpec((chunk, dim), lambda i: (i, 1))],
        out_specs=pl.BlockSpec((dim, dim), lambda i: (0, 0)),
        compiler_params=plain(),
        cost_estimate=pl.CostEstimate(flops=2 * rows * dim * dim, bytes_accessed=8 * rows * dim, transcendentals=0),
        name='outer_weight_grad',
    )(late, late)


def solution(mesh):
    n = mesh.shape['seq']
    row_spec = P(('data', 'seq'), None)
    weight_spec = P()
    part_vec = P('data')
    part_mat = P('data', None)
    part_cube = P('data', None, None)

    def device_step(dec_in, memory, mem_len, grad_out, norm_attn, wq_cross, wk_cross, wv_cross, wo_cross, norm_mlp, w_gate, w_up, w_down):
        q_rows, dim = dec_in.shape
        heads, hd = wq_cross.shape[1], wq_cross.shape[2]
        parts = n // heads
        sources = -(-3 * n // 4)
        total_q = q_rows * n
        key_scale = hd ** -0.5
        scale = key_scale * LOG2E
        wq_t, wk_t, wv_t = (jnp.transpose(w, (1, 2, 0)) for w in (wq_cross, wk_cross, wv_cross))
        source_rows = -(-sources // (parts * math.isqrt(heads)))
        kv, q_in, early_local = exchange(n, heads, source_rows, 0, memory, dec_in, grad_out, norm_attn, wk_t, wv_t, wq_t)
        head_q = q_in.reshape(total_q, 2 * hd)

        early = lax.all_gather(early_local, 'seq', axis=0, tiled=True)

        wo = wo_cross.reshape(heads * hd, dim)
        mine = attention_forward(scale, hd, parts, sources, mem_len, kv, head_q)
        out_t, lse, do_in, factors, grad_hidden, g_norm_mlp = decoder_rows(
            n, heads, 1, mine, dec_in, grad_out, norm_mlp, wo, w_gate, w_up, w_down)
        do_in, factors = lax.optimization_barrier((do_in, factors))
        late = lax.all_gather(factors, 'seq', axis=0, tiled=True)

        dkv, dq_part = attention_backward(scale, key_scale, hd, parts, sources, mem_len, kv, head_q, do_in.reshape(total_q, 2 * hd), out_t, lse)
        dkv_in, dq_rows, gq_share = return_blocks(n, heads, source_rows, 4, dkv, dq_part, norm_attn, early)
        dkv_in, dq_rows, gq_share, late = lax.optimization_barrier((dkv_in, dq_rows, gq_share, late))
        g_wq = lax.all_gather(gq_share, 'seq', axis=0, tiled=True)

        gk_part, gv_part = memory_weight_grads(memory, dkv_in)
        sums, g_dec, norms, n2_all, d1, d3, act = reduce_sums(
            n, heads, 5, gk_part, gv_part, early, late, w_gate, w_up, w_down, wo, wq_t.reshape(heads * hd, dim), norm_attn, norm_mlp,
            dq_rows, dec_in, grad_hidden, g_norm_mlp)
        sums, n2_all, d1, d3, act, dkv_in, late, early, g_wq = lax.optimization_barrier(
            (sums, n2_all, d1, d3, act, dkv_in, late, early, g_wq))
        total = lax.all_gather(sums, 'seq', axis=0, tiled=True)
        g_wo = outer_weight_grad(late, dim)
        g_mem = memory_grad(dkv_in, wk_t, wv_t)
        g_gate, g_up = gate_up_grads(n2_all, d1, d3)
        g_down, g_wk, g_wv = down_grad(early, act, total)

        cube = lambda g: jnp.transpose(g.reshape(heads, hd, dim), (2, 0, 1))
        return (g_dec, g_mem, norms[0], cube(g_wq), cube(g_wk), cube(g_wv), g_wo.reshape(heads, hd, dim), norms[1], g_gate, g_up, g_down)

    return jax.shard_map(device_step, mesh=mesh,
                         in_specs=(row_spec, row_spec, part_vec, row_spec) + (weight_spec,) * 9,
                         out_specs=(row_spec, row_spec, part_vec, part_cube, part_cube, part_cube, part_cube, part_vec, part_mat, part_mat, part_mat),
                         check_vma=False)
```

```python
import functools
import math

import jax
import jax.numpy as jnp
from jax import lax
from jax.experimental import pallas as pl
from jax.experimental.pallas import tpu as pltpu
from jax.sharding import PartitionSpec as P

LOG2E = 1.4426950408889634
NEG = -1e30
VMEM_LIMIT = 60 * 1024 * 1024
MESH = pl.DeviceIdType.MESH
BF16, F32 = jnp.bfloat16, jnp.float32


def rms_norm(tensor, gain):
    mean_sq = jnp.mean(tensor * tensor, axis=-1, keepdims=True)
    return tensor * lax.rsqrt(mean_sq + 1e-6) * gain


def dot(a, b):
    return jnp.dot(a, b, preferred_element_type=F32)


def dot_nt(a, b):
    return lax.dot_general(a, b, (((1,), (1,)), ((), ())), preferred_element_type=F32)


def dot_tn(a, b):
    return lax.dot_general(a, b, (((0,), (0,)), ((), ())), preferred_element_type=F32)


def full(array):
    return pl.BlockSpec(array.shape, lambda *_: (0,) * array.ndim, pipeline_mode=pl.Buffered(1))


def vmem(count):
    return [pl.BlockSpec(memory_space=pltpu.VMEM)] * count


def plain():
    return pltpu.CompilerParams(vmem_limit_bytes=VMEM_LIMIT)


def remote(collective_id):
    return pltpu.CompilerParams(collective_id=collective_id, has_side_effects=True, vmem_limit_bytes=VMEM_LIMIT)


def shape(dims, dtype):
    return jax.ShapeDtypeStruct(dims, dtype)


def meet(peers):
    barrier = pltpu.get_barrier_semaphore()
    for peer in peers:
        pl.semaphore_signal(barrier, inc=1, device_id={'seq': peer}, device_id_type=MESH)
    pl.semaphore_wait(barrier, len(peers))


def send(src, dst, send_sem, recv_sem, peer):
    return pltpu.make_async_remote_copy(src_ref=src, dst_ref=dst, send_sem=send_sem, recv_sem=recv_sem,
                                        device_id={'seq': peer}, device_id_type=MESH)


class Grid:
    def __init__(self, n, heads, source_rows):
        self.n, self.heads, self.source_rows = n, heads, source_rows
        self.parts = n // heads
        self.side = math.isqrt(heads)
        self.me = lax.axis_index('seq')
        self.part = lax.rem(self.me, self.parts)
        self.chip = self.me // self.parts
        self.col = lax.rem(self.chip, self.side)
        self.row = self.chip // self.side
        self.partner = self.chip * self.parts + (self.parts - 1 - self.part)
        self.ties = self.side == 4
        self.direct = (1, 3) if self.ties else (1,)

    def wrap(self, value):
        return lax.rem(value + self.side, self.side)

    def device(self, row, col, part):
        return (row * self.side + col) * self.parts + part

    def near(self, drow, dcol, part=None):
        return self.device(self.wrap(self.row + drow), self.wrap(self.col + dcol), self.part if part is None else part)

    def hop(self, offset):
        return 1 if offset == 1 else -1

    def is_source(self, row):
        return self.wrap(row) < self.source_rows

    def row_peers(self):
        return [lax.rem(self.chip + step, self.heads) * self.parts + self.part for step in range(1, self.heads)]

    def peers(self):
        return self.row_peers() + [self.partner] + [self.near(0, self.hop(d), self.parts - 1 - self.part) for d in self.direct]


def pair_peers(n, heads, me, part):
    parts = n // heads
    head = me // parts
    partner = head * parts + (parts - 1 - part)
    return partner, [partner] + [lax.rem(head + step, heads) * parts + part for step in range(1, heads)]


def pack(rows):
    middle = rows.shape[-2] // 2
    return jnp.concatenate([rows[..., :middle, :], rows[..., middle:, :]], axis=-1)


def unpack(packed):
    middle = packed.shape[-1] // 2
    return jnp.concatenate([packed[..., :middle], packed[..., middle:]], axis=-2)


def start_rows(n, heads, me, part, src, src_of, dst_ref, send_sem, recv_sem):
    parts = n // heads
    head = me // parts
    for step in range(1, heads):
        peer = lax.rem(head + step, heads) * parts + part
        send(src.at[src_of(peer)], dst_ref.at[head], send_sem, recv_sem, peer).start()
    dst_ref[head] = src[src_of(me)]


def wait_rows(heads, me, dst_ref, send_sem, recv_sem):
    others = dst_ref.at[pl.ds(0, heads - 1)]
    whole = send(others, others, send_sem, recv_sem, me)
    whole.wait_send()
    whole.wait_recv()


def swap(src, dst, send_sem, recv_sem, partner):
    copy = send(src, dst, send_sem, recv_sem, partner)
    copy.start()
    copy.wait()


def place(n, heads, part, mine_ref, theirs_ref, wide_ref, low):
    parts = n // heads
    for source, index in ((mine_ref, part), (theirs_ref, parts - 1 - part)):
        for head in range(heads):
            rows = unpack(source[head])
            zeros = jnp.zeros_like(rows)
            wide_ref[head * parts + index] = jnp.concatenate([rows, zeros] if low else [zeros, rows], axis=-1)


def exchange_kernel(n, heads, source_rows, memory_ref, dec_ref, gout_ref, gain_ref, wk_ref, wv_ref, wq_ref, kv_out_ref, q_out_ref, early_ref,
                    kv_ref, stage_ref, up_ref, down_ref, right_ref, left_ref, packed_ref, got_ref, swapped_ref,
                    row_send, row_recv, y_send, pass_send, x_send, fwd_send, stage_recv, up_recv, down_recv, right_recv,
                    left_recv, out_recv):
    g = Grid(n, heads, source_rows)
    side, hd = g.side, wk_ref.shape[1]
    half = kv_out_ref.shape[1]
    chunk_rows = min(256, kv_ref.shape[1])
    barrier = pltpu.get_barrier_semaphore()
    peers = g.peers()
    for peer in peers:
        pl.semaphore_signal(barrier, inc=1, device_id={'seq': peer}, device_id_type=MESH)

    dim = dec_ref.shape[1]
    early_ref[:, :dim] = dec_ref[...]
    early_ref[:, dim:] = gout_ref[...].astype(BF16)
    normed = rms_norm(dec_ref[...].astype(F32), gain_ref[...].astype(F32)).astype(BF16)

    def some_heads(index, carry):
        queries = dot_nt(normed, jnp.concatenate([wq_ref[4 * index + j] for j in range(4)], axis=0)).astype(BF16)
        for j in range(4):
            packed_ref[4 * index + j] = pack(queries[:, hd * j:hd * (j + 1)])
        return carry

    lax.fori_loop(0, heads // 4, some_heads, 0)

    def head(drow, dcol):
        return g.wrap(g.row + drow) * side + g.wrap(g.col + dcol)

    def project(drow, dcols):
        weights = jnp.concatenate([ref[head(drow, d)] for d in dcols for ref in (wk_ref, wv_ref)], axis=0)

        def rows(index, carry):
            at = pl.ds(pl.multiple_of(index * chunk_rows, chunk_rows), chunk_rows)
            both = dot_nt(memory_ref[at, :], weights).astype(BF16)
            for i, d in enumerate(dcols):
                kv_ref[head(drow, d), at, :] = both[:, 2 * hd * i:2 * hd * (i + 1)]
            return carry

        lax.fori_loop(0, kv_ref.shape[1] // chunk_rows, rows, 0)

    def along_column(drow, dcol):
        chunk = kv_ref.at[head(drow, dcol)]
        if drow in g.direct:
            send(chunk, stage_ref.at[drow - 1, dcol], y_send.at[drow - 1], stage_recv.at[drow - 1, dcol], g.near(g.hop(drow), 0)).start()
        elif dcol % 2 == 0:
            send(chunk, up_ref.at[dcol // 2], y_send.at[drow - 1], up_recv.at[dcol // 2], g.near(1, 0)).start()
        else:
            send(chunk, down_ref.at[dcol // 2], y_send.at[drow - 1], down_recv.at[dcol // 2], g.near(-1, 0)).start()

    def along_row(o, dcol):
        chunk = kv_ref.at[head(0, dcol)] if o == 0 else stage_ref.at[o - 1, dcol]
        source = g.device(g.wrap(g.row - o), g.col, g.part)
        if dcol == 0:
            kv_out_ref[source] = chunk[pl.ds(pl.multiple_of(g.part * half, half), half), :]
            away = pl.ds(pl.multiple_of((g.parts - 1 - g.part) * half, half), half)
            send(chunk.at[away], kv_out_ref.at[source], x_send.at[o], out_recv, g.partner).start()
        elif dcol in g.direct:
            for part in range(g.parts):
                send(chunk.at[pl.ds(part * half, half)], kv_out_ref.at[source], x_send.at[o], out_recv,
                     g.near(0, g.hop(dcol), part)).start()
        else:
            send(chunk.at[pl.ds(0, half)], right_ref.at[o], x_send.at[o], right_recv.at[o], g.near(0, 1)).start()
            send(chunk.at[pl.ds(half, half)], left_ref.at[o], x_send.at[o], left_recv.at[o], g.near(0, -1)).start()

    def pass_row(o):
        for ref, sem, come in ((right_ref, right_recv, -1), (left_ref, left_recv, 1)):
            source = g.device(g.wrap(g.row - o), g.wrap(g.col + come), g.part)
            send(ref.at[o], ref.at[o], fwd_send.at[o], sem.at[o], g.me).wait_recv()
            send(ref.at[o], kv_out_ref.at[source], fwd_send.at[o], out_recv, g.near(0, -come, 0 if come < 0 else 1)).start()

    def when_source(row, body):
        pl.when(g.is_source(row))(body)

    if g.ties:
        order = [(2, (2, 1)), (2, (3, 0)), (1, (2, 1)), (3, (2, 3)), (0, (2, 1)), (0, (3, 0))]
        last = [(1, (3, 0)), (3, (1, 0))]
    else:
        order, last = [(1, (1, 0)), (0, (1, 0))], []

    def issue(drow, dcols):
        def body():
            for d in dcols:
                along_row(0, d) if drow == 0 else along_column(drow, d)
        when_source(g.row, body)

    waiting = None
    for drow, dcols in order + last:
        project(drow, dcols)
        if waiting is None:
            pl.semaphore_wait(barrier, len(peers))
            start_rows(n, heads, g.me, g.part, packed_ref, lambda peer: peer // g.parts, got_ref, row_send.at[0], row_recv.at[0])
        elif waiting not in last:
            issue(*waiting)
        waiting = (drow, dcols)
    if not last:
        issue(*waiting)

    if g.ties:
        def up(i):
            send(up_ref.at[i], up_ref.at[i], pass_send.at[0], up_recv.at[i], g.me).wait_recv()
            send(up_ref.at[i], stage_ref.at[1, 2 * i], pass_send.at[0], stage_recv.at[1, 2 * i], g.near(1, 0)).start()

        def down(i):
            send(down_ref.at[i], down_ref.at[i], pass_send.at[1], down_recv.at[i], g.me).wait_recv()
            send(down_ref.at[i], stage_ref.at[1, 2 * i + 1], pass_send.at[1], stage_recv.at[1, 2 * i + 1], g.near(-1, 0)).start()

        for i in range(2):
            when_source(g.row - 1, lambda i=i: up(1 - i))
            when_source(g.row + 1, lambda i=i: down(i))
        for drow, dcols in last:
            issue(drow, dcols)
        when_source(g.row, lambda: pass_row(0))

    wait_rows(heads, g.me, got_ref, row_send.at[0], row_recv.at[0])
    swap(got_ref, swapped_ref, row_send.at[1], row_recv.at[1], g.partner)
    place(n, heads, g.part, got_ref, swapped_ref, q_out_ref, True)

    def arrived(o, dcol):
        def body():
            send(stage_ref.at[o - 1, dcol], stage_ref.at[o - 1, dcol], y_send.at[0], stage_recv.at[o - 1, dcol], g.me).wait_recv()
            along_row(o, dcol)
        when_source(g.row - o, body)

    if g.ties:
        for o, d in ((1, 2), (3, 2), (1, 1), (3, 3)):
            arrived(o, d)
        for o in g.direct:
            when_source(g.row - o, lambda o=o: pass_row(o))
        for d in (2, 1, 0, 3):
            arrived(2, d)
        when_source(g.row - 2, lambda: pass_row(2))
        for o, d in ((1, 3), (3, 1), (1, 0), (3, 0)):
            arrived(o, d)
    else:
        for d in (1, 0):
            arrived(1, d)

    def sent(sem, ref):
        send(ref, ref, sem, out_recv, g.me).wait_send()

    def mine():
        for drow in range(1, side):
            sent(y_send.at[drow - 1], stage_ref.at[0])
    when_source(g.row, mine)
    for o in range(side):
        def passed(o=o):
            sent(x_send.at[o], kv_out_ref.at[pl.ds(0, g.parts * side - 1)])
            if g.ties:
                sent(fwd_send.at[o], kv_out_ref.at[pl.ds(0, 2)])
        when_source(g.row - o, passed)
    if g.ties:
        when_source(g.row - 1, lambda: sent(pass_send.at[0], up_ref))
        when_source(g.row + 1, lambda: sent(pass_send.at[1], down_ref))
    blocks = source_rows * side * g.parts
    others = kv_out_ref.at[pl.ds(0, blocks - source_rows)]
    send(others, others, y_send.at[0], out_recv, g.me).wait_recv()


def row_scratch(heads, q_rows, hd):
    return [pltpu.VMEM((heads, q_rows // 2, 2 * hd), BF16)] * 3


def dma(*dims):
    return pltpu.SemaphoreType.DMA(dims)


def exchange(n, heads, source_rows, collective_id, memory, dec_in, grad_out, gain, wk_t, wv_t, wq_t):
    m_rows, q_rows, hd = memory.shape[0], dec_in.shape[0], wk_t.shape[1]
    side, parts = math.isqrt(heads), n // heads
    half = m_rows // parts
    chunk = lambda *lead: pltpu.VMEM(lead + (m_rows, 2 * hd), BF16)
    block = lambda *lead: pltpu.VMEM(lead + (half, 2 * hd), BF16)
    return pl.pallas_call(
        functools.partial(exchange_kernel, n, heads, source_rows),
        out_shape=[shape((n, half, 2 * hd), BF16), shape((n, q_rows, 2 * hd), BF16), shape((q_rows, 2 * dec_in.shape[1]), BF16)],
        in_specs=vmem(7),
        out_specs=vmem(3),
        scratch_shapes=[chunk(heads), chunk(side - 1, side), chunk(2), chunk(2), block(side), block(side)]
        + row_scratch(heads, q_rows, hd)
        + [dma(2), dma(2), dma(side - 1), dma(2), dma(side), dma(side), dma(side - 1, side), dma(2), dma(2), dma(side), dma(side),
           pltpu.SemaphoreType.DMA],
        compiler_params=remote(collective_id),
        name='exchange',
    )(memory, dec_in, grad_out, gain, wk_t, wv_t, wq_t)


def return_kernel(n, heads, source_rows, chunk, src_ref, dq_ref, gain_ref, early_hbm, dst_ref, rows_ref, gq_ref, stage_ref, right_ref,
                  left_ref, up_ref, down_ref, theirs_ref, packed_ref, got_ref, dqt_ref, decs_ref, dec_sem, row_send, row_recv,
                  x_send, fwd_send, y_send, pass_send, stage_recv, right_recv, left_recv, up_recv, down_recv, out_recv):
    g = Grid(n, heads, source_rows)
    side = g.side
    half = src_ref.shape[1]
    total_rows, dim = dqt_ref.shape[1], gq_ref.shape[1]

    def dec_load(index, slot):
        at = pl.ds(pl.multiple_of(index * chunk, chunk), chunk)
        return pltpu.make_async_copy(early_hbm.at[at, pl.ds(0, dim)], decs_ref.at[slot], dec_sem.at[slot])

    dec_load(0, 0).start()
    meet(g.peers())
    mine = pl.ds(pl.multiple_of(g.part * half, half), half)

    def landing(drow, dcol, head_col):
        if drow == 0:
            return dst_ref.at[g.row * side + head_col, mine], out_recv
        return stage_ref.at[drow - 1, dcol, mine], stage_recv.at[drow - 1, dcol]

    def along_row(drow, dcol):
        row = g.wrap(g.row + drow)
        col = g.wrap(g.col + dcol)
        for part in range(g.parts):
            source = src_ref.at[g.device(row, col, part)]
            if dcol in g.direct:
                dst, sem = landing(drow, dcol, g.col)
                send(source, dst, x_send.at[drow], sem, g.near(0, g.hop(dcol), part)).start()
            elif part == 0:
                send(source, right_ref.at[drow], x_send.at[drow], right_recv.at[drow], g.near(0, 1)).start()
            else:
                send(source, left_ref.at[drow], x_send.at[drow], left_recv.at[drow], g.near(0, -1)).start()

    def own_chip(drow):
        row = g.wrap(g.row + drow)
        away = src_ref.at[g.device(row, g.col, g.parts - 1 - g.part)]
        dst, sem = landing(drow, 0, g.col)
        dst[...] = src_ref[g.device(row, g.col, g.part)]
        send(away, dst, x_send.at[drow], sem, g.partner).start()

    def pass_row(drow):
        for ref, come_sem, come in ((right_ref, right_recv, -1), (left_ref, left_recv, 1)):
            send(ref.at[drow], ref.at[drow], fwd_send.at[drow], come_sem.at[drow], g.me).wait_recv()
            dst, sem = landing(drow, 2, g.wrap(g.col + come))
            send(ref.at[drow], dst, fwd_send.at[drow], sem, g.near(0, -come, 0 if come < 0 else 1)).start()

    def along_column(drow, dcol):
        chunk = stage_ref.at[drow - 1, dcol]
        got = chunk.at[pl.ds(0, half)] if dcol == 0 else chunk
        send(got, got, y_send.at[drow - 1], stage_recv.at[drow - 1, dcol], g.me).wait_recv()
        head = g.row * side + g.wrap(g.col - dcol)
        if drow in g.direct:
            send(chunk, dst_ref.at[head], y_send.at[drow - 1], out_recv, g.near(g.hop(drow), 0)).start()
        elif dcol % 2 == 0:
            send(chunk, up_ref.at[dcol // 2], y_send.at[drow - 1], up_recv.at[dcol // 2], g.near(1, 0)).start()
        else:
            send(chunk, down_ref.at[dcol // 2], y_send.at[drow - 1], down_recv.at[dcol // 2], g.near(-1, 0)).start()

    def when_source(row, body):
        pl.when(g.is_source(row))(body)

    def rows_of(drow):
        def body():
            for d in (2, 1, 3) if g.ties else (1,):
                along_row(drow, d)
        when_source(g.row + drow, body)

    def relay(drow):
        when_source(g.row + drow, lambda: pass_row(drow))

    def column(drow, d):
        when_source(g.row + drow, lambda: along_column(drow, d))

    def up(i):
        def body():
            send(up_ref.at[i], up_ref.at[i], pass_send.at[0], up_recv.at[i], g.me).wait_recv()
            head = g.wrap(g.row - 1) * side + g.wrap(g.col - 2 * i)
            send(up_ref.at[i], dst_ref.at[head], pass_send.at[0], out_recv, g.near(1, 0)).start()
        when_source(g.row + 1, body)

    def down(i):
        def body():
            send(down_ref.at[i], down_ref.at[i], pass_send.at[1], down_recv.at[i], g.me).wait_recv()
            head = g.wrap(g.row + 1) * side + g.wrap(g.col - 2 * i - 1)
            send(down_ref.at[i], dst_ref.at[head], pass_send.at[1], out_recv, g.near(-1, 0)).start()
        when_source(g.row - 1, body)

    def start_dq():
        swap(dq_ref, theirs_ref, row_send.at[0], row_recv.at[0], g.partner)
        both = (dq_ref[...] + theirs_ref[...]).astype(BF16)
        share = dqt_ref.shape[0]
        dqt_ref[...] = jnp.where(g.part == 0, both[:share], both[share:])
        total = both.T
        packed_ref[...] = pack(total.reshape(n, total.shape[0] // n, total.shape[1]))
        start_rows(n, heads, g.me, g.part, packed_ref, lambda peer: peer, got_ref, row_send.at[1], row_recv.at[1])

    def query_weight(index, carry):
        slot = lax.rem(index, 2)
        dec_load(index, slot).wait()

        @pl.when(index + 1 < chunks)
        def _():
            dec_load(index + 1, 1 - slot).start()

        normed = rms_norm(decs_ref[slot].astype(F32), gain_ref[...].astype(F32)).astype(BF16)
        gq_ref[...] += dot(dqt_ref[:, pl.ds(pl.multiple_of(index * chunk, chunk), chunk)], normed)
        return carry

    chunks = total_rows // chunk
    for drow in (2, 1, 3, 0) if g.ties else (1, 0):
        when_source(g.row + drow, lambda drow=drow: own_chip(drow))
    if g.ties:
        rows_of(2)
        for drow in (2, 1, 3):
            column(drow, 0)
        relay(2)
        rows_of(1)
        column(2, 1)
        column(2, 3)
        column(2, 2)
        relay(1)
        rows_of(3)
        start_dq()
        up(0)
        down(0)
        column(1, 1)
        column(1, 3)
        column(1, 2)
        relay(3)
        rows_of(0)
        up(1)
        down(1)
        column(3, 1)
        column(3, 3)
        column(3, 2)
        relay(0)
    else:
        rows_of(1)
        rows_of(0)
        start_dq()
        column(1, 0)
        column(1, 1)
    gq_ref[...] = jnp.zeros_like(gq_ref)
    lax.fori_loop(0, chunks, query_weight, 0)
    wait_rows(heads, g.me, got_ref, row_send.at[1], row_recv.at[1])
    rows_ref[...] = unpack(got_ref[...])

    def sent(sem, ref):
        send(ref, ref, sem, out_recv, g.me).wait_send()

    for drow in range(side):
        def done(drow=drow):
            sent(x_send.at[drow], src_ref.at[pl.ds(0, g.parts * side - 1)])
            if g.ties:
                sent(fwd_send.at[drow], src_ref.at[pl.ds(0, 2)])
            if drow:
                sent(y_send.at[drow - 1], stage_ref.at[0])
        when_source(g.row + drow, done)
    if g.ties:
        when_source(g.row + 1, lambda: sent(pass_send.at[0], up_ref))
        when_source(g.row - 1, lambda: sent(pass_send.at[1], down_ref))

    @pl.when(g.is_source(g.row))
    def _():
        blocks = src_ref.at[pl.ds(0, n - 1)]
        send(blocks, blocks, y_send.at[0], out_recv, g.me).wait_recv()

    @pl.when(jnp.logical_not(g.is_source(g.row)))
    def _():
        def clear(index, carry):
            dst_ref[index] = jnp.zeros(dst_ref.shape[1:], dst_ref.dtype)
            return carry
        lax.fori_loop(0, heads, clear, 0)


def return_blocks(n, heads, source_rows, collective_id, blocks, dq, gain, early):
    half, width = blocks.shape[1], blocks.shape[2]
    hd, total_q = dq.shape
    q_rows = total_q // n
    side, parts = math.isqrt(heads), n // heads
    chunk = lambda *lead: pltpu.VMEM(lead + (half * parts, width), BF16)
    block = lambda *lead: pltpu.VMEM(lead + (half, width), BF16)
    piece, dim = min(512, total_q), early.shape[1] // 2
    return pl.pallas_call(
        functools.partial(return_kernel, n, heads, source_rows, piece),
        out_shape=[shape((heads, half * parts, width), BF16), shape((heads, q_rows, hd), BF16), shape((hd // parts, dim), F32)],
        in_specs=vmem(3) + [pl.BlockSpec(memory_space=pl.ANY)],
        out_specs=vmem(3),
        scratch_shapes=[chunk(side - 1, side), block(side), block(side), chunk(2), chunk(2), pltpu.VMEM(dq.shape, F32),
                        pltpu.VMEM((n, q_rows // 2, 2 * hd), BF16), pltpu.VMEM((heads, q_rows // 2, 2 * hd), BF16),
                        pltpu.VMEM((hd // parts, total_q), BF16), pltpu.VMEM((2, piece, dim), BF16), dma(2), dma(2), dma(2),
                        dma(side), dma(side), dma(side - 1), dma(2), dma(side - 1, side), dma(side), dma(side), dma(2), dma(2),
                        pltpu.SemaphoreType.DMA],
        compiler_params=remote(collective_id),
        name='return_blocks',
    )(blocks, dq, gain, early)


def decoder_kernel(n, heads, mine_ref, dec_ref, gout_ref, gain_ref, wo_hbm, wg_hbm, wu_hbm, wd_hbm,
                   out_ref, lse_ref, do_ref, factors_ref, gh_ref, gnorm_ref,
                   theirs_ref, packed_ref, got_ref, sent_ref, back_ref, swapped_ref, wo_ref, wg_ref, wu_ref, wd_ref, gact_ref,
                   load_sem, send_sem, recv_sem):
    me = lax.axis_index('seq')
    part = lax.rem(me, n // heads)
    partner, peers = pair_peers(n, heads, me, part)
    q_rows, dim = dec_ref.shape
    hd = out_ref.shape[0]
    loads = [pltpu.make_async_copy(src, dst, load_sem.at[i]) for i, (src, dst) in enumerate(
        ((wd_hbm, wd_ref), (wo_hbm, wo_ref), (wg_hbm, wg_ref), (wu_hbm, wu_ref)))]
    for load in loads:
        load.start()
    meet(peers)

    swap(mine_ref, theirs_ref, send_sem.at[0], recv_sem.at[0], partner)
    m_a, m_b = mine_ref[hd + 8:hd + 9], theirs_ref[hd + 8:hd + 9]
    top = jnp.maximum(m_a, m_b)
    s_a, s_b = jnp.exp2(m_a - top), jnp.exp2(m_b - top)
    den = mine_ref[hd:hd + 1] * s_a + theirs_ref[hd:hd + 1] * s_b
    out = (mine_ref[:hd] * s_a + theirs_ref[:hd] * s_b) / den
    packed_ref[...] = pack(out.T.astype(BF16).reshape(n, q_rows, hd))
    start_rows(n, heads, me, part, packed_ref, lambda peer: peer, got_ref, send_sem.at[1], recv_sem.at[1])
    out_ref[...] = out
    lse_ref[...] = top + jnp.log2(den)

    loads[0].wait()
    top_rows = gout_ref[...].astype(BF16)
    tile = 256

    def act_tile(index, carry):
        at = pl.ds(pl.multiple_of(index * tile, tile), tile)
        gact_ref[:, at] = dot_nt(top_rows, wd_ref[at, :])
        return carry

    lax.fori_loop(0, wd_ref.shape[0] // tile, act_tile, 0)
    wait_rows(heads, me, got_ref, send_sem.at[1], recv_sem.at[1])

    attended = jnp.concatenate([unpack(got_ref[h]) for h in range(heads)], axis=1)
    loads[1].wait()
    hidden = (dec_ref[...].astype(F32) + dot(attended, wo_ref[...])).astype(BF16).astype(F32)
    gain = gain_ref[...].astype(F32)
    inverse = lax.rsqrt(jnp.mean(hidden * hidden, axis=-1, keepdims=True) + 1e-6)
    scaled = hidden * inverse
    normed = (scaled * gain).astype(BF16)
    loads[2].wait()
    gate = dot(normed, wg_ref[...])
    loads[3].wait()
    up = dot(normed, wu_ref[...])
    sig = jax.nn.sigmoid(gate)
    silu = gate * sig
    grad_act = gact_ref[...]
    grad_gate = (grad_act * up * (sig + silu * (1.0 - sig))).astype(BF16)
    grad_up = (grad_act * silu).astype(BF16)
    grad_normed = (dot_nt(wg_ref[...], grad_gate) + dot_nt(wu_ref[...], grad_up)).T
    gnorm_ref[...] = jnp.sum(grad_normed * scaled, axis=0, keepdims=True)
    inner = grad_normed * gain
    grad_hidden = gout_ref[...] + inverse * (inner - scaled * jnp.mean(inner * scaled, axis=-1, keepdims=True))
    rounded = grad_hidden.astype(BF16)
    grad_att = dot_nt(wo_ref[...], rounded).T.astype(BF16)
    for h in range(heads):
        sent_ref[h] = pack(grad_att[:, hd * h:hd * (h + 1)])
    factors_ref[:, :dim] = attended
    factors_ref[:, dim:] = rounded
    gh_ref[...] = grad_hidden

    start_rows(n, heads, me, part, sent_ref, lambda peer: peer // (n // heads), back_ref, send_sem.at[2], recv_sem.at[2])
    wait_rows(heads, me, back_ref, send_sem.at[2], recv_sem.at[2])
    swap(back_ref, swapped_ref, send_sem.at[3], recv_sem.at[3], partner)
    place(n, heads, part, back_ref, swapped_ref, do_ref, False)


def decoder_rows(n, heads, collective_id, mine, dec_in, grad_out, gain, wo, w_gate, w_up, w_down):
    q_rows, dim = dec_in.shape
    hd, total_q = wo.shape[0] // heads, mine.shape[1]
    hbm = pl.BlockSpec(memory_space=pl.ANY)
    return pl.pallas_call(
        functools.partial(decoder_kernel, n, heads),
        out_shape=[shape((hd, total_q), F32), shape((1, total_q), F32), shape((n, q_rows, 2 * hd), BF16),
                   shape((q_rows, 2 * dim), BF16), shape((q_rows, dim), F32), shape((1, dim), F32)],
        in_specs=vmem(4) + [hbm] * 4,
        out_specs=vmem(6),
        scratch_shapes=[pltpu.VMEM(mine.shape, F32), pltpu.VMEM((n, q_rows // 2, 2 * hd), BF16)]
        + [pltpu.VMEM((heads, q_rows // 2, 2 * hd), BF16)] * 4
        + [pltpu.VMEM(w.shape, BF16) for w in (wo, w_gate, w_up, w_down)] + [pltpu.VMEM((q_rows, w_down.shape[0]), F32), dma(4), dma(4), dma(4)],
        compiler_params=remote(collective_id),
        name='decoder_rows',
    )(mine, dec_in, grad_out, gain, wo, w_gate, w_up, w_down)


def valid_blocks(mem_len, rows, parts, sources):
    reach = mem_len - lax.rem(lax.axis_index('seq'), parts) * rows
    blocks = jnp.minimum((reach + parts * rows - 1) // (parts * rows), sources)
    return blocks, jnp.minimum(reach - (blocks - 1) * parts * rows, rows)


def forward_kernel(scale, hd, parts, q_block, len_ref, kv_ref, q_ref, out_ref, qt_ref, top_ref):
    rows, total_q = kv_ref.shape[1], q_ref.shape[0]
    blocks, last_valid = valid_blocks(len_ref[0], rows, parts, kv_ref.shape[0])
    groups = [slice(first, first + q_block) for first in range(0, total_q, q_block)]
    base = slice(hd + 8, hd + 9)
    qt_ref[...] = q_ref[...].T

    def values_of(keys):
        return jnp.concatenate([keys.T[hd:], jnp.ones((16, rows), keys.dtype)], axis=0)

    def group_of(index):
        return pl.ds(pl.multiple_of(index * q_block, q_block), q_block)

    def first_step(group, carry):
        cols = group_of(group)
        top = jnp.max(dot(kv_ref[0], qt_ref[:, cols]), axis=0, keepdims=True)
        out_ref[hd + 8:, cols] = jnp.broadcast_to(top * scale, (8, q_block))
        top_ref[:, cols] = jnp.broadcast_to(top, (8, q_block))
        return carry

    lax.fori_loop(0, len(groups), first_step, 0)
    out_ref[:hd + 8, :] = jnp.zeros((hd + 8, total_q), F32)

    def finish(values, scores, cols):
        top_ref[:, cols] = jnp.maximum(top_ref[:, cols], jnp.max(scores.reshape(rows // 8, 8, q_block), axis=0))
        weights = jnp.exp2(scores * scale - out_ref[base, cols]).astype(values.dtype)
        out_ref[:hd + 8, cols] += dot(values, weights)[:hd + 8]

    def step(index, carry):
        keys = kv_ref[index]
        values = values_of(keys)
        for cols in groups:
            finish(values, dot(keys, qt_ref[:, cols]), cols)
        return carry

    def last_step(group, carry):
        cols = group_of(group)
        keys = kv_ref[blocks - 1]
        scores = dot(keys, qt_ref[:, cols])
        position = lax.broadcasted_iota(jnp.int32, scores.shape, 0)
        finish(values_of(keys), jnp.where(position < last_valid, scores, NEG), cols)
        return carry

    lax.fori_loop(0, blocks - 1, step, 0)
    lax.fori_loop(0, len(groups), last_step, 0)

    excess = jnp.max(top_ref[...] * scale - out_ref[hd + 8:, :])
    broken = jnp.max(jnp.where(jnp.abs(out_ref[:hd + 8, :]) <= 3e38, 0.0, 1.0))

    @pl.when(jnp.logical_or(jnp.logical_not(excess <= 64.0), broken > 0.0))
    def _():
        out_ref[:hd + 8, :] = jnp.zeros((hd + 8, total_q), F32)
        out_ref[hd + 8:, :] = jnp.full((8, total_q), NEG, F32)

        def running(step_index, carry):
            index, group = step_index // len(groups), lax.rem(step_index, len(groups))
            cols = group_of(group)
            keys = kv_ref[index]
            limit = jnp.where(index == blocks - 1, last_valid, rows)
            scores = dot(keys, qt_ref[:, cols]) * scale
            position = lax.broadcasted_iota(jnp.int32, scores.shape, 0)
            scores = jnp.where(position < limit, scores, NEG)
            old = out_ref[base, cols]
            new = jnp.maximum(old, jnp.max(scores, axis=0, keepdims=True))
            weights = jnp.exp2(scores - new).astype(keys.dtype)
            out_ref[:hd + 8, cols] = out_ref[:hd + 8, cols] * jnp.exp2(old - new) + dot(values_of(keys), weights)[:hd + 8]
            out_ref[hd + 8:, cols] = jnp.broadcast_to(new, (8, q_block))
            return carry

        lax.fori_loop(0, blocks * len(groups), running, 0)


def attention_forward(scale, hd, parts, sources, mem_len, kv, q):
    rows, width = kv.shape[1], kv.shape[2]
    total_q = q.shape[0]
    return pl.pallas_call(
        functools.partial(forward_kernel, scale, hd, parts, min(1024, total_q)),
        out_shape=shape((hd + 16, total_q), F32),
        grid=(1,),
        in_specs=[pl.BlockSpec(memory_space=pltpu.SMEM),
                  pl.BlockSpec((sources, rows, width), lambda i: (0, 0, 0), pipeline_mode=pl.Buffered(1)), full(q)],
        out_specs=pl.BlockSpec((hd + 16, total_q), lambda i: (0, 0)),
        scratch_shapes=[pltpu.VMEM((width, total_q), BF16), pltpu.VMEM((8, total_q), F32)],
        compiler_params=plain(),
        cost_estimate=pl.CostEstimate(flops=4 * total_q * sources * rows * hd, bytes_accessed=kv.size * 2,
                                      transcendentals=total_q * sources * rows),
        name='attention_forward',
    )(mem_len, kv, q)


def backward_kernel(scale, key_scale, hd, parts, q_block, len_ref, kv_ref, q_ref, do_ref, out_ref, lse_ref, dkv_ref, dq_ref,
                    qt_ref, dot_ref, delta_ref):
    rows, total_q = kv_ref.shape[1], q_ref.shape[0]
    blocks, last_valid = valid_blocks(len_ref[0], rows, parts, kv_ref.shape[0])
    width = kv_ref.shape[2]
    groups = [slice(first, first + q_block) for first in range(0, total_q, q_block)]
    dq_ref[...] = jnp.zeros_like(dq_ref)
    qt_ref[...] = q_ref[...].T
    do_t = do_ref[...].T
    dot_ref[...] = do_t
    delta_ref[...] = jnp.sum(do_t[hd:].astype(F32) * out_ref[...], axis=0, keepdims=True)

    lane_scale = jnp.where(lax.broadcasted_iota(jnp.int32, (1, width), 1) < hd, key_scale, 1.0)

    def products(keys, cols):
        return dot(keys, qt_ref[:, cols]), dot(keys, dot_ref[:, cols])

    def finish(keys, keys_t, scores, grads, cols, valid):
        prob = jnp.exp2(scores * scale - lse_ref[:, cols])
        if valid is not None:
            position = lax.broadcasted_iota(jnp.int32, scores.shape, 0)
            prob = jnp.where(position < valid, prob, 0.0)
        grad_scores = (prob * (grads - delta_ref[:, cols])).astype(keys.dtype)
        update = dot(grad_scores, q_ref[cols, :]) + dot(prob.astype(keys.dtype), do_ref[cols, :])
        dq_ref[:, cols] += dot(keys_t, grad_scores)
        return update

    def step(index, carry):
        keys = kv_ref[index]
        keys_t = keys.T[:hd]
        total = jnp.zeros((rows, width), F32)
        for cols in groups:
            scores, grads = products(keys, cols)
            total += finish(keys, keys_t, scores, grads, cols, None)
        dkv_ref[index] = (total * lane_scale).astype(dkv_ref.dtype)
        return carry

    def last_step(group, total):
        keys = kv_ref[blocks - 1]
        cols = pl.ds(pl.multiple_of(group * q_block, q_block), q_block)
        scores, grads = products(keys, cols)
        return total + finish(keys, keys.T[:hd], scores, grads, cols, last_valid)

    def clear(index, carry):
        dkv_ref[index] = jnp.zeros((rows, width), dkv_ref.dtype)
        return carry

    lax.fori_loop(0, blocks - 1, step, 0)
    total = lax.fori_loop(0, len(groups), last_step, jnp.zeros((rows, width), F32))
    dkv_ref[blocks - 1] = (total * lane_scale).astype(dkv_ref.dtype)
    lax.fori_loop(blocks, dkv_ref.shape[0], clear, 0)
    dq_ref[...] = dq_ref[...] * key_scale


def attention_backward(scale, key_scale, hd, parts, sources, mem_len, kv, q, do, out_t, lse):
    n, rows, width = kv.shape
    total_q = q.shape[0]
    return pl.pallas_call(
        functools.partial(backward_kernel, scale, key_scale, hd, parts, min(512, total_q)),
        out_shape=[shape((n, rows, width), BF16), shape((hd, total_q), F32)],
        grid=(1,),
        in_specs=[pl.BlockSpec(memory_space=pltpu.SMEM),
                  pl.BlockSpec((sources, rows, width), lambda i: (0, 0, 0), pipeline_mode=pl.Buffered(1)),
                  full(q), full(do), full(out_t), full(lse)],
        out_specs=[pl.BlockSpec((n, rows, width), lambda i: (0, 0, 0)),
                   pl.BlockSpec((hd, total_q), lambda i: (0, 0))],
        scratch_shapes=[pltpu.VMEM((width, total_q), BF16), pltpu.VMEM((width, total_q), BF16), pltpu.VMEM((1, total_q), F32)],
        compiler_params=plain(),
        cost_estimate=pl.CostEstimate(flops=10 * total_q * sources * rows * hd, bytes_accessed=kv.size * 4,
                                      transcendentals=total_q * sources * rows),
        name='attention_backward',
    )(mem_len, kv, q, do, out_t, lse)


def reduce_kernel(n, heads, tile, chunk, gk_hbm, gv_hbm, early_hbm, late_hbm, w1_hbm, w3_hbm, w2_hbm, wo_ref, wq_ref, gain1_ref,
                  gain2_ref, dqr_ref, dec_ref, gh_ref, gnorm_ref,
                  sums_ref, gdec_ref, norms_ref, n2_hbm, d1_hbm, d3_hbm, act_hbm,
                  acc_ref, pair_ref, far_ref, near_ref, n2_ref, top_ref, att_ref, decs_ref, w1_ref, w3_ref, w2_ref, w2t_ref, made_ref,
                  d1_ref, d3_ref, act_ref, mine_ref, all_ref,
                  own_sem, share_send, share_recv, pair_send, pair_recv, far_send, far_recv, near_send, near_recv, rows_sem, top_sem, w_sem, out_sem, n2_sem,
                  norm_send, norm_recv):
    g = Grid(n, heads, 0)
    side = g.side
    rows, dim = n2_ref.shape
    tiles = d1_hbm.shape[0]
    own_tiles = (tiles + g.parts - 1 - g.part) // g.parts
    part_rows = acc_ref.shape[1]

    def start_rows_of(index):
        slot = lax.rem(index, 2)
        at = pl.ds(pl.multiple_of(index * chunk, chunk), chunk)
        for i, (src, dst) in enumerate(((late_hbm, att_ref), (early_hbm, decs_ref))):
            pltpu.make_async_copy(src.at[at, pl.ds(0, dim)], dst.at[slot], rows_sem.at[slot, i]).start()

    def tile_at(index):
        return pl.ds(pl.multiple_of(index * tile, tile), tile)

    def weights(index):
        slot = lax.rem(index, 2)
        at = tile_at(index * g.parts + g.part)
        return [pltpu.make_async_copy(src, dst.at[slot], w_sem.at[slot, i]) for i, (src, dst) in enumerate(
            ((w1_hbm.at[:, at], w1_ref), (w3_hbm.at[:, at], w3_ref), (w2_hbm.at[at, :], w2_ref)))]

    def results(index):
        slot, number = lax.rem(index, 2), index * g.parts + g.part
        pairs = ((d1_ref, d1_hbm), (d3_ref, d3_hbm), (act_ref, act_hbm))
        return ([pltpu.make_async_copy(src.at[slot], dst.at[number], out_sem.at[slot, i]) for i, (src, dst) in enumerate(pairs)],
                [send(src.at[slot], dst.at[number], share_send.at[slot, i], share_recv.at[i], g.partner)
                 for i, (src, dst) in enumerate(pairs)])

    start_rows_of(0)
    top_load = pltpu.make_async_copy(early_hbm.at[:, pl.ds(dim, dim)], top_ref, top_sem)
    top_load.start()
    for copy in weights(0):
        copy.start()

    def summand(c, core):
        source = gk_hbm if c < heads // g.parts else gv_hbm
        first = ((g.parts * c) % heads + core) * part_rows
        return source.at[pl.ds(pl.multiple_of(first, part_rows), part_rows), :]

    owns = [pltpu.make_async_copy(summand(c, g.part), acc_ref.at[c], own_sem.at[c]) for c in range(heads)]
    for copy in owns:
        copy.start()

    meet([lax.rem(g.me + step, n) for step in range(1, n)])
    for c in range(heads):
        send(summand(c, g.parts - 1 - g.part), pair_ref.at[c], pair_send, pair_recv, g.partner).start()

    grad_query = jnp.concatenate([dqr_ref[h] for h in range(heads)], axis=1)
    grad_normed = dot(grad_query, wq_ref[...])
    x = dec_ref[...].astype(F32)
    inverse = lax.rsqrt(jnp.mean(x * x, axis=-1, keepdims=True) + 1e-6)
    scaled = x * inverse
    inner = grad_normed * gain1_ref[...].astype(F32)
    gdec_ref[...] = gh_ref[...] + inverse * (inner - scaled * jnp.mean(inner * scaled, axis=-1, keepdims=True))
    mine_ref[0:1, :] = jnp.sum(grad_normed * scaled, axis=0, keepdims=True)
    mine_ref[1:2, :] = gnorm_ref[...]

    for step in range(1, n):
        send(mine_ref, all_ref.at[g.me], norm_send, norm_recv, lax.rem(g.me + step, n)).start()
    all_ref[g.me] = mine_ref[...]

    quarter = part_rows // 4
    streams = [(axis, way, pl.ds((2 * axis + (way < 0)) * quarter, quarter)) for axis in (0, 1) for way in (1, -1)]

    def place_of(axis, line, other):
        return other * side + line if axis == 0 else line * side + other

    def pieces(stage, axis, line):
        position = g.row if axis == 0 else g.col
        return [place_of(axis, line, o) for o in range(side)] if stage == 0 else [place_of(axis, line, position)]

    def ring(stage, stream, step):
        axis, way, part = streams[stream]
        axis = axis if stage == 0 else 1 - axis
        here = g.col if axis == 0 else g.row
        ref, sends, recvs = (far_ref, far_send, far_recv) if stage == 0 else (near_ref, near_send, near_recv)
        to = g.near(0, way) if axis == 0 else g.near(way, 0)
        return axis, way, part, here, ref.at[stream, step - 1], sends.at[stream, step - 1], recvs.at[stream, step - 1], to

    def line_of(here, way, step):
        return lax.rem(here - way * step + 2 * side, side)

    def start_step(stage, step):
        for stream in range(4):
            axis, way, part, here, buffer, sem, recv, to = ring(stage, stream, step)
            for i, c in enumerate(pieces(stage, axis, line_of(here, way, step))):
                send(acc_ref.at[c, part], buffer.at[i], sem, recv, to).start()

    def end_step(stage, step):
        for stream in range(4):
            axis, way, part, here, buffer, sem, recv, to = ring(stage, stream, step)
            whole = send(buffer, buffer, sem, recv, g.me)
            whole.wait_recv()
            for i, c in enumerate(pieces(stage, axis, line_of(here, way, step + 1))):
                acc_ref[c, part, :] = acc_ref[c, part, :] + buffer[i]
            whole.wait_send()

    def add_pair():
        for copy in owns:
            copy.wait()
        whole = send(pair_ref, pair_ref, pair_send, pair_recv, g.me)
        whole.wait_recv()

        def add(c, carry):
            acc_ref[c] = acc_ref[c] + pair_ref[c]
            return carry

        lax.fori_loop(0, heads, add, 0)
        whole.wait_send()

    def first():
        add_pair()
        start_step(0, 1)

    def turn():
        end_step(0, side - 1)
        start_step(1, 1)

    def between(stage, step):
        def body():
            end_step(stage, step)
            start_step(stage, step + 1)
        return body

    def prepare(index, carry):
        slot = lax.rem(index, 2)
        at = pl.ds(pl.multiple_of(index * chunk, chunk), chunk)
        for i, (src, dst) in enumerate(((late_hbm, att_ref), (early_hbm, decs_ref))):
            pltpu.make_async_copy(src.at[at, pl.ds(0, dim)], dst.at[slot], rows_sem.at[slot, i]).wait()

        @pl.when(index + 1 < rows // chunk)
        def _():
            start_rows_of(index + 1)

        pl.when(index == rows // chunk // 2)(first)
        dec = decs_ref[slot].astype(F32)
        hidden = (dec + dot(att_ref[slot], wo_ref[...])).astype(BF16).astype(F32)
        n2_ref[at, :] = rms_norm(hidden, gain2_ref[...].astype(F32)).astype(BF16)
        return carry

    lax.fori_loop(0, rows // chunk, prepare, 0)
    top_load.wait()
    n2_store = pltpu.make_async_copy(n2_ref, n2_hbm, n2_sem)
    n2_store.start()

    events = ([between(0, t) for t in range(1, side - 1)] + [turn] + [between(1, t) for t in range(1, side - 1)]
              + [lambda: end_step(1, side - 1)])
    at_tile = (1, 3)
    inside = tiles // 2 > at_tile[-1] and len(events) > len(at_tile)

    def finish_results(index):
        stores, shares = results(index)
        for copy in stores:
            copy.wait()
        for copy in shares:
            copy.wait_send()

    def activations(index, carry):
        slot = lax.rem(index, 2)
        for copy in weights(index):
            copy.wait()

        @pl.when(index + 1 < own_tiles)
        def _():
            for copy in weights(index + 1):
                copy.start()

        @pl.when(index >= 2)
        def _():
            finish_results(index - 2)

        if inside:
            for event, when in zip(events, at_tile):
                pl.when(index == when)(event)

        w2t_ref[...] = w2_ref[slot].T

        def products(j):
            part = pl.ds(pl.multiple_of(j * chunk, chunk), chunk)
            keep = lax.rem(j, 2)
            made_ref[keep, 0] = dot(n2_ref[part, :], w1_ref[slot])
            made_ref[keep, 1] = dot(n2_ref[part, :], w3_ref[slot])
            made_ref[keep, 2] = dot(top_ref[part, :], w2t_ref[...])

        def factors(j):
            part = pl.ds(pl.multiple_of(j * chunk, chunk), chunk)
            keep = lax.rem(j, 2)
            gate, up, grad = made_ref[keep, 0], made_ref[keep, 1], made_ref[keep, 2]
            sig = jax.nn.sigmoid(gate)
            silu = gate * sig
            act_ref[slot, part, :] = (silu * up).astype(BF16)
            d3_ref[slot, part, :] = (grad * silu).astype(BF16)
            d1_ref[slot, part, :] = (grad * up * (sig + silu * (1.0 - sig))).astype(BF16)

        def both(j, carry):
            part = pl.ds(pl.multiple_of(j * chunk, chunk), chunk)
            fresh = dot(n2_ref[part, :], w1_ref[slot]), dot(n2_ref[part, :], w3_ref[slot]), dot(top_ref[part, :], w2t_ref[...])
            factors(j - 1)
            for i, value in enumerate(fresh):
                made_ref[lax.rem(j, 2), i] = value
            return carry

        products(0)
        lax.fori_loop(1, rows // chunk, both, 0)
        factors(rows // chunk - 1)
        for copies in results(index):
            for copy in copies:
                copy.start()
        return carry

    lax.fori_loop(0, own_tiles, activations, 0)
    for event in events[len(at_tile):] if inside else events:
        event()
    sums_ref[...] = acc_ref[g.chip]

    others = all_ref.at[pl.ds(0, n - 1)]
    whole = send(others, others, norm_send, norm_recv, g.me)
    whole.wait_send()
    whole.wait_recv()
    norms_ref[...] = jnp.sum(all_ref[...], axis=0)
    n2_store.wait()
    @pl.when(own_tiles >= 2)
    def _():
        finish_results(own_tiles - 2)

    finish_results(own_tiles - 1)
    for core in range(g.parts):
        others_tiles = (tiles + core) // g.parts

        @pl.when(g.part == core)
        def _(others_tiles=others_tiles):
            for i, ref in enumerate((d1_hbm, d3_hbm, act_hbm)):
                come = ref.at[pl.ds(0, others_tiles)]
                send(come, come, share_send.at[0, i], share_recv.at[i], g.me).wait_recv()


def reduce_sums(n, heads, collective_id, gk, gv, early, late, w_gate, w_up, w_down, wo, wq, gain1, gain2, dq_rows, dec_in, gh, gnorm):
    rows, dim = early.shape[0], gk.shape[1]
    ff, tile, chunk = w_gate.shape[1], 256, min(512, early.shape[0] // 2)
    part_rows = 2 * gk.shape[0] // n
    side = math.isqrt(heads)
    hbm = pl.BlockSpec(memory_space=pl.ANY)
    return pl.pallas_call(
        functools.partial(reduce_kernel, n, heads, tile, chunk),
        out_shape=[shape((part_rows, dim), F32), shape(gh.shape, F32), shape((2, dim), F32), shape((rows, dim), BF16)]
        + [shape((ff // tile, rows, tile), BF16)] * 3,
        in_specs=[hbm] * 7 + vmem(8),
        out_specs=vmem(3) + [hbm] * 4,
        scratch_shapes=[pltpu.VMEM((heads, part_rows, dim), F32)] * 2
        + [pltpu.VMEM((4, side - 1, side, part_rows // 4, dim), F32), pltpu.VMEM((4, side - 1, 1, part_rows // 4, dim), F32)]
        + [pltpu.VMEM((rows, dim), BF16)] * 2 + [pltpu.VMEM((2, chunk, dim), BF16)] * 2
        + [pltpu.VMEM((2, dim, tile), BF16)] * 2 + [pltpu.VMEM((2, tile, dim), BF16), pltpu.VMEM((dim, tile), BF16),
           pltpu.VMEM((2, 3, chunk, tile), F32)] + [pltpu.VMEM((2, rows, tile), BF16)] * 3
        + [pltpu.VMEM((2, dim), F32), pltpu.VMEM((n, 2, dim), F32)]
        + [dma(heads), dma(2, 3), dma(3), pltpu.SemaphoreType.DMA, pltpu.SemaphoreType.DMA, dma(4, side - 1), dma(4, side - 1), dma(4, side - 1),
           dma(4, side - 1), dma(2, 2), pltpu.SemaphoreType.DMA, dma(2, 3), dma(2, 3), pltpu.SemaphoreType.DMA,
           pltpu.SemaphoreType.DMA, pltpu.SemaphoreType.DMA],
        compiler_params=remote(collective_id),
        cost_estimate=pl.CostEstimate(flops=6 * rows * dim * ff, bytes_accessed=12 * rows * ff, transcendentals=rows * ff),
        name='reduce_sums',
    )(gk, gv, early, late, w_gate, w_up, w_down, wo, wq, gain1, gain2, dq_rows, dec_in, gh, gnorm)


def gate_up_kernel(n2_ref, d1_ref, d3_ref, g1_ref, g3_ref, n2t_ref):
    @pl.when(pl.program_id(0) == 0)
    def _():
        n2t_ref[...] = n2_ref[...].T

    g1_ref[...] = dot(n2t_ref[...], d1_ref[...])
    g3_ref[...] = dot(n2t_ref[...], d3_ref[...])


def gate_up_grads(n2, d1, d3):
    rows, dim = n2.shape
    tiles, _, tile = d1.shape
    cols = pl.BlockSpec((dim, tile), lambda i: (0, i))
    part = pl.BlockSpec((pl.Squeezed(), rows, tile), lambda i: (i, 0, 0))
    return pl.pallas_call(
        gate_up_kernel,
        out_shape=[shape((dim, tiles * tile), F32)] * 2,
        grid=(tiles,),
        in_specs=[full(n2), part, part],
        out_specs=[cols, cols],
        scratch_shapes=[pltpu.VMEM((dim, rows), BF16)],
        compiler_params=plain(),
        cost_estimate=pl.CostEstimate(flops=4 * rows * dim * tiles * tile, bytes_accessed=12 * dim * tiles * tile, transcendentals=0),
        name='gate_up_grads',
    )(n2, d1, d3)


def down_kernel(top_ref, act_ref, k_in_ref, v_in_ref, g2_ref, k_ref, v_ref):
    g2_ref[...] = dot_tn(act_ref[...], top_ref[...])
    k_ref[...] = k_in_ref[...]
    v_ref[...] = v_in_ref[...]


def down_grad(early, act, total):
    rows, dim = early.shape[0], early.shape[1] // 2
    tiles, _, tile = act.shape
    blocks = 1 << (tiles.bit_length() - 1)
    height = total.shape[0] // 2 // blocks
    block = lambda first: pl.BlockSpec((height, dim), lambda i: (jnp.minimum(i, blocks - 1) + first, 0))
    return pl.pallas_call(
        down_kernel,
        out_shape=[shape((tiles * tile, dim), F32)] + [shape((total.shape[0] // 2, dim), F32)] * 2,
        grid=(tiles,),
        in_specs=[pl.BlockSpec((rows, dim), lambda i: (0, 1), pipeline_mode=pl.Buffered(1)),
                  pl.BlockSpec((pl.Squeezed(), rows, tile), lambda i: (i, 0, 0)), block(0), block(blocks)],
        out_specs=[pl.BlockSpec((tile, dim), lambda i: (i, 0)), block(0), block(0)],
        compiler_params=plain(),
        cost_estimate=pl.CostEstimate(flops=2 * rows * dim * tiles * tile, bytes_accessed=12 * dim * tiles * tile, transcendentals=0),
        name='down_grad',
    )(early, act, total, total)


def memory_weight_kernel(memory_ref, dkv_ref, gk_ref, gv_ref):
    group, hd = dkv_ref.shape[0], dkv_ref.shape[2] // 2
    for i in range(group):
        both = dot_tn(dkv_ref[i], memory_ref[...])
        gk_ref[i * hd:(i + 1) * hd, :] = both[:hd]
        gv_ref[i * hd:(i + 1) * hd, :] = both[hd:]


def memory_weight_grads(memory, dkv):
    heads, rows, width = dkv.shape
    dim, hd = memory.shape[1], width // 2
    group = 4
    out = pl.BlockSpec((group * hd, dim), lambda i: (i, 0))
    return pl.pallas_call(
        memory_weight_kernel,
        out_shape=[shape((heads * hd, dim), F32)] * 2,
        grid=(heads // group,),
        in_specs=[full(memory), pl.BlockSpec((group, rows, width), lambda i: (i, 0, 0))],
        out_specs=[out, out],
        compiler_params=plain(),
        cost_estimate=pl.CostEstimate(flops=2 * rows * dim * heads * width, bytes_accessed=16 * rows * dim, transcendentals=0),
        name='memory_weight_grads',
    )(memory, dkv)


def memory_grad_kernel(dkv_ref, wk_ref, wv_ref, gq_in_ref, out_ref, gq_ref):
    group = dkv_ref.shape[0]
    gq_ref[...] = gq_in_ref[...]
    left = jnp.concatenate([dkv_ref[i] for i in range(group)], axis=1)
    right = jnp.concatenate([part[i] for i in range(group) for part in (wk_ref, wv_ref)], axis=0)

    @pl.when(pl.program_id(0) == 0)
    def _():
        out_ref[...] = dot(left, right)

    @pl.when(pl.program_id(0) > 0)
    def _():
        out_ref[...] += dot(left, right)


def memory_grad(dkv, wk_t, wv_t, gq):
    heads, rows, width = dkv.shape
    hd, dim = wk_t.shape[1], wk_t.shape[2]
    group = 4
    weight = pl.BlockSpec((group, hd, dim), lambda i: (i, 0, 0))
    passing = pl.BlockSpec((group * hd, dim), lambda i: (i, 0))
    return pl.pallas_call(
        memory_grad_kernel,
        out_shape=[shape((rows, dim), F32), shape(gq.shape, F32)],
        grid=(heads // group,),
        in_specs=[pl.BlockSpec((group, rows, width), lambda i: (i, 0, 0)), weight, weight, passing],
        out_specs=[pl.BlockSpec((rows, dim), lambda i: (0, 0)), passing],
        compiler_params=plain(),
        cost_estimate=pl.CostEstimate(flops=2 * rows * dim * heads * width, bytes_accessed=12 * rows * dim, transcendentals=0),
        name='memory_grad',
    )(dkv, wk_t, wv_t, gq)


def outer_kernel(att_ref, gh_ref, out_ref):
    @pl.when(pl.program_id(0) == 0)
    def _():
        out_ref[...] = jnp.zeros_like(out_ref)

    out_ref[...] += dot_tn(att_ref[...], gh_ref[...])


def outer_weight_grad(late, dim):
    rows = late.shape[0]
    chunk = min(512, rows)
    return pl.pallas_call(
        outer_kernel,
        out_shape=shape((dim, dim), F32),
        grid=(rows // chunk,),
        in_specs=[pl.BlockSpec((chunk, dim), lambda i: (i, 0)), pl.BlockSpec((chunk, dim), lambda i: (i, 1))],
        out_specs=pl.BlockSpec((dim, dim), lambda i: (0, 0)),
        compiler_params=plain(),
        cost_estimate=pl.CostEstimate(flops=2 * rows * dim * dim, bytes_accessed=8 * rows * dim, transcendentals=0),
        name='outer_weight_grad',
    )(late, late)


def solution(mesh):
    n = mesh.shape['seq']
    row_spec = P(('data', 'seq'), None)
    weight_spec = P()
    part_vec = P('data')
    part_mat = P('data', None)
    part_cube = P('data', None, None)

    def device_step(dec_in, memory, mem_len, grad_out, norm_attn, wq_cross, wk_cross, wv_cross, wo_cross, norm_mlp, w_gate, w_up, w_down):
        q_rows, dim = dec_in.shape
        heads, hd = wq_cross.shape[1], wq_cross.shape[2]
        parts = n // heads
        sources = -(-3 * n // 4)
        total_q = q_rows * n
        key_scale = hd ** -0.5
        scale = key_scale * LOG2E
        wq_t, wk_t, wv_t = (jnp.transpose(w, (1, 2, 0)) for w in (wq_cross, wk_cross, wv_cross))
        source_rows = -(-sources // (parts * math.isqrt(heads)))
        kv, q_in, early_local = exchange(n, heads, source_rows, 0, memory, dec_in, grad_out, norm_attn, wk_t, wv_t, wq_t)
        head_q = q_in.reshape(total_q, 2 * hd)

        early = lax.all_gather(early_local, 'seq', axis=0, tiled=True)

        wo = wo_cross.reshape(heads * hd, dim)
        mine = attention_forward(scale, hd, parts, sources, mem_len, kv, head_q)
        out_t, lse, do_in, factors, grad_hidden, g_norm_mlp = decoder_rows(
            n, heads, 1, mine, dec_in, grad_out, norm_mlp, wo, w_gate, w_up, w_down)
        do_in, factors = lax.optimization_barrier((do_in, factors))
        late = lax.all_gather(factors, 'seq', axis=0, tiled=True)

        dkv, dq_part = attention_backward(scale, key_scale, hd, parts, sources, mem_len, kv, head_q, do_in.reshape(total_q, 2 * hd), out_t, lse)
        dkv_in, dq_rows, gq_share = return_blocks(n, heads, source_rows, 4, dkv, dq_part, norm_attn, early)
        dkv_in, dq_rows, gq_share, late = lax.optimization_barrier((dkv_in, dq_rows, gq_share, late))
        g_wq = lax.all_gather(gq_share, 'seq', axis=0, tiled=True)

        gk_part, gv_part = memory_weight_grads(memory, dkv_in)
        sums, g_dec, norms, n2_all, d1, d3, act = reduce_sums(
            n, heads, 5, gk_part, gv_part, early, late, w_gate, w_up, w_down, wo, wq_t.reshape(heads * hd, dim), norm_attn, norm_mlp,
            dq_rows, dec_in, grad_hidden, g_norm_mlp)
        sums, n2_all, d1, d3, act, dkv_in, late, early, g_wq = lax.optimization_barrier(
            (sums, n2_all, d1, d3, act, dkv_in, late, early, g_wq))
        total = lax.all_gather(sums, 'seq', axis=0, tiled=True)
        g_wo = outer_weight_grad(late, dim)
        g_mem, g_wq = memory_grad(dkv_in, wk_t, wv_t, g_wq)
        g_gate, g_up = gate_up_grads(n2_all, d1, d3)
        g_down, g_wk, g_wv = down_grad(early, act, total)

        cube = lambda g: jnp.transpose(g.reshape(heads, hd, dim), (2, 0, 1))
        return (g_dec, g_mem, norms[0], cube(g_wq), cube(g_wk), cube(g_wv), g_wo.reshape(heads, hd, dim), norms[1], g_gate, g_up, g_down)

    return jax.shard_map(device_step, mesh=mesh,
                         in_specs=(row_spec, row_spec, part_vec, row_spec) + (weight_spec,) * 9,
                         out_specs=(row_spec, row_spec, part_vec, part_cube, part_cube, part_cube, part_cube, part_vec, part_mat, part_mat, part_mat),
                         check_vma=False)
```

```python
import functools
import math

import jax
import jax.numpy as jnp
from jax import lax
from jax.experimental import pallas as pl
from jax.experimental.pallas import tpu as pltpu
from jax.sharding import PartitionSpec as P

LOG2E = 1.4426950408889634
NEG = -1e30
VMEM_LIMIT = 60 * 1024 * 1024
MESH = pl.DeviceIdType.MESH
BF16, F32 = jnp.bfloat16, jnp.float32


def rms_norm(tensor, gain):
    mean_sq = jnp.mean(tensor * tensor, axis=-1, keepdims=True)
    return tensor * lax.rsqrt(mean_sq + 1e-6) * gain


def dot(a, b):
    return jnp.dot(a, b, preferred_element_type=F32)


def dot_nt(a, b):
    return lax.dot_general(a, b, (((1,), (1,)), ((), ())), preferred_element_type=F32)


def dot_tn(a, b):
    return lax.dot_general(a, b, (((0,), (0,)), ((), ())), preferred_element_type=F32)


def full(array):
    return pl.BlockSpec(array.shape, lambda *_: (0,) * array.ndim, pipeline_mode=pl.Buffered(1))


def vmem(count):
    return [pl.BlockSpec(memory_space=pltpu.VMEM)] * count


def plain():
    return pltpu.CompilerParams(vmem_limit_bytes=VMEM_LIMIT)


def remote(collective_id):
    return pltpu.CompilerParams(collective_id=collective_id, has_side_effects=True, vmem_limit_bytes=VMEM_LIMIT)


def shape(dims, dtype):
    return jax.ShapeDtypeStruct(dims, dtype)


def meet(peers):
    barrier = pltpu.get_barrier_semaphore()
    for peer in peers:
        pl.semaphore_signal(barrier, inc=1, device_id={'seq': peer}, device_id_type=MESH)
    pl.semaphore_wait(barrier, len(peers))


def send(src, dst, send_sem, recv_sem, peer):
    return pltpu.make_async_remote_copy(src_ref=src, dst_ref=dst, send_sem=send_sem, recv_sem=recv_sem,
                                        device_id={'seq': peer}, device_id_type=MESH)


class Grid:
    def __init__(self, n, heads, source_rows):
        self.n, self.heads, self.source_rows = n, heads, source_rows
        self.parts = n // heads
        self.side = math.isqrt(heads)
        self.me = lax.axis_index('seq')
        self.part = lax.rem(self.me, self.parts)
        self.chip = self.me // self.parts
        self.col = lax.rem(self.chip, self.side)
        self.row = self.chip // self.side
        self.partner = self.chip * self.parts + (self.parts - 1 - self.part)
        self.ties = self.side == 4
        self.direct = (1, 3) if self.ties else (1,)

    def wrap(self, value):
        return lax.rem(value + self.side, self.side)

    def device(self, row, col, part):
        return (row * self.side + col) * self.parts + part

    def near(self, drow, dcol, part=None):
        return self.device(self.wrap(self.row + drow), self.wrap(self.col + dcol), self.part if part is None else part)

    def hop(self, offset):
        return 1 if offset == 1 else -1

    def is_source(self, row):
        return self.wrap(row) < self.source_rows

    def row_peers(self):
        return [lax.rem(self.chip + step, self.heads) * self.parts + self.part for step in range(1, self.heads)]

    def peers(self):
        return self.row_peers() + [self.partner] + [self.near(0, self.hop(d), self.parts - 1 - self.part) for d in self.direct]


def pair_peers(n, heads, me, part):
    parts = n // heads
    head = me // parts
    partner = head * parts + (parts - 1 - part)
    return partner, [partner] + [lax.rem(head + step, heads) * parts + part for step in range(1, heads)]


def pack(rows):
    middle = rows.shape[-2] // 2
    return jnp.concatenate([rows[..., :middle, :], rows[..., middle:, :]], axis=-1)


def unpack(packed):
    middle = packed.shape[-1] // 2
    return jnp.concatenate([packed[..., :middle], packed[..., middle:]], axis=-2)


def start_rows(n, heads, me, part, src, src_of, dst_ref, send_sem, recv_sem):
    parts = n // heads
    head = me // parts
    for step in range(1, heads):
        peer = lax.rem(head + step, heads) * parts + part
        send(src.at[src_of(peer)], dst_ref.at[head], send_sem, recv_sem, peer).start()
    dst_ref[head] = src[src_of(me)]


def wait_rows(heads, me, dst_ref, send_sem, recv_sem):
    others = dst_ref.at[pl.ds(0, heads - 1)]
    whole = send(others, others, send_sem, recv_sem, me)
    whole.wait_send()
    whole.wait_recv()


def swap(src, dst, send_sem, recv_sem, partner):
    copy = send(src, dst, send_sem, recv_sem, partner)
    copy.start()
    copy.wait()


def place(n, heads, part, mine_ref, theirs_ref, wide_ref, low):
    parts = n // heads
    for source, index in ((mine_ref, part), (theirs_ref, parts - 1 - part)):
        for head in range(heads):
            rows = unpack(source[head])
            zeros = jnp.zeros_like(rows)
            wide_ref[head * parts + index] = jnp.concatenate([rows, zeros] if low else [zeros, rows], axis=-1)


def exchange_kernel(n, heads, source_rows, memory_ref, dec_ref, gout_ref, gain_ref, wk_ref, wv_ref, wq_ref, kv_out_ref, q_out_ref, early_ref,
                    kv_ref, stage_ref, up_ref, down_ref, right_ref, left_ref, packed_ref, got_ref, swapped_ref,
                    row_send, row_recv, y_send, pass_send, x_send, fwd_send, stage_recv, up_recv, down_recv, right_recv,
                    left_recv, out_recv):
    g = Grid(n, heads, source_rows)
    side, hd = g.side, wk_ref.shape[1]
    half = kv_out_ref.shape[1]
    chunk_rows = min(256, kv_ref.shape[1])
    barrier = pltpu.get_barrier_semaphore()
    peers = g.peers()
    for peer in peers:
        pl.semaphore_signal(barrier, inc=1, device_id={'seq': peer}, device_id_type=MESH)

    dim = dec_ref.shape[1]
    early_ref[:, :dim] = dec_ref[...]
    early_ref[:, dim:] = gout_ref[...].astype(BF16)
    normed = rms_norm(dec_ref[...].astype(F32), gain_ref[...].astype(F32)).astype(BF16)

    def some_heads(index, carry):
        queries = dot_nt(normed, jnp.concatenate([wq_ref[4 * index + j] for j in range(4)], axis=0)).astype(BF16)
        for j in range(4):
            packed_ref[4 * index + j] = pack(queries[:, hd * j:hd * (j + 1)])
        return carry

    lax.fori_loop(0, heads // 4, some_heads, 0)

    def head(drow, dcol):
        return g.wrap(g.row + drow) * side + g.wrap(g.col + dcol)

    def project(drow, dcols):
        weights = jnp.concatenate([ref[head(drow, d)] for d in dcols for ref in (wk_ref, wv_ref)], axis=0)

        def rows(index, carry):
            at = pl.ds(pl.multiple_of(index * chunk_rows, chunk_rows), chunk_rows)
            both = dot_nt(memory_ref[at, :], weights).astype(BF16)
            for i, d in enumerate(dcols):
                kv_ref[head(drow, d), at, :] = both[:, 2 * hd * i:2 * hd * (i + 1)]
            return carry

        lax.fori_loop(0, kv_ref.shape[1] // chunk_rows, rows, 0)

    def along_column(drow, dcol):
        chunk = kv_ref.at[head(drow, dcol)]
        if drow in g.direct:
            send(chunk, stage_ref.at[drow - 1, dcol], y_send.at[drow - 1], stage_recv.at[drow - 1, dcol], g.near(g.hop(drow), 0)).start()
        elif dcol % 2 == 0:
            send(chunk, up_ref.at[dcol // 2], y_send.at[drow - 1], up_recv.at[dcol // 2], g.near(1, 0)).start()
        else:
            send(chunk, down_ref.at[dcol // 2], y_send.at[drow - 1], down_recv.at[dcol // 2], g.near(-1, 0)).start()

    def along_row(o, dcol):
        chunk = kv_ref.at[head(0, dcol)] if o == 0 else stage_ref.at[o - 1, dcol]
        source = g.device(g.wrap(g.row - o), g.col, g.part)
        if dcol == 0:
            kv_out_ref[source] = chunk[pl.ds(pl.multiple_of(g.part * half, half), half), :]
            away = pl.ds(pl.multiple_of((g.parts - 1 - g.part) * half, half), half)
            send(chunk.at[away], kv_out_ref.at[source], x_send.at[o], out_recv, g.partner).start()
        elif dcol in g.direct:
            for part in range(g.parts):
                send(chunk.at[pl.ds(part * half, half)], kv_out_ref.at[source], x_send.at[o], out_recv,
                     g.near(0, g.hop(dcol), part)).start()
        else:
            send(chunk.at[pl.ds(0, half)], right_ref.at[o], x_send.at[o], right_recv.at[o], g.near(0, 1)).start()
            send(chunk.at[pl.ds(half, half)], left_ref.at[o], x_send.at[o], left_recv.at[o], g.near(0, -1)).start()

    def pass_row(o):
        for ref, sem, come in ((right_ref, right_recv, -1), (left_ref, left_recv, 1)):
            source = g.device(g.wrap(g.row - o), g.wrap(g.col + come), g.part)
            send(ref.at[o], ref.at[o], fwd_send.at[o], sem.at[o], g.me).wait_recv()
            send(ref.at[o], kv_out_ref.at[source], fwd_send.at[o], out_recv, g.near(0, -come, 0 if come < 0 else 1)).start()

    def when_source(row, body):
        pl.when(g.is_source(row))(body)

    if g.ties:
        order = [(2, (2, 1)), (2, (3, 0)), (1, (2, 1)), (3, (2, 3)), (0, (2, 1)), (0, (3, 0))]
        last = [(1, (3, 0)), (3, (1, 0))]
    else:
        order, last = [(1, (1, 0)), (0, (1, 0))], []

    def issue(drow, dcols):
        def body():
            for d in dcols:
                along_row(0, d) if drow == 0 else along_column(drow, d)
        when_source(g.row, body)

    waiting = None
    for drow, dcols in order + last:
        project(drow, dcols)
        if waiting is None:
            pl.semaphore_wait(barrier, len(peers))
            start_rows(n, heads, g.me, g.part, packed_ref, lambda peer: peer // g.parts, got_ref, row_send.at[0], row_recv.at[0])
        elif waiting not in last:
            issue(*waiting)
        waiting = (drow, dcols)
    if not last:
        issue(*waiting)

    if g.ties:
        def up(i):
            send(up_ref.at[i], up_ref.at[i], pass_send.at[0], up_recv.at[i], g.me).wait_recv()
            send(up_ref.at[i], stage_ref.at[1, 2 * i], pass_send.at[0], stage_recv.at[1, 2 * i], g.near(1, 0)).start()

        def down(i):
            send(down_ref.at[i], down_ref.at[i], pass_send.at[1], down_recv.at[i], g.me).wait_recv()
            send(down_ref.at[i], stage_ref.at[1, 2 * i + 1], pass_send.at[1], stage_recv.at[1, 2 * i + 1], g.near(-1, 0)).start()

        for i in range(2):
            when_source(g.row - 1, lambda i=i: up(1 - i))
            when_source(g.row + 1, lambda i=i: down(i))
        for drow, dcols in last:
            issue(drow, dcols)
        when_source(g.row, lambda: pass_row(0))

    wait_rows(heads, g.me, got_ref, row_send.at[0], row_recv.at[0])
    swap(got_ref, swapped_ref, row_send.at[1], row_recv.at[1], g.partner)
    place(n, heads, g.part, got_ref, swapped_ref, q_out_ref, True)

    def arrived(o, dcol):
        def body():
            send(stage_ref.at[o - 1, dcol], stage_ref.at[o - 1, dcol], y_send.at[0], stage_recv.at[o - 1, dcol], g.me).wait_recv()
            along_row(o, dcol)
        when_source(g.row - o, body)

    if g.ties:
        for o, d in ((1, 2), (3, 2), (1, 1), (3, 3)):
            arrived(o, d)
        for o in g.direct:
            when_source(g.row - o, lambda o=o: pass_row(o))
        for d in (2, 1, 0, 3):
            arrived(2, d)
        when_source(g.row - 2, lambda: pass_row(2))
        for o, d in ((1, 3), (3, 1), (1, 0), (3, 0)):
            arrived(o, d)
    else:
        for d in (1, 0):
            arrived(1, d)

    def sent(sem, ref):
        send(ref, ref, sem, out_recv, g.me).wait_send()

    def mine():
        for drow in range(1, side):
            sent(y_send.at[drow - 1], stage_ref.at[0])
    when_source(g.row, mine)
    for o in range(side):
        def passed(o=o):
            sent(x_send.at[o], kv_out_ref.at[pl.ds(0, g.parts * side - 1)])
            if g.ties:
                sent(fwd_send.at[o], kv_out_ref.at[pl.ds(0, 2)])
        when_source(g.row - o, passed)
    if g.ties:
        when_source(g.row - 1, lambda: sent(pass_send.at[0], up_ref))
        when_source(g.row + 1, lambda: sent(pass_send.at[1], down_ref))
    blocks = source_rows * side * g.parts
    others = kv_out_ref.at[pl.ds(0, blocks - source_rows)]
    send(others, others, y_send.at[0], out_recv, g.me).wait_recv()


def row_scratch(heads, q_rows, hd):
    return [pltpu.VMEM((heads, q_rows // 2, 2 * hd), BF16)] * 3


def dma(*dims):
    return pltpu.SemaphoreType.DMA(dims)


def exchange(n, heads, source_rows, collective_id, memory, dec_in, grad_out, gain, wk_t, wv_t, wq_t):
    m_rows, q_rows, hd = memory.shape[0], dec_in.shape[0], wk_t.shape[1]
    side, parts = math.isqrt(heads), n // heads
    half = m_rows // parts
    chunk = lambda *lead: pltpu.VMEM(lead + (m_rows, 2 * hd), BF16)
    block = lambda *lead: pltpu.VMEM(lead + (half, 2 * hd), BF16)
    return pl.pallas_call(
        functools.partial(exchange_kernel, n, heads, source_rows),
        out_shape=[shape((n, half, 2 * hd), BF16), shape((n, q_rows, 2 * hd), BF16), shape((q_rows, 2 * dec_in.shape[1]), BF16)],
        in_specs=vmem(7),
        out_specs=vmem(3),
        scratch_shapes=[chunk(heads), chunk(side - 1, side), chunk(2), chunk(2), block(side), block(side)]
        + row_scratch(heads, q_rows, hd)
        + [dma(2), dma(2), dma(side - 1), dma(2), dma(side), dma(side), dma(side - 1, side), dma(2), dma(2), dma(side), dma(side),
           pltpu.SemaphoreType.DMA],
        compiler_params=remote(collective_id),
        name='exchange',
    )(memory, dec_in, grad_out, gain, wk_t, wv_t, wq_t)


def return_kernel(n, heads, source_rows, chunk, src_ref, dq_ref, gain_ref, early_hbm, dst_ref, rows_ref, gq_ref, stage_ref, right_ref,
                  left_ref, up_ref, down_ref, theirs_ref, packed_ref, got_ref, dqt_ref, decs_ref, dec_sem, row_send, row_recv,
                  x_send, fwd_send, y_send, pass_send, stage_recv, right_recv, left_recv, up_recv, down_recv, out_recv):
    g = Grid(n, heads, source_rows)
    side = g.side
    half = src_ref.shape[1]
    total_rows, dim = dqt_ref.shape[1], gq_ref.shape[1]

    def dec_load(index, slot):
        at = pl.ds(pl.multiple_of(index * chunk, chunk), chunk)
        return pltpu.make_async_copy(early_hbm.at[at, pl.ds(0, dim)], decs_ref.at[slot], dec_sem.at[slot])

    dec_load(0, 0).start()
    meet(g.peers())
    mine = pl.ds(pl.multiple_of(g.part * half, half), half)

    def landing(drow, dcol, head_col):
        if drow == 0:
            return dst_ref.at[g.row * side + head_col, mine], out_recv
        return stage_ref.at[drow - 1, dcol, mine], stage_recv.at[drow - 1, dcol]

    def along_row(drow, dcol):
        row = g.wrap(g.row + drow)
        col = g.wrap(g.col + dcol)
        for part in range(g.parts):
            source = src_ref.at[g.device(row, col, part)]
            if dcol in g.direct:
                dst, sem = landing(drow, dcol, g.col)
                send(source, dst, x_send.at[drow], sem, g.near(0, g.hop(dcol), part)).start()
            elif part == 0:
                send(source, right_ref.at[drow], x_send.at[drow], right_recv.at[drow], g.near(0, 1)).start()
            else:
                send(source, left_ref.at[drow], x_send.at[drow], left_recv.at[drow], g.near(0, -1)).start()

    def own_chip(drow):
        row = g.wrap(g.row + drow)
        away = src_ref.at[g.device(row, g.col, g.parts - 1 - g.part)]
        dst, sem = landing(drow, 0, g.col)
        dst[...] = src_ref[g.device(row, g.col, g.part)]
        send(away, dst, x_send.at[drow], sem, g.partner).start()

    def pass_row(drow):
        for ref, come_sem, come in ((right_ref, right_recv, -1), (left_ref, left_recv, 1)):
            send(ref.at[drow], ref.at[drow], fwd_send.at[drow], come_sem.at[drow], g.me).wait_recv()
            dst, sem = landing(drow, 2, g.wrap(g.col + come))
            send(ref.at[drow], dst, fwd_send.at[drow], sem, g.near(0, -come, 0 if come < 0 else 1)).start()

    def along_column(drow, dcol):
        chunk = stage_ref.at[drow - 1, dcol]
        got = chunk.at[pl.ds(0, half)] if dcol == 0 else chunk
        send(got, got, y_send.at[drow - 1], stage_recv.at[drow - 1, dcol], g.me).wait_recv()
        head = g.row * side + g.wrap(g.col - dcol)
        if drow in g.direct:
            send(chunk, dst_ref.at[head], y_send.at[drow - 1], out_recv, g.near(g.hop(drow), 0)).start()
        elif dcol % 2 == 0:
            send(chunk, up_ref.at[dcol // 2], y_send.at[drow - 1], up_recv.at[dcol // 2], g.near(1, 0)).start()
        else:
            send(chunk, down_ref.at[dcol // 2], y_send.at[drow - 1], down_recv.at[dcol // 2], g.near(-1, 0)).start()

    def when_source(row, body):
        pl.when(g.is_source(row))(body)

    def rows_of(drow):
        def body():
            for d in (2, 1, 3) if g.ties else (1,):
                along_row(drow, d)
        when_source(g.row + drow, body)

    def relay(drow):
        when_source(g.row + drow, lambda: pass_row(drow))

    def column(drow, d):
        when_source(g.row + drow, lambda: along_column(drow, d))

    def up(i):
        def body():
            send(up_ref.at[i], up_ref.at[i], pass_send.at[0], up_recv.at[i], g.me).wait_recv()
            head = g.wrap(g.row - 1) * side + g.wrap(g.col - 2 * i)
            send(up_ref.at[i], dst_ref.at[head], pass_send.at[0], out_recv, g.near(1, 0)).start()
        when_source(g.row + 1, body)

    def down(i):
        def body():
            send(down_ref.at[i], down_ref.at[i], pass_send.at[1], down_recv.at[i], g.me).wait_recv()
            head = g.wrap(g.row + 1) * side + g.wrap(g.col - 2 * i - 1)
            send(down_ref.at[i], dst_ref.at[head], pass_send.at[1], out_recv, g.near(-1, 0)).start()
        when_source(g.row - 1, body)

    def start_dq():
        swap(dq_ref, theirs_ref, row_send.at[0], row_recv.at[0], g.partner)
        both = (dq_ref[...] + theirs_ref[...]).astype(BF16)
        share = dqt_ref.shape[0]
        dqt_ref[...] = jnp.where(g.part == 0, both[:share], both[share:])
        total = both.T
        packed_ref[...] = pack(total.reshape(n, total.shape[0] // n, total.shape[1]))
        start_rows(n, heads, g.me, g.part, packed_ref, lambda peer: peer, got_ref, row_send.at[1], row_recv.at[1])

    def query_weight(index, carry):
        slot = lax.rem(index, 2)
        dec_load(index, slot).wait()

        @pl.when(index + 1 < chunks)
        def _():
            dec_load(index + 1, 1 - slot).start()

        normed = rms_norm(decs_ref[slot].astype(F32), gain_ref[...].astype(F32)).astype(BF16)
        gq_ref[...] += dot(dqt_ref[:, pl.ds(pl.multiple_of(index * chunk, chunk), chunk)], normed)
        return carry

    chunks = total_rows // chunk
    for drow in (2, 1, 3, 0) if g.ties else (1, 0):
        when_source(g.row + drow, lambda drow=drow: own_chip(drow))
    if g.ties:
        rows_of(2)
        for drow in (2, 1, 3):
            column(drow, 0)
        relay(2)
        rows_of(1)
        column(2, 1)
        column(2, 3)
        column(2, 2)
        relay(1)
        rows_of(3)
        start_dq()
        up(0)
        down(0)
        column(1, 1)
        column(1, 3)
        column(1, 2)
        relay(3)
        rows_of(0)
        up(1)
        down(1)
        column(3, 1)
        column(3, 3)
        column(3, 2)
        relay(0)
    else:
        rows_of(1)
        rows_of(0)
        start_dq()
        column(1, 0)
        column(1, 1)
    gq_ref[...] = jnp.zeros_like(gq_ref)
    lax.fori_loop(0, chunks, query_weight, 0)
    wait_rows(heads, g.me, got_ref, row_send.at[1], row_recv.at[1])
    rows_ref[...] = unpack(got_ref[...])

    def sent(sem, ref):
        send(ref, ref, sem, out_recv, g.me).wait_send()

    for drow in range(side):
        def done(drow=drow):
            sent(x_send.at[drow], src_ref.at[pl.ds(0, g.parts * side - 1)])
            if g.ties:
                sent(fwd_send.at[drow], src_ref.at[pl.ds(0, 2)])
            if drow:
                sent(y_send.at[drow - 1], stage_ref.at[0])
        when_source(g.row + drow, done)
    if g.ties:
        when_source(g.row + 1, lambda: sent(pass_send.at[0], up_ref))
        when_source(g.row - 1, lambda: sent(pass_send.at[1], down_ref))

    @pl.when(g.is_source(g.row))
    def _():
        blocks = src_ref.at[pl.ds(0, n - 1)]
        send(blocks, blocks, y_send.at[0], out_recv, g.me).wait_recv()

    @pl.when(jnp.logical_not(g.is_source(g.row)))
    def _():
        def clear(index, carry):
            dst_ref[index] = jnp.zeros(dst_ref.shape[1:], dst_ref.dtype)
            return carry
        lax.fori_loop(0, heads, clear, 0)


def return_blocks(n, heads, source_rows, collective_id, blocks, dq, gain, early):
    half, width = blocks.shape[1], blocks.shape[2]
    hd, total_q = dq.shape
    q_rows = total_q // n
    side, parts = math.isqrt(heads), n // heads
    chunk = lambda *lead: pltpu.VMEM(lead + (half * parts, width), BF16)
    block = lambda *lead: pltpu.VMEM(lead + (half, width), BF16)
    piece, dim = min(512, total_q), early.shape[1] // 2
    return pl.pallas_call(
        functools.partial(return_kernel, n, heads, source_rows, piece),
        out_shape=[shape((heads, half * parts, width), BF16), shape((heads, q_rows, hd), BF16), shape((hd // parts, dim), F32)],
        in_specs=vmem(3) + [pl.BlockSpec(memory_space=pl.ANY)],
        out_specs=vmem(3),
        scratch_shapes=[chunk(side - 1, side), block(side), block(side), chunk(2), chunk(2), pltpu.VMEM(dq.shape, F32),
                        pltpu.VMEM((n, q_rows // 2, 2 * hd), BF16), pltpu.VMEM((heads, q_rows // 2, 2 * hd), BF16),
                        pltpu.VMEM((hd // parts, total_q), BF16), pltpu.VMEM((2, piece, dim), BF16), dma(2), dma(2), dma(2),
                        dma(side), dma(side), dma(side - 1), dma(2), dma(side - 1, side), dma(side), dma(side), dma(2), dma(2),
                        pltpu.SemaphoreType.DMA],
        compiler_params=remote(collective_id),
        name='return_blocks',
    )(blocks, dq, gain, early)


def decoder_kernel(n, heads, mine_ref, dec_ref, gout_ref, gain_ref, wo_hbm, wg_hbm, wu_hbm, wd_hbm,
                   out_ref, lse_ref, do_ref, factors_ref, gh_ref, gnorm_ref,
                   theirs_ref, packed_ref, got_ref, sent_ref, back_ref, swapped_ref, wo_ref, wg_ref, wu_ref, wd_ref, gact_ref,
                   load_sem, send_sem, recv_sem):
    me = lax.axis_index('seq')
    part = lax.rem(me, n // heads)
    partner, peers = pair_peers(n, heads, me, part)
    q_rows, dim = dec_ref.shape
    hd = out_ref.shape[0]
    loads = [pltpu.make_async_copy(src, dst, load_sem.at[i]) for i, (src, dst) in enumerate(
        ((wd_hbm, wd_ref), (wo_hbm, wo_ref), (wg_hbm, wg_ref), (wu_hbm, wu_ref)))]
    for load in loads:
        load.start()
    meet(peers)

    swap(mine_ref, theirs_ref, send_sem.at[0], recv_sem.at[0], partner)
    m_a, m_b = mine_ref[hd + 8:hd + 9], theirs_ref[hd + 8:hd + 9]
    top = jnp.maximum(m_a, m_b)
    s_a, s_b = jnp.exp2(m_a - top), jnp.exp2(m_b - top)
    den = mine_ref[hd:hd + 1] * s_a + theirs_ref[hd:hd + 1] * s_b
    out = (mine_ref[:hd] * s_a + theirs_ref[:hd] * s_b) / den
    packed_ref[...] = pack(out.T.astype(BF16).reshape(n, q_rows, hd))
    start_rows(n, heads, me, part, packed_ref, lambda peer: peer, got_ref, send_sem.at[1], recv_sem.at[1])
    out_ref[...] = out
    lse_ref[...] = top + jnp.log2(den)

    loads[0].wait()
    top_rows = gout_ref[...].astype(BF16)
    tile = 256

    def act_tile(index, carry):
        at = pl.ds(pl.multiple_of(index * tile, tile), tile)
        gact_ref[:, at] = dot_nt(top_rows, wd_ref[at, :])
        return carry

    lax.fori_loop(0, wd_ref.shape[0] // tile, act_tile, 0)
    wait_rows(heads, me, got_ref, send_sem.at[1], recv_sem.at[1])

    attended = jnp.concatenate([unpack(got_ref[h]) for h in range(heads)], axis=1)
    loads[1].wait()
    hidden = (dec_ref[...].astype(F32) + dot(attended, wo_ref[...])).astype(BF16).astype(F32)
    gain = gain_ref[...].astype(F32)
    inverse = lax.rsqrt(jnp.mean(hidden * hidden, axis=-1, keepdims=True) + 1e-6)
    scaled = hidden * inverse
    normed = (scaled * gain).astype(BF16)
    loads[2].wait()
    gate = dot(normed, wg_ref[...])
    loads[3].wait()
    up = dot(normed, wu_ref[...])
    sig = jax.nn.sigmoid(gate)
    silu = gate * sig
    grad_act = gact_ref[...]
    grad_gate = (grad_act * up * (sig + silu * (1.0 - sig))).astype(BF16)
    grad_up = (grad_act * silu).astype(BF16)
    grad_normed = (dot_nt(wg_ref[...], grad_gate) + dot_nt(wu_ref[...], grad_up)).T
    gnorm_ref[...] = jnp.sum(grad_normed * scaled, axis=0, keepdims=True)
    inner = grad_normed * gain
    grad_hidden = gout_ref[...] + inverse * (inner - scaled * jnp.mean(inner * scaled, axis=-1, keepdims=True))
    rounded = grad_hidden.astype(BF16)
    grad_att = dot_nt(wo_ref[...], rounded).T.astype(BF16)
    for h in range(heads):
        sent_ref[h] = pack(grad_att[:, hd * h:hd * (h + 1)])
    factors_ref[:, :dim] = attended
    factors_ref[:, dim:] = rounded
    gh_ref[...] = grad_hidden

    start_rows(n, heads, me, part, sent_ref, lambda peer: peer // (n // heads), back_ref, send_sem.at[2], recv_sem.at[2])
    wait_rows(heads, me, back_ref, send_sem.at[2], recv_sem.at[2])
    swap(back_ref, swapped_ref, send_sem.at[3], recv_sem.at[3], partner)
    place(n, heads, part, back_ref, swapped_ref, do_ref, False)


def decoder_rows(n, heads, collective_id, mine, dec_in, grad_out, gain, wo, w_gate, w_up, w_down):
    q_rows, dim = dec_in.shape
    hd, total_q = wo.shape[0] // heads, mine.shape[1]
    hbm = pl.BlockSpec(memory_space=pl.ANY)
    return pl.pallas_call(
        functools.partial(decoder_kernel, n, heads),
        out_shape=[shape((hd, total_q), F32), shape((1, total_q), F32), shape((n, q_rows, 2 * hd), BF16),
                   shape((q_rows, 2 * dim), BF16), shape((q_rows, dim), F32), shape((1, dim), F32)],
        in_specs=vmem(4) + [hbm] * 4,
        out_specs=vmem(6),
        scratch_shapes=[pltpu.VMEM(mine.shape, F32), pltpu.VMEM((n, q_rows // 2, 2 * hd), BF16)]
        + [pltpu.VMEM((heads, q_rows // 2, 2 * hd), BF16)] * 4
        + [pltpu.VMEM(w.shape, BF16) for w in (wo, w_gate, w_up, w_down)] + [pltpu.VMEM((q_rows, w_down.shape[0]), F32), dma(4), dma(4), dma(4)],
        compiler_params=remote(collective_id),
        name='decoder_rows',
    )(mine, dec_in, grad_out, gain, wo, w_gate, w_up, w_down)


def valid_blocks(mem_len, rows, parts, sources):
    reach = mem_len - lax.rem(lax.axis_index('seq'), parts) * rows
    blocks = jnp.minimum((reach + parts * rows - 1) // (parts * rows), sources)
    return blocks, jnp.minimum(reach - (blocks - 1) * parts * rows, rows)


def forward_kernel(scale, hd, parts, q_block, len_ref, kv_ref, q_ref, out_ref, qt_ref, top_ref):
    rows, total_q = kv_ref.shape[1], q_ref.shape[0]
    blocks, last_valid = valid_blocks(len_ref[0], rows, parts, kv_ref.shape[0])
    groups = [slice(first, first + q_block) for first in range(0, total_q, q_block)]
    base = slice(hd + 8, hd + 9)
    qt_ref[...] = q_ref[...].T

    def values_of(keys):
        return jnp.concatenate([keys.T[hd:], jnp.ones((16, rows), keys.dtype)], axis=0)

    def group_of(index):
        return pl.ds(pl.multiple_of(index * q_block, q_block), q_block)

    def first_step(group, carry):
        cols = group_of(group)
        top = jnp.max(dot(kv_ref[0], qt_ref[:, cols]), axis=0, keepdims=True)
        out_ref[hd + 8:, cols] = jnp.broadcast_to(top * scale, (8, q_block))
        top_ref[:, cols] = jnp.broadcast_to(top, (8, q_block))
        return carry

    lax.fori_loop(0, len(groups), first_step, 0)
    out_ref[:hd + 8, :] = jnp.zeros((hd + 8, total_q), F32)

    def finish(values, scores, cols):
        top_ref[:, cols] = jnp.maximum(top_ref[:, cols], jnp.max(scores.reshape(rows // 8, 8, q_block), axis=0))
        weights = jnp.exp2(scores * scale - out_ref[base, cols]).astype(values.dtype)
        out_ref[:hd + 8, cols] += dot(values, weights)[:hd + 8]

    def step(index, carry):
        keys = kv_ref[index]
        values = values_of(keys)
        for cols in groups:
            finish(values, dot(keys, qt_ref[:, cols]), cols)
        return carry

    def last_step(group, carry):
        cols = group_of(group)
        keys = kv_ref[blocks - 1]
        scores = dot(keys, qt_ref[:, cols])
        position = lax.broadcasted_iota(jnp.int32, scores.shape, 0)
        finish(values_of(keys), jnp.where(position < last_valid, scores, NEG), cols)
        return carry

    lax.fori_loop(0, blocks - 1, step, 0)
    lax.fori_loop(0, len(groups), last_step, 0)

    excess = jnp.max(top_ref[...] * scale - out_ref[hd + 8:, :])
    broken = jnp.max(jnp.where(jnp.abs(out_ref[:hd + 8, :]) <= 3e38, 0.0, 1.0))

    @pl.when(jnp.logical_or(jnp.logical_not(excess <= 64.0), broken > 0.0))
    def _():
        out_ref[:hd + 8, :] = jnp.zeros((hd + 8, total_q), F32)
        out_ref[hd + 8:, :] = jnp.full((8, total_q), NEG, F32)

        def running(step_index, carry):
            index, group = step_index // len(groups), lax.rem(step_index, len(groups))
            cols = group_of(group)
            keys = kv_ref[index]
            limit = jnp.where(index == blocks - 1, last_valid, rows)
            scores = dot(keys, qt_ref[:, cols]) * scale
            position = lax.broadcasted_iota(jnp.int32, scores.shape, 0)
            scores = jnp.where(position < limit, scores, NEG)
            old = out_ref[base, cols]
            new = jnp.maximum(old, jnp.max(scores, axis=0, keepdims=True))
            weights = jnp.exp2(scores - new).astype(keys.dtype)
            out_ref[:hd + 8, cols] = out_ref[:hd + 8, cols] * jnp.exp2(old - new) + dot(values_of(keys), weights)[:hd + 8]
            out_ref[hd + 8:, cols] = jnp.broadcast_to(new, (8, q_block))
            return carry

        lax.fori_loop(0, blocks * len(groups), running, 0)


def attention_forward(scale, hd, parts, sources, mem_len, kv, q):
    rows, width = kv.shape[1], kv.shape[2]
    total_q = q.shape[0]
    return pl.pallas_call(
        functools.partial(forward_kernel, scale, hd, parts, min(1024, total_q)),
        out_shape=shape((hd + 16, total_q), F32),
        grid=(1,),
        in_specs=[pl.BlockSpec(memory_space=pltpu.SMEM),
                  pl.BlockSpec((sources, rows, width), lambda i: (0, 0, 0), pipeline_mode=pl.Buffered(1)), full(q)],
        out_specs=pl.BlockSpec((hd + 16, total_q), lambda i: (0, 0)),
        scratch_shapes=[pltpu.VMEM((width, total_q), BF16), pltpu.VMEM((8, total_q), F32)],
        compiler_params=plain(),
        cost_estimate=pl.CostEstimate(flops=4 * total_q * sources * rows * hd, bytes_accessed=kv.size * 2,
                                      transcendentals=total_q * sources * rows),
        name='attention_forward',
    )(mem_len, kv, q)


def backward_kernel(scale, key_scale, hd, parts, q_block, len_ref, kv_ref, q_ref, do_ref, out_ref, lse_ref, dkv_ref, dq_ref,
                    qt_ref, dot_ref, delta_ref):
    rows, total_q = kv_ref.shape[1], q_ref.shape[0]
    blocks, last_valid = valid_blocks(len_ref[0], rows, parts, kv_ref.shape[0])
    width = kv_ref.shape[2]
    groups = [slice(first, first + q_block) for first in range(0, total_q, q_block)]
    dq_ref[...] = jnp.zeros_like(dq_ref)
    qt_ref[...] = q_ref[...].T
    do_t = do_ref[...].T
    dot_ref[...] = do_t
    delta_ref[...] = jnp.sum(do_t[hd:].astype(F32) * out_ref[...], axis=0, keepdims=True)

    lane_scale = jnp.where(lax.broadcasted_iota(jnp.int32, (1, width), 1) < hd, key_scale, 1.0)

    def products(keys, cols):
        return dot(keys, qt_ref[:, cols]), dot(keys, dot_ref[:, cols])

    def finish(keys, keys_t, scores, grads, cols, valid):
        prob = jnp.exp2(scores * scale - lse_ref[:, cols])
        if valid is not None:
            position = lax.broadcasted_iota(jnp.int32, scores.shape, 0)
            prob = jnp.where(position < valid, prob, 0.0)
        grad_scores = (prob * (grads - delta_ref[:, cols])).astype(keys.dtype)
        update = dot(grad_scores, q_ref[cols, :]) + dot(prob.astype(keys.dtype), do_ref[cols, :])
        dq_ref[:, cols] += dot(keys_t, grad_scores)
        return update

    def step(index, carry):
        keys = kv_ref[index]
        keys_t = keys.T[:hd]
        total = jnp.zeros((rows, width), F32)
        for cols in groups:
            scores, grads = products(keys, cols)
            total += finish(keys, keys_t, scores, grads, cols, None)
        dkv_ref[index] = (total * lane_scale).astype(dkv_ref.dtype)
        return carry

    def last_step(group, total):
        keys = kv_ref[blocks - 1]
        cols = pl.ds(pl.multiple_of(group * q_block, q_block), q_block)
        scores, grads = products(keys, cols)
        return total + finish(keys, keys.T[:hd], scores, grads, cols, last_valid)

    def clear(index, carry):
        dkv_ref[index] = jnp.zeros((rows, width), dkv_ref.dtype)
        return carry

    lax.fori_loop(0, blocks - 1, step, 0)
    total = lax.fori_loop(0, len(groups), last_step, jnp.zeros((rows, width), F32))
    dkv_ref[blocks - 1] = (total * lane_scale).astype(dkv_ref.dtype)
    lax.fori_loop(blocks, dkv_ref.shape[0], clear, 0)
    dq_ref[...] = dq_ref[...] * key_scale


def attention_backward(scale, key_scale, hd, parts, sources, mem_len, kv, q, do, out_t, lse):
    n, rows, width = kv.shape
    total_q = q.shape[0]
    return pl.pallas_call(
        functools.partial(backward_kernel, scale, key_scale, hd, parts, min(512, total_q)),
        out_shape=[shape((n, rows, width), BF16), shape((hd, total_q), F32)],
        grid=(1,),
        in_specs=[pl.BlockSpec(memory_space=pltpu.SMEM),
                  pl.BlockSpec((sources, rows, width), lambda i: (0, 0, 0), pipeline_mode=pl.Buffered(1)),
                  full(q), full(do), full(out_t), full(lse)],
        out_specs=[pl.BlockSpec((n, rows, width), lambda i: (0, 0, 0)),
                   pl.BlockSpec((hd, total_q), lambda i: (0, 0))],
        scratch_shapes=[pltpu.VMEM((width, total_q), BF16), pltpu.VMEM((width, total_q), BF16), pltpu.VMEM((1, total_q), F32)],
        compiler_params=plain(),
        cost_estimate=pl.CostEstimate(flops=10 * total_q * sources * rows * hd, bytes_accessed=kv.size * 4,
                                      transcendentals=total_q * sources * rows),
        name='attention_backward',
    )(mem_len, kv, q, do, out_t, lse)


def reduce_kernel(n, heads, tile, chunk, gk_hbm, gv_hbm, early_hbm, late_hbm, w1_hbm, w3_hbm, w2_hbm, wo_ref, wq_ref, gain1_ref,
                  gain2_ref, dqr_ref, dec_ref, gh_ref, gnorm_ref,
                  sums_ref, gdec_ref, norms_ref, n2_hbm, d1_hbm, d3_hbm, act_hbm,
                  acc_ref, pair_ref, far_ref, near_ref, n2_ref, top_ref, att_ref, decs_ref, w1_ref, w3_ref, w2_ref, w2t_ref, made_ref,
                  d1_ref, d3_ref, act_ref, mine_ref, all_ref,
                  own_sem, share_send, share_recv, pair_send, pair_recv, far_send, far_recv, near_send, near_recv, rows_sem, top_sem, w_sem, out_sem, n2_sem,
                  norm_send, norm_recv):
    g = Grid(n, heads, 0)
    side = g.side
    rows, dim = n2_ref.shape
    tiles = d1_hbm.shape[0]
    shared = max(1, 4 * tiles // 11)
    own_tiles = tiles - (g.parts - 1) * shared
    part_rows = acc_ref.shape[1]

    def start_rows_of(index):
        slot = lax.rem(index, 2)
        at = pl.ds(pl.multiple_of(index * chunk, chunk), chunk)
        for i, (src, dst) in enumerate(((late_hbm, att_ref), (early_hbm, decs_ref))):
            pltpu.make_async_copy(src.at[at, pl.ds(0, dim)], dst.at[slot], rows_sem.at[slot, i]).start()

    def tile_at(index):
        return pl.ds(pl.multiple_of(index * tile, tile), tile)

    def number_of(index):
        rest = index // shared
        return (1 - rest) * (index * g.parts + g.part) + rest * (index + (g.parts - 1) * shared)

    def weights(index):
        slot = lax.rem(index, 2)
        at = tile_at(number_of(index))
        return [pltpu.make_async_copy(src, dst.at[slot], w_sem.at[slot, i]) for i, (src, dst) in enumerate(
            ((w1_hbm.at[:, at], w1_ref), (w3_hbm.at[:, at], w3_ref), (w2_hbm.at[at, :], w2_ref)))]

    def results(index):
        slot, number = lax.rem(index, 2), number_of(index)
        pairs = ((d1_ref, d1_hbm), (d3_ref, d3_hbm), (act_ref, act_hbm))
        return ([pltpu.make_async_copy(src.at[slot], dst.at[number], out_sem.at[slot, i]) for i, (src, dst) in enumerate(pairs)],
                [send(src.at[slot], dst.at[number], share_send.at[slot, i], share_recv.at[i], g.partner)
                 for i, (src, dst) in enumerate(pairs)])

    start_rows_of(0)
    top_load = pltpu.make_async_copy(early_hbm.at[:, pl.ds(dim, dim)], top_ref, top_sem)
    top_load.start()
    for copy in weights(0):
        copy.start()

    def summand(c, core):
        source = gk_hbm if c < heads // g.parts else gv_hbm
        first = ((g.parts * c) % heads + core) * part_rows
        return source.at[pl.ds(pl.multiple_of(first, part_rows), part_rows), :]

    owns = [pltpu.make_async_copy(summand(c, g.part), acc_ref.at[c], own_sem.at[c]) for c in range(heads)]
    for copy in owns:
        copy.start()

    meet([lax.rem(g.me + step, n) for step in range(1, n)])
    for c in range(heads):
        send(summand(c, g.parts - 1 - g.part), pair_ref.at[c], pair_send, pair_recv, g.partner).start()

    grad_query = jnp.concatenate([dqr_ref[h] for h in range(heads)], axis=1)
    grad_normed = dot(grad_query, wq_ref[...])
    x = dec_ref[...].astype(F32)
    inverse = lax.rsqrt(jnp.mean(x * x, axis=-1, keepdims=True) + 1e-6)
    scaled = x * inverse
    inner = grad_normed * gain1_ref[...].astype(F32)
    gdec_ref[...] = gh_ref[...] + inverse * (inner - scaled * jnp.mean(inner * scaled, axis=-1, keepdims=True))
    mine_ref[0:1, :] = jnp.sum(grad_normed * scaled, axis=0, keepdims=True)
    mine_ref[1:2, :] = gnorm_ref[...]

    for step in range(1, n):
        send(mine_ref, all_ref.at[g.me], norm_send, norm_recv, lax.rem(g.me + step, n)).start()
    all_ref[g.me] = mine_ref[...]

    quarter = part_rows // 4
    streams = [(axis, way, pl.ds((2 * axis + (way < 0)) * quarter, quarter)) for axis in (0, 1) for way in (1, -1)]

    def place_of(axis, line, other):
        return other * side + line if axis == 0 else line * side + other

    def pieces(stage, axis, line):
        position = g.row if axis == 0 else g.col
        return [place_of(axis, line, o) for o in range(side)] if stage == 0 else [place_of(axis, line, position)]

    def ring(stage, stream, step):
        axis, way, part = streams[stream]
        axis = axis if stage == 0 else 1 - axis
        here = g.col if axis == 0 else g.row
        ref, sends, recvs = (far_ref, far_send, far_recv) if stage == 0 else (near_ref, near_send, near_recv)
        to = g.near(0, way) if axis == 0 else g.near(way, 0)
        return axis, way, part, here, ref.at[stream, step - 1], sends.at[stream, step - 1], recvs.at[stream, step - 1], to

    def line_of(here, way, step):
        return lax.rem(here - way * step + 2 * side, side)

    def start_step(stage, step):
        for stream in range(4):
            axis, way, part, here, buffer, sem, recv, to = ring(stage, stream, step)
            for i, c in enumerate(pieces(stage, axis, line_of(here, way, step))):
                send(acc_ref.at[c, part], buffer.at[i], sem, recv, to).start()

    def end_step(stage, step):
        for stream in range(4):
            axis, way, part, here, buffer, sem, recv, to = ring(stage, stream, step)
            whole = send(buffer, buffer, sem, recv, g.me)
            whole.wait_recv()
            for i, c in enumerate(pieces(stage, axis, line_of(here, way, step + 1))):
                acc_ref[c, part, :] = acc_ref[c, part, :] + buffer[i]
            whole.wait_send()

    def add_pair():
        for copy in owns:
            copy.wait()
        whole = send(pair_ref, pair_ref, pair_send, pair_recv, g.me)
        whole.wait_recv()

        def add(c, carry):
            acc_ref[c] = acc_ref[c] + pair_ref[c]
            return carry

        lax.fori_loop(0, heads, add, 0)
        whole.wait_send()

    def first():
        add_pair()
        start_step(0, 1)

    def turn():
        end_step(0, side - 1)
        start_step(1, 1)

    def between(stage, step):
        def body():
            end_step(stage, step)
            start_step(stage, step + 1)
        return body

    def prepare(index, carry):
        slot = lax.rem(index, 2)
        at = pl.ds(pl.multiple_of(index * chunk, chunk), chunk)
        for i, (src, dst) in enumerate(((late_hbm, att_ref), (early_hbm, decs_ref))):
            pltpu.make_async_copy(src.at[at, pl.ds(0, dim)], dst.at[slot], rows_sem.at[slot, i]).wait()

        @pl.when(index + 1 < rows // chunk)
        def _():
            start_rows_of(index + 1)

        pl.when(index == rows // chunk // 2)(first)
        dec = decs_ref[slot].astype(F32)
        hidden = (dec + dot(att_ref[slot], wo_ref[...])).astype(BF16).astype(F32)
        n2_ref[at, :] = rms_norm(hidden, gain2_ref[...].astype(F32)).astype(BF16)
        return carry

    lax.fori_loop(0, rows // chunk, prepare, 0)
    top_load.wait()
    n2_store = pltpu.make_async_copy(n2_ref, n2_hbm, n2_sem)
    n2_store.start()

    events = ([between(0, t) for t in range(1, side - 1)] + [turn] + [between(1, t) for t in range(1, side - 1)]
              + [lambda: end_step(1, side - 1)])
    at_tile = (1, 3, 5, 6)
    inside = own_tiles > at_tile[-1] and len(events) > len(at_tile)

    def finish_results(index):
        stores, shares = results(index)
        for copy in stores:
            copy.wait()

        @pl.when(index < shared)
        def _():
            for copy in shares:
                copy.wait_send()

    def activations(index, carry):
        slot = lax.rem(index, 2)
        for copy in weights(index):
            copy.wait()

        @pl.when(index + 1 < own_tiles)
        def _():
            for copy in weights(index + 1):
                copy.start()

        @pl.when(index >= 2)
        def _():
            finish_results(index - 2)

        if inside:
            for event, when in zip(events, at_tile):
                pl.when(index == when)(event)

        w2t_ref[...] = w2_ref[slot].T

        def products(j):
            part = pl.ds(pl.multiple_of(j * chunk, chunk), chunk)
            keep = lax.rem(j, 2)
            made_ref[keep, 0] = dot(n2_ref[part, :], w1_ref[slot])
            made_ref[keep, 1] = dot(n2_ref[part, :], w3_ref[slot])
            made_ref[keep, 2] = dot(top_ref[part, :], w2t_ref[...])

        def factors(j):
            part = pl.ds(pl.multiple_of(j * chunk, chunk), chunk)
            keep = lax.rem(j, 2)
            gate, up, grad = made_ref[keep, 0], made_ref[keep, 1], made_ref[keep, 2]
            sig = jax.nn.sigmoid(gate)
            silu = gate * sig
            act_ref[slot, part, :] = (silu * up).astype(BF16)
            d3_ref[slot, part, :] = (grad * silu).astype(BF16)
            d1_ref[slot, part, :] = (grad * up * (sig + silu * (1.0 - sig))).astype(BF16)

        def both(j, carry):
            part = pl.ds(pl.multiple_of(j * chunk, chunk), chunk)
            fresh = dot(n2_ref[part, :], w1_ref[slot]), dot(n2_ref[part, :], w3_ref[slot]), dot(top_ref[part, :], w2t_ref[...])
            factors(j - 1)
            for i, value in enumerate(fresh):
                made_ref[lax.rem(j, 2), i] = value
            return carry

        products(0)
        lax.fori_loop(1, rows // chunk, both, 0)
        factors(rows // chunk - 1)
        stores, shares = results(index)
        for copy in stores:
            copy.start()

        @pl.when(index < shared)
        def _():
            for copy in shares:
                copy.start()
        return carry

    lax.fori_loop(0, own_tiles, activations, 0)
    for event in events[len(at_tile):] if inside else events:
        event()
    sums_ref[...] = acc_ref[g.chip]

    others = all_ref.at[pl.ds(0, n - 1)]
    whole = send(others, others, norm_send, norm_recv, g.me)
    whole.wait_send()
    whole.wait_recv()
    norms_ref[...] = jnp.sum(all_ref[...], axis=0)
    n2_store.wait()
    for index in range(max(own_tiles - 2, 0), own_tiles):
        finish_results(index)
    for i, ref in enumerate((d1_hbm, d3_hbm, act_hbm)):
        come = ref.at[pl.ds(0, shared)]
        send(come, come, share_send.at[0, i], share_recv.at[i], g.me).wait_recv()


def reduce_sums(n, heads, collective_id, gk, gv, early, late, w_gate, w_up, w_down, wo, wq, gain1, gain2, dq_rows, dec_in, gh, gnorm):
    rows, dim = early.shape[0], gk.shape[1]
    ff, tile, chunk = w_gate.shape[1], 256, min(512, early.shape[0] // 2)
    part_rows = 2 * gk.shape[0] // n
    side = math.isqrt(heads)
    hbm = pl.BlockSpec(memory_space=pl.ANY)
    return pl.pallas_call(
        functools.partial(reduce_kernel, n, heads, tile, chunk),
        out_shape=[shape((part_rows, dim), F32), shape(gh.shape, F32), shape((2, dim), F32), shape((rows, dim), BF16)]
        + [shape((ff // tile, rows, tile), BF16)] * 3,
        in_specs=[hbm] * 7 + vmem(8),
        out_specs=vmem(3) + [hbm] * 4,
        scratch_shapes=[pltpu.VMEM((heads, part_rows, dim), F32)] * 2
        + [pltpu.VMEM((4, side - 1, side, part_rows // 4, dim), F32), pltpu.VMEM((4, side - 1, 1, part_rows // 4, dim), F32)]
        + [pltpu.VMEM((rows, dim), BF16)] * 2 + [pltpu.VMEM((2, chunk, dim), BF16)] * 2
        + [pltpu.VMEM((2, dim, tile), BF16)] * 2 + [pltpu.VMEM((2, tile, dim), BF16), pltpu.VMEM((dim, tile), BF16),
           pltpu.VMEM((2, 3, chunk, tile), F32)] + [pltpu.VMEM((2, rows, tile), BF16)] * 3
        + [pltpu.VMEM((2, dim), F32), pltpu.VMEM((n, 2, dim), F32)]
        + [dma(heads), dma(2, 3), dma(3), pltpu.SemaphoreType.DMA, pltpu.SemaphoreType.DMA, dma(4, side - 1), dma(4, side - 1), dma(4, side - 1),
           dma(4, side - 1), dma(2, 2), pltpu.SemaphoreType.DMA, dma(2, 3), dma(2, 3), pltpu.SemaphoreType.DMA,
           pltpu.SemaphoreType.DMA, pltpu.SemaphoreType.DMA],
        compiler_params=remote(collective_id),
        cost_estimate=pl.CostEstimate(flops=6 * rows * dim * ff, bytes_accessed=12 * rows * ff, transcendentals=rows * ff),
        name='reduce_sums',
    )(gk, gv, early, late, w_gate, w_up, w_down, wo, wq, gain1, gain2, dq_rows, dec_in, gh, gnorm)


def gate_up_kernel(n2_ref, d1_ref, d3_ref, g1_ref, g3_ref, n2t_ref):
    @pl.when(pl.program_id(0) == 0)
    def _():
        n2t_ref[...] = n2_ref[...].T

    g1_ref[...] = dot(n2t_ref[...], d1_ref[...])
    g3_ref[...] = dot(n2t_ref[...], d3_ref[...])


def gate_up_grads(n2, d1, d3):
    rows, dim = n2.shape
    tiles, _, tile = d1.shape
    cols = pl.BlockSpec((dim, tile), lambda i: (0, i))
    part = pl.BlockSpec((pl.Squeezed(), rows, tile), lambda i: (i, 0, 0))
    return pl.pallas_call(
        gate_up_kernel,
        out_shape=[shape((dim, tiles * tile), F32)] * 2,
        grid=(tiles,),
        in_specs=[full(n2), part, part],
        out_specs=[cols, cols],
        scratch_shapes=[pltpu.VMEM((dim, rows), BF16)],
        compiler_params=plain(),
        cost_estimate=pl.CostEstimate(flops=4 * rows * dim * tiles * tile, bytes_accessed=12 * dim * tiles * tile, transcendentals=0),
        name='gate_up_grads',
    )(n2, d1, d3)


def down_kernel(top_ref, act_ref, k_in_ref, v_in_ref, g2_ref, k_ref, v_ref):
    g2_ref[...] = dot_tn(act_ref[...], top_ref[...])
    k_ref[...] = k_in_ref[...]
    v_ref[...] = v_in_ref[...]


def down_grad(early, act, total):
    rows, dim = early.shape[0], early.shape[1] // 2
    tiles, _, tile = act.shape
    blocks = 1 << (tiles.bit_length() - 1)
    height = total.shape[0] // 2 // blocks
    block = lambda first: pl.BlockSpec((height, dim), lambda i: (jnp.minimum(i, blocks - 1) + first, 0))
    return pl.pallas_call(
        down_kernel,
        out_shape=[shape((tiles * tile, dim), F32)] + [shape((total.shape[0] // 2, dim), F32)] * 2,
        grid=(tiles,),
        in_specs=[pl.BlockSpec((rows, dim), lambda i: (0, 1), pipeline_mode=pl.Buffered(1)),
                  pl.BlockSpec((pl.Squeezed(), rows, tile), lambda i: (i, 0, 0)), block(0), block(blocks)],
        out_specs=[pl.BlockSpec((tile, dim), lambda i: (i, 0)), block(0), block(0)],
        compiler_params=plain(),
        cost_estimate=pl.CostEstimate(flops=2 * rows * dim * tiles * tile, bytes_accessed=12 * dim * tiles * tile, transcendentals=0),
        name='down_grad',
    )(early, act, total, total)


def memory_weight_kernel(memory_ref, dkv_ref, gk_ref, gv_ref):
    group, hd = dkv_ref.shape[0], dkv_ref.shape[2] // 2
    for i in range(group):
        both = dot_tn(dkv_ref[i], memory_ref[...])
        gk_ref[i * hd:(i + 1) * hd, :] = both[:hd]
        gv_ref[i * hd:(i + 1) * hd, :] = both[hd:]


def memory_weight_grads(memory, dkv):
    heads, rows, width = dkv.shape
    dim, hd = memory.shape[1], width // 2
    group = 4
    out = pl.BlockSpec((group * hd, dim), lambda i: (i, 0))
    return pl.pallas_call(
        memory_weight_kernel,
        out_shape=[shape((heads * hd, dim), F32)] * 2,
        grid=(heads // group,),
        in_specs=[full(memory), pl.BlockSpec((group, rows, width), lambda i: (i, 0, 0))],
        out_specs=[out, out],
        compiler_params=plain(),
        cost_estimate=pl.CostEstimate(flops=2 * rows * dim * heads * width, bytes_accessed=16 * rows * dim, transcendentals=0),
        name='memory_weight_grads',
    )(memory, dkv)


def memory_grad_kernel(dkv_ref, wk_ref, wv_ref, gq_in_ref, out_ref, gq_ref):
    group = dkv_ref.shape[0]
    gq_ref[...] = gq_in_ref[...]
    left = jnp.concatenate([dkv_ref[i] for i in range(group)], axis=1)
    right = jnp.concatenate([part[i] for i in range(group) for part in (wk_ref, wv_ref)], axis=0)

    @pl.when(pl.program_id(0) == 0)
    def _():
        out_ref[...] = dot(left, right)

    @pl.when(pl.program_id(0) > 0)
    def _():
        out_ref[...] += dot(left, right)


def memory_grad(dkv, wk_t, wv_t, gq):
    heads, rows, width = dkv.shape
    hd, dim = wk_t.shape[1], wk_t.shape[2]
    group = 4
    weight = pl.BlockSpec((group, hd, dim), lambda i: (i, 0, 0))
    passing = pl.BlockSpec((group * hd, dim), lambda i: (i, 0))
    return pl.pallas_call(
        memory_grad_kernel,
        out_shape=[shape((rows, dim), F32), shape(gq.shape, F32)],
        grid=(heads // group,),
        in_specs=[pl.BlockSpec((group, rows, width), lambda i: (i, 0, 0)), weight, weight, passing],
        out_specs=[pl.BlockSpec((rows, dim), lambda i: (0, 0)), passing],
        compiler_params=plain(),
        cost_estimate=pl.CostEstimate(flops=2 * rows * dim * heads * width, bytes_accessed=12 * rows * dim, transcendentals=0),
        name='memory_grad',
    )(dkv, wk_t, wv_t, gq)


def outer_kernel(att_ref, gh_ref, out_ref):
    @pl.when(pl.program_id(0) == 0)
    def _():
        out_ref[...] = jnp.zeros_like(out_ref)

    out_ref[...] += dot_tn(att_ref[...], gh_ref[...])


def outer_weight_grad(late, dim):
    rows = late.shape[0]
    chunk = min(512, rows)
    return pl.pallas_call(
        outer_kernel,
        out_shape=shape((dim, dim), F32),
        grid=(rows // chunk,),
        in_specs=[pl.BlockSpec((chunk, dim), lambda i: (i, 0)), pl.BlockSpec((chunk, dim), lambda i: (i, 1))],
        out_specs=pl.BlockSpec((dim, dim), lambda i: (0, 0)),
        compiler_params=plain(),
        cost_estimate=pl.CostEstimate(flops=2 * rows * dim * dim, bytes_accessed=8 * rows * dim, transcendentals=0),
        name='outer_weight_grad',
    )(late, late)


def solution(mesh):
    n = mesh.shape['seq']
    row_spec = P(('data', 'seq'), None)
    weight_spec = P()
    part_vec = P('data')
    part_mat = P('data', None)
    part_cube = P('data', None, None)

    def device_step(dec_in, memory, mem_len, grad_out, norm_attn, wq_cross, wk_cross, wv_cross, wo_cross, norm_mlp, w_gate, w_up, w_down):
        q_rows, dim = dec_in.shape
        heads, hd = wq_cross.shape[1], wq_cross.shape[2]
        parts = n // heads
        sources = -(-3 * n // 4)
        total_q = q_rows * n
        key_scale = hd ** -0.5
        scale = key_scale * LOG2E
        wq_t, wk_t, wv_t = (jnp.transpose(w, (1, 2, 0)) for w in (wq_cross, wk_cross, wv_cross))
        source_rows = -(-sources // (parts * math.isqrt(heads)))
        kv, q_in, early_local = exchange(n, heads, source_rows, 0, memory, dec_in, grad_out, norm_attn, wk_t, wv_t, wq_t)
        head_q = q_in.reshape(total_q, 2 * hd)

        early = lax.all_gather(early_local, 'seq', axis=0, tiled=True)

        wo = wo_cross.reshape(heads * hd, dim)
        mine = attention_forward(scale, hd, parts, sources, mem_len, kv, head_q)
        out_t, lse, do_in, factors, grad_hidden, g_norm_mlp = decoder_rows(
            n, heads, 1, mine, dec_in, grad_out, norm_mlp, wo, w_gate, w_up, w_down)
        do_in, factors = lax.optimization_barrier((do_in, factors))
        late = lax.all_gather(factors, 'seq', axis=0, tiled=True)

        dkv, dq_part = attention_backward(scale, key_scale, hd, parts, sources, mem_len, kv, head_q, do_in.reshape(total_q, 2 * hd), out_t, lse)
        dkv_in, dq_rows, gq_share = return_blocks(n, heads, source_rows, 4, dkv, dq_part, norm_attn, early)
        dkv_in, dq_rows, gq_share, late = lax.optimization_barrier((dkv_in, dq_rows, gq_share, late))
        g_wq = lax.all_gather(gq_share, 'seq', axis=0, tiled=True)

        gk_part, gv_part = memory_weight_grads(memory, dkv_in)
        sums, g_dec, norms, n2_all, d1, d3, act = reduce_sums(
            n, heads, 5, gk_part, gv_part, early, late, w_gate, w_up, w_down, wo, wq_t.reshape(heads * hd, dim), norm_attn, norm_mlp,
            dq_rows, dec_in, grad_hidden, g_norm_mlp)
        sums, n2_all, d1, d3, act, dkv_in, late, early, g_wq = lax.optimization_barrier(
            (sums, n2_all, d1, d3, act, dkv_in, late, early, g_wq))
        total = lax.all_gather(sums, 'seq', axis=0, tiled=True)
        g_wo = outer_weight_grad(late, dim)
        g_mem, g_wq = memory_grad(dkv_in, wk_t, wv_t, g_wq)
        g_gate, g_up = gate_up_grads(n2_all, d1, d3)
        g_down, g_wk, g_wv = down_grad(early, act, total)

        cube = lambda g: jnp.transpose(g.reshape(heads, hd, dim), (2, 0, 1))
        return (g_dec, g_mem, norms[0], cube(g_wq), cube(g_wk), cube(g_wv), g_wo.reshape(heads, hd, dim), norms[1], g_gate, g_up, g_down)

    return jax.shard_map(device_step, mesh=mesh,
                         in_specs=(row_spec, row_spec, part_vec, row_spec) + (weight_spec,) * 9,
                         out_specs=(row_spec, row_spec, part_vec, part_cube, part_cube, part_cube, part_cube, part_vec, part_mat, part_mat, part_mat),
                         check_vma=False)
```

```python
import functools
import math

import jax
import jax.numpy as jnp
from jax import lax
from jax.experimental import pallas as pl
from jax.experimental.pallas import tpu as pltpu
from jax.sharding import PartitionSpec as P

LOG2E = 1.4426950408889634
NEG = -1e30
VMEM_LIMIT = 60 * 1024 * 1024
MESH = pl.DeviceIdType.MESH
BF16, F32 = jnp.bfloat16, jnp.float32


def rms_norm(tensor, gain):
    mean_sq = jnp.mean(tensor * tensor, axis=-1, keepdims=True)
    return tensor * lax.rsqrt(mean_sq + 1e-6) * gain


def dot(a, b):
    return jnp.dot(a, b, preferred_element_type=F32)


def dot_nt(a, b):
    return lax.dot_general(a, b, (((1,), (1,)), ((), ())), preferred_element_type=F32)


def dot_tn(a, b):
    return lax.dot_general(a, b, (((0,), (0,)), ((), ())), preferred_element_type=F32)


def full(array):
    return pl.BlockSpec(array.shape, lambda *_: (0,) * array.ndim, pipeline_mode=pl.Buffered(1))


def vmem(count):
    return [pl.BlockSpec(memory_space=pltpu.VMEM)] * count


def plain():
    return pltpu.CompilerParams(vmem_limit_bytes=VMEM_LIMIT)


def remote(collective_id):
    return pltpu.CompilerParams(collective_id=collective_id, has_side_effects=True, vmem_limit_bytes=VMEM_LIMIT)


def shape(dims, dtype):
    return jax.ShapeDtypeStruct(dims, dtype)


def meet(peers):
    barrier = pltpu.get_barrier_semaphore()
    for peer in peers:
        pl.semaphore_signal(barrier, inc=1, device_id={'seq': peer}, device_id_type=MESH)
    pl.semaphore_wait(barrier, len(peers))


def send(src, dst, send_sem, recv_sem, peer):
    return pltpu.make_async_remote_copy(src_ref=src, dst_ref=dst, send_sem=send_sem, recv_sem=recv_sem,
                                        device_id={'seq': peer}, device_id_type=MESH)


class Grid:
    def __init__(self, n, heads, source_rows):
        self.n, self.heads, self.source_rows = n, heads, source_rows
        self.parts = n // heads
        self.side = math.isqrt(heads)
        self.me = lax.axis_index('seq')
        self.part = lax.rem(self.me, self.parts)
        self.chip = self.me // self.parts
        self.col = lax.rem(self.chip, self.side)
        self.row = self.chip // self.side
        self.partner = self.chip * self.parts + (self.parts - 1 - self.part)
        self.ties = self.side == 4
        self.direct = (1, 3) if self.ties else (1,)

    def wrap(self, value):
        return lax.rem(value + self.side, self.side)

    def device(self, row, col, part):
        return (row * self.side + col) * self.parts + part

    def near(self, drow, dcol, part=None):
        return self.device(self.wrap(self.row + drow), self.wrap(self.col + dcol), self.part if part is None else part)

    def hop(self, offset):
        return 1 if offset == 1 else -1

    def is_source(self, row):
        return self.wrap(row) < self.source_rows

    def row_peers(self):
        return [lax.rem(self.chip + step, self.heads) * self.parts + self.part for step in range(1, self.heads)]

    def peers(self):
        return self.row_peers() + [self.partner] + [self.near(0, self.hop(d), self.parts - 1 - self.part) for d in self.direct]


def pair_peers(n, heads, me, part):
    parts = n // heads
    head = me // parts
    partner = head * parts + (parts - 1 - part)
    return partner, [partner] + [lax.rem(head + step, heads) * parts + part for step in range(1, heads)]


def pack(rows):
    middle = rows.shape[-2] // 2
    return jnp.concatenate([rows[..., :middle, :], rows[..., middle:, :]], axis=-1)


def unpack(packed):
    middle = packed.shape[-1] // 2
    return jnp.concatenate([packed[..., :middle], packed[..., middle:]], axis=-2)


def start_rows(n, heads, me, part, src, src_of, dst_ref, send_sem, recv_sem):
    parts = n // heads
    head = me // parts
    for step in range(1, heads):
        peer = lax.rem(head + step, heads) * parts + part
        send(src.at[src_of(peer)], dst_ref.at[head], send_sem, recv_sem, peer).start()
    dst_ref[head] = src[src_of(me)]


def wait_rows(heads, me, dst_ref, send_sem, recv_sem):
    others = dst_ref.at[pl.ds(0, heads - 1)]
    whole = send(others, others, send_sem, recv_sem, me)
    whole.wait_send()
    whole.wait_recv()


def swap(src, dst, send_sem, recv_sem, partner):
    copy = send(src, dst, send_sem, recv_sem, partner)
    copy.start()
    copy.wait()


def place(n, heads, part, mine_ref, theirs_ref, wide_ref, low):
    parts = n // heads
    for source, index in ((mine_ref, part), (theirs_ref, parts - 1 - part)):
        def one(head, carry, source=source, index=index):
            rows = unpack(source[head])
            zeros = jnp.zeros_like(rows)
            wide_ref[head * parts + index] = jnp.concatenate([rows, zeros] if low else [zeros, rows], axis=-1)
            return carry

        lax.fori_loop(0, heads, one, 0)


def exchange_kernel(n, heads, source_rows, memory_ref, dec_ref, gout_ref, gain_ref, wk_ref, wv_ref, wq_ref, kv_out_ref, q_out_ref, early_ref,
                    kv_ref, stage_ref, up_ref, down_ref, right_ref, left_ref, packed_ref, got_ref, swapped_ref,
                    row_send, row_recv, y_send, pass_send, x_send, fwd_send, stage_recv, up_recv, down_recv, right_recv,
                    left_recv, out_recv):
    g = Grid(n, heads, source_rows)
    side, hd = g.side, wk_ref.shape[1]
    half = kv_out_ref.shape[1]
    chunk_rows = min(256, kv_ref.shape[1])
    barrier = pltpu.get_barrier_semaphore()
    peers = g.peers()
    for peer in peers:
        pl.semaphore_signal(barrier, inc=1, device_id={'seq': peer}, device_id_type=MESH)

    dim = dec_ref.shape[1]
    early_ref[:, :dim] = dec_ref[...]
    early_ref[:, dim:] = gout_ref[...].astype(BF16)
    normed = rms_norm(dec_ref[...].astype(F32), gain_ref[...].astype(F32)).astype(BF16)

    def some_heads(index, carry):
        queries = dot_nt(normed, jnp.concatenate([wq_ref[4 * index + j] for j in range(4)], axis=0)).astype(BF16)
        for j in range(4):
            packed_ref[4 * index + j] = pack(queries[:, hd * j:hd * (j + 1)])
        return carry

    lax.fori_loop(0, heads // 4, some_heads, 0)

    def head(drow, dcol):
        return g.wrap(g.row + drow) * side + g.wrap(g.col + dcol)

    def project(drow, dcols):
        weights = jnp.concatenate([ref[head(drow, d)] for d in dcols for ref in (wk_ref, wv_ref)], axis=0)

        def rows(index, carry):
            at = pl.ds(pl.multiple_of(index * chunk_rows, chunk_rows), chunk_rows)
            both = dot_nt(memory_ref[at, :], weights).astype(BF16)
            for i, d in enumerate(dcols):
                kv_ref[head(drow, d), at, :] = both[:, 2 * hd * i:2 * hd * (i + 1)]
            return carry

        lax.fori_loop(0, kv_ref.shape[1] // chunk_rows, rows, 0)

    def along_column(drow, dcol):
        chunk = kv_ref.at[head(drow, dcol)]
        if drow in g.direct:
            send(chunk, stage_ref.at[drow - 1, dcol], y_send.at[drow - 1], stage_recv.at[drow - 1, dcol], g.near(g.hop(drow), 0)).start()
        elif dcol % 2 == 0:
            send(chunk, up_ref.at[dcol // 2], y_send.at[drow - 1], up_recv.at[dcol // 2], g.near(1, 0)).start()
        else:
            send(chunk, down_ref.at[dcol // 2], y_send.at[drow - 1], down_recv.at[dcol // 2], g.near(-1, 0)).start()

    def along_row(o, dcol):
        chunk = kv_ref.at[head(0, dcol)] if o == 0 else stage_ref.at[o - 1, dcol]
        source = g.device(g.wrap(g.row - o), g.col, g.part)
        if dcol == 0:
            kv_out_ref[source] = chunk[pl.ds(pl.multiple_of(g.part * half, half), half), :]
            away = pl.ds(pl.multiple_of((g.parts - 1 - g.part) * half, half), half)
            send(chunk.at[away], kv_out_ref.at[source], x_send.at[o], out_recv, g.partner).start()
        elif dcol in g.direct:
            for part in range(g.parts):
                send(chunk.at[pl.ds(part * half, half)], kv_out_ref.at[source], x_send.at[o], out_recv,
                     g.near(0, g.hop(dcol), part)).start()
        else:
            send(chunk.at[pl.ds(0, half)], right_ref.at[o], x_send.at[o], right_recv.at[o], g.near(0, 1)).start()
            send(chunk.at[pl.ds(half, half)], left_ref.at[o], x_send.at[o], left_recv.at[o], g.near(0, -1)).start()

    def pass_row(o):
        for ref, sem, come in ((right_ref, right_recv, -1), (left_ref, left_recv, 1)):
            source = g.device(g.wrap(g.row - o), g.wrap(g.col + come), g.part)
            send(ref.at[o], ref.at[o], fwd_send.at[o], sem.at[o], g.me).wait_recv()
            send(ref.at[o], kv_out_ref.at[source], fwd_send.at[o], out_recv, g.near(0, -come, 0 if come < 0 else 1)).start()

    def when_source(row, body):
        pl.when(g.is_source(row))(body)

    if g.ties:
        order = [(2, (2, 1)), (2, (3, 0)), (1, (2, 1)), (3, (2, 3)), (0, (2, 1)), (0, (3, 0))]
        last = [(1, (3, 0)), (3, (1, 0))]
    else:
        order, last = [(1, (1, 0)), (0, (1, 0))], []

    def issue(drow, dcols):
        def body():
            for d in dcols:
                along_row(0, d) if drow == 0 else along_column(drow, d)
        when_source(g.row, body)

    waiting = None
    for drow, dcols in order + last:
        project(drow, dcols)
        if waiting is None:
            pl.semaphore_wait(barrier, len(peers))
            start_rows(n, heads, g.me, g.part, packed_ref, lambda peer: peer // g.parts, got_ref, row_send.at[0], row_recv.at[0])
        elif waiting not in last:
            issue(*waiting)
        waiting = (drow, dcols)
    if not last:
        issue(*waiting)

    if g.ties:
        def up(i):
            send(up_ref.at[i], up_ref.at[i], pass_send.at[0], up_recv.at[i], g.me).wait_recv()
            send(up_ref.at[i], stage_ref.at[1, 2 * i], pass_send.at[0], stage_recv.at[1, 2 * i], g.near(1, 0)).start()

        def down(i):
            send(down_ref.at[i], down_ref.at[i], pass_send.at[1], down_recv.at[i], g.me).wait_recv()
            send(down_ref.at[i], stage_ref.at[1, 2 * i + 1], pass_send.at[1], stage_recv.at[1, 2 * i + 1], g.near(-1, 0)).start()

        for i in range(2):
            when_source(g.row - 1, lambda i=i: up(1 - i))
            when_source(g.row + 1, lambda i=i: down(i))
        for drow, dcols in last:
            issue(drow, dcols)
        when_source(g.row, lambda: pass_row(0))

    wait_rows(heads, g.me, got_ref, row_send.at[0], row_recv.at[0])
    swap(got_ref, swapped_ref, row_send.at[1], row_recv.at[1], g.partner)
    place(n, heads, g.part, got_ref, swapped_ref, q_out_ref, True)

    def arrived(o, dcol):
        def body():
            send(stage_ref.at[o - 1, dcol], stage_ref.at[o - 1, dcol], y_send.at[0], stage_recv.at[o - 1, dcol], g.me).wait_recv()
            along_row(o, dcol)
        when_source(g.row - o, body)

    if g.ties:
        for o, d in ((1, 2), (3, 2), (1, 1), (3, 3)):
            arrived(o, d)
        for o in g.direct:
            when_source(g.row - o, lambda o=o: pass_row(o))
        for d in (2, 1, 0, 3):
            arrived(2, d)
        when_source(g.row - 2, lambda: pass_row(2))
        for o, d in ((1, 3), (3, 1), (1, 0), (3, 0)):
            arrived(o, d)
    else:
        for d in (1, 0):
            arrived(1, d)

    def sent(sem, ref):
        send(ref, ref, sem, out_recv, g.me).wait_send()

    def mine():
        for drow in range(1, side):
            sent(y_send.at[drow - 1], stage_ref.at[0])
    when_source(g.row, mine)
    for o in range(side):
        def passed(o=o):
            sent(x_send.at[o], kv_out_ref.at[pl.ds(0, g.parts * side - 1)])
            if g.ties:
                sent(fwd_send.at[o], kv_out_ref.at[pl.ds(0, 2)])
        when_source(g.row - o, passed)
    if g.ties:
        when_source(g.row - 1, lambda: sent(pass_send.at[0], up_ref))
        when_source(g.row + 1, lambda: sent(pass_send.at[1], down_ref))
    blocks = source_rows * side * g.parts
    others = kv_out_ref.at[pl.ds(0, blocks - source_rows)]
    send(others, others, y_send.at[0], out_recv, g.me).wait_recv()


def row_scratch(heads, q_rows, hd):
    return [pltpu.VMEM((heads, q_rows // 2, 2 * hd), BF16)] * 3


def dma(*dims):
    return pltpu.SemaphoreType.DMA(dims)


def exchange(n, heads, source_rows, collective_id, memory, dec_in, grad_out, gain, wk_t, wv_t, wq_t):
    m_rows, q_rows, hd = memory.shape[0], dec_in.shape[0], wk_t.shape[1]
    side, parts = math.isqrt(heads), n // heads
    half = m_rows // parts
    chunk = lambda *lead: pltpu.VMEM(lead + (m_rows, 2 * hd), BF16)
    block = lambda *lead: pltpu.VMEM(lead + (half, 2 * hd), BF16)
    return pl.pallas_call(
        functools.partial(exchange_kernel, n, heads, source_rows),
        out_shape=[shape((n, half, 2 * hd), BF16), shape((n, q_rows, 2 * hd), BF16), shape((q_rows, 2 * dec_in.shape[1]), BF16)],
        in_specs=vmem(7),
        out_specs=vmem(3),
        scratch_shapes=[chunk(heads), chunk(side - 1, side), chunk(2), chunk(2), block(side), block(side)]
        + row_scratch(heads, q_rows, hd)
        + [dma(2), dma(2), dma(side - 1), dma(2), dma(side), dma(side), dma(side - 1, side), dma(2), dma(2), dma(side), dma(side),
           pltpu.SemaphoreType.DMA],
        compiler_params=remote(collective_id),
        name='exchange',
    )(memory, dec_in, grad_out, gain, wk_t, wv_t, wq_t)


def return_kernel(n, heads, source_rows, chunk, src_ref, dq_ref, gain_ref, early_hbm, dst_ref, rows_ref, gq_ref, stage_ref, right_ref,
                  left_ref, up_ref, down_ref, theirs_ref, packed_ref, got_ref, dqt_ref, decs_ref, dec_sem, row_send, row_recv,
                  x_send, fwd_send, y_send, pass_send, stage_recv, right_recv, left_recv, up_recv, down_recv, out_recv):
    g = Grid(n, heads, source_rows)
    side = g.side
    half = src_ref.shape[1]
    total_rows, dim = dqt_ref.shape[1], gq_ref.shape[1]

    def dec_load(index, slot):
        at = pl.ds(pl.multiple_of(index * chunk, chunk), chunk)
        return pltpu.make_async_copy(early_hbm.at[at, pl.ds(0, dim)], decs_ref.at[slot], dec_sem.at[slot])

    dec_load(0, 0).start()
    meet(g.peers())
    mine = pl.ds(pl.multiple_of(g.part * half, half), half)

    def landing(drow, dcol, head_col):
        if drow == 0:
            return dst_ref.at[g.row * side + head_col, mine], out_recv
        return stage_ref.at[drow - 1, dcol, mine], stage_recv.at[drow - 1, dcol]

    def along_row(drow, dcol):
        row = g.wrap(g.row + drow)
        col = g.wrap(g.col + dcol)
        for part in range(g.parts):
            source = src_ref.at[g.device(row, col, part)]
            if dcol in g.direct:
                dst, sem = landing(drow, dcol, g.col)
                send(source, dst, x_send.at[drow], sem, g.near(0, g.hop(dcol), part)).start()
            elif part == 0:
                send(source, right_ref.at[drow], x_send.at[drow], right_recv.at[drow], g.near(0, 1)).start()
            else:
                send(source, left_ref.at[drow], x_send.at[drow], left_recv.at[drow], g.near(0, -1)).start()

    def own_chip(drow):
        row = g.wrap(g.row + drow)
        away = src_ref.at[g.device(row, g.col, g.parts - 1 - g.part)]
        dst, sem = landing(drow, 0, g.col)
        dst[...] = src_ref[g.device(row, g.col, g.part)]
        send(away, dst, x_send.at[drow], sem, g.partner).start()

    def pass_row(drow):
        for ref, come_sem, come in ((right_ref, right_recv, -1), (left_ref, left_recv, 1)):
            send(ref.at[drow], ref.at[drow], fwd_send.at[drow], come_sem.at[drow], g.me).wait_recv()
            dst, sem = landing(drow, 2, g.wrap(g.col + come))
            send(ref.at[drow], dst, fwd_send.at[drow], sem, g.near(0, -come, 0 if come < 0 else 1)).start()

    def along_column(drow, dcol):
        chunk = stage_ref.at[drow - 1, dcol]
        got = chunk.at[pl.ds(0, half)] if dcol == 0 else chunk
        send(got, got, y_send.at[drow - 1], stage_recv.at[drow - 1, dcol], g.me).wait_recv()
        head = g.row * side + g.wrap(g.col - dcol)
        if drow in g.direct:
            send(chunk, dst_ref.at[head], y_send.at[drow - 1], out_recv, g.near(g.hop(drow), 0)).start()
        elif dcol % 2 == 0:
            send(chunk, up_ref.at[dcol // 2], y_send.at[drow - 1], up_recv.at[dcol // 2], g.near(1, 0)).start()
        else:
            send(chunk, down_ref.at[dcol // 2], y_send.at[drow - 1], down_recv.at[dcol // 2], g.near(-1, 0)).start()

    def when_source(row, body):
        pl.when(g.is_source(row))(body)

    def rows_of(drow):
        def body():
            for d in (2, 1, 3) if g.ties else (1,):
                along_row(drow, d)
        when_source(g.row + drow, body)

    def relay(drow):
        when_source(g.row + drow, lambda: pass_row(drow))

    def column(drow, d):
        when_source(g.row + drow, lambda: along_column(drow, d))

    def up(i):
        def body():
            send(up_ref.at[i], up_ref.at[i], pass_send.at[0], up_recv.at[i], g.me).wait_recv()
            head = g.wrap(g.row - 1) * side + g.wrap(g.col - 2 * i)
            send(up_ref.at[i], dst_ref.at[head], pass_send.at[0], out_recv, g.near(1, 0)).start()
        when_source(g.row + 1, body)

    def down(i):
        def body():
            send(down_ref.at[i], down_ref.at[i], pass_send.at[1], down_recv.at[i], g.me).wait_recv()
            head = g.wrap(g.row + 1) * side + g.wrap(g.col - 2 * i - 1)
            send(down_ref.at[i], dst_ref.at[head], pass_send.at[1], out_recv, g.near(-1, 0)).start()
        when_source(g.row - 1, body)

    def start_dq():
        swap(dq_ref, theirs_ref, row_send.at[0], row_recv.at[0], g.partner)
        both = (dq_ref[...] + theirs_ref[...]).astype(BF16)
        share = dqt_ref.shape[0]
        dqt_ref[...] = jnp.where(g.part == 0, both[:share], both[share:])
        total = both.T
        packed_ref[...] = pack(total.reshape(n, total.shape[0] // n, total.shape[1]))
        start_rows(n, heads, g.me, g.part, packed_ref, lambda peer: peer, got_ref, row_send.at[1], row_recv.at[1])

    def query_weight(index, carry):
        slot = lax.rem(index, 2)
        dec_load(index, slot).wait()

        @pl.when(index + 1 < chunks)
        def _():
            dec_load(index + 1, 1 - slot).start()

        normed = rms_norm(decs_ref[slot].astype(F32), gain_ref[...].astype(F32)).astype(BF16)
        gq_ref[...] += dot(dqt_ref[:, pl.ds(pl.multiple_of(index * chunk, chunk), chunk)], normed)
        return carry

    chunks = total_rows // chunk
    for drow in (2, 1, 3, 0) if g.ties else (1, 0):
        when_source(g.row + drow, lambda drow=drow: own_chip(drow))
    if g.ties:
        rows_of(2)
        for drow in (2, 1, 3):
            column(drow, 0)
        relay(2)
        rows_of(1)
        column(2, 1)
        column(2, 3)
        column(2, 2)
        relay(1)
        rows_of(3)
        start_dq()
        up(0)
        down(0)
        column(1, 1)
        column(1, 3)
        column(1, 2)
        relay(3)
        rows_of(0)
        up(1)
        down(1)
        column(3, 1)
        column(3, 3)
        column(3, 2)
        relay(0)
    else:
        rows_of(1)
        rows_of(0)
        start_dq()
        column(1, 0)
        column(1, 1)
    gq_ref[...] = jnp.zeros_like(gq_ref)
    lax.fori_loop(0, chunks, query_weight, 0)
    wait_rows(heads, g.me, got_ref, row_send.at[1], row_recv.at[1])
    rows_ref[...] = unpack(got_ref[...])

    def sent(sem, ref):
        send(ref, ref, sem, out_recv, g.me).wait_send()

    for drow in range(side):
        def done(drow=drow):
            sent(x_send.at[drow], src_ref.at[pl.ds(0, g.parts * side - 1)])
            if g.ties:
                sent(fwd_send.at[drow], src_ref.at[pl.ds(0, 2)])
            if drow:
                sent(y_send.at[drow - 1], stage_ref.at[0])
        when_source(g.row + drow, done)
    if g.ties:
        when_source(g.row + 1, lambda: sent(pass_send.at[0], up_ref))
        when_source(g.row - 1, lambda: sent(pass_send.at[1], down_ref))

    @pl.when(g.is_source(g.row))
    def _():
        blocks = src_ref.at[pl.ds(0, n - 1)]
        send(blocks, blocks, y_send.at[0], out_recv, g.me).wait_recv()

    @pl.when(jnp.logical_not(g.is_source(g.row)))
    def _():
        def clear(index, carry):
            dst_ref[index] = jnp.zeros(dst_ref.shape[1:], dst_ref.dtype)
            return carry
        lax.fori_loop(0, heads, clear, 0)


def return_blocks(n, heads, source_rows, collective_id, blocks, dq, gain, early):
    half, width = blocks.shape[1], blocks.shape[2]
    hd, total_q = dq.shape
    q_rows = total_q // n
    side, parts = math.isqrt(heads), n // heads
    chunk = lambda *lead: pltpu.VMEM(lead + (half * parts, width), BF16)
    block = lambda *lead: pltpu.VMEM(lead + (half, width), BF16)
    piece, dim = min(512, total_q), early.shape[1] // 2
    return pl.pallas_call(
        functools.partial(return_kernel, n, heads, source_rows, piece),
        out_shape=[shape((heads, half * parts, width), BF16), shape((heads, q_rows, hd), BF16), shape((hd // parts, dim), F32)],
        in_specs=vmem(3) + [pl.BlockSpec(memory_space=pl.ANY)],
        out_specs=vmem(3),
        scratch_shapes=[chunk(side - 1, side), block(side), block(side), chunk(2), chunk(2), pltpu.VMEM(dq.shape, F32),
                        pltpu.VMEM((n, q_rows // 2, 2 * hd), BF16), pltpu.VMEM((heads, q_rows // 2, 2 * hd), BF16),
                        pltpu.VMEM((hd // parts, total_q), BF16), pltpu.VMEM((2, piece, dim), BF16), dma(2), dma(2), dma(2),
                        dma(side), dma(side), dma(side - 1), dma(2), dma(side - 1, side), dma(side), dma(side), dma(2), dma(2),
                        pltpu.SemaphoreType.DMA],
        compiler_params=remote(collective_id),
        name='return_blocks',
    )(blocks, dq, gain, early)


def decoder_kernel(n, heads, mine_ref, dec_ref, gout_ref, gain_ref, wo_hbm, wg_hbm, wu_hbm, wd_hbm,
                   out_ref, lse_ref, do_ref, factors_ref, gh_ref, gnorm_ref,
                   theirs_ref, packed_ref, got_ref, sent_ref, back_ref, swapped_ref, wo_ref, wg_ref, wu_ref, wd_ref, gact_ref,
                   load_sem, send_sem, recv_sem):
    me = lax.axis_index('seq')
    part = lax.rem(me, n // heads)
    partner, peers = pair_peers(n, heads, me, part)
    q_rows, dim = dec_ref.shape
    hd = out_ref.shape[0]
    loads = [pltpu.make_async_copy(src, dst, load_sem.at[i]) for i, (src, dst) in enumerate(
        ((wd_hbm, wd_ref), (wo_hbm, wo_ref), (wg_hbm, wg_ref), (wu_hbm, wu_ref)))]
    for load in loads:
        load.start()
    meet(peers)

    swap(mine_ref, theirs_ref, send_sem.at[0], recv_sem.at[0], partner)
    m_a, m_b = mine_ref[hd + 8:hd + 9], theirs_ref[hd + 8:hd + 9]
    top = jnp.maximum(m_a, m_b)
    s_a, s_b = jnp.exp2(m_a - top), jnp.exp2(m_b - top)
    den = mine_ref[hd:hd + 1] * s_a + theirs_ref[hd:hd + 1] * s_b
    out = (mine_ref[:hd] * s_a + theirs_ref[:hd] * s_b) / den
    packed_ref[...] = pack(out.T.astype(BF16).reshape(n, q_rows, hd))
    start_rows(n, heads, me, part, packed_ref, lambda peer: peer, got_ref, send_sem.at[1], recv_sem.at[1])
    out_ref[...] = out
    lse_ref[...] = top + jnp.log2(den)

    loads[0].wait()
    top_rows = gout_ref[...].astype(BF16)
    tile = 256

    def act_tile(index, carry):
        at = pl.ds(pl.multiple_of(index * tile, tile), tile)
        gact_ref[:, at] = dot_nt(top_rows, wd_ref[at, :])
        return carry

    lax.fori_loop(0, wd_ref.shape[0] // tile, act_tile, 0)
    wait_rows(heads, me, got_ref, send_sem.at[1], recv_sem.at[1])

    attended = jnp.concatenate([unpack(got_ref[h]) for h in range(heads)], axis=1)
    loads[1].wait()
    hidden = (dec_ref[...].astype(F32) + dot(attended, wo_ref[...])).astype(BF16).astype(F32)
    gain = gain_ref[...].astype(F32)
    inverse = lax.rsqrt(jnp.mean(hidden * hidden, axis=-1, keepdims=True) + 1e-6)
    scaled = hidden * inverse
    normed = (scaled * gain).astype(BF16)
    loads[2].wait()
    gate = dot(normed, wg_ref[...])
    loads[3].wait()
    up = dot(normed, wu_ref[...])
    sig = jax.nn.sigmoid(gate)
    silu = gate * sig
    grad_act = gact_ref[...]
    grad_gate = (grad_act * up * (sig + silu * (1.0 - sig))).astype(BF16)
    grad_up = (grad_act * silu).astype(BF16)
    grad_normed = (dot_nt(wg_ref[...], grad_gate) + dot_nt(wu_ref[...], grad_up)).T
    gnorm_ref[...] = jnp.sum(grad_normed * scaled, axis=0, keepdims=True)
    inner = grad_normed * gain
    grad_hidden = gout_ref[...] + inverse * (inner - scaled * jnp.mean(inner * scaled, axis=-1, keepdims=True))
    rounded = grad_hidden.astype(BF16)
    grad_att = dot_nt(wo_ref[...], rounded).T.astype(BF16)
    for h in range(heads):
        sent_ref[h] = pack(grad_att[:, hd * h:hd * (h + 1)])
    factors_ref[:, :dim] = attended
    factors_ref[:, dim:] = rounded
    gh_ref[...] = grad_hidden

    start_rows(n, heads, me, part, sent_ref, lambda peer: peer // (n // heads), back_ref, send_sem.at[2], recv_sem.at[2])
    wait_rows(heads, me, back_ref, send_sem.at[2], recv_sem.at[2])
    swap(back_ref, swapped_ref, send_sem.at[3], recv_sem.at[3], partner)
    place(n, heads, part, back_ref, swapped_ref, do_ref, False)


def decoder_rows(n, heads, collective_id, mine, dec_in, grad_out, gain, wo, w_gate, w_up, w_down):
    q_rows, dim = dec_in.shape
    hd, total_q = wo.shape[0] // heads, mine.shape[1]
    hbm = pl.BlockSpec(memory_space=pl.ANY)
    return pl.pallas_call(
        functools.partial(decoder_kernel, n, heads),
        out_shape=[shape((hd, total_q), F32), shape((1, total_q), F32), shape((n, q_rows, 2 * hd), BF16),
                   shape((q_rows, 2 * dim), BF16), shape((q_rows, dim), F32), shape((1, dim), F32)],
        in_specs=vmem(4) + [hbm] * 4,
        out_specs=vmem(6),
        scratch_shapes=[pltpu.VMEM(mine.shape, F32), pltpu.VMEM((n, q_rows // 2, 2 * hd), BF16)]
        + [pltpu.VMEM((heads, q_rows // 2, 2 * hd), BF16)] * 4
        + [pltpu.VMEM(w.shape, BF16) for w in (wo, w_gate, w_up, w_down)] + [pltpu.VMEM((q_rows, w_down.shape[0]), F32), dma(4), dma(4), dma(4)],
        compiler_params=remote(collective_id),
        name='decoder_rows',
    )(mine, dec_in, grad_out, gain, wo, w_gate, w_up, w_down)


def valid_blocks(mem_len, rows, parts, sources):
    reach = mem_len - lax.rem(lax.axis_index('seq'), parts) * rows
    blocks = jnp.minimum((reach + parts * rows - 1) // (parts * rows), sources)
    return blocks, jnp.minimum(reach - (blocks - 1) * parts * rows, rows)


def forward_kernel(scale, hd, parts, q_block, len_ref, kv_ref, q_ref, out_ref, qt_ref, top_ref):
    rows, total_q = kv_ref.shape[1], q_ref.shape[0]
    blocks, last_valid = valid_blocks(len_ref[0], rows, parts, kv_ref.shape[0])
    groups = [slice(first, first + q_block) for first in range(0, total_q, q_block)]
    base = slice(hd + 8, hd + 9)
    qt_ref[...] = q_ref[...].T

    def values_of(keys):
        return jnp.concatenate([keys.T[hd:], jnp.ones((16, rows), keys.dtype)], axis=0)

    def group_of(index):
        return pl.ds(pl.multiple_of(index * q_block, q_block), q_block)

    def first_step(group, carry):
        cols = group_of(group)
        top = jnp.max(dot(kv_ref[0], qt_ref[:, cols]), axis=0, keepdims=True)
        out_ref[hd + 8:, cols] = jnp.broadcast_to(top * scale, (8, q_block))
        top_ref[:, cols] = jnp.broadcast_to(top, (8, q_block))
        return carry

    lax.fori_loop(0, len(groups), first_step, 0)
    out_ref[:hd + 8, :] = jnp.zeros((hd + 8, total_q), F32)

    def finish(values, scores, cols):
        top_ref[:, cols] = jnp.maximum(top_ref[:, cols], jnp.max(scores.reshape(rows // 8, 8, q_block), axis=0))
        weights = jnp.exp2(scores * scale - out_ref[base, cols]).astype(values.dtype)
        out_ref[:hd + 8, cols] += dot(values, weights)[:hd + 8]

    def step(index, carry):
        keys = kv_ref[index]
        values = values_of(keys)
        for cols in groups:
            finish(values, dot(keys, qt_ref[:, cols]), cols)
        return carry

    def last_step(group, carry):
        cols = group_of(group)
        keys = kv_ref[blocks - 1]
        scores = dot(keys, qt_ref[:, cols])
        position = lax.broadcasted_iota(jnp.int32, scores.shape, 0)
        finish(values_of(keys), jnp.where(position < last_valid, scores, NEG), cols)
        return carry

    lax.fori_loop(0, blocks - 1, step, 0)
    lax.fori_loop(0, len(groups), last_step, 0)

    excess = jnp.max(top_ref[...] * scale - out_ref[hd + 8:, :])
    broken = jnp.max(jnp.where(jnp.abs(out_ref[:hd + 8, :]) <= 3e38, 0.0, 1.0))

    @pl.when(jnp.logical_or(jnp.logical_not(excess <= 64.0), broken > 0.0))
    def _():
        out_ref[:hd + 8, :] = jnp.zeros((hd + 8, total_q), F32)
        out_ref[hd + 8:, :] = jnp.full((8, total_q), NEG, F32)

        def running(step_index, carry):
            index, group = step_index // len(groups), lax.rem(step_index, len(groups))
            cols = group_of(group)
            keys = kv_ref[index]
            limit = jnp.where(index == blocks - 1, last_valid, rows)
            scores = dot(keys, qt_ref[:, cols]) * scale
            position = lax.broadcasted_iota(jnp.int32, scores.shape, 0)
            scores = jnp.where(position < limit, scores, NEG)
            old = out_ref[base, cols]
            new = jnp.maximum(old, jnp.max(scores, axis=0, keepdims=True))
            weights = jnp.exp2(scores - new).astype(keys.dtype)
            out_ref[:hd + 8, cols] = out_ref[:hd + 8, cols] * jnp.exp2(old - new) + dot(values_of(keys), weights)[:hd + 8]
            out_ref[hd + 8:, cols] = jnp.broadcast_to(new, (8, q_block))
            return carry

        lax.fori_loop(0, blocks * len(groups), running, 0)


def attention_forward(scale, hd, parts, sources, mem_len, kv, q):
    rows, width = kv.shape[1], kv.shape[2]
    total_q = q.shape[0]
    return pl.pallas_call(
        functools.partial(forward_kernel, scale, hd, parts, min(1024, total_q)),
        out_shape=shape((hd + 16, total_q), F32),
        grid=(1,),
        in_specs=[pl.BlockSpec(memory_space=pltpu.SMEM),
                  pl.BlockSpec((sources, rows, width), lambda i: (0, 0, 0), pipeline_mode=pl.Buffered(1)), full(q)],
        out_specs=pl.BlockSpec((hd + 16, total_q), lambda i: (0, 0)),
        scratch_shapes=[pltpu.VMEM((width, total_q), BF16), pltpu.VMEM((8, total_q), F32)],
        compiler_params=plain(),
        cost_estimate=pl.CostEstimate(flops=4 * total_q * sources * rows * hd, bytes_accessed=kv.size * 2,
                                      transcendentals=total_q * sources * rows),
        name='attention_forward',
    )(mem_len, kv, q)


def backward_kernel(scale, key_scale, hd, parts, q_block, len_ref, kv_ref, q_ref, do_ref, out_ref, lse_ref, dkv_ref, dq_ref,
                    qt_ref, dot_ref, delta_ref):
    rows, total_q = kv_ref.shape[1], q_ref.shape[0]
    blocks, last_valid = valid_blocks(len_ref[0], rows, parts, kv_ref.shape[0])
    width = kv_ref.shape[2]
    groups = [slice(first, first + q_block) for first in range(0, total_q, q_block)]
    dq_ref[...] = jnp.zeros_like(dq_ref)
    qt_ref[...] = q_ref[...].T
    do_t = do_ref[...].T
    dot_ref[...] = do_t
    delta_ref[...] = jnp.sum(do_t[hd:].astype(F32) * out_ref[...], axis=0, keepdims=True)

    lane_scale = jnp.where(lax.broadcasted_iota(jnp.int32, (1, width), 1) < hd, key_scale, 1.0)

    def products(keys, cols):
        return dot(keys, qt_ref[:, cols]), dot(keys, dot_ref[:, cols])

    def finish(keys, keys_t, scores, grads, cols, valid):
        prob = jnp.exp2(scores * scale - lse_ref[:, cols])
        if valid is not None:
            position = lax.broadcasted_iota(jnp.int32, scores.shape, 0)
            prob = jnp.where(position < valid, prob, 0.0)
        grad_scores = (prob * (grads - delta_ref[:, cols])).astype(keys.dtype)
        update = dot(grad_scores, q_ref[cols, :]) + dot(prob.astype(keys.dtype), do_ref[cols, :])
        dq_ref[:, cols] += dot(keys_t, grad_scores)
        return update

    def step(index, carry):
        keys = kv_ref[index]
        keys_t = keys.T[:hd]
        total = jnp.zeros((rows, width), F32)
        for cols in groups:
            scores, grads = products(keys, cols)
            total += finish(keys, keys_t, scores, grads, cols, None)
        dkv_ref[index] = (total * lane_scale).astype(dkv_ref.dtype)
        return carry

    def last_step(group, total):
        keys = kv_ref[blocks - 1]
        cols = pl.ds(pl.multiple_of(group * q_block, q_block), q_block)
        scores, grads = products(keys, cols)
        return total + finish(keys, keys.T[:hd], scores, grads, cols, last_valid)

    def clear(index, carry):
        dkv_ref[index] = jnp.zeros((rows, width), dkv_ref.dtype)
        return carry

    lax.fori_loop(0, blocks - 1, step, 0)
    total = lax.fori_loop(0, len(groups), last_step, jnp.zeros((rows, width), F32))
    dkv_ref[blocks - 1] = (total * lane_scale).astype(dkv_ref.dtype)
    lax.fori_loop(blocks, dkv_ref.shape[0], clear, 0)
    dq_ref[...] = dq_ref[...] * key_scale


def attention_backward(scale, key_scale, hd, parts, sources, mem_len, kv, q, do, out_t, lse):
    n, rows, width = kv.shape
    total_q = q.shape[0]
    return pl.pallas_call(
        functools.partial(backward_kernel, scale, key_scale, hd, parts, min(512, total_q)),
        out_shape=[shape((n, rows, width), BF16), shape((hd, total_q), F32)],
        grid=(1,),
        in_specs=[pl.BlockSpec(memory_space=pltpu.SMEM),
                  pl.BlockSpec((sources, rows, width), lambda i: (0, 0, 0), pipeline_mode=pl.Buffered(1)),
                  full(q), full(do), full(out_t), full(lse)],
        out_specs=[pl.BlockSpec((n, rows, width), lambda i: (0, 0, 0)),
                   pl.BlockSpec((hd, total_q), lambda i: (0, 0))],
        scratch_shapes=[pltpu.VMEM((width, total_q), BF16), pltpu.VMEM((width, total_q), BF16), pltpu.VMEM((1, total_q), F32)],
        compiler_params=plain(),
        cost_estimate=pl.CostEstimate(flops=10 * total_q * sources * rows * hd, bytes_accessed=kv.size * 4,
                                      transcendentals=total_q * sources * rows),
        name='attention_backward',
    )(mem_len, kv, q, do, out_t, lse)


def reduce_kernel(n, heads, tile, chunk, gk_hbm, gv_hbm, early_hbm, late_hbm, w1_hbm, w3_hbm, w2_hbm, wo_ref, wq_ref, gain1_ref,
                  gain2_ref, dqr_ref, dec_ref, gh_ref, gnorm_ref,
                  sums_ref, gdec_ref, norms_ref, n2_hbm, d1_hbm, d3_hbm, act_hbm,
                  acc_ref, pair_ref, far_ref, near_ref, n2_ref, top_ref, att_ref, decs_ref, w1_ref, w3_ref, w2_ref,
                  d1_ref, d3_ref, act_ref, mine_ref, all_ref,
                  own_sem, share_send, share_recv, pair_send, pair_recv, far_send, far_recv, near_send, near_recv, rows_sem, top_sem, w_sem, out_sem, n2_sem,
                  norm_send, norm_recv):
    g = Grid(n, heads, 0)
    side = g.side
    rows, dim = n2_ref.shape
    tiles = d1_hbm.shape[0]
    shared = max(1, 4 * tiles // 11)
    own_tiles = tiles - (g.parts - 1) * shared
    part_rows = acc_ref.shape[1]

    def start_rows_of(index):
        slot = lax.rem(index, 2)
        at = pl.ds(pl.multiple_of(index * chunk, chunk), chunk)
        for i, (src, dst) in enumerate(((late_hbm, att_ref), (early_hbm, decs_ref))):
            pltpu.make_async_copy(src.at[at, pl.ds(0, dim)], dst.at[slot], rows_sem.at[slot, i]).start()

    def tile_at(index):
        return pl.ds(pl.multiple_of(index * tile, tile), tile)

    def number_of(index):
        rest = index // shared
        return (1 - rest) * (index * g.parts + g.part) + rest * (index + (g.parts - 1) * shared)

    def weights(index):
        slot = lax.rem(index, 2)
        at = tile_at(number_of(index))
        return [pltpu.make_async_copy(src, dst.at[slot], w_sem.at[slot, i]) for i, (src, dst) in enumerate(
            ((w1_hbm.at[:, at], w1_ref), (w3_hbm.at[:, at], w3_ref), (w2_hbm.at[at, :], w2_ref)))]

    def results(index):
        slot, number = lax.rem(index, 2), number_of(index)
        pairs = ((d1_ref, d1_hbm), (d3_ref, d3_hbm), (act_ref, act_hbm))
        return ([pltpu.make_async_copy(src.at[slot], dst.at[number], out_sem.at[slot, i]) for i, (src, dst) in enumerate(pairs)],
                [send(src.at[slot], dst.at[number], share_send.at[slot, i], share_recv.at[i], g.partner)
                 for i, (src, dst) in enumerate(pairs)])

    start_rows_of(0)
    top_load = pltpu.make_async_copy(early_hbm.at[:, pl.ds(dim, dim)], top_ref, top_sem)
    top_load.start()
    for copy in weights(0):
        copy.start()

    def summand(c, core):
        source = gk_hbm if c < heads // g.parts else gv_hbm
        first = ((g.parts * c) % heads + core) * part_rows
        return source.at[pl.ds(pl.multiple_of(first, part_rows), part_rows), :]

    owns = [pltpu.make_async_copy(summand(c, g.part), acc_ref.at[c], own_sem.at[c]) for c in range(heads)]
    for copy in owns:
        copy.start()

    barrier = pltpu.get_barrier_semaphore()

    def signal(step, carry):
        pl.semaphore_signal(barrier, inc=1, device_id={'seq': lax.rem(g.me + step, n)}, device_id_type=MESH)
        return carry

    lax.fori_loop(1, n, signal, 0)
    pl.semaphore_wait(barrier, n - 1)
    for c in range(heads):
        send(summand(c, g.parts - 1 - g.part), pair_ref.at[c], pair_send, pair_recv, g.partner).start()

    grad_query = jnp.concatenate([dqr_ref[h] for h in range(heads)], axis=1)
    grad_normed = dot(grad_query, wq_ref[...])
    x = dec_ref[...].astype(F32)
    inverse = lax.rsqrt(jnp.mean(x * x, axis=-1, keepdims=True) + 1e-6)
    scaled = x * inverse
    inner = grad_normed * gain1_ref[...].astype(F32)
    gdec_ref[...] = gh_ref[...] + inverse * (inner - scaled * jnp.mean(inner * scaled, axis=-1, keepdims=True))
    mine_ref[0:1, :] = jnp.sum(grad_normed * scaled, axis=0, keepdims=True)
    mine_ref[1:2, :] = gnorm_ref[...]

    def give(step, carry):
        send(mine_ref, all_ref.at[g.me], norm_send, norm_recv, lax.rem(g.me + step, n)).start()
        return carry

    lax.fori_loop(1, n, give, 0)
    all_ref[g.me] = mine_ref[...]

    quarter = part_rows // 4
    streams = [(axis, way, pl.ds((2 * axis + (way < 0)) * quarter, quarter)) for axis in (0, 1) for way in (1, -1)]

    def place_of(axis, line, other):
        return other * side + line if axis == 0 else line * side + other

    def pieces(stage, axis, line):
        position = g.row if axis == 0 else g.col
        return [place_of(axis, line, o) for o in range(side)] if stage == 0 else [place_of(axis, line, position)]

    def ring(stage, stream, step):
        axis, way, part = streams[stream]
        axis = axis if stage == 0 else 1 - axis
        here = g.col if axis == 0 else g.row
        ref, sends, recvs = (far_ref, far_send, far_recv) if stage == 0 else (near_ref, near_send, near_recv)
        to = g.near(0, way) if axis == 0 else g.near(way, 0)
        return axis, way, part, here, ref.at[stream, step - 1], sends.at[stream, step - 1], recvs.at[stream, step - 1], to

    def line_of(here, way, step):
        return lax.rem(here - way * step + 2 * side, side)

    def start_step(stage, step):
        for stream in range(4):
            axis, way, part, here, buffer, sem, recv, to = ring(stage, stream, step)
            for i, c in enumerate(pieces(stage, axis, line_of(here, way, step))):
                send(acc_ref.at[c, part], buffer.at[i], sem, recv, to).start()

    def end_step(stage, step):
        for stream in range(4):
            axis, way, part, here, buffer, sem, recv, to = ring(stage, stream, step)
            whole = send(buffer, buffer, sem, recv, g.me)
            whole.wait_recv()
            for i, c in enumerate(pieces(stage, axis, line_of(here, way, step + 1))):
                acc_ref[c, part, :] = acc_ref[c, part, :] + buffer[i]
            whole.wait_send()

    def add_pair():
        for copy in owns:
            copy.wait()
        whole = send(pair_ref, pair_ref, pair_send, pair_recv, g.me)
        whole.wait_recv()

        def add(c, carry):
            acc_ref[c] = acc_ref[c] + pair_ref[c]
            return carry

        lax.fori_loop(0, heads, add, 0)
        whole.wait_send()

    def first():
        add_pair()
        start_step(0, 1)

    def turn():
        end_step(0, side - 1)
        start_step(1, 1)

    def between(stage, step):
        def body():
            end_step(stage, step)
            start_step(stage, step + 1)
        return body

    def prepare(index, carry):
        slot = lax.rem(index, 2)
        at = pl.ds(pl.multiple_of(index * chunk, chunk), chunk)
        for i, (src, dst) in enumerate(((late_hbm, att_ref), (early_hbm, decs_ref))):
            pltpu.make_async_copy(src.at[at, pl.ds(0, dim)], dst.at[slot], rows_sem.at[slot, i]).wait()

        @pl.when(index + 1 < rows // chunk)
        def _():
            start_rows_of(index + 1)

        pl.when(index == rows // chunk // 2)(first)
        dec = decs_ref[slot].astype(F32)
        hidden = (dec + dot(att_ref[slot], wo_ref[...])).astype(BF16).astype(F32)
        n2_ref[at, :] = rms_norm(hidden, gain2_ref[...].astype(F32)).astype(BF16)
        return carry

    lax.fori_loop(0, rows // chunk, prepare, 0)
    top_load.wait()
    n2_store = pltpu.make_async_copy(n2_ref, n2_hbm, n2_sem)
    n2_store.start()

    events = ([between(0, t) for t in range(1, side - 1)] + [turn] + [between(1, t) for t in range(1, side - 1)]
              + [lambda: end_step(1, side - 1)])
    at_tile = (1, 3, 5, 6)
    inside = own_tiles > at_tile[-1] and len(events) > len(at_tile)

    def finish_results(index):
        stores, shares = results(index)
        for copy in stores:
            copy.wait()

        @pl.when(index < shared)
        def _():
            for copy in shares:
                copy.wait_send()

    def activations(index, carry):
        slot = lax.rem(index, 2)
        for copy in weights(index):
            copy.wait()

        @pl.when(index + 1 < own_tiles)
        def _():
            for copy in weights(index + 1):
                copy.start()

        @pl.when(index >= 2)
        def _():
            finish_results(index - 2)

        if inside:
            for event, when in zip(events, at_tile):
                pl.when(index == when)(event)

        w1, w3, w2t = w1_ref[slot], w3_ref[slot], w2_ref[slot].T
        for first_row in range(0, rows, chunk):
            part = slice(first_row, first_row + chunk)
            gate = dot(n2_ref[part, :], w1)
            up = dot(n2_ref[part, :], w3)
            grad = dot(top_ref[part, :], w2t)
            sig = jax.nn.sigmoid(gate)
            silu = gate * sig
            act_ref[slot, part, :] = (silu * up).astype(BF16)
            d3_ref[slot, part, :] = (grad * silu).astype(BF16)
            d1_ref[slot, part, :] = (grad * up * (sig + silu * (1.0 - sig))).astype(BF16)
        stores, shares = results(index)
        for copy in stores:
            copy.start()

        @pl.when(index < shared)
        def _():
            for copy in shares:
                copy.start()
        return carry

    lax.fori_loop(0, own_tiles, activations, 0)
    for event in events[len(at_tile):] if inside else events:
        event()
    sums_ref[...] = acc_ref[g.chip]

    others = all_ref.at[pl.ds(0, n - 1)]
    whole = send(others, others, norm_send, norm_recv, g.me)
    whole.wait_send()
    whole.wait_recv()
    norms_ref[...] = jnp.sum(all_ref[...], axis=0)
    n2_store.wait()
    for index in range(max(own_tiles - 2, 0), own_tiles):
        finish_results(index)
    for i, ref in enumerate((d1_hbm, d3_hbm, act_hbm)):
        come = ref.at[pl.ds(0, shared)]
        send(come, come, share_send.at[0, i], share_recv.at[i], g.me).wait_recv()


def reduce_sums(n, heads, collective_id, gk, gv, early, late, w_gate, w_up, w_down, wo, wq, gain1, gain2, dq_rows, dec_in, gh, gnorm):
    rows, dim = early.shape[0], gk.shape[1]
    ff, tile, chunk = w_gate.shape[1], 256, min(512, early.shape[0] // 2)
    part_rows = 2 * gk.shape[0] // n
    side = math.isqrt(heads)
    hbm = pl.BlockSpec(memory_space=pl.ANY)
    return pl.pallas_call(
        functools.partial(reduce_kernel, n, heads, tile, chunk),
        out_shape=[shape((part_rows, dim), F32), shape(gh.shape, F32), shape((2, dim), F32), shape((rows, dim), BF16)]
        + [shape((ff // tile, rows, tile), BF16)] * 3,
        in_specs=[hbm] * 7 + vmem(8),
        out_specs=vmem(3) + [hbm] * 4,
        scratch_shapes=[pltpu.VMEM((heads, part_rows, dim), F32)] * 2
        + [pltpu.VMEM((4, side - 1, side, part_rows // 4, dim), F32), pltpu.VMEM((4, side - 1, 1, part_rows // 4, dim), F32)]
        + [pltpu.VMEM((rows, dim), BF16)] * 2 + [pltpu.VMEM((2, chunk, dim), BF16)] * 2
        + [pltpu.VMEM((2, dim, tile), BF16)] * 2 + [pltpu.VMEM((2, tile, dim), BF16)] + [pltpu.VMEM((2, rows, tile), BF16)] * 3
        + [pltpu.VMEM((2, dim), F32), pltpu.VMEM((n, 2, dim), F32)]
        + [dma(heads), dma(2, 3), dma(3), pltpu.SemaphoreType.DMA, pltpu.SemaphoreType.DMA, dma(4, side - 1), dma(4, side - 1), dma(4, side - 1),
           dma(4, side - 1), dma(2, 2), pltpu.SemaphoreType.DMA, dma(2, 3), dma(2, 3), pltpu.SemaphoreType.DMA,
           pltpu.SemaphoreType.DMA, pltpu.SemaphoreType.DMA],
        compiler_params=remote(collective_id),
        cost_estimate=pl.CostEstimate(flops=6 * rows * dim * ff, bytes_accessed=12 * rows * ff, transcendentals=rows * ff),
        name='reduce_sums',
    )(gk, gv, early, late, w_gate, w_up, w_down, wo, wq, gain1, gain2, dq_rows, dec_in, gh, gnorm)


def gate_up_kernel(n2_ref, d1_ref, d3_ref, g1_ref, g3_ref, n2t_ref):
    @pl.when(pl.program_id(0) == 0)
    def _():
        n2t_ref[...] = n2_ref[...].T

    g1_ref[...] = dot(n2t_ref[...], d1_ref[...])
    g3_ref[...] = dot(n2t_ref[...], d3_ref[...])


def gate_up_grads(n2, d1, d3):
    rows, dim = n2.shape
    tiles, _, tile = d1.shape
    cols = pl.BlockSpec((dim, tile), lambda i: (0, i))
    part = pl.BlockSpec((pl.Squeezed(), rows, tile), lambda i: (i, 0, 0))
    return pl.pallas_call(
        gate_up_kernel,
        out_shape=[shape((dim, tiles * tile), F32)] * 2,
        grid=(tiles,),
        in_specs=[full(n2), part, part],
        out_specs=[cols, cols],
        scratch_shapes=[pltpu.VMEM((dim, rows), BF16)],
        compiler_params=plain(),
        cost_estimate=pl.CostEstimate(flops=4 * rows * dim * tiles * tile, bytes_accessed=12 * dim * tiles * tile, transcendentals=0),
        name='gate_up_grads',
    )(n2, d1, d3)


def down_kernel(top_ref, act_ref, k_in_ref, v_in_ref, g2_ref, k_ref, v_ref):
    g2_ref[...] = dot_tn(act_ref[...], top_ref[...])
    k_ref[...] = k_in_ref[...]
    v_ref[...] = v_in_ref[...]


def down_grad(early, act, total):
    rows, dim = early.shape[0], early.shape[1] // 2
    tiles, _, tile = act.shape
    blocks = 1 << (tiles.bit_length() - 1)
    height = total.shape[0] // 2 // blocks
    block = lambda first: pl.BlockSpec((height, dim), lambda i: (jnp.minimum(i, blocks - 1) + first, 0))
    return pl.pallas_call(
        down_kernel,
        out_shape=[shape((tiles * tile, dim), F32)] + [shape((total.shape[0] // 2, dim), F32)] * 2,
        grid=(tiles,),
        in_specs=[pl.BlockSpec((rows, dim), lambda i: (0, 1), pipeline_mode=pl.Buffered(1)),
                  pl.BlockSpec((pl.Squeezed(), rows, tile), lambda i: (i, 0, 0)), block(0), block(blocks)],
        out_specs=[pl.BlockSpec((tile, dim), lambda i: (i, 0)), block(0), block(0)],
        compiler_params=plain(),
        cost_estimate=pl.CostEstimate(flops=2 * rows * dim * tiles * tile, bytes_accessed=12 * dim * tiles * tile, transcendentals=0),
        name='down_grad',
    )(early, act, total, total)


def memory_weight_kernel(memory_ref, dkv_ref, gk_ref, gv_ref):
    group, hd = dkv_ref.shape[0], dkv_ref.shape[2] // 2
    for i in range(group):
        both = dot_tn(dkv_ref[i], memory_ref[...])
        gk_ref[i * hd:(i + 1) * hd, :] = both[:hd]
        gv_ref[i * hd:(i + 1) * hd, :] = both[hd:]


def memory_weight_grads(memory, dkv):
    heads, rows, width = dkv.shape
    dim, hd = memory.shape[1], width // 2
    group = 4
    out = pl.BlockSpec((group * hd, dim), lambda i: (i, 0))
    return pl.pallas_call(
        memory_weight_kernel,
        out_shape=[shape((heads * hd, dim), F32)] * 2,
        grid=(heads // group,),
        in_specs=[full(memory), pl.BlockSpec((group, rows, width), lambda i: (i, 0, 0))],
        out_specs=[out, out],
        compiler_params=plain(),
        cost_estimate=pl.CostEstimate(flops=2 * rows * dim * heads * width, bytes_accessed=16 * rows * dim, transcendentals=0),
        name='memory_weight_grads',
    )(memory, dkv)


def memory_grad_kernel(dkv_ref, wk_ref, wv_ref, gq_in_ref, out_ref, gq_ref):
    group = dkv_ref.shape[0]
    gq_ref[...] = gq_in_ref[...]
    left = jnp.concatenate([dkv_ref[i] for i in range(group)], axis=1)
    right = jnp.concatenate([part[i] for i in range(group) for part in (wk_ref, wv_ref)], axis=0)

    @pl.when(pl.program_id(0) == 0)
    def _():
        out_ref[...] = dot(left, right)

    @pl.when(pl.program_id(0) > 0)
    def _():
        out_ref[...] += dot(left, right)


def memory_grad(dkv, wk_t, wv_t, gq):
    heads, rows, width = dkv.shape
    hd, dim = wk_t.shape[1], wk_t.shape[2]
    group = 4
    weight = pl.BlockSpec((group, hd, dim), lambda i: (i, 0, 0))
    passing = pl.BlockSpec((group * hd, dim), lambda i: (i, 0))
    return pl.pallas_call(
        memory_grad_kernel,
        out_shape=[shape((rows, dim), F32), shape(gq.shape, F32)],
        grid=(heads // group,),
        in_specs=[pl.BlockSpec((group, rows, width), lambda i: (i, 0, 0)), weight, weight, passing],
        out_specs=[pl.BlockSpec((rows, dim), lambda i: (0, 0)), passing],
        compiler_params=plain(),
        cost_estimate=pl.CostEstimate(flops=2 * rows * dim * heads * width, bytes_accessed=12 * rows * dim, transcendentals=0),
        name='memory_grad',
    )(dkv, wk_t, wv_t, gq)


def outer_kernel(att_ref, gh_ref, out_ref):
    @pl.when(pl.program_id(0) == 0)
    def _():
        out_ref[...] = jnp.zeros_like(out_ref)

    out_ref[...] += dot_tn(att_ref[...], gh_ref[...])


def outer_weight_grad(late, dim):
    rows = late.shape[0]
    chunk = min(512, rows)
    return pl.pallas_call(
        outer_kernel,
        out_shape=shape((dim, dim), F32),
        grid=(rows // chunk,),
        in_specs=[pl.BlockSpec((chunk, dim), lambda i: (i, 0)), pl.BlockSpec((chunk, dim), lambda i: (i, 1))],
        out_specs=pl.BlockSpec((dim, dim), lambda i: (0, 0)),
        compiler_params=plain(),
        cost_estimate=pl.CostEstimate(flops=2 * rows * dim * dim, bytes_accessed=8 * rows * dim, transcendentals=0),
        name='outer_weight_grad',
    )(late, late)


def solution(mesh):
    n = mesh.shape['seq']
    row_spec = P(('data', 'seq'), None)
    weight_spec = P()
    part_vec = P('data')
    part_mat = P('data', None)
    part_cube = P('data', None, None)

    def device_step(dec_in, memory, mem_len, grad_out, norm_attn, wq_cross, wk_cross, wv_cross, wo_cross, norm_mlp, w_gate, w_up, w_down):
        q_rows, dim = dec_in.shape
        heads, hd = wq_cross.shape[1], wq_cross.shape[2]
        parts = n // heads
        sources = -(-3 * n // 4)
        total_q = q_rows * n
        key_scale = hd ** -0.5
        scale = key_scale * LOG2E
        wq_t, wk_t, wv_t = (jnp.transpose(w, (1, 2, 0)) for w in (wq_cross, wk_cross, wv_cross))
        source_rows = -(-sources // (parts * math.isqrt(heads)))
        kv, q_in, early_local = exchange(n, heads, source_rows, 0, memory, dec_in, grad_out, norm_attn, wk_t, wv_t, wq_t)
        head_q = q_in.reshape(total_q, 2 * hd)

        early = lax.all_gather(early_local, 'seq', axis=0, tiled=True)

        wo = wo_cross.reshape(heads * hd, dim)
        mine = attention_forward(scale, hd, parts, sources, mem_len, kv, head_q)
        out_t, lse, do_in, factors, grad_hidden, g_norm_mlp = decoder_rows(
            n, heads, 1, mine, dec_in, grad_out, norm_mlp, wo, w_gate, w_up, w_down)
        do_in, factors = lax.optimization_barrier((do_in, factors))
        late = lax.all_gather(factors, 'seq', axis=0, tiled=True)

        dkv, dq_part = attention_backward(scale, key_scale, hd, parts, sources, mem_len, kv, head_q, do_in.reshape(total_q, 2 * hd), out_t, lse)
        dkv_in, dq_rows, gq_share = return_blocks(n, heads, source_rows, 4, dkv, dq_part, norm_attn, early)
        dkv_in, dq_rows, gq_share, late = lax.optimization_barrier((dkv_in, dq_rows, gq_share, late))
        g_wq = lax.all_gather(gq_share, 'seq', axis=0, tiled=True)

        gk_part, gv_part = memory_weight_grads(memory, dkv_in)
        sums, g_dec, norms, n2_all, d1, d3, act = reduce_sums(
            n, heads, 5, gk_part, gv_part, early, late, w_gate, w_up, w_down, wo, wq_t.reshape(heads * hd, dim), norm_attn, norm_mlp,
            dq_rows, dec_in, grad_hidden, g_norm_mlp)
        sums, n2_all, d1, d3, act, dkv_in, late, early, g_wq = lax.optimization_barrier(
            (sums, n2_all, d1, d3, act, dkv_in, late, early, g_wq))
        total = lax.all_gather(sums, 'seq', axis=0, tiled=True)
        g_wo = outer_weight_grad(late, dim)
        g_mem, g_wq = memory_grad(dkv_in, wk_t, wv_t, g_wq)
        g_gate, g_up = gate_up_grads(n2_all, d1, d3)
        g_down, g_wk, g_wv = down_grad(early, act, total)

        cube = lambda g: jnp.transpose(g.reshape(heads, hd, dim), (2, 0, 1))
        return (g_dec, g_mem, norms[0], cube(g_wq), cube(g_wk), cube(g_wv), g_wo.reshape(heads, hd, dim), norms[1], g_gate, g_up, g_down)

    return jax.shard_map(device_step, mesh=mesh,
                         in_specs=(row_spec, row_spec, part_vec, row_spec) + (weight_spec,) * 9,
                         out_specs=(row_spec, row_spec, part_vec, part_cube, part_cube, part_cube, part_cube, part_vec, part_mat, part_mat, part_mat),
                         check_vma=False)
```

```python
import functools
import math

import jax
import jax.numpy as jnp
from jax import lax
from jax.experimental import pallas as pl
from jax.experimental.pallas import tpu as pltpu
from jax.sharding import PartitionSpec as P

LOG2E = 1.4426950408889634
NEG = -1e30
VMEM_LIMIT = 60 * 1024 * 1024
MESH = pl.DeviceIdType.MESH
BF16, F32 = jnp.bfloat16, jnp.float32


def rms_norm(tensor, gain):
    mean_sq = jnp.mean(tensor * tensor, axis=-1, keepdims=True)
    return tensor * lax.rsqrt(mean_sq + 1e-6) * gain


def dot(a, b):
    return jnp.dot(a, b, preferred_element_type=F32)


def dot_nt(a, b):
    return lax.dot_general(a, b, (((1,), (1,)), ((), ())), preferred_element_type=F32)


def dot_tn(a, b):
    return lax.dot_general(a, b, (((0,), (0,)), ((), ())), preferred_element_type=F32)


def full(array):
    return pl.BlockSpec(array.shape, lambda *_: (0,) * array.ndim, pipeline_mode=pl.Buffered(1))


def vmem(count):
    return [pl.BlockSpec(memory_space=pltpu.VMEM)] * count


def plain():
    return pltpu.CompilerParams(vmem_limit_bytes=VMEM_LIMIT)


def remote(collective_id):
    return pltpu.CompilerParams(collective_id=collective_id, has_side_effects=True, vmem_limit_bytes=VMEM_LIMIT)


def shape(dims, dtype):
    return jax.ShapeDtypeStruct(dims, dtype)


def meet(peers):
    barrier = pltpu.get_barrier_semaphore()
    for peer in peers:
        pl.semaphore_signal(barrier, inc=1, device_id={'seq': peer}, device_id_type=MESH)
    pl.semaphore_wait(barrier, len(peers))


def send(src, dst, send_sem, recv_sem, peer):
    return pltpu.make_async_remote_copy(src_ref=src, dst_ref=dst, send_sem=send_sem, recv_sem=recv_sem,
                                        device_id={'seq': peer}, device_id_type=MESH)


class Grid:
    def __init__(self, n, heads, source_rows):
        self.n, self.heads, self.source_rows = n, heads, source_rows
        self.parts = n // heads
        self.side = math.isqrt(heads)
        self.me = lax.axis_index('seq')
        self.part = lax.rem(self.me, self.parts)
        self.chip = self.me // self.parts
        self.col = lax.rem(self.chip, self.side)
        self.row = self.chip // self.side
        self.partner = self.chip * self.parts + (self.parts - 1 - self.part)
        self.ties = self.side == 4
        self.direct = (1, 3) if self.ties else (1,)

    def wrap(self, value):
        return lax.rem(value + self.side, self.side)

    def device(self, row, col, part):
        return (row * self.side + col) * self.parts + part

    def near(self, drow, dcol, part=None):
        return self.device(self.wrap(self.row + drow), self.wrap(self.col + dcol), self.part if part is None else part)

    def hop(self, offset):
        return 1 if offset == 1 else -1

    def is_source(self, row):
        return self.wrap(row) < self.source_rows

    def row_peers(self):
        return [lax.rem(self.chip + step, self.heads) * self.parts + self.part for step in range(1, self.heads)]

    def peers(self):
        return self.row_peers() + [self.partner] + [self.near(0, self.hop(d), self.parts - 1 - self.part) for d in self.direct]


def pair_peers(n, heads, me, part):
    parts = n // heads
    head = me // parts
    partner = head * parts + (parts - 1 - part)
    return partner, [partner] + [lax.rem(head + step, heads) * parts + part for step in range(1, heads)]


def pack(rows):
    middle = rows.shape[-2] // 2
    return jnp.concatenate([rows[..., :middle, :], rows[..., middle:, :]], axis=-1)


def unpack(packed):
    middle = packed.shape[-1] // 2
    return jnp.concatenate([packed[..., :middle], packed[..., middle:]], axis=-2)


def start_rows(n, heads, me, part, src, src_of, dst_ref, send_sem, recv_sem):
    parts = n // heads
    head = me // parts
    for step in range(1, heads):
        peer = lax.rem(head + step, heads) * parts + part
        send(src.at[src_of(peer)], dst_ref.at[head], send_sem, recv_sem, peer).start()
    dst_ref[head] = src[src_of(me)]


def wait_rows(heads, me, dst_ref, send_sem, recv_sem):
    others = dst_ref.at[pl.ds(0, heads - 1)]
    whole = send(others, others, send_sem, recv_sem, me)
    whole.wait_send()
    whole.wait_recv()


def swap(src, dst, send_sem, recv_sem, partner):
    copy = send(src, dst, send_sem, recv_sem, partner)
    copy.start()
    copy.wait()


def place(n, heads, part, mine_ref, theirs_ref, wide_ref, low, unroll):
    parts = n // heads
    for source, index in ((mine_ref, part), (theirs_ref, parts - 1 - part)):
        def one(head, carry, source=source, index=index):
            rows = unpack(source[head])
            zeros = jnp.zeros_like(rows)
            wide_ref[head * parts + index] = jnp.concatenate([rows, zeros] if low else [zeros, rows], axis=-1)
            return carry

        if unroll:
            for head in range(heads):
                one(head, 0)
        else:
            lax.fori_loop(0, heads, one, 0)


def exchange_kernel(n, heads, source_rows, memory_ref, dec_ref, gout_ref, gain_ref, wk_ref, wv_ref, wq_ref, kv_out_ref, q_out_ref, early_ref,
                    kv_ref, stage_ref, up_ref, down_ref, right_ref, left_ref, packed_ref, got_ref, swapped_ref,
                    row_send, row_recv, y_send, pass_send, x_send, fwd_send, stage_recv, up_recv, down_recv, right_recv,
                    left_recv, out_recv):
    g = Grid(n, heads, source_rows)
    side, hd = g.side, wk_ref.shape[1]
    half = kv_out_ref.shape[1]
    chunk_rows = min(256, kv_ref.shape[1])
    barrier = pltpu.get_barrier_semaphore()
    peers = g.peers()
    for peer in peers:
        pl.semaphore_signal(barrier, inc=1, device_id={'seq': peer}, device_id_type=MESH)

    dim = dec_ref.shape[1]
    early_ref[:, :dim] = dec_ref[...]
    early_ref[:, dim:] = gout_ref[...].astype(BF16)
    normed = rms_norm(dec_ref[...].astype(F32), gain_ref[...].astype(F32)).astype(BF16)

    def some_heads(index, carry):
        queries = dot_nt(normed, jnp.concatenate([wq_ref[4 * index + j] for j in range(4)], axis=0)).astype(BF16)
        for j in range(4):
            packed_ref[4 * index + j] = pack(queries[:, hd * j:hd * (j + 1)])
        return carry

    lax.fori_loop(0, heads // 4, some_heads, 0)

    def head(drow, dcol):
        return g.wrap(g.row + drow) * side + g.wrap(g.col + dcol)

    def project(drow, dcols):
        weights = jnp.concatenate([ref[head(drow, d)] for d in dcols for ref in (wk_ref, wv_ref)], axis=0)

        def rows(index, carry):
            at = pl.ds(pl.multiple_of(index * chunk_rows, chunk_rows), chunk_rows)
            both = dot_nt(memory_ref[at, :], weights).astype(BF16)
            for i, d in enumerate(dcols):
                kv_ref[head(drow, d), at, :] = both[:, 2 * hd * i:2 * hd * (i + 1)]
            return carry

        lax.fori_loop(0, kv_ref.shape[1] // chunk_rows, rows, 0)

    def along_column(drow, dcol):
        chunk = kv_ref.at[head(drow, dcol)]
        if drow in g.direct:
            send(chunk, stage_ref.at[drow - 1, dcol], y_send.at[drow - 1], stage_recv.at[drow - 1, dcol], g.near(g.hop(drow), 0)).start()
        elif dcol % 2 == 0:
            send(chunk, up_ref.at[dcol // 2], y_send.at[drow - 1], up_recv.at[dcol // 2], g.near(1, 0)).start()
        else:
            send(chunk, down_ref.at[dcol // 2], y_send.at[drow - 1], down_recv.at[dcol // 2], g.near(-1, 0)).start()

    def along_row(o, dcol):
        chunk = kv_ref.at[head(0, dcol)] if o == 0 else stage_ref.at[o - 1, dcol]
        source = g.device(g.wrap(g.row - o), g.col, g.part)
        if dcol == 0:
            kv_out_ref[source] = chunk[pl.ds(pl.multiple_of(g.part * half, half), half), :]
            away = pl.ds(pl.multiple_of((g.parts - 1 - g.part) * half, half), half)
            send(chunk.at[away], kv_out_ref.at[source], x_send.at[o], out_recv, g.partner).start()
        elif dcol in g.direct:
            for part in range(g.parts):
                send(chunk.at[pl.ds(part * half, half)], kv_out_ref.at[source], x_send.at[o], out_recv,
                     g.near(0, g.hop(dcol), part)).start()
        else:
            send(chunk.at[pl.ds(0, half)], right_ref.at[o], x_send.at[o], right_recv.at[o], g.near(0, 1)).start()
            send(chunk.at[pl.ds(half, half)], left_ref.at[o], x_send.at[o], left_recv.at[o], g.near(0, -1)).start()

    def pass_row(o):
        for ref, sem, come in ((right_ref, right_recv, -1), (left_ref, left_recv, 1)):
            source = g.device(g.wrap(g.row - o), g.wrap(g.col + come), g.part)
            send(ref.at[o], ref.at[o], fwd_send.at[o], sem.at[o], g.me).wait_recv()
            send(ref.at[o], kv_out_ref.at[source], fwd_send.at[o], out_recv, g.near(0, -come, 0 if come < 0 else 1)).start()

    def when_source(row, body):
        pl.when(g.is_source(row))(body)

    if g.ties:
        order = [(2, (2, 1)), (2, (3, 0)), (1, (2, 1)), (3, (2, 3)), (0, (2, 1)), (0, (3, 0))]
        last = [(1, (3, 0)), (3, (1, 0))]
    else:
        order, last = [(1, (1, 0)), (0, (1, 0))], []

    def issue(drow, dcols):
        def body():
            for d in dcols:
                along_row(0, d) if drow == 0 else along_column(drow, d)
        when_source(g.row, body)

    waiting = None
    for drow, dcols in order + last:
        project(drow, dcols)
        if waiting is None:
            pl.semaphore_wait(barrier, len(peers))
            start_rows(n, heads, g.me, g.part, packed_ref, lambda peer: peer // g.parts, got_ref, row_send.at[0], row_recv.at[0])
        elif waiting not in last:
            issue(*waiting)
        waiting = (drow, dcols)
    if not last:
        issue(*waiting)

    if g.ties:
        def up(i):
            send(up_ref.at[i], up_ref.at[i], pass_send.at[0], up_recv.at[i], g.me).wait_recv()
            send(up_ref.at[i], stage_ref.at[1, 2 * i], pass_send.at[0], stage_recv.at[1, 2 * i], g.near(1, 0)).start()

        def down(i):
            send(down_ref.at[i], down_ref.at[i], pass_send.at[1], down_recv.at[i], g.me).wait_recv()
            send(down_ref.at[i], stage_ref.at[1, 2 * i + 1], pass_send.at[1], stage_recv.at[1, 2 * i + 1], g.near(-1, 0)).start()

        for i in range(2):
            when_source(g.row - 1, lambda i=i: up(1 - i))
            when_source(g.row + 1, lambda i=i: down(i))
        for drow, dcols in last:
            issue(drow, dcols)
        when_source(g.row, lambda: pass_row(0))

    wait_rows(heads, g.me, got_ref, row_send.at[0], row_recv.at[0])
    swap(got_ref, swapped_ref, row_send.at[1], row_recv.at[1], g.partner)
    place(n, heads, g.part, got_ref, swapped_ref, q_out_ref, True, False)

    def arrived(o, dcol):
        def body():
            send(stage_ref.at[o - 1, dcol], stage_ref.at[o - 1, dcol], y_send.at[0], stage_recv.at[o - 1, dcol], g.me).wait_recv()
            along_row(o, dcol)
        when_source(g.row - o, body)

    if g.ties:
        for o, d in ((1, 2), (3, 2), (1, 1), (3, 3)):
            arrived(o, d)
        for o in g.direct:
            when_source(g.row - o, lambda o=o: pass_row(o))
        for d in (2, 1, 0, 3):
            arrived(2, d)
        when_source(g.row - 2, lambda: pass_row(2))
        for o, d in ((1, 3), (3, 1), (1, 0), (3, 0)):
            arrived(o, d)
    else:
        for d in (1, 0):
            arrived(1, d)

    def sent(sem, ref):
        send(ref, ref, sem, out_recv, g.me).wait_send()

    def mine():
        for drow in range(1, side):
            sent(y_send.at[drow - 1], stage_ref.at[0])
    when_source(g.row, mine)
    for o in range(side):
        def passed(o=o):
            sent(x_send.at[o], kv_out_ref.at[pl.ds(0, g.parts * side - 1)])
            if g.ties:
                sent(fwd_send.at[o], kv_out_ref.at[pl.ds(0, 2)])
        when_source(g.row - o, passed)
    if g.ties:
        when_source(g.row - 1, lambda: sent(pass_send.at[0], up_ref))
        when_source(g.row + 1, lambda: sent(pass_send.at[1], down_ref))
    blocks = source_rows * side * g.parts
    others = kv_out_ref.at[pl.ds(0, blocks - source_rows)]
    send(others, others, y_send.at[0], out_recv, g.me).wait_recv()


def row_scratch(heads, q_rows, hd):
    return [pltpu.VMEM((heads, q_rows // 2, 2 * hd), BF16)] * 3


def dma(*dims):
    return pltpu.SemaphoreType.DMA(dims)


def exchange(n, heads, source_rows, collective_id, memory, dec_in, grad_out, gain, wk_t, wv_t, wq_t):
    m_rows, q_rows, hd = memory.shape[0], dec_in.shape[0], wk_t.shape[1]
    side, parts = math.isqrt(heads), n // heads
    half = m_rows // parts
    chunk = lambda *lead: pltpu.VMEM(lead + (m_rows, 2 * hd), BF16)
    block = lambda *lead: pltpu.VMEM(lead + (half, 2 * hd), BF16)
    return pl.pallas_call(
        functools.partial(exchange_kernel, n, heads, source_rows),
        out_shape=[shape((n, half, 2 * hd), BF16), shape((n, q_rows, 2 * hd), BF16), shape((q_rows, 2 * dec_in.shape[1]), BF16)],
        in_specs=vmem(7),
        out_specs=vmem(3),
        scratch_shapes=[chunk(heads), chunk(side - 1, side), chunk(2), chunk(2), block(side), block(side)]
        + row_scratch(heads, q_rows, hd)
        + [dma(2), dma(2), dma(side - 1), dma(2), dma(side), dma(side), dma(side - 1, side), dma(2), dma(2), dma(side), dma(side),
           pltpu.SemaphoreType.DMA],
        compiler_params=remote(collective_id),
        name='exchange',
    )(memory, dec_in, grad_out, gain, wk_t, wv_t, wq_t)


def return_kernel(n, heads, source_rows, chunk, src_ref, dq_ref, gain_ref, early_hbm, dst_ref, rows_ref, gq_ref, stage_ref, right_ref,
                  left_ref, up_ref, down_ref, theirs_ref, packed_ref, got_ref, dqt_ref, decs_ref, dec_sem, row_send, row_recv,
                  x_send, fwd_send, y_send, pass_send, stage_recv, right_recv, left_recv, up_recv, down_recv, out_recv):
    g = Grid(n, heads, source_rows)
    side = g.side
    half = src_ref.shape[1]
    total_rows, dim = dqt_ref.shape[1], gq_ref.shape[1]

    def dec_load(index, slot):
        at = pl.ds(pl.multiple_of(index * chunk, chunk), chunk)
        return pltpu.make_async_copy(early_hbm.at[at, pl.ds(0, dim)], decs_ref.at[slot], dec_sem.at[slot])

    dec_load(0, 0).start()
    meet(g.peers())
    mine = pl.ds(pl.multiple_of(g.part * half, half), half)

    def landing(drow, dcol, head_col):
        if drow == 0:
            return dst_ref.at[g.row * side + head_col, mine], out_recv
        return stage_ref.at[drow - 1, dcol, mine], stage_recv.at[drow - 1, dcol]

    def along_row(drow, dcol):
        row = g.wrap(g.row + drow)
        col = g.wrap(g.col + dcol)
        for part in range(g.parts):
            source = src_ref.at[g.device(row, col, part)]
            if dcol in g.direct:
                dst, sem = landing(drow, dcol, g.col)
                send(source, dst, x_send.at[drow], sem, g.near(0, g.hop(dcol), part)).start()
            elif part == 0:
                send(source, right_ref.at[drow], x_send.at[drow], right_recv.at[drow], g.near(0, 1)).start()
            else:
                send(source, left_ref.at[drow], x_send.at[drow], left_recv.at[drow], g.near(0, -1)).start()

    def own_chip(drow):
        row = g.wrap(g.row + drow)
        away = src_ref.at[g.device(row, g.col, g.parts - 1 - g.part)]
        dst, sem = landing(drow, 0, g.col)
        dst[...] = src_ref[g.device(row, g.col, g.part)]
        send(away, dst, x_send.at[drow], sem, g.partner).start()

    def pass_row(drow):
        for ref, come_sem, come in ((right_ref, right_recv, -1), (left_ref, left_recv, 1)):
            send(ref.at[drow], ref.at[drow], fwd_send.at[drow], come_sem.at[drow], g.me).wait_recv()
            dst, sem = landing(drow, 2, g.wrap(g.col + come))
            send(ref.at[drow], dst, fwd_send.at[drow], sem, g.near(0, -come, 0 if come < 0 else 1)).start()

    def along_column(drow, dcol):
        chunk = stage_ref.at[drow - 1, dcol]
        got = chunk.at[pl.ds(0, half)] if dcol == 0 else chunk
        send(got, got, y_send.at[drow - 1], stage_recv.at[drow - 1, dcol], g.me).wait_recv()
        head = g.row * side + g.wrap(g.col - dcol)
        if drow in g.direct:
            send(chunk, dst_ref.at[head], y_send.at[drow - 1], out_recv, g.near(g.hop(drow), 0)).start()
        elif dcol % 2 == 0:
            send(chunk, up_ref.at[dcol // 2], y_send.at[drow - 1], up_recv.at[dcol // 2], g.near(1, 0)).start()
        else:
            send(chunk, down_ref.at[dcol // 2], y_send.at[drow - 1], down_recv.at[dcol // 2], g.near(-1, 0)).start()

    def when_source(row, body):
        pl.when(g.is_source(row))(body)

    def rows_of(drow):
        def body():
            for d in (2, 1, 3) if g.ties else (1,):
                along_row(drow, d)
        when_source(g.row + drow, body)

    def relay(drow):
        when_source(g.row + drow, lambda: pass_row(drow))

    def column(drow, d):
        when_source(g.row + drow, lambda: along_column(drow, d))

    def up(i):
        def body():
            send(up_ref.at[i], up_ref.at[i], pass_send.at[0], up_recv.at[i], g.me).wait_recv()
            head = g.wrap(g.row - 1) * side + g.wrap(g.col - 2 * i)
            send(up_ref.at[i], dst_ref.at[head], pass_send.at[0], out_recv, g.near(1, 0)).start()
        when_source(g.row + 1, body)

    def down(i):
        def body():
            send(down_ref.at[i], down_ref.at[i], pass_send.at[1], down_recv.at[i], g.me).wait_recv()
            head = g.wrap(g.row + 1) * side + g.wrap(g.col - 2 * i - 1)
            send(down_ref.at[i], dst_ref.at[head], pass_send.at[1], out_recv, g.near(-1, 0)).start()
        when_source(g.row - 1, body)

    def start_dq():
        swap(dq_ref, theirs_ref, row_send.at[0], row_recv.at[0], g.partner)
        both = (dq_ref[...] + theirs_ref[...]).astype(BF16)
        share = dqt_ref.shape[0]
        dqt_ref[...] = jnp.where(g.part == 0, both[:share], both[share:])
        total = both.T
        packed_ref[...] = pack(total.reshape(n, total.shape[0] // n, total.shape[1]))
        start_rows(n, heads, g.me, g.part, packed_ref, lambda peer: peer, got_ref, row_send.at[1], row_recv.at[1])

    def query_weight(index, carry):
        slot = lax.rem(index, 2)
        dec_load(index, slot).wait()

        @pl.when(index + 1 < chunks)
        def _():
            dec_load(index + 1, 1 - slot).start()

        normed = rms_norm(decs_ref[slot].astype(F32), gain_ref[...].astype(F32)).astype(BF16)
        gq_ref[...] += dot(dqt_ref[:, pl.ds(pl.multiple_of(index * chunk, chunk), chunk)], normed)
        return carry

    chunks = total_rows // chunk
    for drow in (2, 1, 3, 0) if g.ties else (1, 0):
        when_source(g.row + drow, lambda drow=drow: own_chip(drow))
    if g.ties:
        rows_of(2)
        for drow in (2, 1, 3):
            column(drow, 0)
        relay(2)
        rows_of(1)
        column(2, 1)
        column(2, 3)
        column(2, 2)
        relay(1)
        rows_of(3)
        start_dq()
        up(0)
        down(0)
        column(1, 1)
        column(1, 3)
        column(1, 2)
        relay(3)
        rows_of(0)
        up(1)
        down(1)
        column(3, 1)
        column(3, 3)
        column(3, 2)
        relay(0)
    else:
        rows_of(1)
        rows_of(0)
        start_dq()
        column(1, 0)
        column(1, 1)
    gq_ref[...] = jnp.zeros_like(gq_ref)
    lax.fori_loop(0, chunks, query_weight, 0)
    wait_rows(heads, g.me, got_ref, row_send.at[1], row_recv.at[1])
    rows_ref[...] = unpack(got_ref[...])

    def sent(sem, ref):
        send(ref, ref, sem, out_recv, g.me).wait_send()

    for drow in range(side):
        def done(drow=drow):
            sent(x_send.at[drow], src_ref.at[pl.ds(0, g.parts * side - 1)])
            if g.ties:
                sent(fwd_send.at[drow], src_ref.at[pl.ds(0, 2)])
            if drow:
                sent(y_send.at[drow - 1], stage_ref.at[0])
        when_source(g.row + drow, done)
    if g.ties:
        when_source(g.row + 1, lambda: sent(pass_send.at[0], up_ref))
        when_source(g.row - 1, lambda: sent(pass_send.at[1], down_ref))

    @pl.when(g.is_source(g.row))
    def _():
        blocks = src_ref.at[pl.ds(0, n - 1)]
        send(blocks, blocks, y_send.at[0], out_recv, g.me).wait_recv()

    @pl.when(jnp.logical_not(g.is_source(g.row)))
    def _():
        def clear(index, carry):
            dst_ref[index] = jnp.zeros(dst_ref.shape[1:], dst_ref.dtype)
            return carry
        lax.fori_loop(0, heads, clear, 0)


def return_blocks(n, heads, source_rows, collective_id, blocks, dq, gain, early):
    half, width = blocks.shape[1], blocks.shape[2]
    hd, total_q = dq.shape
    q_rows = total_q // n
    side, parts = math.isqrt(heads), n // heads
    chunk = lambda *lead: pltpu.VMEM(lead + (half * parts, width), BF16)
    block = lambda *lead: pltpu.VMEM(lead + (half, width), BF16)
    piece, dim = min(512, total_q), early.shape[1] // 2
    return pl.pallas_call(
        functools.partial(return_kernel, n, heads, source_rows, piece),
        out_shape=[shape((heads, half * parts, width), BF16), shape((heads, q_rows, hd), BF16), shape((hd // parts, dim), F32)],
        in_specs=vmem(3) + [pl.BlockSpec(memory_space=pl.ANY)],
        out_specs=vmem(3),
        scratch_shapes=[chunk(side - 1, side), block(side), block(side), chunk(2), chunk(2), pltpu.VMEM(dq.shape, F32),
                        pltpu.VMEM((n, q_rows // 2, 2 * hd), BF16), pltpu.VMEM((heads, q_rows // 2, 2 * hd), BF16),
                        pltpu.VMEM((hd // parts, total_q), BF16), pltpu.VMEM((2, piece, dim), BF16), dma(2), dma(2), dma(2),
                        dma(side), dma(side), dma(side - 1), dma(2), dma(side - 1, side), dma(side), dma(side), dma(2), dma(2),
                        pltpu.SemaphoreType.DMA],
        compiler_params=remote(collective_id),
        name='return_blocks',
    )(blocks, dq, gain, early)


def decoder_kernel(n, heads, mine_ref, dec_ref, gout_ref, gain_ref, wo_hbm, wg_hbm, wu_hbm, wd_hbm,
                   out_ref, lse_ref, do_ref, factors_ref, gh_ref, gnorm_ref,
                   theirs_ref, packed_ref, got_ref, sent_ref, back_ref, swapped_ref, wo_ref, wg_ref, wu_ref, wd_ref, gact_ref,
                   load_sem, send_sem, recv_sem):
    me = lax.axis_index('seq')
    part = lax.rem(me, n // heads)
    partner, peers = pair_peers(n, heads, me, part)
    q_rows, dim = dec_ref.shape
    hd = out_ref.shape[0]
    loads = [pltpu.make_async_copy(src, dst, load_sem.at[i]) for i, (src, dst) in enumerate(
        ((wd_hbm, wd_ref), (wo_hbm, wo_ref), (wg_hbm, wg_ref), (wu_hbm, wu_ref)))]
    for load in loads:
        load.start()
    meet(peers)

    swap(mine_ref, theirs_ref, send_sem.at[0], recv_sem.at[0], partner)
    m_a, m_b = mine_ref[hd + 8:hd + 9], theirs_ref[hd + 8:hd + 9]
    top = jnp.maximum(m_a, m_b)
    s_a, s_b = jnp.exp2(m_a - top), jnp.exp2(m_b - top)
    den = mine_ref[hd:hd + 1] * s_a + theirs_ref[hd:hd + 1] * s_b
    out = (mine_ref[:hd] * s_a + theirs_ref[:hd] * s_b) / den
    packed_ref[...] = pack(out.T.astype(BF16).reshape(n, q_rows, hd))
    start_rows(n, heads, me, part, packed_ref, lambda peer: peer, got_ref, send_sem.at[1], recv_sem.at[1])
    out_ref[...] = out
    lse_ref[...] = top + jnp.log2(den)

    loads[0].wait()
    top_rows = gout_ref[...].astype(BF16)
    tile = 256

    def act_tile(index, carry):
        at = pl.ds(pl.multiple_of(index * tile, tile), tile)
        gact_ref[:, at] = dot_nt(top_rows, wd_ref[at, :])
        return carry

    lax.fori_loop(0, wd_ref.shape[0] // tile, act_tile, 0)
    wait_rows(heads, me, got_ref, send_sem.at[1], recv_sem.at[1])

    attended = jnp.concatenate([unpack(got_ref[h]) for h in range(heads)], axis=1)
    loads[1].wait()
    hidden = (dec_ref[...].astype(F32) + dot(attended, wo_ref[...])).astype(BF16).astype(F32)
    gain = gain_ref[...].astype(F32)
    inverse = lax.rsqrt(jnp.mean(hidden * hidden, axis=-1, keepdims=True) + 1e-6)
    scaled = hidden * inverse
    normed = (scaled * gain).astype(BF16)
    loads[2].wait()
    gate = dot(normed, wg_ref[...])
    loads[3].wait()
    up = dot(normed, wu_ref[...])
    sig = jax.nn.sigmoid(gate)
    silu = gate * sig
    grad_act = gact_ref[...]
    grad_gate = (grad_act * up * (sig + silu * (1.0 - sig))).astype(BF16)
    grad_up = (grad_act * silu).astype(BF16)
    grad_normed = (dot_nt(wg_ref[...], grad_gate) + dot_nt(wu_ref[...], grad_up)).T
    gnorm_ref[...] = jnp.sum(grad_normed * scaled, axis=0, keepdims=True)
    inner = grad_normed * gain
    grad_hidden = gout_ref[...] + inverse * (inner - scaled * jnp.mean(inner * scaled, axis=-1, keepdims=True))
    rounded = grad_hidden.astype(BF16)
    grad_att = dot_nt(wo_ref[...], rounded).T.astype(BF16)
    for h in range(heads):
        sent_ref[h] = pack(grad_att[:, hd * h:hd * (h + 1)])
    factors_ref[:, :dim] = attended
    factors_ref[:, dim:] = rounded
    gh_ref[...] = grad_hidden

    start_rows(n, heads, me, part, sent_ref, lambda peer: peer // (n // heads), back_ref, send_sem.at[2], recv_sem.at[2])
    wait_rows(heads, me, back_ref, send_sem.at[2], recv_sem.at[2])
    swap(back_ref, swapped_ref, send_sem.at[3], recv_sem.at[3], partner)
    place(n, heads, part, back_ref, swapped_ref, do_ref, False, True)


def decoder_rows(n, heads, collective_id, mine, dec_in, grad_out, gain, wo, w_gate, w_up, w_down):
    q_rows, dim = dec_in.shape
    hd, total_q = wo.shape[0] // heads, mine.shape[1]
    hbm = pl.BlockSpec(memory_space=pl.ANY)
    return pl.pallas_call(
        functools.partial(decoder_kernel, n, heads),
        out_shape=[shape((hd, total_q), F32), shape((1, total_q), F32), shape((n, q_rows, 2 * hd), BF16),
                   shape((q_rows, 2 * dim), BF16), shape((q_rows, dim), F32), shape((1, dim), F32)],
        in_specs=vmem(4) + [hbm] * 4,
        out_specs=vmem(6),
        scratch_shapes=[pltpu.VMEM(mine.shape, F32), pltpu.VMEM((n, q_rows // 2, 2 * hd), BF16)]
        + [pltpu.VMEM((heads, q_rows // 2, 2 * hd), BF16)] * 4
        + [pltpu.VMEM(w.shape, BF16) for w in (wo, w_gate, w_up, w_down)] + [pltpu.VMEM((q_rows, w_down.shape[0]), F32), dma(4), dma(4), dma(4)],
        compiler_params=remote(collective_id),
        name='decoder_rows',
    )(mine, dec_in, grad_out, gain, wo, w_gate, w_up, w_down)


def valid_blocks(mem_len, rows, parts, sources):
    reach = mem_len - lax.rem(lax.axis_index('seq'), parts) * rows
    blocks = jnp.minimum((reach + parts * rows - 1) // (parts * rows), sources)
    return blocks, jnp.minimum(reach - (blocks - 1) * parts * rows, rows)


def forward_kernel(scale, hd, parts, q_block, len_ref, kv_ref, q_ref, out_ref, qt_ref, top_ref):
    rows, total_q = kv_ref.shape[1], q_ref.shape[0]
    blocks, last_valid = valid_blocks(len_ref[0], rows, parts, kv_ref.shape[0])
    groups = [slice(first, first + q_block) for first in range(0, total_q, q_block)]
    base = slice(hd + 8, hd + 9)
    qt_ref[...] = q_ref[...].T

    def values_of(keys):
        return jnp.concatenate([keys.T[hd:], jnp.ones((16, rows), keys.dtype)], axis=0)

    def group_of(index):
        return pl.ds(pl.multiple_of(index * q_block, q_block), q_block)

    def first_step(group, carry):
        cols = group_of(group)
        top = jnp.max(dot(kv_ref[0], qt_ref[:, cols]), axis=0, keepdims=True)
        out_ref[hd + 8:, cols] = jnp.broadcast_to(top * scale, (8, q_block))
        top_ref[:, cols] = jnp.broadcast_to(top, (8, q_block))
        return carry

    lax.fori_loop(0, len(groups), first_step, 0)
    out_ref[:hd + 8, :] = jnp.zeros((hd + 8, total_q), F32)

    def finish(values, scores, cols):
        top_ref[:, cols] = jnp.maximum(top_ref[:, cols], jnp.max(scores.reshape(rows // 8, 8, q_block), axis=0))
        weights = jnp.exp2(scores * scale - out_ref[base, cols]).astype(values.dtype)
        out_ref[:hd + 8, cols] += dot(values, weights)[:hd + 8]

    def step(index, carry):
        keys = kv_ref[index]
        values = values_of(keys)
        for cols in groups:
            finish(values, dot(keys, qt_ref[:, cols]), cols)
        return carry

    def last_step(group, carry):
        cols = group_of(group)
        keys = kv_ref[blocks - 1]
        scores = dot(keys, qt_ref[:, cols])
        position = lax.broadcasted_iota(jnp.int32, scores.shape, 0)
        finish(values_of(keys), jnp.where(position < last_valid, scores, NEG), cols)
        return carry

    lax.fori_loop(0, blocks - 1, step, 0)
    lax.fori_loop(0, len(groups), last_step, 0)

    excess = jnp.max(top_ref[...] * scale - out_ref[hd + 8:, :])
    broken = jnp.max(jnp.where(jnp.abs(out_ref[:hd + 8, :]) <= 3e38, 0.0, 1.0))

    @pl.when(jnp.logical_or(jnp.logical_not(excess <= 64.0), broken > 0.0))
    def _():
        out_ref[:hd + 8, :] = jnp.zeros((hd + 8, total_q), F32)
        out_ref[hd + 8:, :] = jnp.full((8, total_q), NEG, F32)

        small = min(256, total_q)
        count = total_q // small

        def running(step_index, carry):
            index, group = step_index // count, lax.rem(step_index, count)
            cols = pl.ds(pl.multiple_of(group * small, small), small)
            keys = kv_ref[index]
            limit = jnp.where(index == blocks - 1, last_valid, rows)
            scores = dot(keys, qt_ref[:, cols]) * scale
            position = lax.broadcasted_iota(jnp.int32, scores.shape, 0)
            scores = jnp.where(position < limit, scores, NEG)
            old = out_ref[base, cols]
            new = jnp.maximum(old, jnp.max(scores, axis=0, keepdims=True))
            weights = jnp.exp2(scores - new).astype(keys.dtype)
            out_ref[:hd + 8, cols] = out_ref[:hd + 8, cols] * jnp.exp2(old - new) + dot(values_of(keys), weights)[:hd + 8]
            out_ref[hd + 8:, cols] = jnp.broadcast_to(new, (8, small))
            return carry

        lax.fori_loop(0, blocks * count, running, 0)


def attention_forward(scale, hd, parts, sources, mem_len, kv, q):
    rows, width = kv.shape[1], kv.shape[2]
    total_q = q.shape[0]
    return pl.pallas_call(
        functools.partial(forward_kernel, scale, hd, parts, min(1024, total_q)),
        out_shape=shape((hd + 16, total_q), F32),
        grid=(1,),
        in_specs=[pl.BlockSpec(memory_space=pltpu.SMEM),
                  pl.BlockSpec((sources, rows, width), lambda i: (0, 0, 0), pipeline_mode=pl.Buffered(1)), full(q)],
        out_specs=pl.BlockSpec((hd + 16, total_q), lambda i: (0, 0)),
        scratch_shapes=[pltpu.VMEM((width, total_q), BF16), pltpu.VMEM((8, total_q), F32)],
        compiler_params=plain(),
        cost_estimate=pl.CostEstimate(flops=4 * total_q * sources * rows * hd, bytes_accessed=kv.size * 2,
                                      transcendentals=total_q * sources * rows),
        name='attention_forward',
    )(mem_len, kv, q)


def backward_kernel(scale, key_scale, hd, parts, q_block, len_ref, kv_ref, q_ref, do_ref, out_ref, lse_ref, dkv_ref, dq_ref,
                    qt_ref, dot_ref, delta_ref):
    rows, total_q = kv_ref.shape[1], q_ref.shape[0]
    blocks, last_valid = valid_blocks(len_ref[0], rows, parts, kv_ref.shape[0])
    width = kv_ref.shape[2]
    groups = [slice(first, first + q_block) for first in range(0, total_q, q_block)]
    dq_ref[...] = jnp.zeros_like(dq_ref)
    qt_ref[...] = q_ref[...].T
    do_t = do_ref[...].T
    dot_ref[...] = do_t
    delta_ref[...] = jnp.sum(do_t[hd:].astype(F32) * out_ref[...], axis=0, keepdims=True)

    lane_scale = jnp.where(lax.broadcasted_iota(jnp.int32, (1, width), 1) < hd, key_scale, 1.0)

    def products(keys, cols):
        return dot(keys, qt_ref[:, cols]), dot(keys, dot_ref[:, cols])

    def finish(keys, keys_t, scores, grads, cols, valid):
        prob = jnp.exp2(scores * scale - lse_ref[:, cols])
        if valid is not None:
            position = lax.broadcasted_iota(jnp.int32, scores.shape, 0)
            prob = jnp.where(position < valid, prob, 0.0)
        grad_scores = (prob * (grads - delta_ref[:, cols])).astype(keys.dtype)
        update = dot(grad_scores, q_ref[cols, :]) + dot(prob.astype(keys.dtype), do_ref[cols, :])
        dq_ref[:, cols] += dot(keys_t, grad_scores)
        return update

    def step(index, carry):
        keys = kv_ref[index]
        keys_t = keys.T[:hd]
        total = jnp.zeros((rows, width), F32)
        for cols in groups:
            scores, grads = products(keys, cols)
            total += finish(keys, keys_t, scores, grads, cols, None)
        dkv_ref[index] = (total * lane_scale).astype(dkv_ref.dtype)
        return carry

    def last_step(group, total):
        keys = kv_ref[blocks - 1]
        cols = pl.ds(pl.multiple_of(group * q_block, q_block), q_block)
        scores, grads = products(keys, cols)
        return total + finish(keys, keys.T[:hd], scores, grads, cols, last_valid)

    def clear(index, carry):
        dkv_ref[index] = jnp.zeros((rows, width), dkv_ref.dtype)
        return carry

    lax.fori_loop(0, blocks - 1, step, 0)
    total = lax.fori_loop(0, len(groups), last_step, jnp.zeros((rows, width), F32))
    dkv_ref[blocks - 1] = (total * lane_scale).astype(dkv_ref.dtype)
    lax.fori_loop(blocks, dkv_ref.shape[0], clear, 0)
    dq_ref[...] = dq_ref[...] * key_scale


def attention_backward(scale, key_scale, hd, parts, sources, mem_len, kv, q, do, out_t, lse):
    n, rows, width = kv.shape
    total_q = q.shape[0]
    return pl.pallas_call(
        functools.partial(backward_kernel, scale, key_scale, hd, parts, min(512, total_q)),
        out_shape=[shape((n, rows, width), BF16), shape((hd, total_q), F32)],
        grid=(1,),
        in_specs=[pl.BlockSpec(memory_space=pltpu.SMEM),
                  pl.BlockSpec((sources, rows, width), lambda i: (0, 0, 0), pipeline_mode=pl.Buffered(1)),
                  full(q), full(do), full(out_t), full(lse)],
        out_specs=[pl.BlockSpec((n, rows, width), lambda i: (0, 0, 0)),
                   pl.BlockSpec((hd, total_q), lambda i: (0, 0))],
        scratch_shapes=[pltpu.VMEM((width, total_q), BF16), pltpu.VMEM((width, total_q), BF16), pltpu.VMEM((1, total_q), F32)],
        compiler_params=plain(),
        cost_estimate=pl.CostEstimate(flops=10 * total_q * sources * rows * hd, bytes_accessed=kv.size * 4,
                                      transcendentals=total_q * sources * rows),
        name='attention_backward',
    )(mem_len, kv, q, do, out_t, lse)


def reduce_kernel(n, heads, tile, chunk, gk_hbm, gv_hbm, early_hbm, late_hbm, w1_hbm, w3_hbm, w2_hbm, wo_ref, wq_ref, gain1_ref,
                  gain2_ref, dqr_ref, dec_ref, gh_ref, gnorm_ref,
                  sums_ref, gdec_ref, norms_ref, n2_hbm, d1_hbm, d3_hbm, act_hbm,
                  acc_ref, pair_ref, far_ref, near_ref, n2_ref, top_ref, att_ref, decs_ref, w1_ref, w3_ref, w2_ref,
                  d1_ref, d3_ref, act_ref, mine_ref, all_ref,
                  own_sem, share_send, share_recv, pair_send, pair_recv, far_send, far_recv, near_send, near_recv, rows_sem, top_sem, w_sem, out_sem, n2_sem,
                  norm_send, norm_recv):
    g = Grid(n, heads, 0)
    side = g.side
    rows, dim = n2_ref.shape
    tiles = d1_hbm.shape[0]
    shared = max(1, 4 * tiles // 11)
    own_tiles = tiles - (g.parts - 1) * shared
    part_rows = acc_ref.shape[1]

    def start_rows_of(index):
        slot = lax.rem(index, 2)
        at = pl.ds(pl.multiple_of(index * chunk, chunk), chunk)
        for i, (src, dst) in enumerate(((late_hbm, att_ref), (early_hbm, decs_ref))):
            pltpu.make_async_copy(src.at[at, pl.ds(0, dim)], dst.at[slot], rows_sem.at[slot, i]).start()

    def tile_at(index):
        return pl.ds(pl.multiple_of(index * tile, tile), tile)

    def number_of(index):
        rest = index // shared
        return (1 - rest) * (index * g.parts + g.part) + rest * (index + (g.parts - 1) * shared)

    def weights(index):
        slot = lax.rem(index, 2)
        at = tile_at(number_of(index))
        return [pltpu.make_async_copy(src, dst.at[slot], w_sem.at[slot, i]) for i, (src, dst) in enumerate(
            ((w1_hbm.at[:, at], w1_ref), (w3_hbm.at[:, at], w3_ref), (w2_hbm.at[at, :], w2_ref)))]

    def results(index):
        slot, number = lax.rem(index, 2), number_of(index)
        pairs = ((d1_ref, d1_hbm), (d3_ref, d3_hbm), (act_ref, act_hbm))
        return ([pltpu.make_async_copy(src.at[slot], dst.at[number], out_sem.at[slot, i]) for i, (src, dst) in enumerate(pairs)],
                [send(src.at[slot], dst.at[number], share_send.at[slot, i], share_recv.at[i], g.partner)
                 for i, (src, dst) in enumerate(pairs)])

    start_rows_of(0)
    top_load = pltpu.make_async_copy(early_hbm.at[:, pl.ds(dim, dim)], top_ref, top_sem)
    top_load.start()
    for copy in weights(0):
        copy.start()

    def summand(c, core):
        source = gk_hbm if c < heads // g.parts else gv_hbm
        first = ((g.parts * c) % heads + core) * part_rows
        return source.at[pl.ds(pl.multiple_of(first, part_rows), part_rows), :]

    owns = [pltpu.make_async_copy(summand(c, g.part), acc_ref.at[c], own_sem.at[c]) for c in range(heads)]
    for copy in owns:
        copy.start()

    barrier = pltpu.get_barrier_semaphore()

    def signal(step, carry):
        pl.semaphore_signal(barrier, inc=1, device_id={'seq': lax.rem(g.me + step, n)}, device_id_type=MESH)
        return carry

    lax.fori_loop(1, n, signal, 0)
    pl.semaphore_wait(barrier, n - 1)
    for c in range(heads):
        send(summand(c, g.parts - 1 - g.part), pair_ref.at[c], pair_send, pair_recv, g.partner).start()

    grad_query = jnp.concatenate([dqr_ref[h] for h in range(heads)], axis=1)
    grad_normed = dot(grad_query, wq_ref[...])
    x = dec_ref[...].astype(F32)
    inverse = lax.rsqrt(jnp.mean(x * x, axis=-1, keepdims=True) + 1e-6)
    scaled = x * inverse
    inner = grad_normed * gain1_ref[...].astype(F32)
    gdec_ref[...] = gh_ref[...] + inverse * (inner - scaled * jnp.mean(inner * scaled, axis=-1, keepdims=True))
    mine_ref[0:1, :] = jnp.sum(grad_normed * scaled, axis=0, keepdims=True)
    mine_ref[1:2, :] = gnorm_ref[...]

    def give(step, carry):
        send(mine_ref, all_ref.at[g.me], norm_send, norm_recv, lax.rem(g.me + step, n)).start()
        return carry

    lax.fori_loop(1, n, give, 0)
    all_ref[g.me] = mine_ref[...]

    quarter = part_rows // 4
    streams = [(axis, way, pl.ds((2 * axis + (way < 0)) * quarter, quarter)) for axis in (0, 1) for way in (1, -1)]

    def place_of(axis, line, other):
        return other * side + line if axis == 0 else line * side + other

    def pieces(stage, axis, line):
        position = g.row if axis == 0 else g.col
        return [place_of(axis, line, o) for o in range(side)] if stage == 0 else [place_of(axis, line, position)]

    def ring(stage, stream, step):
        axis, way, part = streams[stream]
        axis = axis if stage == 0 else 1 - axis
        here = g.col if axis == 0 else g.row
        ref, sends, recvs = (far_ref, far_send, far_recv) if stage == 0 else (near_ref, near_send, near_recv)
        to = g.near(0, way) if axis == 0 else g.near(way, 0)
        return axis, way, part, here, ref.at[stream, step - 1], sends.at[stream, step - 1], recvs.at[stream, step - 1], to

    def line_of(here, way, step):
        return lax.rem(here - way * step + 2 * side, side)

    def start_step(stage, step):
        for stream in range(4):
            axis, way, part, here, buffer, sem, recv, to = ring(stage, stream, step)
            for i, c in enumerate(pieces(stage, axis, line_of(here, way, step))):
                send(acc_ref.at[c, part], buffer.at[i], sem, recv, to).start()

    def end_step(stage, step):
        for stream in range(4):
            axis, way, part, here, buffer, sem, recv, to = ring(stage, stream, step)
            whole = send(buffer, buffer, sem, recv, g.me)
            whole.wait_recv()
            for i, c in enumerate(pieces(stage, axis, line_of(here, way, step + 1))):
                acc_ref[c, part, :] = acc_ref[c, part, :] + buffer[i]
            whole.wait_send()

    def add_pair():
        for copy in owns:
            copy.wait()
        whole = send(pair_ref, pair_ref, pair_send, pair_recv, g.me)
        whole.wait_recv()

        def add(c, carry):
            acc_ref[c] = acc_ref[c] + pair_ref[c]
            return carry

        lax.fori_loop(0, heads, add, 0)
        whole.wait_send()

    def first():
        add_pair()
        start_step(0, 1)

    def turn():
        end_step(0, side - 1)
        start_step(1, 1)

    def between(stage, step):
        def body():
            end_step(stage, step)
            start_step(stage, step + 1)
        return body

    def prepare(index, carry):
        slot = lax.rem(index, 2)
        at = pl.ds(pl.multiple_of(index * chunk, chunk), chunk)
        for i, (src, dst) in enumerate(((late_hbm, att_ref), (early_hbm, decs_ref))):
            pltpu.make_async_copy(src.at[at, pl.ds(0, dim)], dst.at[slot], rows_sem.at[slot, i]).wait()

        @pl.when(index + 1 < rows // chunk)
        def _():
            start_rows_of(index + 1)

        pl.when(index == rows // chunk // 2)(first)
        dec = decs_ref[slot].astype(F32)
        hidden = (dec + dot(att_ref[slot], wo_ref[...])).astype(BF16).astype(F32)
        n2_ref[at, :] = rms_norm(hidden, gain2_ref[...].astype(F32)).astype(BF16)
        return carry

    lax.fori_loop(0, rows // chunk, prepare, 0)
    top_load.wait()
    n2_store = pltpu.make_async_copy(n2_ref, n2_hbm, n2_sem)
    n2_store.start()

    events = ([between(0, t) for t in range(1, side - 1)] + [turn] + [between(1, t) for t in range(1, side - 1)]
              + [lambda: end_step(1, side - 1)])
    at_tile = (1, 3, 5, 6)
    inside = own_tiles > at_tile[-1] and len(events) > len(at_tile)

    def finish_results(index):
        stores, shares = results(index)
        for copy in stores:
            copy.wait()

        @pl.when(index < shared)
        def _():
            for copy in shares:
                copy.wait_send()

    def activations(index, carry):
        slot = lax.rem(index, 2)
        for copy in weights(index):
            copy.wait()

        @pl.when(index + 1 < own_tiles)
        def _():
            for copy in weights(index + 1):
                copy.start()

        @pl.when(index >= 2)
        def _():
            finish_results(index - 2)

        if inside:
            for event, when in zip(events, at_tile):
                pl.when(index == when)(event)

        w1, w3, w2t = w1_ref[slot], w3_ref[slot], w2_ref[slot].T
        for first_row in range(0, rows, chunk):
            part = slice(first_row, first_row + chunk)
            gate = dot(n2_ref[part, :], w1)
            up = dot(n2_ref[part, :], w3)
            grad = dot(top_ref[part, :], w2t)
            sig = jax.nn.sigmoid(gate)
            silu = gate * sig
            act_ref[slot, part, :] = (silu * up).astype(BF16)
            d3_ref[slot, part, :] = (grad * silu).astype(BF16)
            d1_ref[slot, part, :] = (grad * up * (sig + silu * (1.0 - sig))).astype(BF16)
        stores, shares = results(index)
        for copy in stores:
            copy.start()

        @pl.when(index < shared)
        def _():
            for copy in shares:
                copy.start()
        return carry

    lax.fori_loop(0, own_tiles, activations, 0)
    for event in events[len(at_tile):] if inside else events:
        event()
    sums_ref[...] = acc_ref[g.chip]

    others = all_ref.at[pl.ds(0, n - 1)]
    whole = send(others, others, norm_send, norm_recv, g.me)
    whole.wait_send()
    whole.wait_recv()
    norms_ref[...] = jnp.sum(all_ref[...], axis=0)
    n2_store.wait()
    for index in range(max(own_tiles - 2, 0), own_tiles):
        finish_results(index)
    for i, ref in enumerate((d1_hbm, d3_hbm, act_hbm)):
        come = ref.at[pl.ds(0, shared)]
        send(come, come, share_send.at[0, i], share_recv.at[i], g.me).wait_recv()


def reduce_sums(n, heads, collective_id, gk, gv, early, late, w_gate, w_up, w_down, wo, wq, gain1, gain2, dq_rows, dec_in, gh, gnorm):
    rows, dim = early.shape[0], gk.shape[1]
    ff, tile, chunk = w_gate.shape[1], 256, min(512, early.shape[0] // 2)
    part_rows = 2 * gk.shape[0] // n
    side = math.isqrt(heads)
    hbm = pl.BlockSpec(memory_space=pl.ANY)
    return pl.pallas_call(
        functools.partial(reduce_kernel, n, heads, tile, chunk),
        out_shape=[shape((part_rows, dim), F32), shape(gh.shape, F32), shape((2, dim), F32), shape((rows, dim), BF16)]
        + [shape((ff // tile, rows, tile), BF16)] * 3,
        in_specs=[hbm] * 7 + vmem(8),
        out_specs=vmem(3) + [hbm] * 4,
        scratch_shapes=[pltpu.VMEM((heads, part_rows, dim), F32)] * 2
        + [pltpu.VMEM((4, side - 1, side, part_rows // 4, dim), F32), pltpu.VMEM((4, side - 1, 1, part_rows // 4, dim), F32)]
        + [pltpu.VMEM((rows, dim), BF16)] * 2 + [pltpu.VMEM((2, chunk, dim), BF16)] * 2
        + [pltpu.VMEM((2, dim, tile), BF16)] * 2 + [pltpu.VMEM((2, tile, dim), BF16)] + [pltpu.VMEM((2, rows, tile), BF16)] * 3
        + [pltpu.VMEM((2, dim), F32), pltpu.VMEM((n, 2, dim), F32)]
        + [dma(heads), dma(2, 3), dma(3), pltpu.SemaphoreType.DMA, pltpu.SemaphoreType.DMA, dma(4, side - 1), dma(4, side - 1), dma(4, side - 1),
           dma(4, side - 1), dma(2, 2), pltpu.SemaphoreType.DMA, dma(2, 3), dma(2, 3), pltpu.SemaphoreType.DMA,
           pltpu.SemaphoreType.DMA, pltpu.SemaphoreType.DMA],
        compiler_params=remote(collective_id),
        cost_estimate=pl.CostEstimate(flops=6 * rows * dim * ff, bytes_accessed=12 * rows * ff, transcendentals=rows * ff),
        name='reduce_sums',
    )(gk, gv, early, late, w_gate, w_up, w_down, wo, wq, gain1, gain2, dq_rows, dec_in, gh, gnorm)


def gate_up_kernel(n2_ref, d1_ref, d3_ref, g1_ref, g3_ref, n2t_ref):
    @pl.when(pl.program_id(0) == 0)
    def _():
        n2t_ref[...] = n2_ref[...].T

    g1_ref[...] = dot(n2t_ref[...], d1_ref[...])
    g3_ref[...] = dot(n2t_ref[...], d3_ref[...])


def gate_up_grads(n2, d1, d3):
    rows, dim = n2.shape
    tiles, _, tile = d1.shape
    cols = pl.BlockSpec((dim, tile), lambda i: (0, i))
    part = pl.BlockSpec((pl.Squeezed(), rows, tile), lambda i: (i, 0, 0))
    return pl.pallas_call(
        gate_up_kernel,
        out_shape=[shape((dim, tiles * tile), F32)] * 2,
        grid=(tiles,),
        in_specs=[full(n2), part, part],
        out_specs=[cols, cols],
        scratch_shapes=[pltpu.VMEM((dim, rows), BF16)],
        compiler_params=plain(),
        cost_estimate=pl.CostEstimate(flops=4 * rows * dim * tiles * tile, bytes_accessed=12 * dim * tiles * tile, transcendentals=0),
        name='gate_up_grads',
    )(n2, d1, d3)


def down_kernel(top_ref, act_ref, k_in_ref, v_in_ref, g2_ref, k_ref, v_ref):
    g2_ref[...] = dot_tn(act_ref[...], top_ref[...])
    k_ref[...] = k_in_ref[...]
    v_ref[...] = v_in_ref[...]


def down_grad(early, act, total):
    rows, dim = early.shape[0], early.shape[1] // 2
    tiles, _, tile = act.shape
    blocks = 1 << (tiles.bit_length() - 1)
    height = total.shape[0] // 2 // blocks
    block = lambda first: pl.BlockSpec((height, dim), lambda i: (jnp.minimum(i, blocks - 1) + first, 0))
    return pl.pallas_call(
        down_kernel,
        out_shape=[shape((tiles * tile, dim), F32)] + [shape((total.shape[0] // 2, dim), F32)] * 2,
        grid=(tiles,),
        in_specs=[pl.BlockSpec((rows, dim), lambda i: (0, 1), pipeline_mode=pl.Buffered(1)),
                  pl.BlockSpec((pl.Squeezed(), rows, tile), lambda i: (i, 0, 0)), block(0), block(blocks)],
        out_specs=[pl.BlockSpec((tile, dim), lambda i: (i, 0)), block(0), block(0)],
        compiler_params=plain(),
        cost_estimate=pl.CostEstimate(flops=2 * rows * dim * tiles * tile, bytes_accessed=12 * dim * tiles * tile, transcendentals=0),
        name='down_grad',
    )(early, act, total, total)


def memory_weight_kernel(memory_ref, dkv_ref, gk_ref, gv_ref):
    group, hd = dkv_ref.shape[0], dkv_ref.shape[2] // 2
    for i in range(group):
        both = dot_tn(dkv_ref[i], memory_ref[...])
        gk_ref[i * hd:(i + 1) * hd, :] = both[:hd]
        gv_ref[i * hd:(i + 1) * hd, :] = both[hd:]


def memory_weight_grads(memory, dkv):
    heads, rows, width = dkv.shape
    dim, hd = memory.shape[1], width // 2
    group = 4
    out = pl.BlockSpec((group * hd, dim), lambda i: (i, 0))
    return pl.pallas_call(
        memory_weight_kernel,
        out_shape=[shape((heads * hd, dim), F32)] * 2,
        grid=(heads // group,),
        in_specs=[full(memory), pl.BlockSpec((group, rows, width), lambda i: (i, 0, 0))],
        out_specs=[out, out],
        compiler_params=plain(),
        cost_estimate=pl.CostEstimate(flops=2 * rows * dim * heads * width, bytes_accessed=16 * rows * dim, transcendentals=0),
        name='memory_weight_grads',
    )(memory, dkv)


def memory_grad_kernel(dkv_ref, wk_ref, wv_ref, gq_in_ref, out_ref, gq_ref):
    group = dkv_ref.shape[0]
    gq_ref[...] = gq_in_ref[...]
    left = jnp.concatenate([dkv_ref[i] for i in range(group)], axis=1)
    right = jnp.concatenate([part[i] for i in range(group) for part in (wk_ref, wv_ref)], axis=0)

    @pl.when(pl.program_id(0) == 0)
    def _():
        out_ref[...] = dot(left, right)

    @pl.when(pl.program_id(0) > 0)
    def _():
        out_ref[...] += dot(left, right)


def memory_grad(dkv, wk_t, wv_t, gq):
    heads, rows, width = dkv.shape
    hd, dim = wk_t.shape[1], wk_t.shape[2]
    group = 4
    weight = pl.BlockSpec((group, hd, dim), lambda i: (i, 0, 0))
    passing = pl.BlockSpec((group * hd, dim), lambda i: (i, 0))
    return pl.pallas_call(
        memory_grad_kernel,
        out_shape=[shape((rows, dim), F32), shape(gq.shape, F32)],
        grid=(heads // group,),
        in_specs=[pl.BlockSpec((group, rows, width), lambda i: (i, 0, 0)), weight, weight, passing],
        out_specs=[pl.BlockSpec((rows, dim), lambda i: (0, 0)), passing],
        compiler_params=plain(),
        cost_estimate=pl.CostEstimate(flops=2 * rows * dim * heads * width, bytes_accessed=12 * rows * dim, transcendentals=0),
        name='memory_grad',
    )(dkv, wk_t, wv_t, gq)


def outer_kernel(att_ref, gh_ref, out_ref):
    @pl.when(pl.program_id(0) == 0)
    def _():
        out_ref[...] = jnp.zeros_like(out_ref)

    out_ref[...] += dot_tn(att_ref[...], gh_ref[...])


def outer_weight_grad(late, dim):
    rows = late.shape[0]
    chunk = min(512, rows)
    return pl.pallas_call(
        outer_kernel,
        out_shape=shape((dim, dim), F32),
        grid=(rows // chunk,),
        in_specs=[pl.BlockSpec((chunk, dim), lambda i: (i, 0)), pl.BlockSpec((chunk, dim), lambda i: (i, 1))],
        out_specs=pl.BlockSpec((dim, dim), lambda i: (0, 0)),
        compiler_params=plain(),
        cost_estimate=pl.CostEstimate(flops=2 * rows * dim * dim, bytes_accessed=8 * rows * dim, transcendentals=0),
        name='outer_weight_grad',
    )(late, late)


def solution(mesh):
    n = mesh.shape['seq']
    row_spec = P(('data', 'seq'), None)
    weight_spec = P()
    part_vec = P('data')
    part_mat = P('data', None)
    part_cube = P('data', None, None)

    def device_step(dec_in, memory, mem_len, grad_out, norm_attn, wq_cross, wk_cross, wv_cross, wo_cross, norm_mlp, w_gate, w_up, w_down):
        q_rows, dim = dec_in.shape
        heads, hd = wq_cross.shape[1], wq_cross.shape[2]
        parts = n // heads
        sources = -(-3 * n // 4)
        total_q = q_rows * n
        key_scale = hd ** -0.5
        scale = key_scale * LOG2E
        wq_t, wk_t, wv_t = (jnp.transpose(w, (1, 2, 0)) for w in (wq_cross, wk_cross, wv_cross))
        source_rows = -(-sources // (parts * math.isqrt(heads)))
        kv, q_in, early_local = exchange(n, heads, source_rows, 0, memory, dec_in, grad_out, norm_attn, wk_t, wv_t, wq_t)
        head_q = q_in.reshape(total_q, 2 * hd)

        early = lax.all_gather(early_local, 'seq', axis=0, tiled=True)

        wo = wo_cross.reshape(heads * hd, dim)
        mine = attention_forward(scale, hd, parts, sources, mem_len, kv, head_q)
        out_t, lse, do_in, factors, grad_hidden, g_norm_mlp = decoder_rows(
            n, heads, 1, mine, dec_in, grad_out, norm_mlp, wo, w_gate, w_up, w_down)
        do_in, factors = lax.optimization_barrier((do_in, factors))
        late = lax.all_gather(factors, 'seq', axis=0, tiled=True)

        dkv, dq_part = attention_backward(scale, key_scale, hd, parts, sources, mem_len, kv, head_q, do_in.reshape(total_q, 2 * hd), out_t, lse)
        dkv_in, dq_rows, gq_share = return_blocks(n, heads, source_rows, 4, dkv, dq_part, norm_attn, early)
        dkv_in, dq_rows, gq_share, late = lax.optimization_barrier((dkv_in, dq_rows, gq_share, late))
        g_wq = lax.all_gather(gq_share, 'seq', axis=0, tiled=True)

        gk_part, gv_part = memory_weight_grads(memory, dkv_in)
        sums, g_dec, norms, n2_all, d1, d3, act = reduce_sums(
            n, heads, 5, gk_part, gv_part, early, late, w_gate, w_up, w_down, wo, wq_t.reshape(heads * hd, dim), norm_attn, norm_mlp,
            dq_rows, dec_in, grad_hidden, g_norm_mlp)
        sums, n2_all, d1, d3, act, dkv_in, late, early, g_wq = lax.optimization_barrier(
            (sums, n2_all, d1, d3, act, dkv_in, late, early, g_wq))
        total = lax.all_gather(sums, 'seq', axis=0, tiled=True)
        g_wo = outer_weight_grad(late, dim)
        g_mem, g_wq = memory_grad(dkv_in, wk_t, wv_t, g_wq)
        g_gate, g_up = gate_up_grads(n2_all, d1, d3)
        g_down, g_wk, g_wv = down_grad(early, act, total)

        cube = lambda g: jnp.transpose(g.reshape(heads, hd, dim), (2, 0, 1))
        return (g_dec, g_mem, norms[0], cube(g_wq), cube(g_wk), cube(g_wv), g_wo.reshape(heads, hd, dim), norms[1], g_gate, g_up, g_down)

    return jax.shard_map(device_step, mesh=mesh,
                         in_specs=(row_spec, row_spec, part_vec, row_spec) + (weight_spec,) * 9,
                         out_specs=(row_spec, row_spec, part_vec, part_cube, part_cube, part_cube, part_cube, part_vec, part_mat, part_mat, part_mat),
                         check_vma=False)
```
